32 devices in a mesh: band: 2 (over x), vis: 16 (over z, y, core).
Axes of the slice: x: 2, y: 2, z: 4, core: 2. Of those that a mesh axis runs over, the one named last changes fastest.
Arguments:
- sky_image: float32 [4096, 4096], P(('band', 'vis')), as said below
- coef_dual: float32 [4, 2048, 2048], P(None, ('band', 'vis')), may hold values from -12 to 12
- vis_dual: float32 [2, 16, 16, 4, 2, 32], P('band', 'vis'), may hold values from -12 to 12
- visibilities: float32 [2, 16, 16, 4, 2, 32], P('band', 'vis')
- kernel_blocks: bfloat16 [2, 16, 16, 4, 2, 32, 256], P('band', 'vis'), may hold values from -0.375 to 0.375
- tile_rows: int32 [2, 16, 16, 4], P('band', 'vis'), may hold values from 0 to 2047
- tile_counts: int32 [2, 16, 16], P('band', 'vis'), may hold values from 1 to 4, as said below
Outputs:
- new_image: float32 [4096, 4096], P(('band', 'vis'))
- new_coef_dual: float32 [4, 2048, 2048], P(None, ('band', 'vis'))
- new_vis_dual: float32 [2, 16, 16, 4, 2, 32], P('band', 'vis')
The draws below stay inside these ranges and needn't reach their ends.
Inputs may be any that keep to these rules, and one draw needn't show every extreme that they name: `sky_image`: nonnegative. `tile_counts`: in every band some owner q has all 4 slots live from every device of that band.
All inputs are finite; a program needn't handle non-finite values.
Results may differ from the reference program's by a relative error of at most 0.0018.
Values may be sent and summed in bfloat16 or wider, within the bound.
A program may use at most 128 MiB of HBM per device.

```python
import jax
import jax.numpy as jnp
from jax import lax

IMG = 4096
VT = 32
SLOTS = 4
ITERS = 1
STRIPE = 2048
PIECE_ROWS = 256
HALF = 2048
N_BAND = 2
N_VIS = 16


def draw_sky_image(key, part):
    row_key, col_key, base_key = jax.random.split(key, 3)
    row_scale = jnp.exp(jax.random.uniform(row_key, (IMG, 1), jnp.float32) * jnp.log(10.0))
    col_scale = jnp.exp(jax.random.uniform(col_key, (1, IMG), jnp.float32) * jnp.log(10.0))
    rising = 1.0 + 2.0 * jnp.arange(IMG, dtype=jnp.float32)[:, None] / IMG
    base_values = jax.random.uniform(base_key, (IMG, IMG), jnp.float32)
    return 0.2 * base_values * row_scale * col_scale * rising


def draw_visibilities(key, part):
    full_shape = (N_BAND, N_VIS, N_VIS, SLOTS, 2, VT)
    scale_key, value_key = jax.random.split(key)
    tile_scale = jnp.exp(jax.random.uniform(scale_key, (N_BAND, N_VIS, N_VIS, SLOTS, 1, 1), jnp.float32) * jnp.log(10.0))
    position = (jnp.arange(N_BAND * N_VIS, dtype=jnp.float32) / (N_BAND * N_VIS - 1)).reshape(N_BAND, N_VIS, 1, 1, 1, 1)
    values = jax.random.normal(value_key, full_shape, jnp.float32)
    rising = 1.0 + 2.0 * position
    return values * tile_scale * rising


def draw_tile_counts(key, part):
    count_key, owner_key = jax.random.split(jax.random.fold_in(key, 11))
    counts = jax.random.randint(count_key, (N_BAND, N_VIS, N_VIS), 1, SLOTS + 1)
    full_owner = jax.random.randint(owner_key, (N_BAND, 1, 1), 0, N_VIS)
    owners = jnp.arange(N_VIS, dtype=jnp.int32)[None, None, :]
    return jnp.where(owners == full_owner, SLOTS, counts).astype(jnp.int32)


def plant(values, key, low, largest):
    extent = values.shape
    spot = [jax.random.randint(jax.random.fold_in(key, axis), (), 0, extent[axis]) for axis in range(len(extent))]
    values = values.at[tuple(spot)].set(low)
    longest = extent.index(max(extent))
    spot[longest] = (spot[longest] + 1) % extent[longest]
    return values.at[tuple(spot)].set(largest)


def block_levels(rng, shape, cuts, least, largest):
    loudness, own = 1.0, jax.random.fold_in(rng, 6)
    for dim, shards_of in cuts:
        heights = jnp.exp(jax.random.uniform(jax.random.fold_in(own, dim), (shards_of,), jnp.float32, least / len(cuts), largest / len(cuts)))
        loudness = loudness * jnp.repeat(heights, shape[dim] // shards_of).reshape([-1 if axis == dim else 1 for axis in range(len(shape))])
    return loudness


def centred(own_key, extent, width, limit, cuts=(), held_as=jnp.bfloat16):
    entries = width * jax.random.normal(own_key, extent, jnp.float32)
    if cuts:
        entries = entries * block_levels(own_key, extent, cuts, -0.22, 0.18)
    return jnp.clip(entries, -limit, limit).astype(held_as)


def setup_inputs(seed: int = 0) -> dict:
    splits = jax.random.split(jax.random.key(seed), 8)
    sky_image = draw_sky_image(jax.random.fold_in(splits[7], 71), 0)
    coef_dual = centred(splits[1], (4, HALF, HALF), 2.0, 12.0, ((1, 32),), jnp.float32)
    vis_dual = centred(splits[2], (N_BAND, N_VIS, N_VIS, SLOTS, 2, VT), 2.0, 12.0, ((0, 2), (1, 16)), jnp.float32)
    visibilities = draw_visibilities(jax.random.fold_in(splits[7], 71), 0)
    kernel_blocks = centred(splits[4], (N_BAND, N_VIS, N_VIS, SLOTS, 2, VT, PIECE_ROWS), PIECE_ROWS ** -0.5, 0.375, ((0, 2), (1, 16)))
    tile_rows = plant(jax.random.randint(splits[5], (N_BAND, N_VIS, N_VIS, SLOTS), 0, STRIPE), jax.random.fold_in(splits[5], 1), 0, STRIPE - 1).astype(jnp.int32)
    tile_counts = draw_tile_counts(jax.random.fold_in(splits[7], 71), 0)
    return dict(sky_image=sky_image, coef_dual=coef_dual, vis_dual=vis_dual, visibilities=visibilities, kernel_blocks=kernel_blocks, tile_rows=tile_rows, tile_counts=tile_counts)


low_taps = (-0.010597401784997278, 0.032883011666982945, 0.030841381835986965, -0.18703481171888114, -0.02798376941698385, 0.6308807679295904, 0.7148465705525415, 0.23037781330885523)
high_taps = tuple(((-1.0) ** offset * low_taps[7 - offset] for offset in range(8)))
highest = lax.Precision.HIGHEST

def analyse_axis(field, axis):
    length = field.shape[axis]
    low_part = 0.0
    high_part = 0.0
    for offset in range(8):
        taken = lax.slice_in_dim(jnp.roll(field, -offset, axis=axis), 0, length, 2, axis)
        low_part = low_part + low_taps[offset] * taken
        high_part = high_part + high_taps[offset] * taken
    return (low_part, high_part)

def synthesise_axis(low_part, high_part, axis):
    halves = []
    for parity in range(2):
        summed = 0.0
        for delay in range(4):
            summed = summed + low_taps[parity + 2 * delay] * jnp.roll(low_part, delay, axis=axis)
            summed = summed + high_taps[parity + 2 * delay] * jnp.roll(high_part, delay, axis=axis)
        halves.append(summed)
    joined = jnp.stack(halves, axis=axis + 1)
    new_shape = list(low_part.shape)
    new_shape[axis] = 2 * new_shape[axis]
    return joined.reshape(new_shape)

def analysis(field):
    rows_low, rows_high = analyse_axis(field, 0)
    low_low, low_high = analyse_axis(rows_low, 1)
    high_low, high_high = analyse_axis(rows_high, 1)
    return jnp.stack([low_low, low_high, high_low, high_high])

def synthesis(coeffs):
    rows_low = synthesise_axis(coeffs[0], coeffs[1], 1)
    rows_high = synthesise_axis(coeffs[2], coeffs[3], 1)
    return synthesise_axis(rows_low, rows_high, 0)

def forward_map(extrap, kernel_blocks, tile_rows):
    spectrum = jnp.fft.fft2(extrap) / IMG
    flipped = spectrum.T.reshape(N_BAND, STRIPE, N_VIS, PIECE_ROWS)
    real_grid = lax.optimization_barrier(jnp.real(flipped).astype(jnp.bfloat16))
    imag_grid = lax.optimization_barrier(jnp.imag(flipped).astype(jnp.bfloat16))
    owners = jnp.arange(N_VIS, dtype=jnp.int32)[None, :, None]

    def per_band(inputs):
        kernels, rows_band, real_band, imag_band = inputs
        tile_real = real_band[rows_band, owners].astype(jnp.float32)
        tile_imag = imag_band[rows_band, owners].astype(jnp.float32)
        kernel_real = kernels[:, :, :, 0].astype(jnp.float32)
        kernel_imag = kernels[:, :, :, 1].astype(jnp.float32)
        out_real = jnp.einsum('vqsat,vqst->vqsa', kernel_real, tile_real, precision=highest) - jnp.einsum('vqsat,vqst->vqsa', kernel_imag, tile_imag, precision=highest)
        out_imag = jnp.einsum('vqsat,vqst->vqsa', kernel_real, tile_imag, precision=highest) + jnp.einsum('vqsat,vqst->vqsa', kernel_imag, tile_real, precision=highest)
        return jnp.stack([out_real, out_imag], axis=3)
    return lax.map(per_band, (kernel_blocks, tile_rows, real_grid, imag_grid))

def adjoint_map(weights, kernel_blocks, tile_rows):
    rounded = lax.optimization_barrier(weights.astype(jnp.bfloat16))
    owners = jnp.arange(N_VIS, dtype=jnp.int32)[None, :, None]

    def per_band(inputs):
        kernels, rows_band, vis_band = inputs
        kernel_real = kernels[:, :, :, 0].astype(jnp.float32)
        kernel_imag = kernels[:, :, :, 1].astype(jnp.float32)
        weight_real = vis_band[:, :, :, 0].astype(jnp.float32)
        weight_imag = vis_band[:, :, :, 1].astype(jnp.float32)
        grid_real = jnp.einsum('vqsat,vqsa->vqst', kernel_real, weight_real, precision=highest) + jnp.einsum('vqsat,vqsa->vqst', kernel_imag, weight_imag, precision=highest)
        grid_imag = jnp.einsum('vqsat,vqsa->vqst', kernel_real, weight_imag, precision=highest) - jnp.einsum('vqsat,vqsa->vqst', kernel_imag, weight_real, precision=highest)
        stacked = jnp.stack([grid_real, grid_imag], axis=3)
        segment = (owners * STRIPE + rows_band).astype(jnp.int32)
        summed = jax.ops.segment_sum(stacked.reshape(-1, 2, PIECE_ROWS), segment.reshape(-1), num_segments=N_VIS * STRIPE)
        return summed.reshape(N_VIS, STRIPE, 2, PIECE_ROWS)
    grids = lax.map(per_band, (kernel_blocks, tile_rows, rounded))
    ordered = jnp.transpose(grids, (3, 1, 4, 0, 2)).reshape(2, IMG, IMG)
    spectrum = lax.complex(ordered[0], ordered[1])
    return jnp.real(jnp.fft.ifft2(spectrum)) * IMG

def reference(sky_image, coef_dual, vis_dual, visibilities, kernel_blocks, tile_rows, tile_counts):
    slot_index = jnp.arange(SLOTS, dtype=jnp.int32)
    live_slots = (slot_index < tile_counts[..., None]).astype(jnp.float32)[..., None, None]
    data_square = jnp.sum(live_slots * visibilities * visibilities)
    radius = 0.5 * jnp.sqrt(data_square + 1e-06)
    for iteration in range(ITERS):
        adjoint_part = adjoint_map(live_slots * vis_dual, kernel_blocks, tile_rows)
        smooth = synthesis(coef_dual)
        new_image = jnp.maximum(sky_image - smooth - adjoint_part, 0.0)
        extrap = 2.0 * new_image - sky_image
        coeffs = analysis(extrap)
        threshold = 0.5 * jnp.sum(jnp.abs(coeffs)) / (IMG * IMG)
        coef_dual = jnp.clip(coef_dual + coeffs, -threshold, threshold)
        predicted = forward_map(extrap, kernel_blocks, tile_rows)
        residual = live_slots * (vis_dual + predicted - visibilities)
        size_value = jnp.sqrt(jnp.sum(residual * residual) + 1e-06)
        vis_dual = residual * (1.0 - jnp.minimum(1.0, radius / size_value))
        sky_image = new_image
    return (sky_image, coef_dual, vis_dual)
```

```python
import math

import jax
import numpy as np
import jax.numpy as jnp
from jax import lax
from jax.experimental import pallas as pl
from jax.experimental.pallas import tpu as pltpu
from jax.sharding import PartitionSpec as P

IMG = 4096


low_taps = (
    -0.010597401784997278,
    0.032883011666982945,
    0.030841381835986965,
    -0.18703481171888114,
    -0.02798376941698385,
    0.6308807679295904,
    0.7148465705525415,
    0.23037781330885523,
)
high_taps = tuple(((-1.0) ** offset * low_taps[7 - offset] for offset in range(8)))
highest = lax.Precision.HIGHEST


def shifted(block, axis, distance):
    devices = range(lax.axis_size(axis))
    route = [((i - distance) % len(devices), i) for i in devices]
    return lax.ppermute(block, axis, route)


def dft_table(table_size, sign):
    positions = jnp.arange(table_size, dtype=jnp.int32)
    phase = positions[:, None] * positions[None, :] % table_size
    angle = 2.0 * math.pi / table_size * phase.astype(jnp.float32)
    return (jnp.cos(angle), sign * jnp.sin(angle))


def section_one(table, values):
    return jnp.einsum("kn,...nm->...km", table, values, precision=highest)


def section_two(table, values):
    return jnp.einsum("qm,...km->...qk", table, values, precision=highest)


def dft_last(real_in, imag_in, sign):
    leading = real_in.shape[:-1]
    length = real_in.shape[-1]
    inner_len = 64
    outer_len = length // inner_len
    split_real = real_in.reshape(leading + (outer_len, inner_len))
    table_real, table_imag = dft_table(outer_len, sign)
    first_real = section_one(table_real, split_real)
    first_imag = section_one(table_imag, split_real)
    if imag_in is not None:
        split_imag = imag_in.reshape(leading + (outer_len, inner_len))
        first_real = first_real - section_one(table_imag, split_imag)
        first_imag = first_imag + section_one(table_real, split_imag)
    outer_index = jnp.arange(outer_len, dtype=jnp.int32)
    inner_index = jnp.arange(inner_len, dtype=jnp.int32)
    twist_phase = outer_index[:, None] * inner_index[None, :] % length
    twist_angle = 2.0 * math.pi / length * twist_phase.astype(jnp.float32)
    twist_real = jnp.cos(twist_angle)
    twist_imag = sign * jnp.sin(twist_angle)
    mid_real = first_real * twist_real - first_imag * twist_imag
    mid_imag = first_real * twist_imag + first_imag * twist_real
    last_real, last_imag = dft_table(inner_len, sign)
    out_real = section_two(last_real, mid_real) - section_two(last_imag, mid_imag)
    out_imag = section_two(last_real, mid_imag) + section_two(last_imag, mid_real)
    factor = 1.0 / math.sqrt(length)
    return (
        (out_real * factor).reshape(leading + (length,)),
        (out_imag * factor).reshape(leading + (length,)),
    )


def pieces_from_image(extrap, band_count, group_count):
    rows_dev = extrap.shape[0]
    image_width = extrap.shape[1]
    stripe = image_width // band_count
    piece_cols = stripe // group_count
    piece_rows = image_width // group_count
    col_real, col_imag = dft_last(extrap, None, -1.0)
    shaped = jnp.stack([col_real, col_imag]).reshape(
        2, 1, 1, rows_dev, band_count, group_count, piece_cols
    )
    moved = lax.all_to_all(
        lax.all_to_all(shaped, "band", split_axis=4, concat_axis=1, tiled=True),
        "vis",
        split_axis=5,
        concat_axis=2,
        tiled=True,
    )
    columns = jnp.transpose(moved.reshape(2, image_width, piece_cols), (2, 0, 1))
    row_real, row_imag = dft_last(columns[:, 0], columns[:, 1], -1.0)
    stacked = (
        jnp.stack([row_real, row_imag], axis=1)
        .astype(jnp.bfloat16)
        .reshape(piece_cols, 2, group_count, piece_rows)
    )
    pieces = lax.all_to_all(stacked, "vis", split_axis=2, concat_axis=0, tiled=True)
    return pieces.reshape(stripe, 2, piece_rows)


def image_from_pieces(piece_sum, band_count, group_count):
    stripe = piece_sum.shape[0]
    piece_rows = piece_sum.shape[2]
    piece_cols = stripe // group_count
    image_width = piece_rows * group_count
    rows_dev = image_width // (band_count * group_count)
    spread = lax.all_to_all(
        piece_sum.reshape(stripe, 2, 1, piece_rows), "vis", split_axis=0, concat_axis=2, tiled=True
    )
    spread = spread.reshape(piece_cols, 2, image_width)
    col_real, col_imag = dft_last(spread[:, 0], spread[:, 1], 1.0)
    stacked = jnp.transpose(jnp.stack([col_real, col_imag]), (0, 2, 1))
    shaped = stacked.reshape(2, band_count, group_count, rows_dev, 1, 1, piece_cols)
    moved = lax.all_to_all(
        lax.all_to_all(shaped, "band", split_axis=1, concat_axis=4, tiled=True),
        "vis",
        split_axis=2,
        concat_axis=5,
        tiled=True,
    )
    moved = moved.reshape(2, rows_dev, image_width)
    out_real, out_imag = dft_last(moved[0], moved[1], 1.0)
    return out_real


def cols_down(field):
    image_width = field.shape[1]
    extended = jnp.concatenate([field, field[:, :6]], axis=1)
    low_part = 0.0
    high_part = 0.0
    for offset in range(8):
        taken = extended[:, offset : offset + image_width : 2]
        low_part = low_part + low_taps[offset] * taken
        high_part = high_part + high_taps[offset] * taken
    return (low_part, high_part)


def cols_up(low_part, high_part):
    halves = []
    for parity in range(2):
        summed = 0.0
        for delay in range(4):
            summed = summed + low_taps[parity + 2 * delay] * jnp.roll(low_part, delay, axis=1)
            summed = summed + high_taps[parity + 2 * delay] * jnp.roll(high_part, delay, axis=1)
        halves.append(summed)
    return jnp.stack(halves, axis=2).reshape(low_part.shape[0], 2 * low_part.shape[1])


def rows_up(low_ext, high_ext, half_rows):
    halves = []
    for parity in range(2):
        summed = 0.0
        for delay in range(4):
            begin = 3 - delay
            summed = summed + low_taps[parity + 2 * delay] * low_ext[begin : begin + half_rows]
            summed = summed + high_taps[parity + 2 * delay] * high_ext[begin : begin + half_rows]
        halves.append(summed)
    return jnp.stack(halves, axis=1).reshape(2 * half_rows, low_ext.shape[1])


def analysis(extrap):
    rows_dev = extrap.shape[0]
    taken_rows = min(6, rows_dev)
    parts_list = [extrap]
    parts_list.append(shifted(extrap[:taken_rows], ("band", "vis"), -1))
    extended = jnp.concatenate(parts_list, axis=0)
    half_rows = rows_dev // 2
    rows_low = 0.0
    rows_high = 0.0
    for offset in range(8):
        taken = extended[offset : offset + 2 * half_rows : 2]
        rows_low = rows_low + low_taps[offset] * taken
        rows_high = rows_high + high_taps[offset] * taken
    low_low, low_high = cols_down(rows_low)
    high_low, high_high = cols_down(rows_high)
    return jnp.stack([low_low, low_high, high_low, high_high])


def synthesis(coef_dual):
    half_rows = coef_dual.shape[1]
    taken_rows = min(3, half_rows)
    parts_list = [shifted(coef_dual[:, half_rows - taken_rows :, :], ("band", "vis"), 1)]
    joined = jnp.concatenate(parts_list[::-1] + [coef_dual], axis=1)
    cols_low = rows_up(joined[0], joined[2], half_rows)
    cols_high = rows_up(joined[1], joined[3], half_rows)
    return cols_up(cols_low, cols_high)


def degrid(kernel_here, tiles):
    kernel_real = kernel_here[:, :, 0]
    kernel_imag = kernel_here[:, :, 1]
    tile_real = tiles[:, :, 0]
    tile_imag = tiles[:, :, 1]
    out_real = jnp.einsum(
        "qsat,qst->qsa", kernel_real, tile_real, preferred_element_type=jnp.float32
    ) - jnp.einsum("qsat,qst->qsa", kernel_imag, tile_imag, preferred_element_type=jnp.float32)
    out_imag = jnp.einsum(
        "qsat,qst->qsa", kernel_real, tile_imag, preferred_element_type=jnp.float32
    ) + jnp.einsum("qsat,qst->qsa", kernel_imag, tile_real, preferred_element_type=jnp.float32)
    return jnp.stack([out_real, out_imag], axis=2)


def grid_back(kernel_here, weights):
    kernel_real = kernel_here[:, :, 0]
    kernel_imag = kernel_here[:, :, 1]
    weight_real = weights[:, :, 0]
    weight_imag = weights[:, :, 1]
    grid_real = jnp.einsum(
        "qsat,qsa->qst", kernel_real, weight_real, preferred_element_type=jnp.float32
    ) + jnp.einsum("qsat,qsa->qst", kernel_imag, weight_imag, preferred_element_type=jnp.float32)
    grid_imag = jnp.einsum(
        "qsat,qsa->qst", kernel_real, weight_imag, preferred_element_type=jnp.float32
    ) - jnp.einsum("qsat,qsa->qst", kernel_imag, weight_real, preferred_element_type=jnp.float32)
    return jnp.stack([grid_real, grid_imag], axis=2)


def local(sky_image, coef_dual, vis_dual, visibilities, kernel_blocks, tile_rows, tile_counts):
    band_count = lax.axis_size("band")
    group_count = lax.axis_size("vis")
    kernel_here = kernel_blocks[0, 0]
    rows_here = tile_rows[0, 0]
    slot_count = rows_here.shape[1]
    live_slots = (
        jnp.arange(slot_count, dtype=jnp.int32)[None, :] < tile_counts[0, 0][:, None]
    ).astype(jnp.float32)[:, :, None, None]
    vis_data = visibilities[0, 0]
    vis_state = vis_dual[0, 0]
    image_width = sky_image.shape[1]
    stripe = image_width // band_count
    piece_rows = image_width // group_count
    incoming_rows = lax.all_to_all(rows_here, "vis", split_axis=0, concat_axis=0, tiled=True)
    data_part = jnp.sum(live_slots * vis_data * vis_data)
    weights = (live_slots * vis_state).astype(jnp.bfloat16)
    contrib = grid_back(kernel_here, weights)
    arrived = lax.all_to_all(contrib, "vis", split_axis=0, concat_axis=0, tiled=True)
    piece_sum = jax.ops.segment_sum(
        arrived.reshape(-1, 2, piece_rows), incoming_rows.reshape(-1), num_segments=stripe
    )
    adjoint_part = image_from_pieces(piece_sum, band_count, group_count)
    smooth = synthesis(coef_dual)
    new_image = jnp.maximum(sky_image - smooth - adjoint_part, 0.0)
    extrap = 2.0 * new_image - sky_image
    coeffs = analysis(extrap)
    abs_total = jnp.sum(jnp.abs(coeffs))
    coef_total = lax.psum(abs_total, ("band", "vis"))
    threshold = 0.5 * coef_total / (IMG * IMG)
    coef_dual = jnp.clip(coef_dual + coeffs, -threshold, threshold)
    piece_grid = pieces_from_image(extrap, band_count, group_count)
    tiles = lax.all_to_all(
        piece_grid[incoming_rows], "vis", split_axis=0, concat_axis=0, tiled=True
    )
    predicted = degrid(kernel_here, tiles)
    residual = live_slots * (vis_state + predicted - vis_data)
    resid_square = jnp.sum(residual * residual)
    norm_square, data_square = lax.psum((resid_square, data_part), ("band", "vis"))
    radius = 0.5 * jnp.sqrt(data_square + 1e-06)
    size_value = jnp.sqrt(norm_square + 1e-06)
    vis_state = residual * (1.0 - jnp.minimum(1.0, radius / size_value))
    return (new_image, coef_dual, vis_state[None, None])


high = lax.Precision.HIGH
everywhere = ("band", "vis")


def wave_tables(length, digit_low):
    digit_high = length // digit_low
    low = np.arange(digit_low)
    wide = np.arange(digit_high)
    full = 2.0 * np.pi
    small = full * (low[:, None] * low[None, :] % digit_low) / digit_low
    twist = full * (low[:, None] * wide[None, :]) / length
    large = full * (wide[:, None] * wide[None, :] % digit_high) / digit_high
    return small, twist, large


def complex_matrix(angle, sign):
    c = np.cos(angle)
    s = sign * np.sin(angle)
    return np.stack([np.stack([c, -s], axis=1), np.stack([s, c], axis=1)])


def f32(values):
    return jnp.asarray(np.asarray(values, np.float32))


def bf16(values):
    return f32(values).astype(jnp.bfloat16)


def analysis_matrix(half):
    matrix = np.zeros((2, half, 2 * half + 6))
    for k in range(half):
        for j in range(8):
            matrix[0, k, 2 * k + j] = low_taps[j]
            matrix[1, k, 2 * k + j] = high_taps[j]
    return matrix.reshape(2 * half, 2 * half + 6)


def synthesis_matrix(half):
    matrix = np.zeros((2 * half, 2, half + 3))
    for n in range(2 * half):
        for delay in range(4):
            tap = n % 2 + 2 * delay
            matrix[n, 0, n // 2 - delay + 3] = low_taps[tap]
            matrix[n, 1, n // 2 - delay + 3] = high_taps[tap]
    return matrix


def fast_analysis(extrap, halo):
    rows_dev, width = extrap.shape
    extended = jnp.concatenate([extrap, halo], axis=0)
    by_rows = jnp.einsum("ij,jn->in", f32(analysis_matrix(rows_dev // 2)), extended, precision=high)
    size = 256
    blocks = by_rows.reshape(rows_dev, width // size, size)
    following = jnp.roll(blocks, -1, axis=1)[:, :, :6]
    matrix = analysis_matrix(size // 2)
    out = jnp.einsum("rbi,ji->rbj", blocks, f32(matrix[:, :size]), precision=high)
    out = out + jnp.einsum("rbi,ji->rbj", following, f32(matrix[:, size:]), precision=high)
    out = out.reshape(2, rows_dev // 2, width // size, 2, size // 2)
    return jnp.transpose(out, (0, 3, 1, 2, 4)).reshape(4, rows_dev // 2, width // 2)


def fast_synthesis(coef_dual):
    half_rows, half_width = coef_dual.shape[1:]
    halo = shifted(coef_dual[:, half_rows - 3 :, :], everywhere, 1)
    joined = jnp.concatenate([halo, coef_dual], axis=1)
    joined = joined.reshape(2, 2, half_rows + 3, half_width)
    by_rows = jnp.einsum("irj,rcjn->cin", f32(synthesis_matrix(half_rows)), joined, precision=high)
    size = 128
    blocks = by_rows.reshape(2, 2 * half_rows, half_width // size, size)
    before = jnp.roll(blocks, 1, axis=2)[:, :, :, size - 3 :]
    matrix = synthesis_matrix(size)
    out = jnp.einsum("cibk,nck->ibn", blocks, f32(matrix[:, :, 3:]), precision=high)
    out = out + jnp.einsum("cibk,nck->ibn", before, f32(matrix[:, :, :3]), precision=high)
    return out.reshape(2 * half_rows, 2 * half_width)


def cos_sums(values, size):
    half = size // 2
    if half < 2:
        return [values[0] + values[1], values[0] - values[1]]
    quarter = half // 2
    plus = [values[a] + values[half - a] for a in range(quarter)] + [values[quarter]]
    minus = [values[a] - values[half - a] for a in range(quarter)]
    out = [None] * (half + 1)
    out[0::2] = cos_sums(plus, half)
    for k in range(1, half, 2):
        total = minus[0]
        for a in range(1, quarter):
            total = total + minus[a] * math.cos(2 * math.pi * (a * k % size) / size)
        out[k] = total
    return out


def sin_sums(values, size):
    half = size // 2
    if half < 2:
        return [None] * (half + 1)
    quarter = half // 2
    plus = {a: values[a] + values[half - a] for a in range(1, quarter)}
    plus[quarter] = values[quarter]
    minus = [None] + [values[a] - values[half - a] for a in range(1, quarter)]
    out = [None] * (half + 1)
    out[0::2] = sin_sums(minus, half)
    for k in range(1, half, 2):
        total = None
        for a in range(1, quarter + 1):
            factor = math.sin(2 * math.pi * (a * k % size) / size)
            term = plus[a] if a * 4 == size and k % 4 == 1 else plus[a] * factor
            total = term if total is None else total + term
        out[k] = total
    return out


def even_odd(values):
    size = len(values)
    half = size // 2
    even = [values[0]] + [values[a] + values[size - a] for a in range(1, half)] + [values[half]]
    odd = [None] + [values[a] - values[size - a] for a in range(1, half)]
    return even, odd


def split(values):
    upper = values.astype(jnp.bfloat16)
    return upper, (values - upper.astype(jnp.float32)).astype(jnp.bfloat16)


def table_pair(values):
    upper = f32(values).astype(jnp.bfloat16)
    return upper, (f32(values) - upper.astype(jnp.float32)).astype(jnp.bfloat16)


def nt_dot(a, b):
    return lax.dot_general(a, b, (((1,), (1,)), ((), ())), preferred_element_type=jnp.float32)


def nn_dot(a, b):
    return lax.dot_general(a, b, (((1,), (0,)), ((), ())), preferred_element_type=jnp.float32)


LEVELS = 32000.0
MESH = pl.DeviceIdType.MESH
LANES = 128
whole = pl.BlockSpec(memory_space=pltpu.VMEM)


def place():
    band = lax.axis_index("band")
    vis = lax.axis_index("vis")
    groups = lax.axis_size("vis")
    z = vis // 4
    y = vis // 2 % 2
    core = vis % 2
    return band, z, y, core, groups


def gather_kernel(block_ref, cols_ref, out_ref, all_cols_ref, send_a, send_b, recv_a, recv_b):
    x, z, y, core, groups = place()
    levels = groups // 4

    def index(px, pz, py, pc):
        return px * groups + pz * 4 + py * 2 + pc

    def device(px, pz, py, pc):
        return (px, pz * 4 + py * 2 + pc)

    me = index(x, z, y, core)
    fx, fy = x * (1 - core) + (1 - x) * core, (1 - y) * (1 - core) + y * core
    sx, sy = (1 - x) * (1 - core) + x * core, y * (1 - core) + (1 - y) * core
    up, down, first, second, twin = 0, 1, 2, 3, 4
    targets = [
        device(x, z + 1, y, core),
        device(x, z - 1, y, core),
        device(fx, z, fy, core),
        device(sx, z, sy, core),
        device(x, z, y, 1 - core),
    ]
    has_up, has_down = z < levels - 1, z > 0
    barrier = pltpu.get_barrier_semaphore()

    def signal(way):
        pl.semaphore_signal(barrier, inc=1, device_id=targets[way], device_id_type=MESH)

    pl.when(has_up)(lambda: signal(up))
    pl.when(has_down)(lambda: signal(down))
    for way in (first, second, twin):
        signal(way)
    pl.semaphore_wait(barrier, 5 - (z + 1) // levels - (levels - z) // levels)

    def copies(block, way):
        own_a, own_b = out_ref.at[block], all_cols_ref.at[block]
        return [
            pltpu.make_async_remote_copy(
                src_ref=own_a,
                dst_ref=own_a,
                send_sem=send_a.at[way, block],
                recv_sem=recv_a.at[block],
                device_id=targets[way],
                device_id_type=MESH,
            ),
            pltpu.make_async_remote_copy(
                src_ref=own_b,
                dst_ref=own_b,
                send_sem=send_b.at[way, block],
                recv_sem=recv_b.at[block],
                device_id=targets[way],
                device_id_type=MESH,
            ),
        ]

    def start(block, way):
        for copy in copies(block, way):
            copy.start()

    def sent(block, way):
        for copy in copies(block, way):
            copy.wait_send()

    def got(block):
        for copy in copies(block, twin):
            copy.wait_recv()

    out_ref[me] = block_ref[...]
    all_cols_ref[me] = cols_ref[...]

    pl.when(has_up)(lambda: start(me, up))
    pl.when(has_down)(lambda: start(me, down))
    for way in (first, second, twin):
        start(me, way)

    def each_line(px, py, action):
        def at(j):
            if j == 0:
                action(index(px, z, py, core), 0)
                return
            pl.when(z >= j)(lambda: action(index(px, z - j, py, core), 1))
            pl.when(z + j < levels)(lambda: action(index(px, z + j, py, core), -1))

        return at

    def own_line(do):
        def action(block, heading):
            if heading == 0:
                return
            do(block, heading)

        return action

    def take_own(block, heading):
        got(block)
        if heading > 0:
            pl.when(has_up)(lambda: start(block, up))
        else:
            pl.when(has_down)(lambda: start(block, down))
        for way in (first, second, twin):
            start(block, way)

    def take_first(block, heading):
        got(block)
        for way in (second, twin):
            start(block, way)

    def take_second(block, heading):
        got(block)
        start(block, twin)

    dx, dy = 1 - x, 1 - y
    lines = [
        each_line(x, y, own_line(take_own)),
        each_line(fx, fy, take_first),
        each_line(sx, sy, take_second),
        each_line(dx, dy, take_second),
    ]
    for j in range(levels):
        for at in lines:
            at(j)

    for i in range(groups):
        bx, rest = i // (groups // 2), i % (groups // 2)
        got(bx * groups + rest * 2 + 1 - core)

    def end_own(block, heading):
        if heading == 0:
            pl.when(has_up)(lambda: sent(block, up))
            pl.when(has_down)(lambda: sent(block, down))
        elif heading > 0:
            pl.when(has_up)(lambda: sent(block, up))
        else:
            pl.when(has_down)(lambda: sent(block, down))
        for way in (first, second, twin):
            sent(block, way)

    def end_first(block, heading):
        for way in (second, twin):
            sent(block, way)

    def end_second(block, heading):
        sent(block, twin)

    lines = [
        each_line(x, y, end_own),
        each_line(fx, fy, end_first),
        each_line(sx, sy, end_second),
        each_line(dx, dy, end_second),
    ]
    for j in range(levels):
        for at in lines:
            at(j)


def gather_all(block, cols, devices):
    return pl.pallas_call(
        gather_kernel,
        out_shape=(
            jax.ShapeDtypeStruct((devices,) + block.shape, block.dtype),
            jax.ShapeDtypeStruct((devices,) + cols.shape, cols.dtype),
        ),
        in_specs=[whole] * 2,
        out_specs=(whole, whole),
        scratch_shapes=[
            pltpu.SemaphoreType.DMA((5, devices)),
            pltpu.SemaphoreType.DMA((5, devices)),
            pltpu.SemaphoreType.DMA((devices,)),
            pltpu.SemaphoreType.DMA((devices,)),
        ],
        compiler_params=pltpu.CompilerParams(collective_id=0, has_side_effects=True),
        name="gather_all",
    )(block, cols)


def level(values):
    return jnp.round(values).astype(jnp.int32)


def image_kernel(
    low,
    block_ref,
    cols_ref,
    turn_ref,
    phase_ref,
    inv_ref,
    tw_ref,
    fwd_ref,
    sky_ref,
    smooth_ref,
    image_ref,
    extrap_ref,
    picked_ref,
    unit_ref,
    fold_ref,
    grid_ref,
    hot_ref,
    half_ref,
    spec_ref,
    rest_ref,
):
    rows = sky_ref.shape[0]
    tiles = block_ref.shape[0]
    kept = low // 2 + 1
    wide = LANES
    lane = lax.broadcasted_iota(jnp.int32, (1, LANES), 1)
    for i in range(tiles // LANES):
        columns = jnp.where(lane < LANES // 2, cols_ref[2 * i], cols_ref[2 * i + 1])
        k1 = columns % low
        k2 = columns // low
        flip = k1 >= kept
        k1 = jnp.where(flip, low - k1, k1)
        k2 = jnp.where(flip, wide - 1 - k2, k2)
        fold_ref[0, i : i + 1, :] = (k1 * wide + k2).astype(jnp.float32)
        fold_ref[1, i : i + 1, :] = jnp.where(flip, -1.0, 1.0)
    chunk = 512
    for j in range(tiles // chunk):
        both = nt_dot(turn_ref[...], block_ref[j * chunk : (j + 1) * chunk, :])
        for i in range(chunk // LANES):
            b = j * (chunk // LANES) + i
            real = both[:rows, i * LANES : (i + 1) * LANES]
            imag = both[rows:, i * LANES : (i + 1) * LANES]
            out_real = real * phase_ref[0] - imag * phase_ref[1]
            out_imag = (real * phase_ref[1] + imag * phase_ref[0]) * fold_ref[1, b : b + 1, :]
            grid_ref[:rows, b * LANES : (b + 1) * LANES] = out_real.astype(jnp.bfloat16)
            grid_ref[rows:, b * LANES : (b + 1) * LANES] = out_imag.astype(jnp.bfloat16)

    def scatter(p, carry):
        base = pl.multiple_of(p * 2 * wide, 2 * wide)
        row = (lax.broadcasted_iota(jnp.int32, (2 * wide, LANES), 0) + base).astype(jnp.float32)
        for i in range(tiles // LANES):
            hit = row == fold_ref[0, i : i + 1, :]
            hot_ref[pl.ds(base, 2 * wide), i * LANES : (i + 1) * LANES] = jnp.where(
                hit, 1.0, 0.0
            ).astype(jnp.bfloat16)
        folded = nt_dot(grid_ref[...], hot_ref[pl.ds(base, 2 * wide), :]).astype(jnp.bfloat16)
        for e in range(2):
            pair = jnp.concatenate(
                [folded[:rows, e * wide : (e + 1) * wide], folded[rows:, e * wide : (e + 1) * wide]],
                axis=1,
            )
            mid = nn_dot(pair, inv_ref[...])
            k1 = p * 2 + e
            tw_real, tw_imag = tw_ref[0, pl.ds(k1, 1), :], tw_ref[1, pl.ds(k1, 1), :]
            real, imag = mid[:, :wide], mid[:, wide:]
            half_ref[k1, :, :wide] = real * tw_real - imag * tw_imag
            half_ref[k1, :, wide:] = real * tw_imag + imag * tw_real
        return carry

    lax.fori_loop(0, (kept + 1) // 2, scatter, 0)

    def strip(i, carry):
        at = pl.ds(pl.multiple_of(i * 8, 8), 8)
        cos_part = cos_sums([half_ref[k, at, :wide] for k in range(kept)], low)
        sin_part = sin_sums([None] + [half_ref[k, at, wide:] for k in range(1, kept - 1)], low)
        extraps = []
        for a in range(low):
            k = min(a, low - a)
            if a == 0 or a == low // 2:
                adjoint = cos_part[k]
            elif a < low // 2:
                adjoint = cos_part[k] - sin_part[k]
            else:
                adjoint = cos_part[k] + sin_part[k]
            here = slice(a * wide, (a + 1) * wide)
            sky = sky_ref[at, here]
            image = jnp.maximum(sky - smooth_ref[at, here] - adjoint, 0.0)
            extrap = 2.0 * image - sky
            image_ref[at, here] = image
            extrap_ref[at, here] = extrap
            extraps.append(extrap)
        even, odd = even_odd(extraps)
        real_part = cos_sums(even, low)
        imag_part = sin_sums(odd, low)
        for k in range(kept):
            tw_real, tw_imag = tw_ref[0, k : k + 1, :], tw_ref[1, k : k + 1, :]
            real = real_part[k] * tw_real
            imag = -real_part[k] * tw_imag
            if 0 < k < kept - 1:
                real = real - imag_part[k] * tw_imag
                imag = imag - imag_part[k] * tw_real
            half_ref[k, at, :wide] = real
            half_ref[k, at, wide:] = imag
        return carry

    lax.fori_loop(0, rows // 8, strip, 0)

    for k in range(kept):
        upper, lower = split(half_ref[k])
        out = nn_dot(upper, fwd_ref[0]) + nn_dot(lower, fwd_ref[0]) + nn_dot(upper, fwd_ref[1])
        here = slice(k * wide, (k + 1) * wide)
        upper, lower = split(out)
        spec_ref[:rows, here] = upper[:, :wide]
        spec_ref[rows:, here] = upper[:, wide:]
        rest_ref[:rows, here] = lower[:, :wide]
        rest_ref[rows:, here] = lower[:, wide:]

    def pick(j, carry):
        at = pl.multiple_of(j * 2 * LANES, 2 * LANES)
        hot = hot_ref[: kept * wide, pl.ds(at, 2 * LANES)]
        got = nn_dot(spec_ref[...], hot) + nn_dot(rest_ref[...], hot)
        for h in range(2):
            sign = fold_ref[1, pl.ds(2 * j + h, 1), :]
            real = got[:rows, h * LANES : (h + 1) * LANES]
            imag = got[rows:, h * LANES : (h + 1) * LANES] * sign
            most = jnp.max(jnp.maximum(jnp.abs(real), jnp.abs(imag)), axis=0, keepdims=True)
            most = jnp.maximum(most, 1e-30)
            unit_ref[2 * j + h] = most * (1.0 / LEVELS)
            to_level = LEVELS / most
            packed = level(real * to_level) * 65536 + level(imag * to_level)
            to = pl.ds(pl.multiple_of(at + h * LANES, LANES), LANES)
            picked_ref[to, :] = packed.T
        return carry

    lax.fori_loop(0, tiles // (2 * LANES), pick, 0)


def image_step(blocks, cols, me, sky_image, smooth, groups, slots, piece):
    rows, width = sky_image.shape
    tiles = blocks.shape[0] * blocks.shape[1]
    low = width // LANES
    kept = low // 2 + 1
    turn = np.arange(piece)
    angle = (me * rows + jnp.arange(rows, dtype=jnp.int32))[:, None] * turn[None, :] % width
    angle = (2.0 * math.pi / width) * angle.astype(jnp.float32)
    cosine, sine = jnp.cos(angle), jnp.sin(angle)
    turn = jnp.concatenate(
        [jnp.concatenate([cosine, -sine], axis=1), jnp.concatenate([sine, cosine], axis=1)]
    ).astype(jnp.bfloat16)
    owner = np.arange(LANES) // slots % groups
    shift = 2 * np.pi * (np.arange(rows)[:, None] * owner[None, :] % groups) / groups
    phase = f32(np.stack([np.cos(shift), np.sin(shift)]))
    wide = np.arange(LANES)
    full = 2 * np.pi * (wide[:, None] * wide[None, :] % LANES) / LANES
    c, s = np.cos(full) / width, np.sin(full) / width
    inverse = bf16(np.block([[c, s], [-s, c]]))
    forward = jnp.stack(table_pair(np.block([[c, -s], [s, c]])))
    twist = 2 * np.pi * np.arange(kept + 1)[:, None] * wide[None, :] / width
    twist = f32(np.stack([np.cos(twist), np.sin(twist)]))
    return pl.pallas_call(
        lambda *refs: image_kernel(low, *refs),
        out_shape=(
            jax.ShapeDtypeStruct((rows, width), jnp.float32),
            jax.ShapeDtypeStruct((rows, width), jnp.float32),
            jax.ShapeDtypeStruct((tiles, rows), jnp.int32),
            jax.ShapeDtypeStruct((tiles // LANES, 1, LANES), jnp.float32),
        ),
        in_specs=[whole] * 9,
        out_specs=(whole,) * 4,
        scratch_shapes=[
            pltpu.VMEM((2, tiles // LANES, LANES), jnp.float32),
            pltpu.VMEM((2 * rows, tiles), jnp.bfloat16),
            pltpu.VMEM(((kept + 1) * LANES, tiles), jnp.bfloat16),
            pltpu.VMEM((kept + 1, rows, 2 * LANES), jnp.float32),
            pltpu.VMEM((2 * rows, kept * LANES), jnp.bfloat16),
            pltpu.VMEM((2 * rows, kept * LANES), jnp.bfloat16),
        ],
        compiler_params=pltpu.CompilerParams(vmem_limit_bytes=60 * 2**20),
        name="image_step",
    )(
        blocks.reshape(tiles, -1),
        cols,
        turn,
        phase,
        inverse,
        twist,
        forward,
        sky_image,
        smooth,
    )


def exchange_kernel(
    picked_ref, unit_ref, top_ref, got_ref, units_ref, below_ref, send_a, send_b, recv_a, recv_b, halo
):
    x, z, y, core, groups = place()
    devices = 2 * groups
    tiles = got_ref.shape[1]

    def flipped(value, bit):
        return value + (1 - 2 * (value // bit % 2)) * bit

    me = x * groups + z * 4 + y * 2 + core
    barrier = pltpu.get_barrier_semaphore()
    peers = []
    for code in sorted(range(1, devices), key=lambda code: -(code // 8 % 2)):
        vis = z * 4 + y * 2 + core
        for bit in (1, 2, 4, 8):
            if code & bit:
                vis = flipped(vis, bit)
        band = 1 - x if code & 16 else x
        peers.append((band, vis))
    for peer in peers:
        pl.semaphore_signal(barrier, inc=1, device_id=peer, device_id_type=MESH)
    before = (me + devices - 1) % devices
    pl.semaphore_wait(barrier, devices - 1)
    edge = pltpu.make_async_remote_copy(
        src_ref=top_ref,
        dst_ref=below_ref,
        send_sem=halo.at[0],
        recv_sem=halo.at[1],
        device_id=(before // groups, before % groups),
        device_id_type=MESH,
    )
    edge.start()
    copies = []
    for i, (band, vis) in enumerate(peers):
        to = band * groups + vis
        at = pl.ds(pl.multiple_of(to * tiles, tiles), tiles)
        copies.append(
            pltpu.make_async_remote_copy(
                src_ref=picked_ref.at[at, :],
                dst_ref=got_ref.at[me],
                send_sem=send_a.at[i],
                recv_sem=recv_a.at[i],
                device_id=(band, vis),
                device_id_type=MESH,
            )
        )
        copies.append(
            pltpu.make_async_remote_copy(
                src_ref=unit_ref.at[to // 2],
                dst_ref=units_ref.at[me],
                send_sem=send_b.at[i],
                recv_sem=recv_b.at[i],
                device_id=(band, vis),
                device_id_type=MESH,
            )
        )
    for copy in copies:
        copy.start()
    here = pl.ds(pl.multiple_of(me * tiles, tiles), tiles)
    got_ref[me] = picked_ref[here, :]
    units_ref[me] = unit_ref[me // 2]
    edge.wait()
    for copy in copies:
        copy.wait()


def exchange(picked, units, extrap, devices):
    tiles = picked.shape[0] // devices
    top = extrap[:8]
    return pl.pallas_call(
        exchange_kernel,
        out_shape=(
            jax.ShapeDtypeStruct((devices, tiles) + picked.shape[1:], picked.dtype),
            jax.ShapeDtypeStruct((devices,) + units.shape[1:], units.dtype),
            jax.ShapeDtypeStruct(top.shape, top.dtype),
        ),
        in_specs=[whole] * 3,
        out_specs=(whole,) * 3,
        scratch_shapes=[
            pltpu.SemaphoreType.DMA((devices - 1,)),
            pltpu.SemaphoreType.DMA((devices - 1,)),
            pltpu.SemaphoreType.DMA((devices - 1,)),
            pltpu.SemaphoreType.DMA((devices - 1,)),
            pltpu.SemaphoreType.DMA((2,)),
        ],
        compiler_params=pltpu.CompilerParams(collective_id=1, has_side_effects=True),
        name="exchange",
    )(picked, units, top)


def tile_kernel(
    devices, got_ref, units_ref, phase_ref, last_ref, order_ref, out_ref, mid_ref, unit_ref
):
    tiles, rows = phase_ref.shape[1:]
    group = LANES * 2 // 16
    units = jnp.concatenate([units_ref[d] for d in range(devices)], axis=0)
    units = jnp.concatenate([units] * (LANES // devices), axis=0).T
    unit_ref[...] = jnp.where(lax.axis_index("vis") % 2 == 0, units[:tiles], units[tiles:])

    def strip(i, carry):
        at = pl.multiple_of(i * 8, 8)
        here = pl.ds(at, 8)
        cosine, sine = phase_ref[0, here, :], phase_ref[1, here, :]
        reals, imags = [], []
        for d in range(devices):
            packed = got_ref[d, here, :]
            real = (packed + 32768) >> 16
            imag = packed - (real << 16)
            unit = unit_ref[here, d : d + 1]
            real = real.astype(jnp.float32) * unit
            imag = imag.astype(jnp.float32) * unit
            reals.append(real * cosine + imag * sine)
            imags.append(imag * cosine - real * sine)
        even, odd = even_odd(reals)
        cos_real, sin_real = cos_sums(even, devices), sin_sums(odd, devices)
        even, odd = even_odd(imags)
        cos_imag, sin_imag = cos_sums(even, devices), sin_sums(odd, devices)
        half = devices // 2
        for k in range(half + 1):
            if k == 0 or k == half:
                outs = [(k, cos_real[k], cos_imag[k])]
            else:
                outs = [
                    (k, cos_real[k] + sin_imag[k], cos_imag[k] - sin_real[k]),
                    (devices - k, cos_real[k] - sin_imag[k], cos_imag[k] + sin_real[k]),
                ]
            for t, real, imag in outs:
                mid_ref[t, here, :rows] = real
                mid_ref[t, here, rows:] = imag
        return carry

    lax.fori_loop(0, tiles // 8, strip, 0)
    lane = lax.broadcasted_iota(jnp.int32, (1, 2 * LANES), 1) // 16
    pieces = []
    for g in range(devices // group):
        total = None
        for e in range(group):
            upper, lower = split(mid_ref[g * group + e])
            out = nn_dot(upper, last_ref[0, g]) + nn_dot(lower, last_ref[0, g])
            out = out + nn_dot(upper, last_ref[1, g])
            out = jnp.where(lane == e, out, 0.0)
            total = out if total is None else total + out
        pieces.append(total.astype(jnp.bfloat16))
    tile = jnp.concatenate(pieces, axis=1)
    out_ref[...] = nn_dot(tile, order_ref[...])


def finish_tiles(got, units, devices, groups, slots, rows, piece):
    width = devices * rows
    tiles = groups * slots
    shift = np.arange(tiles)[:, None] // slots * np.arange(rows)[None, :] % groups
    shift = 2 * np.pi * shift / groups
    phase = f32(np.stack([np.cos(shift), np.sin(shift)]))
    each = piece // devices
    t = np.arange(devices)[:, None] + devices * np.arange(each)[None, :]
    angle = 2 * np.pi * (np.arange(rows)[:, None, None] * t[None] % width) / width
    c, s = np.cos(angle), np.sin(angle)
    table = np.stack([np.stack([c, -s], axis=2), np.stack([s, c], axis=2)])
    table = table.reshape(2 * rows, -1, 2 * LANES).transpose(1, 0, 2)
    last = jnp.stack(table_pair(table))
    order = np.zeros((2 * piece, 2 * piece))
    for a in range(devices):
        for part in range(2):
            for b in range(each):
                order[(a * 2 + part) * each + b, part * piece + a + devices * b] = 1.0
    return pl.pallas_call(
        lambda *refs: tile_kernel(devices, *refs),
        out_shape=jax.ShapeDtypeStruct((tiles, 2 * piece), jnp.float32),
        in_specs=[whole] * 5,
        out_specs=whole,
        scratch_shapes=[
            pltpu.VMEM((devices, tiles, 2 * rows), jnp.float32),
            pltpu.VMEM((tiles, LANES), jnp.float32),
        ],
        compiler_params=pltpu.CompilerParams(vmem_limit_bytes=40 * 2**20),
        name="finish_tiles",
    )(got, units, phase, last, bf16(order))


def to_all(values, devices):
    flat = jnp.broadcast_to(values.reshape(1, -1), (devices, values.size))
    return lax.all_to_all(flat, everywhere, split_axis=0, concat_axis=0, tiled=True)


def fast_local(sky_image, coef_dual, vis_dual, visibilities, kernel_blocks, tile_rows, tile_counts):
    bands = lax.axis_size("band")
    groups = lax.axis_size("vis")
    devices = bands * groups
    me = lax.axis_index(everywhere)
    kernel_here = kernel_blocks[0, 0]
    slots = tile_rows.shape[3]
    rows_dev, width = sky_image.shape
    piece = width // groups
    stripe = width // bands
    tiles = groups * slots
    live_slots = (
        jnp.arange(slots, dtype=jnp.int32)[None, :] < tile_counts[0, 0][:, None]
    ).astype(jnp.float32)[:, :, None, None]
    vis_data = visibilities[0, 0]
    vis_state = vis_dual[0, 0]
    columns_here = (tile_rows[0, 0] + lax.axis_index("band") * stripe).reshape(1, tiles)
    columns_here = jnp.concatenate([columns_here, columns_here], axis=1)
    weights = (live_slots * vis_state).astype(jnp.bfloat16)
    contrib = grid_back(kernel_here, weights).astype(jnp.bfloat16).reshape(tiles, 2 * piece)
    blocks, cols = gather_all(contrib, columns_here, devices)
    smooth = fast_synthesis(coef_dual)
    new_image, extrap, picked, units = image_step(
        blocks, cols, me, sky_image, smooth, groups, slots, piece
    )
    got, units, below = exchange(picked, units, extrap, devices)
    tile = finish_tiles(got, units, devices, groups, slots, rows_dev, piece)
    tile = tile.astype(jnp.bfloat16).reshape(groups, slots, 2, piece)
    coeffs = fast_analysis(extrap, below[:6])
    predicted = degrid(kernel_here, tile)
    residual = live_slots * (vis_state + predicted - vis_data)
    sums = jnp.stack(
        [
            jnp.sum(jnp.abs(coeffs)),
            jnp.sum(residual * residual),
            jnp.sum(live_slots * vis_data * vis_data),
        ]
    )
    sums = jnp.sum(to_all(sums, devices), axis=0)
    threshold = 0.5 * sums[0] / (width * width)
    coef_dual = jnp.clip(coef_dual + coeffs, -threshold, threshold)
    radius = 0.5 * jnp.sqrt(sums[2] + 1e-06)
    size_value = jnp.sqrt(sums[1] + 1e-06)
    vis_state = residual * (1.0 - jnp.minimum(1.0, radius / size_value))
    return (new_image, coef_dual, vis_state[None, None])


def body_for(mesh):
    devices = mesh.shape["band"] * mesh.shape["vis"]
    relayed = mesh.shape["band"] == 2 and mesh.shape["vis"] % 4 == 0 and devices == 32

    def body(sky_image, *rest):
        rows, width = sky_image.shape
        piece = width // mesh.shape["vis"]
        tiles = rest[4].shape[2] * rest[4].shape[3]
        if relayed and rows == LANES and piece == 2 * LANES and 2 * tiles == LANES:
            return fast_local(sky_image, *rest)
        return local(sky_image, *rest)

    return body


def solution(mesh):
    return jax.shard_map(
        body_for(mesh),
        mesh=mesh,
        in_specs=(
            P(("band", "vis"), None),
            P(None, ("band", "vis"), None),
            P("band", "vis", None, None, None, None),
            P("band", "vis", None, None, None, None),
            P("band", "vis", None, None, None, None, None),
            P("band", "vis", None, None),
            P("band", "vis", None),
        ),
        out_specs=(
            P(("band", "vis"), None),
            P(None, ("band", "vis"), None),
            P("band", "vis", None, None, None, None),
        ),
        check_vma=False,
    )
```

```python
import math

import jax
import numpy as np
import jax.numpy as jnp
from jax import lax
from jax.experimental import pallas as pl
from jax.experimental.pallas import tpu as pltpu
from jax.sharding import PartitionSpec as P

IMG = 4096


low_taps = (
    -0.010597401784997278,
    0.032883011666982945,
    0.030841381835986965,
    -0.18703481171888114,
    -0.02798376941698385,
    0.6308807679295904,
    0.7148465705525415,
    0.23037781330885523,
)
high_taps = tuple(((-1.0) ** offset * low_taps[7 - offset] for offset in range(8)))
highest = lax.Precision.HIGHEST


def shifted(block, axis, distance):
    devices = range(lax.axis_size(axis))
    route = [((i - distance) % len(devices), i) for i in devices]
    return lax.ppermute(block, axis, route)


def dft_table(table_size, sign):
    positions = jnp.arange(table_size, dtype=jnp.int32)
    phase = positions[:, None] * positions[None, :] % table_size
    angle = 2.0 * math.pi / table_size * phase.astype(jnp.float32)
    return (jnp.cos(angle), sign * jnp.sin(angle))


def section_one(table, values):
    return jnp.einsum("kn,...nm->...km", table, values, precision=highest)


def section_two(table, values):
    return jnp.einsum("qm,...km->...qk", table, values, precision=highest)


def dft_last(real_in, imag_in, sign):
    leading = real_in.shape[:-1]
    length = real_in.shape[-1]
    inner_len = 64
    outer_len = length // inner_len
    split_real = real_in.reshape(leading + (outer_len, inner_len))
    table_real, table_imag = dft_table(outer_len, sign)
    first_real = section_one(table_real, split_real)
    first_imag = section_one(table_imag, split_real)
    if imag_in is not None:
        split_imag = imag_in.reshape(leading + (outer_len, inner_len))
        first_real = first_real - section_one(table_imag, split_imag)
        first_imag = first_imag + section_one(table_real, split_imag)
    outer_index = jnp.arange(outer_len, dtype=jnp.int32)
    inner_index = jnp.arange(inner_len, dtype=jnp.int32)
    twist_phase = outer_index[:, None] * inner_index[None, :] % length
    twist_angle = 2.0 * math.pi / length * twist_phase.astype(jnp.float32)
    twist_real = jnp.cos(twist_angle)
    twist_imag = sign * jnp.sin(twist_angle)
    mid_real = first_real * twist_real - first_imag * twist_imag
    mid_imag = first_real * twist_imag + first_imag * twist_real
    last_real, last_imag = dft_table(inner_len, sign)
    out_real = section_two(last_real, mid_real) - section_two(last_imag, mid_imag)
    out_imag = section_two(last_real, mid_imag) + section_two(last_imag, mid_real)
    factor = 1.0 / math.sqrt(length)
    return (
        (out_real * factor).reshape(leading + (length,)),
        (out_imag * factor).reshape(leading + (length,)),
    )


def pieces_from_image(extrap, band_count, group_count):
    rows_dev = extrap.shape[0]
    image_width = extrap.shape[1]
    stripe = image_width // band_count
    piece_cols = stripe // group_count
    piece_rows = image_width // group_count
    col_real, col_imag = dft_last(extrap, None, -1.0)
    shaped = jnp.stack([col_real, col_imag]).reshape(
        2, 1, 1, rows_dev, band_count, group_count, piece_cols
    )
    moved = lax.all_to_all(
        lax.all_to_all(shaped, "band", split_axis=4, concat_axis=1, tiled=True),
        "vis",
        split_axis=5,
        concat_axis=2,
        tiled=True,
    )
    columns = jnp.transpose(moved.reshape(2, image_width, piece_cols), (2, 0, 1))
    row_real, row_imag = dft_last(columns[:, 0], columns[:, 1], -1.0)
    stacked = (
        jnp.stack([row_real, row_imag], axis=1)
        .astype(jnp.bfloat16)
        .reshape(piece_cols, 2, group_count, piece_rows)
    )
    pieces = lax.all_to_all(stacked, "vis", split_axis=2, concat_axis=0, tiled=True)
    return pieces.reshape(stripe, 2, piece_rows)


def image_from_pieces(piece_sum, band_count, group_count):
    stripe = piece_sum.shape[0]
    piece_rows = piece_sum.shape[2]
    piece_cols = stripe // group_count
    image_width = piece_rows * group_count
    rows_dev = image_width // (band_count * group_count)
    spread = lax.all_to_all(
        piece_sum.reshape(stripe, 2, 1, piece_rows), "vis", split_axis=0, concat_axis=2, tiled=True
    )
    spread = spread.reshape(piece_cols, 2, image_width)
    col_real, col_imag = dft_last(spread[:, 0], spread[:, 1], 1.0)
    stacked = jnp.transpose(jnp.stack([col_real, col_imag]), (0, 2, 1))
    shaped = stacked.reshape(2, band_count, group_count, rows_dev, 1, 1, piece_cols)
    moved = lax.all_to_all(
        lax.all_to_all(shaped, "band", split_axis=1, concat_axis=4, tiled=True),
        "vis",
        split_axis=2,
        concat_axis=5,
        tiled=True,
    )
    moved = moved.reshape(2, rows_dev, image_width)
    out_real, out_imag = dft_last(moved[0], moved[1], 1.0)
    return out_real


def cols_down(field):
    image_width = field.shape[1]
    extended = jnp.concatenate([field, field[:, :6]], axis=1)
    low_part = 0.0
    high_part = 0.0
    for offset in range(8):
        taken = extended[:, offset : offset + image_width : 2]
        low_part = low_part + low_taps[offset] * taken
        high_part = high_part + high_taps[offset] * taken
    return (low_part, high_part)


def cols_up(low_part, high_part):
    halves = []
    for parity in range(2):
        summed = 0.0
        for delay in range(4):
            summed = summed + low_taps[parity + 2 * delay] * jnp.roll(low_part, delay, axis=1)
            summed = summed + high_taps[parity + 2 * delay] * jnp.roll(high_part, delay, axis=1)
        halves.append(summed)
    return jnp.stack(halves, axis=2).reshape(low_part.shape[0], 2 * low_part.shape[1])


def rows_up(low_ext, high_ext, half_rows):
    halves = []
    for parity in range(2):
        summed = 0.0
        for delay in range(4):
            begin = 3 - delay
            summed = summed + low_taps[parity + 2 * delay] * low_ext[begin : begin + half_rows]
            summed = summed + high_taps[parity + 2 * delay] * high_ext[begin : begin + half_rows]
        halves.append(summed)
    return jnp.stack(halves, axis=1).reshape(2 * half_rows, low_ext.shape[1])


def analysis(extrap):
    rows_dev = extrap.shape[0]
    taken_rows = min(6, rows_dev)
    parts_list = [extrap]
    parts_list.append(shifted(extrap[:taken_rows], ("band", "vis"), -1))
    extended = jnp.concatenate(parts_list, axis=0)
    half_rows = rows_dev // 2
    rows_low = 0.0
    rows_high = 0.0
    for offset in range(8):
        taken = extended[offset : offset + 2 * half_rows : 2]
        rows_low = rows_low + low_taps[offset] * taken
        rows_high = rows_high + high_taps[offset] * taken
    low_low, low_high = cols_down(rows_low)
    high_low, high_high = cols_down(rows_high)
    return jnp.stack([low_low, low_high, high_low, high_high])


def synthesis(coef_dual):
    half_rows = coef_dual.shape[1]
    taken_rows = min(3, half_rows)
    parts_list = [shifted(coef_dual[:, half_rows - taken_rows :, :], ("band", "vis"), 1)]
    joined = jnp.concatenate(parts_list[::-1] + [coef_dual], axis=1)
    cols_low = rows_up(joined[0], joined[2], half_rows)
    cols_high = rows_up(joined[1], joined[3], half_rows)
    return cols_up(cols_low, cols_high)


def degrid(kernel_here, tiles):
    kernel_real = kernel_here[:, :, 0]
    kernel_imag = kernel_here[:, :, 1]
    tile_real = tiles[:, :, 0]
    tile_imag = tiles[:, :, 1]
    out_real = jnp.einsum(
        "qsat,qst->qsa", kernel_real, tile_real, preferred_element_type=jnp.float32
    ) - jnp.einsum("qsat,qst->qsa", kernel_imag, tile_imag, preferred_element_type=jnp.float32)
    out_imag = jnp.einsum(
        "qsat,qst->qsa", kernel_real, tile_imag, preferred_element_type=jnp.float32
    ) + jnp.einsum("qsat,qst->qsa", kernel_imag, tile_real, preferred_element_type=jnp.float32)
    return jnp.stack([out_real, out_imag], axis=2)


def grid_back(kernel_here, weights):
    kernel_real = kernel_here[:, :, 0]
    kernel_imag = kernel_here[:, :, 1]
    weight_real = weights[:, :, 0]
    weight_imag = weights[:, :, 1]
    grid_real = jnp.einsum(
        "qsat,qsa->qst", kernel_real, weight_real, preferred_element_type=jnp.float32
    ) + jnp.einsum("qsat,qsa->qst", kernel_imag, weight_imag, preferred_element_type=jnp.float32)
    grid_imag = jnp.einsum(
        "qsat,qsa->qst", kernel_real, weight_imag, preferred_element_type=jnp.float32
    ) - jnp.einsum("qsat,qsa->qst", kernel_imag, weight_real, preferred_element_type=jnp.float32)
    return jnp.stack([grid_real, grid_imag], axis=2)


def local(sky_image, coef_dual, vis_dual, visibilities, kernel_blocks, tile_rows, tile_counts):
    band_count = lax.axis_size("band")
    group_count = lax.axis_size("vis")
    kernel_here = kernel_blocks[0, 0]
    rows_here = tile_rows[0, 0]
    slot_count = rows_here.shape[1]
    live_slots = (
        jnp.arange(slot_count, dtype=jnp.int32)[None, :] < tile_counts[0, 0][:, None]
    ).astype(jnp.float32)[:, :, None, None]
    vis_data = visibilities[0, 0]
    vis_state = vis_dual[0, 0]
    image_width = sky_image.shape[1]
    stripe = image_width // band_count
    piece_rows = image_width // group_count
    incoming_rows = lax.all_to_all(rows_here, "vis", split_axis=0, concat_axis=0, tiled=True)
    data_part = jnp.sum(live_slots * vis_data * vis_data)
    weights = (live_slots * vis_state).astype(jnp.bfloat16)
    contrib = grid_back(kernel_here, weights)
    arrived = lax.all_to_all(contrib, "vis", split_axis=0, concat_axis=0, tiled=True)
    piece_sum = jax.ops.segment_sum(
        arrived.reshape(-1, 2, piece_rows), incoming_rows.reshape(-1), num_segments=stripe
    )
    adjoint_part = image_from_pieces(piece_sum, band_count, group_count)
    smooth = synthesis(coef_dual)
    new_image = jnp.maximum(sky_image - smooth - adjoint_part, 0.0)
    extrap = 2.0 * new_image - sky_image
    coeffs = analysis(extrap)
    abs_total = jnp.sum(jnp.abs(coeffs))
    coef_total = lax.psum(abs_total, ("band", "vis"))
    threshold = 0.5 * coef_total / (IMG * IMG)
    coef_dual = jnp.clip(coef_dual + coeffs, -threshold, threshold)
    piece_grid = pieces_from_image(extrap, band_count, group_count)
    tiles = lax.all_to_all(
        piece_grid[incoming_rows], "vis", split_axis=0, concat_axis=0, tiled=True
    )
    predicted = degrid(kernel_here, tiles)
    residual = live_slots * (vis_state + predicted - vis_data)
    resid_square = jnp.sum(residual * residual)
    norm_square, data_square = lax.psum((resid_square, data_part), ("band", "vis"))
    radius = 0.5 * jnp.sqrt(data_square + 1e-06)
    size_value = jnp.sqrt(norm_square + 1e-06)
    vis_state = residual * (1.0 - jnp.minimum(1.0, radius / size_value))
    return (new_image, coef_dual, vis_state[None, None])


high = lax.Precision.HIGH
everywhere = ("band", "vis")


def wave_tables(length, digit_low):
    digit_high = length // digit_low
    low = np.arange(digit_low)
    wide = np.arange(digit_high)
    full = 2.0 * np.pi
    small = full * (low[:, None] * low[None, :] % digit_low) / digit_low
    twist = full * (low[:, None] * wide[None, :]) / length
    large = full * (wide[:, None] * wide[None, :] % digit_high) / digit_high
    return small, twist, large


def complex_matrix(angle, sign):
    c = np.cos(angle)
    s = sign * np.sin(angle)
    return np.stack([np.stack([c, -s], axis=1), np.stack([s, c], axis=1)])


def f32(values):
    return jnp.asarray(np.asarray(values, np.float32))


def bf16(values):
    return f32(values).astype(jnp.bfloat16)


def analysis_matrix(half):
    matrix = np.zeros((2, half, 2 * half + 6))
    for k in range(half):
        for j in range(8):
            matrix[0, k, 2 * k + j] = low_taps[j]
            matrix[1, k, 2 * k + j] = high_taps[j]
    return matrix.reshape(2 * half, 2 * half + 6)


def synthesis_matrix(half):
    matrix = np.zeros((2 * half, 2, half + 3))
    for n in range(2 * half):
        for delay in range(4):
            tap = n % 2 + 2 * delay
            matrix[n, 0, n // 2 - delay + 3] = low_taps[tap]
            matrix[n, 1, n // 2 - delay + 3] = high_taps[tap]
    return matrix


def fast_analysis(extrap, halo):
    rows_dev, width = extrap.shape
    extended = jnp.concatenate([extrap, halo], axis=0)
    by_rows = jnp.einsum("ij,jn->in", f32(analysis_matrix(rows_dev // 2)), extended, precision=high)
    size = 256
    blocks = by_rows.reshape(rows_dev, width // size, size)
    following = jnp.roll(blocks, -1, axis=1)[:, :, :6]
    matrix = analysis_matrix(size // 2)
    out = jnp.einsum("rbi,ji->rbj", blocks, f32(matrix[:, :size]), precision=high)
    out = out + jnp.einsum("rbi,ji->rbj", following, f32(matrix[:, size:]), precision=high)
    out = out.reshape(2, rows_dev // 2, width // size, 2, size // 2)
    return jnp.transpose(out, (0, 3, 1, 2, 4)).reshape(4, rows_dev // 2, width // 2)


def fast_synthesis(coef_dual):
    half_rows, half_width = coef_dual.shape[1:]
    halo = shifted(coef_dual[:, half_rows - 3 :, :], everywhere, 1)
    joined = jnp.concatenate([halo, coef_dual], axis=1)
    joined = joined.reshape(2, 2, half_rows + 3, half_width)
    by_rows = jnp.einsum("irj,rcjn->cin", f32(synthesis_matrix(half_rows)), joined, precision=high)
    size = 128
    blocks = by_rows.reshape(2, 2 * half_rows, half_width // size, size)
    before = jnp.roll(blocks, 1, axis=2)[:, :, :, size - 3 :]
    matrix = synthesis_matrix(size)
    out = jnp.einsum("cibk,nck->ibn", blocks, f32(matrix[:, :, 3:]), precision=high)
    out = out + jnp.einsum("cibk,nck->ibn", before, f32(matrix[:, :, :3]), precision=high)
    return out.reshape(2 * half_rows, 2 * half_width)


def cos_sums(values, size):
    half = size // 2
    if half < 2:
        return [values[0] + values[1], values[0] - values[1]]
    quarter = half // 2
    plus = [values[a] + values[half - a] for a in range(quarter)] + [values[quarter]]
    minus = [values[a] - values[half - a] for a in range(quarter)]
    out = [None] * (half + 1)
    out[0::2] = cos_sums(plus, half)
    for k in range(1, half, 2):
        total = minus[0]
        for a in range(1, quarter):
            total = total + minus[a] * math.cos(2 * math.pi * (a * k % size) / size)
        out[k] = total
    return out


def sin_sums(values, size):
    half = size // 2
    if half < 2:
        return [None] * (half + 1)
    quarter = half // 2
    plus = {a: values[a] + values[half - a] for a in range(1, quarter)}
    plus[quarter] = values[quarter]
    minus = [None] + [values[a] - values[half - a] for a in range(1, quarter)]
    out = [None] * (half + 1)
    out[0::2] = sin_sums(minus, half)
    for k in range(1, half, 2):
        total = None
        for a in range(1, quarter + 1):
            factor = math.sin(2 * math.pi * (a * k % size) / size)
            term = plus[a] if a * 4 == size and k % 4 == 1 else plus[a] * factor
            total = term if total is None else total + term
        out[k] = total
    return out


def even_odd(values):
    size = len(values)
    half = size // 2
    even = [values[0]] + [values[a] + values[size - a] for a in range(1, half)] + [values[half]]
    odd = [None] + [values[a] - values[size - a] for a in range(1, half)]
    return even, odd


def split(values):
    upper = values.astype(jnp.bfloat16)
    return upper, (values - upper.astype(jnp.float32)).astype(jnp.bfloat16)


def table_pair(values):
    upper = f32(values).astype(jnp.bfloat16)
    return upper, (f32(values) - upper.astype(jnp.float32)).astype(jnp.bfloat16)


def nt_dot(a, b):
    return lax.dot_general(a, b, (((1,), (1,)), ((), ())), preferred_element_type=jnp.float32)


def nn_dot(a, b):
    return lax.dot_general(a, b, (((1,), (0,)), ((), ())), preferred_element_type=jnp.float32)


LEVELS = 32000.0
MESH = pl.DeviceIdType.MESH
LANES = 128
whole = pl.BlockSpec(memory_space=pltpu.VMEM)


def place():
    band = lax.axis_index("band")
    vis = lax.axis_index("vis")
    groups = lax.axis_size("vis")
    z = vis // 4
    y = vis // 2 % 2
    core = vis % 2
    return band, z, y, core, groups


def taps_dot(values, tables):
    upper, lower = split(values)
    return nn_dot(upper, tables[0]) + nn_dot(lower, tables[0]) + nn_dot(upper, tables[1])


def gather_kernel(
    kernels_ref,
    weights_ref,
    cols_ref,
    coef_ref,
    up_ref,
    edge_ref,
    out_ref,
    all_cols_ref,
    smooth_ref,
    tail_ref,
    halo_ref,
    joined_ref,
    tall_ref,
    send_a,
    send_b,
    recv_a,
    recv_b,
    halo_sem,
):
    x, z, y, core, groups = place()
    levels = groups // 4
    devices = 2 * groups
    half_rows, half_width = coef_ref.shape[1:]

    def index(px, pz, py, pc):
        return px * groups + pz * 4 + py * 2 + pc

    def device(px, pz, py, pc):
        return (px, pz * 4 + py * 2 + pc)

    me = index(x, z, y, core)
    after, before = (me + 1) % devices, (me + devices - 1) % devices
    twin = device(x, z, y, 1 - core)
    line = [device(x, (z + k) % levels, y, core) for k in range(1, levels)]
    corners = [(1 - x, y), (x, 1 - y), (1 - x, 1 - y)]
    plane = [device(px, z, py, core) for px, py in corners]
    follower = (after // groups, after % groups)
    leader = (before // groups, before % groups)
    barrier = pltpu.get_barrier_semaphore()
    peers = line + plane + [twin, follower, leader]
    for peer in peers:
        pl.semaphore_signal(barrier, inc=1, device_id=peer, device_id_type=MESH)

    for c in range(4):
        tail_ref[3 * c : 3 * c + 3, :] = coef_ref[c, half_rows - 3 :, :]
    count = 16
    span = kernels_ref.shape[0] * count // out_ref.shape[1]
    lane = lax.broadcasted_iota(jnp.int32, (count, span), 1) // (span // count)
    mine = lane == lax.broadcasted_iota(jnp.int32, (count, span), 0)
    for i in range(out_ref.shape[1] // count):
        spread = [jnp.where(mine, weights_ref[part, i : i + 1, :], 0.0) for part in range(2)]
        spread = jnp.concatenate(spread, axis=0).astype(jnp.bfloat16)
        both = nn_dot(spread, kernels_ref[i * span : (i + 1) * span, :])
        both = jnp.concatenate([both[:count], both[count:]], axis=1)
        out_ref[me, i * count : (i + 1) * count, :] = both.astype(jnp.bfloat16)
    all_cols_ref[me] = cols_ref[...]
    pl.semaphore_wait(barrier, len(peers))

    started = []

    def start(block, target, slot):
        own_a, own_b = out_ref.at[block], all_cols_ref.at[block]
        for own, send, recv in ((own_a, send_a, recv_a), (own_b, send_b, recv_b)):
            copy = pltpu.make_async_remote_copy(
                src_ref=own,
                dst_ref=own,
                send_sem=send.at[slot],
                recv_sem=recv.at[block],
                device_id=target,
                device_id_type=MESH,
            )
            copy.start()
            started.append(copy)

    def got(block):
        for ref, send, recv in ((out_ref, send_a, recv_a), (all_cols_ref, send_b, recv_b)):
            pltpu.make_async_remote_copy(
                src_ref=ref.at[block],
                dst_ref=ref.at[block],
                send_sem=send.at[0],
                recv_sem=recv.at[block],
                device_id=twin,
                device_id_type=MESH,
            ).wait_recv()

    slots = iter(range(send_a.shape[0]))
    far = sorted(range(1, levels), key=lambda k: abs(k - levels / 2))
    for k in far:
        start(me, line[k - 1], next(slots))
    for target in plane:
        start(me, target, next(slots))
    edge = pltpu.make_async_remote_copy(
        src_ref=tail_ref,
        dst_ref=halo_ref,
        send_sem=halo_sem.at[0],
        recv_sem=halo_sem.at[1],
        device_id=follower,
        device_id_type=MESH,
    )
    edge.start()
    start(me, twin, next(slots))

    for c in range(4):
        joined_ref[c, 8:, :] = coef_ref[c]
    edge.wait()
    for c in range(4):
        joined_ref[c, 5:8, :] = halo_ref[3 * c : 3 * c + 3, :]

    line_blocks = [index(x, (z + levels - k) % levels, y, core) for k in range(1, levels)]
    for block in line_blocks:
        got(block)
        for target in plane:
            start(block, target, next(slots))
        start(block, twin, next(slots))

    def tall(i, carry):
        here = pl.ds(pl.multiple_of(i * LANES, LANES), LANES)
        for c in range(2):
            for k in range(half_rows // 8):
                low = [joined_ref[c, 8 + 8 * k - d : 16 + 8 * k - d, here] for d in range(4)]
                high = [joined_ref[c + 2, 8 + 8 * k - d : 16 + 8 * k - d, here] for d in range(4)]
                for parity in range(2):
                    total = 0.0
                    for d in range(4):
                        total = total + low_taps[parity + 2 * d] * low[d]
                        total = total + high_taps[parity + 2 * d] * high[d]
                    tall_ref[c, i, pl.ds(16 * k + parity, 8, stride=2), :] = total
        return carry

    lax.fori_loop(0, half_width // LANES, tall, 0)

    for px, py in corners:
        block = index(px, z, py, core)
        got(block)
        start(block, twin, next(slots))
    for k in range(1, levels):
        for px, py in corners:
            block = index(px, (z + levels - k) % levels, py, core)
            got(block)
            start(block, twin, next(slots))

    blocks = half_width // LANES

    def broad(i, carry):
        there = (i + blocks - 1) % blocks
        near = jnp.concatenate([tall_ref[0, i], tall_ref[1, i]], axis=1)
        last = jnp.concatenate([tall_ref[0, there], tall_ref[1, there]], axis=1)
        out = taps_dot(near, up_ref)
        first = taps_dot(last, edge_ref)
        at = pl.multiple_of(i * 2 * LANES, 2 * LANES)
        smooth_ref[:, pl.ds(at, LANES)] = out[:, :LANES] + first
        smooth_ref[:, pl.ds(pl.multiple_of(at + LANES, LANES), LANES)] = out[:, LANES:]
        return carry

    lax.fori_loop(0, blocks, broad, 0)

    for i in range(groups):
        bx, rest = i // (groups // 2), i % (groups // 2)
        got(bx * groups + rest * 2 + 1 - core)
    for copy in started:
        copy.wait_send()


def gather_all(kernels, weights, cols, coef, devices):
    tiles = weights.shape[1] * 16
    half_rows, half_width = coef.shape[1:]
    matrix = synthesis_matrix(LANES)
    near = matrix[:, :, 3:].transpose(1, 2, 0).reshape(2 * LANES, 2 * LANES)
    edge = np.zeros((2, LANES, LANES))
    edge[:, LANES - 3 :, :] = matrix[:LANES, :, :3].transpose(1, 2, 0)
    copies = 3 * 4 + 7 + 12
    return pl.pallas_call(
        gather_kernel,
        out_shape=(
            jax.ShapeDtypeStruct((devices, tiles, 2 * kernels.shape[1]), jnp.bfloat16),
            jax.ShapeDtypeStruct((devices,) + cols.shape, cols.dtype),
            jax.ShapeDtypeStruct((2 * half_rows, 2 * half_width), jnp.float32),
        ),
        in_specs=[whole] * 6,
        out_specs=(whole,) * 3,
        scratch_shapes=[
            pltpu.VMEM((16, half_width), jnp.float32),
            pltpu.VMEM((16, half_width), jnp.float32),
            pltpu.VMEM((4, half_rows + 8, half_width), jnp.float32),
            pltpu.VMEM((2, half_width // LANES, 2 * half_rows, LANES), jnp.float32),
            pltpu.SemaphoreType.DMA((copies,)),
            pltpu.SemaphoreType.DMA((copies,)),
            pltpu.SemaphoreType.DMA((devices,)),
            pltpu.SemaphoreType.DMA((devices,)),
            pltpu.SemaphoreType.DMA((2,)),
        ],
        compiler_params=pltpu.CompilerParams(
            collective_id=0, has_side_effects=True, vmem_limit_bytes=40 * 2**20
        ),
        name="gather_all",
    )(
        kernels,
        weights,
        cols,
        coef,
        jnp.stack(table_pair(near)),
        jnp.stack(table_pair(edge.reshape(2 * LANES, LANES))),
    )


def level(values):
    return jnp.round(values).astype(jnp.int32)


def image_kernel(
    low,
    block_ref,
    cols_ref,
    turn_ref,
    phase_ref,
    inv_ref,
    tw_ref,
    fwd_ref,
    sky_ref,
    smooth_ref,
    image_ref,
    extrap_ref,
    picked_ref,
    unit_ref,
    fold_ref,
    grid_ref,
    hot_ref,
    half_ref,
    spec_ref,
    rest_ref,
):
    rows = sky_ref.shape[0]
    tiles = block_ref.shape[0]
    kept = low // 2 + 1
    wide = LANES
    lane = lax.broadcasted_iota(jnp.int32, (1, LANES), 1)
    for i in range(tiles // LANES):
        columns = jnp.where(lane < LANES // 2, cols_ref[2 * i], cols_ref[2 * i + 1])
        k1 = columns % low
        k2 = columns // low
        flip = k1 >= kept
        k1 = jnp.where(flip, low - k1, k1)
        k2 = jnp.where(flip, wide - 1 - k2, k2)
        fold_ref[0, i : i + 1, :] = (k1 * wide + k2).astype(jnp.float32)
        fold_ref[1, i : i + 1, :] = jnp.where(flip, -1.0, 1.0)
    chunk = 512
    for j in range(tiles // chunk):
        both = nt_dot(turn_ref[...], block_ref[j * chunk : (j + 1) * chunk, :])
        for i in range(chunk // LANES):
            b = j * (chunk // LANES) + i
            real = both[:rows, i * LANES : (i + 1) * LANES]
            imag = both[rows:, i * LANES : (i + 1) * LANES]
            out_real = real * phase_ref[0] - imag * phase_ref[1]
            out_imag = (real * phase_ref[1] + imag * phase_ref[0]) * fold_ref[1, b : b + 1, :]
            grid_ref[:rows, b * LANES : (b + 1) * LANES] = out_real.astype(jnp.bfloat16)
            grid_ref[rows:, b * LANES : (b + 1) * LANES] = out_imag.astype(jnp.bfloat16)

    def scatter(p, carry):
        base = pl.multiple_of(p * 2 * wide, 2 * wide)
        row = (lax.broadcasted_iota(jnp.int32, (2 * wide, LANES), 0) + base).astype(jnp.float32)
        for i in range(tiles // LANES):
            hit = row == fold_ref[0, i : i + 1, :]
            hot_ref[pl.ds(base, 2 * wide), i * LANES : (i + 1) * LANES] = jnp.where(
                hit, 1.0, 0.0
            ).astype(jnp.bfloat16)
        folded = nt_dot(grid_ref[...], hot_ref[pl.ds(base, 2 * wide), :]).astype(jnp.bfloat16)
        for e in range(2):
            pair = jnp.concatenate(
                [folded[:rows, e * wide : (e + 1) * wide], folded[rows:, e * wide : (e + 1) * wide]],
                axis=1,
            )
            mid = nn_dot(pair, inv_ref[...])
            k1 = p * 2 + e
            tw_real, tw_imag = tw_ref[0, pl.ds(k1, 1), :], tw_ref[1, pl.ds(k1, 1), :]
            real, imag = mid[:, :wide], mid[:, wide:]
            half_ref[k1, :, :wide] = real * tw_real - imag * tw_imag
            half_ref[k1, :, wide:] = real * tw_imag + imag * tw_real
        return carry

    lax.fori_loop(0, (kept + 1) // 2, scatter, 0)

    def strip(i, carry):
        at = pl.ds(pl.multiple_of(i * 8, 8), 8)
        cos_part = cos_sums([half_ref[k, at, :wide] for k in range(kept)], low)
        sin_part = sin_sums([None] + [half_ref[k, at, wide:] for k in range(1, kept - 1)], low)
        extraps = []
        for a in range(low):
            k = min(a, low - a)
            if a == 0 or a == low // 2:
                adjoint = cos_part[k]
            elif a < low // 2:
                adjoint = cos_part[k] - sin_part[k]
            else:
                adjoint = cos_part[k] + sin_part[k]
            here = slice(a * wide, (a + 1) * wide)
            sky = sky_ref[at, here]
            image = jnp.maximum(sky - smooth_ref[at, here] - adjoint, 0.0)
            extrap = 2.0 * image - sky
            image_ref[at, here] = image
            extrap_ref[at, here] = extrap
            extraps.append(extrap)
        even, odd = even_odd(extraps)
        real_part = cos_sums(even, low)
        imag_part = sin_sums(odd, low)
        for k in range(kept):
            tw_real, tw_imag = tw_ref[0, k : k + 1, :], tw_ref[1, k : k + 1, :]
            real = real_part[k] * tw_real
            imag = -real_part[k] * tw_imag
            if 0 < k < kept - 1:
                real = real - imag_part[k] * tw_imag
                imag = imag - imag_part[k] * tw_real
            half_ref[k, at, :wide] = real
            half_ref[k, at, wide:] = imag
        return carry

    lax.fori_loop(0, rows // 8, strip, 0)

    for k in range(kept):
        upper, lower = split(half_ref[k])
        out = nn_dot(upper, fwd_ref[0]) + nn_dot(lower, fwd_ref[0]) + nn_dot(upper, fwd_ref[1])
        here = slice(k * wide, (k + 1) * wide)
        upper, lower = split(out)
        spec_ref[:rows, here] = upper[:, :wide]
        spec_ref[rows:, here] = upper[:, wide:]
        rest_ref[:rows, here] = lower[:, :wide]
        rest_ref[rows:, here] = lower[:, wide:]

    def pick(j, carry):
        at = pl.multiple_of(j * 2 * LANES, 2 * LANES)
        hot = hot_ref[: kept * wide, pl.ds(at, 2 * LANES)]
        got = nn_dot(spec_ref[...], hot) + nn_dot(rest_ref[...], hot)
        for h in range(2):
            sign = fold_ref[1, pl.ds(2 * j + h, 1), :]
            real = got[:rows, h * LANES : (h + 1) * LANES]
            imag = got[rows:, h * LANES : (h + 1) * LANES] * sign
            most = jnp.max(jnp.maximum(jnp.abs(real), jnp.abs(imag)), axis=0, keepdims=True)
            most = jnp.maximum(most, 1e-30)
            unit_ref[2 * j + h] = most * (1.0 / LEVELS)
            to_level = LEVELS / most
            packed = level(real * to_level) * 65536 + level(imag * to_level)
            to = pl.ds(pl.multiple_of(at + h * LANES, LANES), LANES)
            picked_ref[to, :] = packed.T
        return carry

    lax.fori_loop(0, tiles // (2 * LANES), pick, 0)


def image_step(blocks, cols, me, sky_image, smooth, groups, slots, piece):
    rows, width = sky_image.shape
    tiles = blocks.shape[0] * blocks.shape[1]
    low = width // LANES
    kept = low // 2 + 1
    turn = np.arange(piece)
    angle = (me * rows + jnp.arange(rows, dtype=jnp.int32))[:, None] * turn[None, :] % width
    angle = (2.0 * math.pi / width) * angle.astype(jnp.float32)
    cosine, sine = jnp.cos(angle), jnp.sin(angle)
    turn = jnp.concatenate(
        [jnp.concatenate([cosine, -sine], axis=1), jnp.concatenate([sine, cosine], axis=1)]
    ).astype(jnp.bfloat16)
    owner = np.arange(LANES) // slots % groups
    shift = 2 * np.pi * (np.arange(rows)[:, None] * owner[None, :] % groups) / groups
    phase = f32(np.stack([np.cos(shift), np.sin(shift)]))
    wide = np.arange(LANES)
    full = 2 * np.pi * (wide[:, None] * wide[None, :] % LANES) / LANES
    c, s = np.cos(full) / width, np.sin(full) / width
    inverse = bf16(np.block([[c, s], [-s, c]]))
    forward = jnp.stack(table_pair(np.block([[c, -s], [s, c]])))
    twist = 2 * np.pi * np.arange(kept + 1)[:, None] * wide[None, :] / width
    twist = f32(np.stack([np.cos(twist), np.sin(twist)]))
    return pl.pallas_call(
        lambda *refs: image_kernel(low, *refs),
        out_shape=(
            jax.ShapeDtypeStruct((rows, width), jnp.float32),
            jax.ShapeDtypeStruct((rows, width), jnp.float32),
            jax.ShapeDtypeStruct((tiles, rows), jnp.int32),
            jax.ShapeDtypeStruct((tiles // LANES, 1, LANES), jnp.float32),
        ),
        in_specs=[whole] * 9,
        out_specs=(whole,) * 4,
        scratch_shapes=[
            pltpu.VMEM((2, tiles // LANES, LANES), jnp.float32),
            pltpu.VMEM((2 * rows, tiles), jnp.bfloat16),
            pltpu.VMEM(((kept + 1) * LANES, tiles), jnp.bfloat16),
            pltpu.VMEM((kept + 1, rows, 2 * LANES), jnp.float32),
            pltpu.VMEM((2 * rows, kept * LANES), jnp.bfloat16),
            pltpu.VMEM((2 * rows, kept * LANES), jnp.bfloat16),
        ],
        compiler_params=pltpu.CompilerParams(vmem_limit_bytes=60 * 2**20),
        name="image_step",
    )(
        blocks.reshape(tiles, -1),
        cols,
        turn,
        phase,
        inverse,
        twist,
        forward,
        sky_image,
        smooth,
    )


def exchange_kernel(
    picked_ref, unit_ref, top_ref, got_ref, units_ref, below_ref, send_a, send_b, recv_a, recv_b, halo
):
    x, z, y, core, groups = place()
    devices = 2 * groups
    tiles = got_ref.shape[1]

    def flipped(value, bit):
        return value + (1 - 2 * (value // bit % 2)) * bit

    me = x * groups + z * 4 + y * 2 + core
    barrier = pltpu.get_barrier_semaphore()
    peers = []
    for code in sorted(range(1, devices), key=lambda code: -(code // 8 % 2)):
        vis = z * 4 + y * 2 + core
        for bit in (1, 2, 4, 8):
            if code & bit:
                vis = flipped(vis, bit)
        band = 1 - x if code & 16 else x
        peers.append((band, vis))
    for peer in peers:
        pl.semaphore_signal(barrier, inc=1, device_id=peer, device_id_type=MESH)
    before = (me + devices - 1) % devices
    pl.semaphore_wait(barrier, devices - 1)
    edge = pltpu.make_async_remote_copy(
        src_ref=top_ref,
        dst_ref=below_ref,
        send_sem=halo.at[0],
        recv_sem=halo.at[1],
        device_id=(before // groups, before % groups),
        device_id_type=MESH,
    )
    edge.start()
    copies = []
    for i, (band, vis) in enumerate(peers):
        to = band * groups + vis
        at = pl.ds(pl.multiple_of(to * tiles, tiles), tiles)
        copies.append(
            pltpu.make_async_remote_copy(
                src_ref=picked_ref.at[at, :],
                dst_ref=got_ref.at[me],
                send_sem=send_a.at[i],
                recv_sem=recv_a.at[i],
                device_id=(band, vis),
                device_id_type=MESH,
            )
        )
        copies.append(
            pltpu.make_async_remote_copy(
                src_ref=unit_ref.at[to // 2],
                dst_ref=units_ref.at[me],
                send_sem=send_b.at[i],
                recv_sem=recv_b.at[i],
                device_id=(band, vis),
                device_id_type=MESH,
            )
        )
    for copy in copies:
        copy.start()
    here = pl.ds(pl.multiple_of(me * tiles, tiles), tiles)
    got_ref[me] = picked_ref[here, :]
    units_ref[me] = unit_ref[me // 2]
    edge.wait()
    for copy in copies:
        copy.wait()


def exchange(picked, units, extrap, devices):
    tiles = picked.shape[0] // devices
    top = extrap[:8]
    return pl.pallas_call(
        exchange_kernel,
        out_shape=(
            jax.ShapeDtypeStruct((devices, tiles) + picked.shape[1:], picked.dtype),
            jax.ShapeDtypeStruct((devices,) + units.shape[1:], units.dtype),
            jax.ShapeDtypeStruct(top.shape, top.dtype),
        ),
        in_specs=[whole] * 3,
        out_specs=(whole,) * 3,
        scratch_shapes=[
            pltpu.SemaphoreType.DMA((devices - 1,)),
            pltpu.SemaphoreType.DMA((devices - 1,)),
            pltpu.SemaphoreType.DMA((devices - 1,)),
            pltpu.SemaphoreType.DMA((devices - 1,)),
            pltpu.SemaphoreType.DMA((2,)),
        ],
        compiler_params=pltpu.CompilerParams(collective_id=1, has_side_effects=True),
        name="exchange",
    )(picked, units, top)


def tile_kernel(
    devices, got_ref, units_ref, phase_ref, last_ref, order_ref, out_ref, mid_ref, unit_ref
):
    tiles, rows = phase_ref.shape[1:]
    group = LANES * 2 // 16
    units = jnp.concatenate([units_ref[d] for d in range(devices)], axis=0)
    units = jnp.concatenate([units] * (LANES // devices), axis=0).T
    unit_ref[...] = jnp.where(lax.axis_index("vis") % 2 == 0, units[:tiles], units[tiles:])

    def strip(i, carry):
        at = pl.multiple_of(i * 8, 8)
        here = pl.ds(at, 8)
        cosine, sine = phase_ref[0, here, :], phase_ref[1, here, :]
        reals, imags = [], []
        for d in range(devices):
            packed = got_ref[d, here, :]
            real = (packed + 32768) >> 16
            imag = packed - (real << 16)
            unit = unit_ref[here, d : d + 1]
            real = real.astype(jnp.float32) * unit
            imag = imag.astype(jnp.float32) * unit
            reals.append(real * cosine + imag * sine)
            imags.append(imag * cosine - real * sine)
        even, odd = even_odd(reals)
        cos_real, sin_real = cos_sums(even, devices), sin_sums(odd, devices)
        even, odd = even_odd(imags)
        cos_imag, sin_imag = cos_sums(even, devices), sin_sums(odd, devices)
        half = devices // 2
        for k in range(half + 1):
            if k == 0 or k == half:
                outs = [(k, cos_real[k], cos_imag[k])]
            else:
                outs = [
                    (k, cos_real[k] + sin_imag[k], cos_imag[k] - sin_real[k]),
                    (devices - k, cos_real[k] - sin_imag[k], cos_imag[k] + sin_real[k]),
                ]
            for t, real, imag in outs:
                mid_ref[t, here, :rows] = real
                mid_ref[t, here, rows:] = imag
        return carry

    lax.fori_loop(0, tiles // 8, strip, 0)
    lane = lax.broadcasted_iota(jnp.int32, (1, 2 * LANES), 1) // 16
    pieces = []
    for g in range(devices // group):
        total = None
        for e in range(group):
            upper, lower = split(mid_ref[g * group + e])
            out = nn_dot(upper, last_ref[0, g]) + nn_dot(lower, last_ref[0, g])
            out = out + nn_dot(upper, last_ref[1, g])
            out = jnp.where(lane == e, out, 0.0)
            total = out if total is None else total + out
        pieces.append(total.astype(jnp.bfloat16))
    tile = jnp.concatenate(pieces, axis=1)
    out_ref[...] = nn_dot(tile, order_ref[...])


def finish_tiles(got, units, devices, groups, slots, rows, piece):
    width = devices * rows
    tiles = groups * slots
    shift = np.arange(tiles)[:, None] // slots * np.arange(rows)[None, :] % groups
    shift = 2 * np.pi * shift / groups
    phase = f32(np.stack([np.cos(shift), np.sin(shift)]))
    each = piece // devices
    t = np.arange(devices)[:, None] + devices * np.arange(each)[None, :]
    angle = 2 * np.pi * (np.arange(rows)[:, None, None] * t[None] % width) / width
    c, s = np.cos(angle), np.sin(angle)
    table = np.stack([np.stack([c, -s], axis=2), np.stack([s, c], axis=2)])
    table = table.reshape(2 * rows, -1, 2 * LANES).transpose(1, 0, 2)
    last = jnp.stack(table_pair(table))
    order = np.zeros((2 * piece, 2 * piece))
    for a in range(devices):
        for part in range(2):
            for b in range(each):
                order[(a * 2 + part) * each + b, part * piece + a + devices * b] = 1.0
    return pl.pallas_call(
        lambda *refs: tile_kernel(devices, *refs),
        out_shape=jax.ShapeDtypeStruct((tiles, 2 * piece), jnp.float32),
        in_specs=[whole] * 5,
        out_specs=whole,
        scratch_shapes=[
            pltpu.VMEM((devices, tiles, 2 * rows), jnp.float32),
            pltpu.VMEM((tiles, LANES), jnp.float32),
        ],
        compiler_params=pltpu.CompilerParams(vmem_limit_bytes=40 * 2**20),
        name="finish_tiles",
    )(got, units, phase, last, bf16(order))


def to_all(values, devices):
    flat = jnp.broadcast_to(values.reshape(1, -1), (devices, values.size))
    return lax.all_to_all(flat, everywhere, split_axis=0, concat_axis=0, tiled=True)


def fast_local(sky_image, coef_dual, vis_dual, visibilities, kernel_blocks, tile_rows, tile_counts):
    bands = lax.axis_size("band")
    groups = lax.axis_size("vis")
    devices = bands * groups
    me = lax.axis_index(everywhere)
    kernel_here = kernel_blocks[0, 0]
    slots = tile_rows.shape[3]
    rows_dev, width = sky_image.shape
    piece = width // groups
    stripe = width // bands
    tiles = groups * slots
    live_slots = (
        jnp.arange(slots, dtype=jnp.int32)[None, :] < tile_counts[0, 0][:, None]
    ).astype(jnp.float32)[:, :, None, None]
    vis_data = visibilities[0, 0]
    vis_state = vis_dual[0, 0]
    columns_here = (tile_rows[0, 0] + lax.axis_index("band") * stripe).reshape(1, tiles)
    columns_here = jnp.concatenate([columns_here, columns_here], axis=1)
    weights = live_slots * vis_state
    weights = jnp.stack([weights, jnp.stack([weights[:, :, 1], -weights[:, :, 0]], axis=2)])
    weights = weights.reshape(2, tiles // 16, -1)
    kernels = kernel_here.reshape(-1, piece)
    blocks, cols, smooth = gather_all(kernels, weights, columns_here, coef_dual, devices)
    new_image, extrap, picked, units = image_step(
        blocks, cols, me, sky_image, smooth, groups, slots, piece
    )
    got, units, below = exchange(picked, units, extrap, devices)
    tile = finish_tiles(got, units, devices, groups, slots, rows_dev, piece)
    tile = tile.astype(jnp.bfloat16).reshape(groups, slots, 2, piece)
    coeffs = fast_analysis(extrap, below[:6])
    predicted = degrid(kernel_here, tile)
    residual = live_slots * (vis_state + predicted - vis_data)
    sums = jnp.stack(
        [
            jnp.sum(jnp.abs(coeffs)),
            jnp.sum(residual * residual),
            jnp.sum(live_slots * vis_data * vis_data),
        ]
    )
    sums = jnp.sum(to_all(sums, devices), axis=0)
    threshold = 0.5 * sums[0] / (width * width)
    coef_dual = jnp.clip(coef_dual + coeffs, -threshold, threshold)
    radius = 0.5 * jnp.sqrt(sums[2] + 1e-06)
    size_value = jnp.sqrt(sums[1] + 1e-06)
    vis_state = residual * (1.0 - jnp.minimum(1.0, radius / size_value))
    return (new_image, coef_dual, vis_state[None, None])


def body_for(mesh):
    devices = mesh.shape["band"] * mesh.shape["vis"]
    relayed = mesh.shape["band"] == 2 and mesh.shape["vis"] % 4 == 0 and devices == 32

    def body(sky_image, *rest):
        rows, width = sky_image.shape
        piece = width // mesh.shape["vis"]
        tiles = rest[4].shape[2] * rest[4].shape[3]
        if relayed and rows == LANES and piece == 2 * LANES and 2 * tiles == LANES:
            return fast_local(sky_image, *rest)
        return local(sky_image, *rest)

    return body


def solution(mesh):
    return jax.shard_map(
        body_for(mesh),
        mesh=mesh,
        in_specs=(
            P(("band", "vis"), None),
            P(None, ("band", "vis"), None),
            P("band", "vis", None, None, None, None),
            P("band", "vis", None, None, None, None),
            P("band", "vis", None, None, None, None, None),
            P("band", "vis", None, None),
            P("band", "vis", None),
        ),
        out_specs=(
            P(("band", "vis"), None),
            P(None, ("band", "vis"), None),
            P("band", "vis", None, None, None, None),
        ),
        check_vma=False,
    )
```

```python
import math

import jax
import numpy as np
import jax.numpy as jnp
from jax import lax
from jax.experimental import pallas as pl
from jax.experimental.pallas import tpu as pltpu
from jax.sharding import PartitionSpec as P

IMG = 4096


low_taps = (
    -0.010597401784997278,
    0.032883011666982945,
    0.030841381835986965,
    -0.18703481171888114,
    -0.02798376941698385,
    0.6308807679295904,
    0.7148465705525415,
    0.23037781330885523,
)
high_taps = tuple(((-1.0) ** offset * low_taps[7 - offset] for offset in range(8)))
highest = lax.Precision.HIGHEST


def shifted(block, axis, distance):
    devices = range(lax.axis_size(axis))
    route = [((i - distance) % len(devices), i) for i in devices]
    return lax.ppermute(block, axis, route)


def dft_table(table_size, sign):
    positions = jnp.arange(table_size, dtype=jnp.int32)
    phase = positions[:, None] * positions[None, :] % table_size
    angle = 2.0 * math.pi / table_size * phase.astype(jnp.float32)
    return (jnp.cos(angle), sign * jnp.sin(angle))


def section_one(table, values):
    return jnp.einsum("kn,...nm->...km", table, values, precision=highest)


def section_two(table, values):
    return jnp.einsum("qm,...km->...qk", table, values, precision=highest)


def dft_last(real_in, imag_in, sign):
    leading = real_in.shape[:-1]
    length = real_in.shape[-1]
    inner_len = 64
    outer_len = length // inner_len
    split_real = real_in.reshape(leading + (outer_len, inner_len))
    table_real, table_imag = dft_table(outer_len, sign)
    first_real = section_one(table_real, split_real)
    first_imag = section_one(table_imag, split_real)
    if imag_in is not None:
        split_imag = imag_in.reshape(leading + (outer_len, inner_len))
        first_real = first_real - section_one(table_imag, split_imag)
        first_imag = first_imag + section_one(table_real, split_imag)
    outer_index = jnp.arange(outer_len, dtype=jnp.int32)
    inner_index = jnp.arange(inner_len, dtype=jnp.int32)
    twist_phase = outer_index[:, None] * inner_index[None, :] % length
    twist_angle = 2.0 * math.pi / length * twist_phase.astype(jnp.float32)
    twist_real = jnp.cos(twist_angle)
    twist_imag = sign * jnp.sin(twist_angle)
    mid_real = first_real * twist_real - first_imag * twist_imag
    mid_imag = first_real * twist_imag + first_imag * twist_real
    last_real, last_imag = dft_table(inner_len, sign)
    out_real = section_two(last_real, mid_real) - section_two(last_imag, mid_imag)
    out_imag = section_two(last_real, mid_imag) + section_two(last_imag, mid_real)
    factor = 1.0 / math.sqrt(length)
    return (
        (out_real * factor).reshape(leading + (length,)),
        (out_imag * factor).reshape(leading + (length,)),
    )


def pieces_from_image(extrap, band_count, group_count):
    rows_dev = extrap.shape[0]
    image_width = extrap.shape[1]
    stripe = image_width // band_count
    piece_cols = stripe // group_count
    piece_rows = image_width // group_count
    col_real, col_imag = dft_last(extrap, None, -1.0)
    shaped = jnp.stack([col_real, col_imag]).reshape(
        2, 1, 1, rows_dev, band_count, group_count, piece_cols
    )
    moved = lax.all_to_all(
        lax.all_to_all(shaped, "band", split_axis=4, concat_axis=1, tiled=True),
        "vis",
        split_axis=5,
        concat_axis=2,
        tiled=True,
    )
    columns = jnp.transpose(moved.reshape(2, image_width, piece_cols), (2, 0, 1))
    row_real, row_imag = dft_last(columns[:, 0], columns[:, 1], -1.0)
    stacked = (
        jnp.stack([row_real, row_imag], axis=1)
        .astype(jnp.bfloat16)
        .reshape(piece_cols, 2, group_count, piece_rows)
    )
    pieces = lax.all_to_all(stacked, "vis", split_axis=2, concat_axis=0, tiled=True)
    return pieces.reshape(stripe, 2, piece_rows)


def image_from_pieces(piece_sum, band_count, group_count):
    stripe = piece_sum.shape[0]
    piece_rows = piece_sum.shape[2]
    piece_cols = stripe // group_count
    image_width = piece_rows * group_count
    rows_dev = image_width // (band_count * group_count)
    spread = lax.all_to_all(
        piece_sum.reshape(stripe, 2, 1, piece_rows), "vis", split_axis=0, concat_axis=2, tiled=True
    )
    spread = spread.reshape(piece_cols, 2, image_width)
    col_real, col_imag = dft_last(spread[:, 0], spread[:, 1], 1.0)
    stacked = jnp.transpose(jnp.stack([col_real, col_imag]), (0, 2, 1))
    shaped = stacked.reshape(2, band_count, group_count, rows_dev, 1, 1, piece_cols)
    moved = lax.all_to_all(
        lax.all_to_all(shaped, "band", split_axis=1, concat_axis=4, tiled=True),
        "vis",
        split_axis=2,
        concat_axis=5,
        tiled=True,
    )
    moved = moved.reshape(2, rows_dev, image_width)
    out_real, out_imag = dft_last(moved[0], moved[1], 1.0)
    return out_real


def cols_down(field):
    image_width = field.shape[1]
    extended = jnp.concatenate([field, field[:, :6]], axis=1)
    low_part = 0.0
    high_part = 0.0
    for offset in range(8):
        taken = extended[:, offset : offset + image_width : 2]
        low_part = low_part + low_taps[offset] * taken
        high_part = high_part + high_taps[offset] * taken
    return (low_part, high_part)


def cols_up(low_part, high_part):
    halves = []
    for parity in range(2):
        summed = 0.0
        for delay in range(4):
            summed = summed + low_taps[parity + 2 * delay] * jnp.roll(low_part, delay, axis=1)
            summed = summed + high_taps[parity + 2 * delay] * jnp.roll(high_part, delay, axis=1)
        halves.append(summed)
    return jnp.stack(halves, axis=2).reshape(low_part.shape[0], 2 * low_part.shape[1])


def rows_up(low_ext, high_ext, half_rows):
    halves = []
    for parity in range(2):
        summed = 0.0
        for delay in range(4):
            begin = 3 - delay
            summed = summed + low_taps[parity + 2 * delay] * low_ext[begin : begin + half_rows]
            summed = summed + high_taps[parity + 2 * delay] * high_ext[begin : begin + half_rows]
        halves.append(summed)
    return jnp.stack(halves, axis=1).reshape(2 * half_rows, low_ext.shape[1])


def analysis(extrap):
    rows_dev = extrap.shape[0]
    taken_rows = min(6, rows_dev)
    parts_list = [extrap]
    parts_list.append(shifted(extrap[:taken_rows], ("band", "vis"), -1))
    extended = jnp.concatenate(parts_list, axis=0)
    half_rows = rows_dev // 2
    rows_low = 0.0
    rows_high = 0.0
    for offset in range(8):
        taken = extended[offset : offset + 2 * half_rows : 2]
        rows_low = rows_low + low_taps[offset] * taken
        rows_high = rows_high + high_taps[offset] * taken
    low_low, low_high = cols_down(rows_low)
    high_low, high_high = cols_down(rows_high)
    return jnp.stack([low_low, low_high, high_low, high_high])


def synthesis(coef_dual):
    half_rows = coef_dual.shape[1]
    taken_rows = min(3, half_rows)
    parts_list = [shifted(coef_dual[:, half_rows - taken_rows :, :], ("band", "vis"), 1)]
    joined = jnp.concatenate(parts_list[::-1] + [coef_dual], axis=1)
    cols_low = rows_up(joined[0], joined[2], half_rows)
    cols_high = rows_up(joined[1], joined[3], half_rows)
    return cols_up(cols_low, cols_high)


def degrid(kernel_here, tiles):
    kernel_real = kernel_here[:, :, 0]
    kernel_imag = kernel_here[:, :, 1]
    tile_real = tiles[:, :, 0]
    tile_imag = tiles[:, :, 1]
    out_real = jnp.einsum(
        "qsat,qst->qsa", kernel_real, tile_real, preferred_element_type=jnp.float32
    ) - jnp.einsum("qsat,qst->qsa", kernel_imag, tile_imag, preferred_element_type=jnp.float32)
    out_imag = jnp.einsum(
        "qsat,qst->qsa", kernel_real, tile_imag, preferred_element_type=jnp.float32
    ) + jnp.einsum("qsat,qst->qsa", kernel_imag, tile_real, preferred_element_type=jnp.float32)
    return jnp.stack([out_real, out_imag], axis=2)


def grid_back(kernel_here, weights):
    kernel_real = kernel_here[:, :, 0]
    kernel_imag = kernel_here[:, :, 1]
    weight_real = weights[:, :, 0]
    weight_imag = weights[:, :, 1]
    grid_real = jnp.einsum(
        "qsat,qsa->qst", kernel_real, weight_real, preferred_element_type=jnp.float32
    ) + jnp.einsum("qsat,qsa->qst", kernel_imag, weight_imag, preferred_element_type=jnp.float32)
    grid_imag = jnp.einsum(
        "qsat,qsa->qst", kernel_real, weight_imag, preferred_element_type=jnp.float32
    ) - jnp.einsum("qsat,qsa->qst", kernel_imag, weight_real, preferred_element_type=jnp.float32)
    return jnp.stack([grid_real, grid_imag], axis=2)


def local(sky_image, coef_dual, vis_dual, visibilities, kernel_blocks, tile_rows, tile_counts):
    band_count = lax.axis_size("band")
    group_count = lax.axis_size("vis")
    kernel_here = kernel_blocks[0, 0]
    rows_here = tile_rows[0, 0]
    slot_count = rows_here.shape[1]
    live_slots = (
        jnp.arange(slot_count, dtype=jnp.int32)[None, :] < tile_counts[0, 0][:, None]
    ).astype(jnp.float32)[:, :, None, None]
    vis_data = visibilities[0, 0]
    vis_state = vis_dual[0, 0]
    image_width = sky_image.shape[1]
    stripe = image_width // band_count
    piece_rows = image_width // group_count
    incoming_rows = lax.all_to_all(rows_here, "vis", split_axis=0, concat_axis=0, tiled=True)
    data_part = jnp.sum(live_slots * vis_data * vis_data)
    weights = (live_slots * vis_state).astype(jnp.bfloat16)
    contrib = grid_back(kernel_here, weights)
    arrived = lax.all_to_all(contrib, "vis", split_axis=0, concat_axis=0, tiled=True)
    piece_sum = jax.ops.segment_sum(
        arrived.reshape(-1, 2, piece_rows), incoming_rows.reshape(-1), num_segments=stripe
    )
    adjoint_part = image_from_pieces(piece_sum, band_count, group_count)
    smooth = synthesis(coef_dual)
    new_image = jnp.maximum(sky_image - smooth - adjoint_part, 0.0)
    extrap = 2.0 * new_image - sky_image
    coeffs = analysis(extrap)
    abs_total = jnp.sum(jnp.abs(coeffs))
    coef_total = lax.psum(abs_total, ("band", "vis"))
    threshold = 0.5 * coef_total / (IMG * IMG)
    coef_dual = jnp.clip(coef_dual + coeffs, -threshold, threshold)
    piece_grid = pieces_from_image(extrap, band_count, group_count)
    tiles = lax.all_to_all(
        piece_grid[incoming_rows], "vis", split_axis=0, concat_axis=0, tiled=True
    )
    predicted = degrid(kernel_here, tiles)
    residual = live_slots * (vis_state + predicted - vis_data)
    resid_square = jnp.sum(residual * residual)
    norm_square, data_square = lax.psum((resid_square, data_part), ("band", "vis"))
    radius = 0.5 * jnp.sqrt(data_square + 1e-06)
    size_value = jnp.sqrt(norm_square + 1e-06)
    vis_state = residual * (1.0 - jnp.minimum(1.0, radius / size_value))
    return (new_image, coef_dual, vis_state[None, None])


high = lax.Precision.HIGH
everywhere = ("band", "vis")


def wave_tables(length, digit_low):
    digit_high = length // digit_low
    low = np.arange(digit_low)
    wide = np.arange(digit_high)
    full = 2.0 * np.pi
    small = full * (low[:, None] * low[None, :] % digit_low) / digit_low
    twist = full * (low[:, None] * wide[None, :]) / length
    large = full * (wide[:, None] * wide[None, :] % digit_high) / digit_high
    return small, twist, large


def complex_matrix(angle, sign):
    c = np.cos(angle)
    s = sign * np.sin(angle)
    return np.stack([np.stack([c, -s], axis=1), np.stack([s, c], axis=1)])


def f32(values):
    return jnp.asarray(np.asarray(values, np.float32))


def bf16(values):
    return f32(values).astype(jnp.bfloat16)


def analysis_matrix(half):
    matrix = np.zeros((2, half, 2 * half + 6))
    for k in range(half):
        for j in range(8):
            matrix[0, k, 2 * k + j] = low_taps[j]
            matrix[1, k, 2 * k + j] = high_taps[j]
    return matrix.reshape(2 * half, 2 * half + 6)


def synthesis_matrix(half):
    matrix = np.zeros((2 * half, 2, half + 3))
    for n in range(2 * half):
        for delay in range(4):
            tap = n % 2 + 2 * delay
            matrix[n, 0, n // 2 - delay + 3] = low_taps[tap]
            matrix[n, 1, n // 2 - delay + 3] = high_taps[tap]
    return matrix


def cos_sums(values, size):
    half = size // 2
    if half < 2:
        return [values[0] + values[1], values[0] - values[1]]
    quarter = half // 2
    plus = [values[a] + values[half - a] for a in range(quarter)] + [values[quarter]]
    minus = [values[a] - values[half - a] for a in range(quarter)]
    out = [None] * (half + 1)
    out[0::2] = cos_sums(plus, half)
    for k in range(1, half, 2):
        total = minus[0]
        for a in range(1, quarter):
            total = total + minus[a] * math.cos(2 * math.pi * (a * k % size) / size)
        out[k] = total
    return out


def sin_sums(values, size):
    half = size // 2
    if half < 2:
        return [None] * (half + 1)
    quarter = half // 2
    plus = {a: values[a] + values[half - a] for a in range(1, quarter)}
    plus[quarter] = values[quarter]
    minus = [None] + [values[a] - values[half - a] for a in range(1, quarter)]
    out = [None] * (half + 1)
    out[0::2] = sin_sums(minus, half)
    for k in range(1, half, 2):
        total = None
        for a in range(1, quarter + 1):
            factor = math.sin(2 * math.pi * (a * k % size) / size)
            term = plus[a] if a * 4 == size and k % 4 == 1 else plus[a] * factor
            total = term if total is None else total + term
        out[k] = total
    return out


def even_odd(values):
    size = len(values)
    half = size // 2
    even = [values[0]] + [values[a] + values[size - a] for a in range(1, half)] + [values[half]]
    odd = [None] + [values[a] - values[size - a] for a in range(1, half)]
    return even, odd


def split(values):
    upper = values.astype(jnp.bfloat16)
    return upper, (values - upper.astype(jnp.float32)).astype(jnp.bfloat16)


def table_pair(values):
    upper = f32(values).astype(jnp.bfloat16)
    return upper, (f32(values) - upper.astype(jnp.float32)).astype(jnp.bfloat16)


def nt_dot(a, b):
    return lax.dot_general(a, b, (((1,), (1,)), ((), ())), preferred_element_type=jnp.float32)


def nn_dot(a, b):
    return lax.dot_general(a, b, (((1,), (0,)), ((), ())), preferred_element_type=jnp.float32)


LEVELS = 32000.0
MESH = pl.DeviceIdType.MESH
LANES = 128
whole = pl.BlockSpec(memory_space=pltpu.VMEM)


def place():
    band = lax.axis_index("band")
    vis = lax.axis_index("vis")
    groups = lax.axis_size("vis")
    z = vis // 4
    y = vis // 2 % 2
    core = vis % 2
    return band, z, y, core, groups


def taps_dot(values, tables):
    upper, lower = split(values)
    return nn_dot(upper, tables[0]) + nn_dot(lower, tables[0]) + nn_dot(upper, tables[1])


def level(values):
    return jnp.round(values).astype(jnp.int32)


def step_kernel(
    low,
    kernels_hbm,
    coef_hbm,
    sky_hbm,
    up_hbm,
    edge_hbm,
    turn_hbm,
    inv_hbm,
    fwd_hbm,
    near_hbm,
    next_hbm,
    last_hbm,
    order_hbm,
    weights_ref,
    cols_ref,
    vis_ref,
    phase_ref,
    shift_ref,
    tw_ref,
    image_hbm,
    merged_ref,
    residual_ref,
    sums_ref,
    kernels_ref,
    joined_ref,
    sky_ref,
    up_ref,
    edge_ref,
    turn_ref,
    inv_ref,
    fwd_ref,
    near_ref,
    next_ref,
    last_ref,
    order_ref,
    load_sem,
    tail_ref,
    halo_ref,
    block_ref,
    all_cols_ref,
    tall_ref,
    smooth_ref,
    fold_ref,
    grid_ref,
    hot_ref,
    half_ref,
    spec_ref,
    rest_ref,
    extrap_ref,
    picked_ref,
    unit_ref,
    got_ref,
    units_ref,
    mid_ref,
    column_ref,
    all_sums_ref,
    send_a,
    send_b,
    recv_a,
    recv_b,
    send_p,
    send_u,
    recv_p,
    recv_u,
    send_s,
    recv_s,
    halo_sem,
):
    x, z, y, core, groups = place()
    levels = groups // 4
    devices = 2 * groups
    half_rows, half_width = coef_hbm.shape[1:]
    rows = 2 * half_rows
    tiles = block_ref.shape[1]
    kept = low // 2 + 1
    wide = LANES

    def index(px, pz, py, pc):
        return px * groups + pz * 4 + py * 2 + pc

    def device(px, pz, py, pc):
        return (px, pz * 4 + py * 2 + pc)

    def ident(number):
        return (number // groups, number % groups)

    def remote(src, dst, send, recv, target):
        return pltpu.make_async_remote_copy(
            src_ref=src,
            dst_ref=dst,
            send_sem=send,
            recv_sem=recv,
            device_id=target,
            device_id_type=MESH,
        )

    me = index(x, z, y, core)
    after, before = (me + 1) % devices, (me + devices - 1) % devices
    twin = device(x, z, y, 1 - core)
    line = [device(x, (z + k) % levels, y, core) for k in range(1, levels)]
    corners = [(1 - x, y), (x, 1 - y), (1 - x, 1 - y)]
    plane = [device(px, z, py, core) for px, py in corners]
    barrier = pltpu.get_barrier_semaphore()
    peers = line + plane + [twin, ident(after), ident(before)]
    for peer in peers:
        pl.semaphore_signal(barrier, inc=1, device_id=peer, device_id_type=MESH)

    sources = [
        (kernels_hbm, kernels_ref),
        (coef_hbm, joined_ref.at[:, pl.ds(8, half_rows), :]),
        (up_hbm, up_ref),
        (edge_hbm, edge_ref),
        (turn_hbm, turn_ref),
        (inv_hbm, inv_ref),
        (sky_hbm, sky_ref),
        (fwd_hbm, fwd_ref),
        (near_hbm, near_ref),
        (next_hbm, next_ref),
        (last_hbm, last_ref),
        (order_hbm, order_ref),
    ]
    loads = [
        pltpu.make_async_copy(src, dst, load_sem.at[i]) for i, (src, dst) in enumerate(sources)
    ]
    for load in loads:
        load.start()
    loads[0].wait()
    count = 16
    span = kernels_ref.shape[0] * count // tiles
    lane = lax.broadcasted_iota(jnp.int32, (count, span), 1) // (span // count)
    mine = lane == lax.broadcasted_iota(jnp.int32, (count, span), 0)
    for i in range(tiles // count):
        spread = [jnp.where(mine, weights_ref[part, i : i + 1, :], 0.0) for part in range(2)]
        spread = jnp.concatenate(spread, axis=0).astype(jnp.bfloat16)
        both = nn_dot(spread, kernels_ref[i * span : (i + 1) * span, :])
        both = jnp.concatenate([both[:count], both[count:]], axis=1)
        block_ref[me, i * count : (i + 1) * count, :] = both.astype(jnp.bfloat16)
    all_cols_ref[me] = cols_ref[...]
    loads[1].wait()
    for c in range(4):
        tail_ref[3 * c : 3 * c + 3, :] = joined_ref[c, half_rows + 5 :, :]
    pl.semaphore_wait(barrier, len(peers))

    started = []

    def start(block, target, slot):
        own_a, own_b = block_ref.at[block], all_cols_ref.at[block]
        for own, send, recv in ((own_a, send_a, recv_a), (own_b, send_b, recv_b)):
            copy = remote(own, own, send.at[slot], recv.at[block], target)
            copy.start()
            started.append(copy)

    def got(block):
        for ref, send, recv in ((block_ref, send_a, recv_a), (all_cols_ref, send_b, recv_b)):
            own = ref.at[block]
            remote(own, own, send.at[0], recv.at[block], twin).wait_recv()

    slots = iter(range(send_a.shape[0]))
    far = sorted(range(1, levels), key=lambda k: abs(k - levels / 2))
    for k in far:
        start(me, line[k - 1], next(slots))
    for target in plane:
        start(me, target, next(slots))
    edge = remote(tail_ref, halo_ref, halo_sem.at[0], halo_sem.at[1], ident(after))
    edge.start()
    start(me, twin, next(slots))
    edge.wait()
    for c in range(4):
        joined_ref[c, 5:8, :] = halo_ref[3 * c : 3 * c + 3, :]

    line_blocks = [index(x, (z + levels - k) % levels, y, core) for k in range(1, levels)]
    for block in line_blocks:
        got(block)
        for target in plane:
            start(block, target, next(slots))
        start(block, twin, next(slots))
    strips = half_width // LANES

    def tall(i, carry):
        here = pl.ds(pl.multiple_of(i * LANES, LANES), LANES)
        for c in range(2):
            for k in range(half_rows // 8):
                lows = [joined_ref[c, 8 + 8 * k - d : 16 + 8 * k - d, here] for d in range(4)]
                highs = [joined_ref[c + 2, 8 + 8 * k - d : 16 + 8 * k - d, here] for d in range(4)]
                for parity in range(2):
                    total = 0.0
                    for d in range(4):
                        total = total + low_taps[parity + 2 * d] * lows[d]
                        total = total + high_taps[parity + 2 * d] * highs[d]
                    tall_ref[c * strips + i, pl.ds(16 * k + parity, 8, stride=2), :] = total
        return carry

    lax.fori_loop(0, strips, tall, 0)

    for px, py in corners:
        block = index(px, z, py, core)
        got(block)
        start(block, twin, next(slots))
    for k in range(1, levels):
        for px, py in corners:
            block = index(px, (z + levels - k) % levels, py, core)
            got(block)
            start(block, twin, next(slots))
    loads[2].wait()
    loads[3].wait()

    def broad(i, carry):
        there = (i + strips - 1) % strips
        near = jnp.concatenate([tall_ref[i], tall_ref[strips + i]], axis=1)
        last = jnp.concatenate([tall_ref[there], tall_ref[strips + there]], axis=1)
        out = taps_dot(near, up_ref)
        first = taps_dot(last, edge_ref)
        smooth_ref[2 * i] = out[:, :LANES] + first
        smooth_ref[2 * i + 1] = out[:, LANES:]
        return carry

    lax.fori_loop(0, strips, broad, 0)
    loads[4].wait()
    loads[5].wait()

    for i in range(groups):
        bx, rest = i // (groups // 2), i % (groups // 2)
        got(bx * groups + rest * 2 + 1 - core)

    total_tiles = devices * tiles
    lane = lax.broadcasted_iota(jnp.int32, (1, LANES), 1)
    for i in range(devices // 2):
        columns = jnp.where(lane < tiles, all_cols_ref[2 * i], all_cols_ref[2 * i + 1])
        k1 = columns % low
        k2 = columns // low
        flip = k1 >= kept
        k1 = jnp.where(flip, low - k1, k1)
        k2 = jnp.where(flip, wide - 1 - k2, k2)
        fold_ref[0, i : i + 1, :] = (k1 * wide + k2).astype(jnp.float32)
        fold_ref[1, i : i + 1, :] = jnp.where(flip, -1.0, 1.0)
    chunk = 512
    for j in range(total_tiles // chunk):
        some = block_ref[j * chunk // tiles : (j + 1) * chunk // tiles]
        both = nt_dot(turn_ref[...], some.reshape(chunk, -1))
        for i in range(chunk // LANES):
            b = j * (chunk // LANES) + i
            real = both[:rows, i * LANES : (i + 1) * LANES]
            imag = both[rows:, i * LANES : (i + 1) * LANES]
            out_real = real * phase_ref[0] - imag * phase_ref[1]
            out_imag = (real * phase_ref[1] + imag * phase_ref[0]) * fold_ref[1, b : b + 1, :]
            grid_ref[:rows, b * LANES : (b + 1) * LANES] = out_real.astype(jnp.bfloat16)
            grid_ref[rows:, b * LANES : (b + 1) * LANES] = out_imag.astype(jnp.bfloat16)

    def scatter(p, carry):
        base = pl.multiple_of(p * 2 * wide, 2 * wide)
        row = (lax.broadcasted_iota(jnp.int32, (2 * wide, LANES), 0) + base).astype(jnp.float32)
        for i in range(total_tiles // LANES):
            hit = row == fold_ref[0, i : i + 1, :]
            hot_ref[pl.ds(base, 2 * wide), i * LANES : (i + 1) * LANES] = jnp.where(
                hit, 1.0, 0.0
            ).astype(jnp.bfloat16)
        folded = nt_dot(grid_ref[...], hot_ref[pl.ds(base, 2 * wide), :]).astype(jnp.bfloat16)
        for e in range(2):
            here = slice(e * wide, (e + 1) * wide)
            pair = jnp.concatenate([folded[:rows, here], folded[rows:, here]], axis=1)
            mid = nn_dot(pair, inv_ref[...])
            k1 = p * 2 + e
            tw_real, tw_imag = tw_ref[0, pl.ds(k1, 1), :], tw_ref[1, pl.ds(k1, 1), :]
            real, imag = mid[:, :wide], mid[:, wide:]
            half_ref[k1, :, :wide] = real * tw_real - imag * tw_imag
            half_ref[k1, :, wide:] = real * tw_imag + imag * tw_real
        return carry

    lax.fori_loop(0, (kept + 1) // 2, scatter, 0)
    loads[6].wait()

    def strip(i, carry):
        at = pl.ds(pl.multiple_of(i * 8, 8), 8)
        cos_part = cos_sums([half_ref[k, at, :wide] for k in range(kept)], low)
        sin_part = sin_sums([None] + [half_ref[k, at, wide:] for k in range(1, kept - 1)], low)
        extraps = []
        for a in range(low):
            k = min(a, low - a)
            if a == 0 or a == low // 2:
                adjoint = cos_part[k]
            elif a < low // 2:
                adjoint = cos_part[k] - sin_part[k]
            else:
                adjoint = cos_part[k] + sin_part[k]
            here = slice(a * wide, (a + 1) * wide)
            sky = sky_ref[at, here]
            image = jnp.maximum(sky - smooth_ref[a, at, :] - adjoint, 0.0)
            extrap = 2.0 * image - sky
            sky_ref[at, here] = image
            extrap_ref[a, at, :] = extrap
            extraps.append(extrap)
        even, odd = even_odd(extraps)
        real_part = cos_sums(even, low)
        imag_part = sin_sums(odd, low)
        for k in range(kept):
            tw_real, tw_imag = tw_ref[0, k : k + 1, :], tw_ref[1, k : k + 1, :]
            real = real_part[k] * tw_real
            imag = -real_part[k] * tw_imag
            if 0 < k < kept - 1:
                real = real - imag_part[k] * tw_imag
                imag = imag - imag_part[k] * tw_real
            half_ref[k, at, :wide] = real
            half_ref[k, at, wide:] = imag
        return carry

    lax.fori_loop(0, rows // 8, strip, 0)
    store = pltpu.make_async_copy(sky_ref, image_hbm, load_sem.at[len(loads)])
    store.start()
    top = remote(
        extrap_ref.at[:, pl.ds(0, 8), :],
        extrap_ref.at[:, pl.ds(rows, 8), :],
        halo_sem.at[2],
        halo_sem.at[3],
        ident(before),
    )
    top.start()
    loads[7].wait()

    def spectrum(k, carry):
        out = taps_dot(half_ref[k], fwd_ref)
        here = pl.ds(pl.multiple_of(k * wide, wide), wide)
        upper, lower = split(out)
        spec_ref[:rows, here] = upper[:, :wide]
        spec_ref[rows:, here] = upper[:, wide:]
        rest_ref[:rows, here] = lower[:, :wide]
        rest_ref[rows:, here] = lower[:, wide:]
        return carry

    lax.fori_loop(0, kept, spectrum, 0)

    def sends(to):
        at = pl.ds(pl.multiple_of(to * tiles, tiles), tiles)
        return [
            remote(picked_ref.at[at, :], got_ref.at[me], send_p.at[to], recv_p.at[me], ident(to)),
            remote(unit_ref.at[to // 2], units_ref.at[me], send_u.at[to], recv_u.at[me], ident(to)),
        ]

    def arrivals(origin):
        at = pl.ds(0, tiles)
        return [
            remote(
                picked_ref.at[at, :], got_ref.at[origin], send_p.at[0], recv_p.at[origin], twin
            ),
            remote(unit_ref.at[0], units_ref.at[origin], send_u.at[0], recv_u.at[origin], twin),
        ]

    def pick(s, carry):
        half = levels // 2
        to_z = (z // half + 1 + s // levels) % 2 * half + s // 2 % half
        j = (x + 1 + s) % 2 * levels + to_z
        at = pl.multiple_of(j * 2 * LANES, 2 * LANES)
        hot = hot_ref[: kept * wide, pl.ds(at, 2 * LANES)]
        both = nn_dot(spec_ref[...], hot) + nn_dot(rest_ref[...], hot)
        for h in range(2):
            sign = fold_ref[1, pl.ds(2 * j + h, 1), :]
            real = both[:rows, h * LANES : (h + 1) * LANES]
            imag = both[rows:, h * LANES : (h + 1) * LANES] * sign
            most = jnp.max(jnp.maximum(jnp.abs(real), jnp.abs(imag)), axis=0, keepdims=True)
            most = jnp.maximum(most, 1e-30)
            unit_ref[2 * j + h] = most * (1.0 / LEVELS)
            to_level = LEVELS / most
            packed = level(real * to_level) * 65536 + level(imag * to_level)
            to = pl.ds(pl.multiple_of(at + h * LANES, LANES), LANES)
            picked_ref[to, :] = packed.T
        for i in range(4):
            to = j * 4 + i

            @pl.when(to != me)
            def _():
                for copy in sends(to):
                    copy.start()

        return carry

    lax.fori_loop(0, devices // 4, pick, 0)
    got_ref[me] = picked_ref[pl.ds(pl.multiple_of(me * tiles, tiles), tiles), :]
    units_ref[me] = unit_ref[me // 2]
    top.wait()
    loads[8].wait()
    loads[9].wait()

    def rows_down(i, carry):
        for k in range(half_rows // 8):
            lows, highs = 0.0, 0.0
            for tap in range(8):
                taken = extrap_ref[i, pl.ds(16 * k + tap, 8, stride=2), :]
                lows = lows + low_taps[tap] * taken
                highs = highs + high_taps[tap] * taken
            tall_ref[i, 8 * k : 8 * k + 8, :] = lows
            tall_ref[i, half_rows + 8 * k : half_rows + 8 * k + 8, :] = highs
        return carry

    lax.fori_loop(0, low, rows_down, 0)

    def cols_down(b, absolute):
        here = jnp.concatenate([tall_ref[2 * b], tall_ref[2 * b + 1]], axis=1)
        out = taps_dot(here, near_ref) + taps_dot(tall_ref[(2 * b + 2) % low], next_ref)
        at = pl.ds(pl.multiple_of(b * LANES, LANES), LANES)
        for c in range(4):
            top_row, left = c // 2 * half_rows, c % 2 * LANES
            part = out[top_row : top_row + half_rows, left : left + LANES]
            absolute = absolute + jnp.abs(part)
            merged_ref[c, :, at] = joined_ref[c, 8:, at] + part
        return absolute

    absolute = lax.fori_loop(0, low // 2, cols_down, jnp.zeros((half_rows, LANES), jnp.float32))
    abs_total = jnp.sum(jnp.sum(absolute, axis=0, keepdims=True), axis=1, keepdims=True)
    loads[10].wait()
    loads[11].wait()

    def landed(k, carry):
        for copy in arrivals((me + k) % devices):
            copy.wait_recv()
        return carry

    lax.fori_loop(1, devices, landed, 0)

    units = jnp.concatenate([units_ref[d] for d in range(devices)], axis=0)
    units = jnp.concatenate([units] * (LANES // devices), axis=0).T
    column_ref[...] = jnp.where(core == 0, units[:tiles], units[tiles:])

    def finish(i, carry):
        here = pl.ds(pl.multiple_of(i * 8, 8), 8)
        cosine, sine = shift_ref[0, here, :], shift_ref[1, here, :]
        reals, imags = [], []
        for d in range(devices):
            packed = got_ref[d, here, :]
            real = (packed + 32768) >> 16
            imag = packed - (real << 16)
            unit = column_ref[here, d : d + 1]
            real = real.astype(jnp.float32) * unit
            imag = imag.astype(jnp.float32) * unit
            reals.append(real * cosine + imag * sine)
            imags.append(imag * cosine - real * sine)
        even, odd = even_odd(reals)
        cos_real, sin_real = cos_sums(even, devices), sin_sums(odd, devices)
        even, odd = even_odd(imags)
        cos_imag, sin_imag = cos_sums(even, devices), sin_sums(odd, devices)
        half = devices // 2
        for k in range(half + 1):
            if k == 0 or k == half:
                outs = [(k, cos_real[k], cos_imag[k])]
            else:
                outs = [
                    (k, cos_real[k] + sin_imag[k], cos_imag[k] - sin_real[k]),
                    (devices - k, cos_real[k] - sin_imag[k], cos_imag[k] + sin_real[k]),
                ]
            for t, real, imag in outs:
                mid_ref[t, here, :rows] = real
                mid_ref[t, here, rows:] = imag
        return carry

    lax.fori_loop(0, tiles // 8, finish, 0)
    group = 2 * LANES // 16
    lane = lax.broadcasted_iota(jnp.int32, (1, 2 * LANES), 1) // 16
    pieces = []
    for g in range(devices // group):
        total = None
        for e in range(group):
            upper, lower = split(mid_ref[g * group + e])
            out = nn_dot(upper, last_ref[0, g]) + nn_dot(lower, last_ref[0, g])
            out = out + nn_dot(upper, last_ref[1, g])
            out = jnp.where(lane == e, out, 0.0)
            total = out if total is None else total + out
        pieces.append(total.astype(jnp.bfloat16))
    tile = nn_dot(jnp.concatenate(pieces, axis=1), order_ref[...]).astype(jnp.bfloat16)
    piece = kernels_ref.shape[1]
    first, second = [], []
    for i in range(tiles // count):
        here = tile[i * count : (i + 1) * count]
        pair = jnp.concatenate([here[:, :piece], here[:, piece:]], axis=0)
        out = nt_dot(pair, kernels_ref[i * span : (i + 1) * span, :])
        first.append(jnp.sum(jnp.where(mine, out[:count], 0.0), axis=0, keepdims=True))
        second.append(jnp.sum(jnp.where(mine, out[count:], 0.0), axis=0, keepdims=True))
    first = jnp.concatenate(first, axis=0)
    second = jnp.concatenate(second, axis=0)
    visits = span // count // 2
    lane = lax.broadcasted_iota(jnp.int32, first.shape, 1) // visits % 2
    crossed = jnp.where(
        lane == 0, -pltpu.roll(second, span - visits, 1), pltpu.roll(second, visits, 1)
    )
    live = vis_ref[2]
    residual = live * (vis_ref[0] + first + crossed - vis_ref[1])
    residual_ref[...] = residual
    norms = []
    for values in (residual, vis_ref[1] * live):
        norms.append(jnp.sum(jnp.sum(values * values, axis=0, keepdims=True), axis=1, keepdims=True))
    lane = lax.broadcasted_iota(jnp.int32, (1, LANES), 1)
    row = jnp.where(lane == 0, abs_total, jnp.where(lane == 1, norms[0], norms[1]))
    all_sums_ref[me] = row

    def share(k, carry):
        to = (me + k) % devices
        own = all_sums_ref.at[me]
        remote(own, own, send_s.at[to], recv_s.at[me], ident(to)).start()
        return carry

    lax.fori_loop(1, devices, share, 0)
    for copy in started:
        copy.wait_send()
    store.wait()

    def shared(k, total):
        other = (me + k) % devices
        own = all_sums_ref.at[other]
        remote(own, own, send_s.at[other], recv_s.at[other], twin).wait_recv()
        return total

    lax.fori_loop(1, devices, shared, 0)
    total = all_sums_ref[0]
    for d in range(1, devices):
        total = total + all_sums_ref[d]
    sums_ref[...] = total

    def sent(k, carry):
        to = (me + k) % devices
        for copy in sends(to):
            copy.wait_send()
        own = all_sums_ref.at[me]
        remote(own, own, send_s.at[to], recv_s.at[me], ident(to)).wait_send()
        return carry

    lax.fori_loop(1, devices, sent, 0)


def step(kernels, coef, sky, weights, cols, vis, me, groups, slots, devices):
    rows, width = sky.shape
    piece = kernels.shape[1]
    tiles = groups * slots
    half_rows, half_width = coef.shape[1:]
    low = width // LANES
    kept = low // 2 + 1
    wide = np.arange(LANES)
    matrix = synthesis_matrix(LANES)
    up = matrix[:, :, 3:].transpose(1, 2, 0).reshape(2 * LANES, 2 * LANES)
    edge = np.zeros((2, LANES, LANES))
    edge[:, LANES - 3 :, :] = matrix[:LANES, :, :3].transpose(1, 2, 0)
    matrix = analysis_matrix(LANES).T
    following = np.zeros((LANES, 2 * LANES))
    following[:6] = matrix[2 * LANES :]
    turn = np.arange(piece)
    angle = (me * rows + jnp.arange(rows, dtype=jnp.int32))[:, None] * turn[None, :] % width
    angle = (2.0 * math.pi / width) * angle.astype(jnp.float32)
    cosine, sine = jnp.cos(angle), jnp.sin(angle)
    turn = jnp.concatenate(
        [jnp.concatenate([cosine, -sine], axis=1), jnp.concatenate([sine, cosine], axis=1)]
    ).astype(jnp.bfloat16)
    owner = wide // slots % groups
    shift = 2 * np.pi * (np.arange(rows)[:, None] * owner[None, :] % groups) / groups
    phase = np.stack([np.cos(shift), np.sin(shift)])
    full = 2 * np.pi * (wide[:, None] * wide[None, :] % LANES) / LANES
    c, s = np.cos(full) / width, np.sin(full) / width
    inverse = np.block([[c, s], [-s, c]])
    forward = np.block([[c, -s], [s, c]])
    twist = 2 * np.pi * np.arange(kept + 1)[:, None] * wide[None, :] / width
    each = piece // devices
    t = np.arange(devices)[:, None] + devices * np.arange(each)[None, :]
    angle = 2 * np.pi * (np.arange(rows)[:, None, None] * t[None] % width) / width
    c, s = np.cos(angle), np.sin(angle)
    last = np.stack([np.stack([c, -s], axis=2), np.stack([s, c], axis=2)])
    last = last.reshape(2 * rows, -1, 2 * LANES).transpose(1, 0, 2)
    order = np.zeros((2 * piece, 2 * piece))
    for a in range(devices):
        for part in range(2):
            for b in range(each):
                order[(a * 2 + part) * each + b, part * piece + a + devices * b] = 1.0
    loaded = [
        kernels,
        coef,
        sky,
        jnp.stack(table_pair(up)),
        jnp.stack(table_pair(edge.reshape(2 * LANES, LANES))),
        turn,
        bf16(inverse),
        jnp.stack(table_pair(forward)),
        jnp.stack(table_pair(matrix[: 2 * LANES])),
        jnp.stack(table_pair(following)),
        jnp.stack(table_pair(last)),
        bf16(order),
    ]
    held = [
        weights,
        cols,
        vis,
        f32(phase),
        f32(phase[:, :, :tiles].transpose(0, 2, 1)),
        f32(np.stack([np.cos(twist), np.sin(twist)])),
    ]
    buffers = [pltpu.VMEM(value.shape, value.dtype) for value in loaded]
    buffers[1] = pltpu.VMEM((4, half_rows + 8, half_width), jnp.float32)
    copies = 3 * 4 + 7 + 12
    dma = pltpu.SemaphoreType.DMA
    anywhere = pl.BlockSpec(memory_space=pl.ANY)
    return pl.pallas_call(
        lambda *refs: step_kernel(low, *refs),
        out_shape=(
            jax.ShapeDtypeStruct((rows, width), jnp.float32),
            jax.ShapeDtypeStruct(coef.shape, jnp.float32),
            jax.ShapeDtypeStruct(vis.shape[1:], jnp.float32),
            jax.ShapeDtypeStruct((1, LANES), jnp.float32),
        ),
        in_specs=[anywhere] * len(loaded) + [whole] * len(held),
        out_specs=(anywhere, whole, whole, whole),
        scratch_shapes=buffers[:1]
        + [buffers[1]]
        + buffers[2:]
        + [
            dma((len(loaded) + 1,)),
            pltpu.VMEM((16, half_width), jnp.float32),
            pltpu.VMEM((16, half_width), jnp.float32),
            pltpu.VMEM((devices, tiles, 2 * piece), jnp.bfloat16),
            pltpu.VMEM((devices,) + cols.shape, jnp.int32),
            pltpu.VMEM((low, rows, LANES), jnp.float32),
            pltpu.VMEM((low, rows, LANES), jnp.float32),
            pltpu.VMEM((2, devices // 2, LANES), jnp.float32),
            pltpu.VMEM((2 * rows, devices * tiles), jnp.bfloat16),
            pltpu.VMEM(((kept + 1) * LANES, devices * tiles), jnp.bfloat16),
            pltpu.VMEM((kept + 1, rows, 2 * LANES), jnp.float32),
            pltpu.VMEM((2 * rows, kept * LANES), jnp.bfloat16),
            pltpu.VMEM((2 * rows, kept * LANES), jnp.bfloat16),
            pltpu.VMEM((low, rows + 8, LANES), jnp.float32),
            pltpu.VMEM((devices * tiles, rows), jnp.int32),
            pltpu.VMEM((devices // 2, 1, LANES), jnp.float32),
            pltpu.VMEM((devices, tiles, rows), jnp.int32),
            pltpu.VMEM((devices, 1, LANES), jnp.float32),
            pltpu.VMEM((devices, tiles, 2 * rows), jnp.float32),
            pltpu.VMEM((tiles, LANES), jnp.float32),
            pltpu.VMEM((devices, 1, LANES), jnp.float32),
            dma((copies,)),
            dma((copies,)),
        ]
        + [dma((devices,))] * 8
        + [dma((4,))],
        compiler_params=pltpu.CompilerParams(
            collective_id=0, has_side_effects=True, vmem_limit_bytes=58 * 2**20
        ),
        name="step",
    )(*loaded, *held)


def fast_local(sky_image, coef_dual, vis_dual, visibilities, kernel_blocks, tile_rows, tile_counts):
    bands = lax.axis_size("band")
    groups = lax.axis_size("vis")
    devices = bands * groups
    me = lax.axis_index(everywhere)
    kernel_here = kernel_blocks[0, 0]
    slots = tile_rows.shape[3]
    rows_dev, width = sky_image.shape
    piece = width // groups
    stripe = width // bands
    tiles = groups * slots
    live_slots = (
        jnp.arange(slots, dtype=jnp.int32)[None, :] < tile_counts[0, 0][:, None]
    ).astype(jnp.float32)[:, :, None, None]
    vis_data = visibilities[0, 0]
    vis_state = vis_dual[0, 0]
    columns_here = (tile_rows[0, 0] + lax.axis_index("band") * stripe).reshape(1, tiles)
    columns_here = jnp.concatenate([columns_here, columns_here], axis=1)
    weights = live_slots * vis_state
    weights = jnp.stack([weights, jnp.stack([weights[:, :, 1], -weights[:, :, 0]], axis=2)])
    weights = weights.reshape(2, tiles // 16, -1)
    kernels = kernel_here.reshape(-1, piece)
    vis_rows = (tiles // 16, kernels.shape[0] * 16 // tiles)
    live = jnp.broadcast_to(live_slots, vis_state.shape)
    vis = jnp.stack([vis_state, vis_data, live]).reshape((3,) + vis_rows)
    new_image, merged, residual, sums = step(
        kernels, coef_dual, sky_image, weights, columns_here, vis, me, groups, slots, devices
    )
    threshold = 0.5 * sums[0, 0] / (width * width)
    coef_dual = jnp.clip(merged, -threshold, threshold)
    radius = 0.5 * jnp.sqrt(sums[0, 2] + 1e-06)
    size_value = jnp.sqrt(sums[0, 1] + 1e-06)
    vis_state = residual * (1.0 - jnp.minimum(1.0, radius / size_value))
    return (new_image, coef_dual, vis_state.reshape(vis_dual.shape))


def body_for(mesh):
    devices = mesh.shape["band"] * mesh.shape["vis"]
    relayed = mesh.shape["band"] == 2 and mesh.shape["vis"] % 4 == 0 and devices == 32

    def body(sky_image, *rest):
        rows, width = sky_image.shape
        piece = width // mesh.shape["vis"]
        tiles = rest[4].shape[2] * rest[4].shape[3]
        if relayed and rows == LANES and piece == 2 * LANES and 2 * tiles == LANES:
            return fast_local(sky_image, *rest)
        return local(sky_image, *rest)

    return body


def solution(mesh):
    return jax.shard_map(
        body_for(mesh),
        mesh=mesh,
        in_specs=(
            P(("band", "vis"), None),
            P(None, ("band", "vis"), None),
            P("band", "vis", None, None, None, None),
            P("band", "vis", None, None, None, None),
            P("band", "vis", None, None, None, None, None),
            P("band", "vis", None, None),
            P("band", "vis", None),
        ),
        out_specs=(
            P(("band", "vis"), None),
            P(None, ("band", "vis"), None),
            P("band", "vis", None, None, None, None),
        ),
        check_vma=False,
    )
```

```python
import math

import jax
import numpy as np
import jax.numpy as jnp
from jax import lax
from jax.experimental import pallas as pl
from jax.experimental.pallas import tpu as pltpu
from jax.sharding import PartitionSpec as P

IMG = 4096


low_taps = (
    -0.010597401784997278,
    0.032883011666982945,
    0.030841381835986965,
    -0.18703481171888114,
    -0.02798376941698385,
    0.6308807679295904,
    0.7148465705525415,
    0.23037781330885523,
)
high_taps = tuple(((-1.0) ** offset * low_taps[7 - offset] for offset in range(8)))
highest = lax.Precision.HIGHEST


def shifted(block, axis, distance):
    devices = range(lax.axis_size(axis))
    route = [((i - distance) % len(devices), i) for i in devices]
    return lax.ppermute(block, axis, route)


def dft_table(table_size, sign):
    positions = jnp.arange(table_size, dtype=jnp.int32)
    phase = positions[:, None] * positions[None, :] % table_size
    angle = 2.0 * math.pi / table_size * phase.astype(jnp.float32)
    return (jnp.cos(angle), sign * jnp.sin(angle))


def section_one(table, values):
    return jnp.einsum("kn,...nm->...km", table, values, precision=highest)


def section_two(table, values):
    return jnp.einsum("qm,...km->...qk", table, values, precision=highest)


def dft_last(real_in, imag_in, sign):
    leading = real_in.shape[:-1]
    length = real_in.shape[-1]
    inner_len = 64
    outer_len = length // inner_len
    split_real = real_in.reshape(leading + (outer_len, inner_len))
    table_real, table_imag = dft_table(outer_len, sign)
    first_real = section_one(table_real, split_real)
    first_imag = section_one(table_imag, split_real)
    if imag_in is not None:
        split_imag = imag_in.reshape(leading + (outer_len, inner_len))
        first_real = first_real - section_one(table_imag, split_imag)
        first_imag = first_imag + section_one(table_real, split_imag)
    outer_index = jnp.arange(outer_len, dtype=jnp.int32)
    inner_index = jnp.arange(inner_len, dtype=jnp.int32)
    twist_phase = outer_index[:, None] * inner_index[None, :] % length
    twist_angle = 2.0 * math.pi / length * twist_phase.astype(jnp.float32)
    twist_real = jnp.cos(twist_angle)
    twist_imag = sign * jnp.sin(twist_angle)
    mid_real = first_real * twist_real - first_imag * twist_imag
    mid_imag = first_real * twist_imag + first_imag * twist_real
    last_real, last_imag = dft_table(inner_len, sign)
    out_real = section_two(last_real, mid_real) - section_two(last_imag, mid_imag)
    out_imag = section_two(last_real, mid_imag) + section_two(last_imag, mid_real)
    factor = 1.0 / math.sqrt(length)
    return (
        (out_real * factor).reshape(leading + (length,)),
        (out_imag * factor).reshape(leading + (length,)),
    )


def pieces_from_image(extrap, band_count, group_count):
    rows_dev = extrap.shape[0]
    image_width = extrap.shape[1]
    stripe = image_width // band_count
    piece_cols = stripe // group_count
    piece_rows = image_width // group_count
    col_real, col_imag = dft_last(extrap, None, -1.0)
    shaped = jnp.stack([col_real, col_imag]).reshape(
        2, 1, 1, rows_dev, band_count, group_count, piece_cols
    )
    moved = lax.all_to_all(
        lax.all_to_all(shaped, "band", split_axis=4, concat_axis=1, tiled=True),
        "vis",
        split_axis=5,
        concat_axis=2,
        tiled=True,
    )
    columns = jnp.transpose(moved.reshape(2, image_width, piece_cols), (2, 0, 1))
    row_real, row_imag = dft_last(columns[:, 0], columns[:, 1], -1.0)
    stacked = (
        jnp.stack([row_real, row_imag], axis=1)
        .astype(jnp.bfloat16)
        .reshape(piece_cols, 2, group_count, piece_rows)
    )
    pieces = lax.all_to_all(stacked, "vis", split_axis=2, concat_axis=0, tiled=True)
    return pieces.reshape(stripe, 2, piece_rows)


def image_from_pieces(piece_sum, band_count, group_count):
    stripe = piece_sum.shape[0]
    piece_rows = piece_sum.shape[2]
    piece_cols = stripe // group_count
    image_width = piece_rows * group_count
    rows_dev = image_width // (band_count * group_count)
    spread = lax.all_to_all(
        piece_sum.reshape(stripe, 2, 1, piece_rows), "vis", split_axis=0, concat_axis=2, tiled=True
    )
    spread = spread.reshape(piece_cols, 2, image_width)
    col_real, col_imag = dft_last(spread[:, 0], spread[:, 1], 1.0)
    stacked = jnp.transpose(jnp.stack([col_real, col_imag]), (0, 2, 1))
    shaped = stacked.reshape(2, band_count, group_count, rows_dev, 1, 1, piece_cols)
    moved = lax.all_to_all(
        lax.all_to_all(shaped, "band", split_axis=1, concat_axis=4, tiled=True),
        "vis",
        split_axis=2,
        concat_axis=5,
        tiled=True,
    )
    moved = moved.reshape(2, rows_dev, image_width)
    out_real, out_imag = dft_last(moved[0], moved[1], 1.0)
    return out_real


def cols_down(field):
    image_width = field.shape[1]
    extended = jnp.concatenate([field, field[:, :6]], axis=1)
    low_part = 0.0
    high_part = 0.0
    for offset in range(8):
        taken = extended[:, offset : offset + image_width : 2]
        low_part = low_part + low_taps[offset] * taken
        high_part = high_part + high_taps[offset] * taken
    return (low_part, high_part)


def cols_up(low_part, high_part):
    halves = []
    for parity in range(2):
        summed = 0.0
        for delay in range(4):
            summed = summed + low_taps[parity + 2 * delay] * jnp.roll(low_part, delay, axis=1)
            summed = summed + high_taps[parity + 2 * delay] * jnp.roll(high_part, delay, axis=1)
        halves.append(summed)
    return jnp.stack(halves, axis=2).reshape(low_part.shape[0], 2 * low_part.shape[1])


def rows_up(low_ext, high_ext, half_rows):
    halves = []
    for parity in range(2):
        summed = 0.0
        for delay in range(4):
            begin = 3 - delay
            summed = summed + low_taps[parity + 2 * delay] * low_ext[begin : begin + half_rows]
            summed = summed + high_taps[parity + 2 * delay] * high_ext[begin : begin + half_rows]
        halves.append(summed)
    return jnp.stack(halves, axis=1).reshape(2 * half_rows, low_ext.shape[1])


def analysis(extrap):
    rows_dev = extrap.shape[0]
    taken_rows = min(6, rows_dev)
    parts_list = [extrap]
    parts_list.append(shifted(extrap[:taken_rows], ("band", "vis"), -1))
    extended = jnp.concatenate(parts_list, axis=0)
    half_rows = rows_dev // 2
    rows_low = 0.0
    rows_high = 0.0
    for offset in range(8):
        taken = extended[offset : offset + 2 * half_rows : 2]
        rows_low = rows_low + low_taps[offset] * taken
        rows_high = rows_high + high_taps[offset] * taken
    low_low, low_high = cols_down(rows_low)
    high_low, high_high = cols_down(rows_high)
    return jnp.stack([low_low, low_high, high_low, high_high])


def synthesis(coef_dual):
    half_rows = coef_dual.shape[1]
    taken_rows = min(3, half_rows)
    parts_list = [shifted(coef_dual[:, half_rows - taken_rows :, :], ("band", "vis"), 1)]
    joined = jnp.concatenate(parts_list[::-1] + [coef_dual], axis=1)
    cols_low = rows_up(joined[0], joined[2], half_rows)
    cols_high = rows_up(joined[1], joined[3], half_rows)
    return cols_up(cols_low, cols_high)


def degrid(kernel_here, tiles):
    kernel_real = kernel_here[:, :, 0]
    kernel_imag = kernel_here[:, :, 1]
    tile_real = tiles[:, :, 0]
    tile_imag = tiles[:, :, 1]
    out_real = jnp.einsum(
        "qsat,qst->qsa", kernel_real, tile_real, preferred_element_type=jnp.float32
    ) - jnp.einsum("qsat,qst->qsa", kernel_imag, tile_imag, preferred_element_type=jnp.float32)
    out_imag = jnp.einsum(
        "qsat,qst->qsa", kernel_real, tile_imag, preferred_element_type=jnp.float32
    ) + jnp.einsum("qsat,qst->qsa", kernel_imag, tile_real, preferred_element_type=jnp.float32)
    return jnp.stack([out_real, out_imag], axis=2)


def grid_back(kernel_here, weights):
    kernel_real = kernel_here[:, :, 0]
    kernel_imag = kernel_here[:, :, 1]
    weight_real = weights[:, :, 0]
    weight_imag = weights[:, :, 1]
    grid_real = jnp.einsum(
        "qsat,qsa->qst", kernel_real, weight_real, preferred_element_type=jnp.float32
    ) + jnp.einsum("qsat,qsa->qst", kernel_imag, weight_imag, preferred_element_type=jnp.float32)
    grid_imag = jnp.einsum(
        "qsat,qsa->qst", kernel_real, weight_imag, preferred_element_type=jnp.float32
    ) - jnp.einsum("qsat,qsa->qst", kernel_imag, weight_real, preferred_element_type=jnp.float32)
    return jnp.stack([grid_real, grid_imag], axis=2)


def local(sky_image, coef_dual, vis_dual, visibilities, kernel_blocks, tile_rows, tile_counts):
    band_count = lax.axis_size("band")
    group_count = lax.axis_size("vis")
    kernel_here = kernel_blocks[0, 0]
    rows_here = tile_rows[0, 0]
    slot_count = rows_here.shape[1]
    live_slots = (
        jnp.arange(slot_count, dtype=jnp.int32)[None, :] < tile_counts[0, 0][:, None]
    ).astype(jnp.float32)[:, :, None, None]
    vis_data = visibilities[0, 0]
    vis_state = vis_dual[0, 0]
    image_width = sky_image.shape[1]
    stripe = image_width // band_count
    piece_rows = image_width // group_count
    incoming_rows = lax.all_to_all(rows_here, "vis", split_axis=0, concat_axis=0, tiled=True)
    data_part = jnp.sum(live_slots * vis_data * vis_data)
    weights = (live_slots * vis_state).astype(jnp.bfloat16)
    contrib = grid_back(kernel_here, weights)
    arrived = lax.all_to_all(contrib, "vis", split_axis=0, concat_axis=0, tiled=True)
    piece_sum = jax.ops.segment_sum(
        arrived.reshape(-1, 2, piece_rows), incoming_rows.reshape(-1), num_segments=stripe
    )
    adjoint_part = image_from_pieces(piece_sum, band_count, group_count)
    smooth = synthesis(coef_dual)
    new_image = jnp.maximum(sky_image - smooth - adjoint_part, 0.0)
    extrap = 2.0 * new_image - sky_image
    coeffs = analysis(extrap)
    abs_total = jnp.sum(jnp.abs(coeffs))
    coef_total = lax.psum(abs_total, ("band", "vis"))
    threshold = 0.5 * coef_total / (IMG * IMG)
    coef_dual = jnp.clip(coef_dual + coeffs, -threshold, threshold)
    piece_grid = pieces_from_image(extrap, band_count, group_count)
    tiles = lax.all_to_all(
        piece_grid[incoming_rows], "vis", split_axis=0, concat_axis=0, tiled=True
    )
    predicted = degrid(kernel_here, tiles)
    residual = live_slots * (vis_state + predicted - vis_data)
    resid_square = jnp.sum(residual * residual)
    norm_square, data_square = lax.psum((resid_square, data_part), ("band", "vis"))
    radius = 0.5 * jnp.sqrt(data_square + 1e-06)
    size_value = jnp.sqrt(norm_square + 1e-06)
    vis_state = residual * (1.0 - jnp.minimum(1.0, radius / size_value))
    return (new_image, coef_dual, vis_state[None, None])


high = lax.Precision.HIGH
everywhere = ("band", "vis")


def wave_tables(length, digit_low):
    digit_high = length // digit_low
    low = np.arange(digit_low)
    wide = np.arange(digit_high)
    full = 2.0 * np.pi
    small = full * (low[:, None] * low[None, :] % digit_low) / digit_low
    twist = full * (low[:, None] * wide[None, :]) / length
    large = full * (wide[:, None] * wide[None, :] % digit_high) / digit_high
    return small, twist, large


def complex_matrix(angle, sign):
    c = np.cos(angle)
    s = sign * np.sin(angle)
    return np.stack([np.stack([c, -s], axis=1), np.stack([s, c], axis=1)])


def f32(values):
    return jnp.asarray(np.asarray(values, np.float32))


def bf16(values):
    return f32(values).astype(jnp.bfloat16)


def analysis_matrix(half):
    matrix = np.zeros((2, half, 2 * half + 6))
    for k in range(half):
        for j in range(8):
            matrix[0, k, 2 * k + j] = low_taps[j]
            matrix[1, k, 2 * k + j] = high_taps[j]
    return matrix.reshape(2 * half, 2 * half + 6)


def synthesis_matrix(half):
    matrix = np.zeros((2 * half, 2, half + 3))
    for n in range(2 * half):
        for delay in range(4):
            tap = n % 2 + 2 * delay
            matrix[n, 0, n // 2 - delay + 3] = low_taps[tap]
            matrix[n, 1, n // 2 - delay + 3] = high_taps[tap]
    return matrix


def cos_sums(values, size):
    half = size // 2
    if half < 2:
        return [values[0] + values[1], values[0] - values[1]]
    quarter = half // 2
    plus = [values[a] + values[half - a] for a in range(quarter)] + [values[quarter]]
    minus = [values[a] - values[half - a] for a in range(quarter)]
    out = [None] * (half + 1)
    out[0::2] = cos_sums(plus, half)
    for k in range(1, half, 2):
        total = minus[0]
        for a in range(1, quarter):
            total = total + minus[a] * math.cos(2 * math.pi * (a * k % size) / size)
        out[k] = total
    return out


def sin_sums(values, size):
    half = size // 2
    if half < 2:
        return [None] * (half + 1)
    quarter = half // 2
    plus = {a: values[a] + values[half - a] for a in range(1, quarter)}
    plus[quarter] = values[quarter]
    minus = [None] + [values[a] - values[half - a] for a in range(1, quarter)]
    out = [None] * (half + 1)
    out[0::2] = sin_sums(minus, half)
    for k in range(1, half, 2):
        total = None
        for a in range(1, quarter + 1):
            factor = math.sin(2 * math.pi * (a * k % size) / size)
            term = plus[a] if a * 4 == size and k % 4 == 1 else plus[a] * factor
            total = term if total is None else total + term
        out[k] = total
    return out


def even_odd(values):
    size = len(values)
    half = size // 2
    even = [values[0]] + [values[a] + values[size - a] for a in range(1, half)] + [values[half]]
    odd = [None] + [values[a] - values[size - a] for a in range(1, half)]
    return even, odd


def split(values):
    upper = values.astype(jnp.bfloat16)
    return upper, (values - upper.astype(jnp.float32)).astype(jnp.bfloat16)


def table_pair(values):
    upper = f32(values).astype(jnp.bfloat16)
    return upper, (f32(values) - upper.astype(jnp.float32)).astype(jnp.bfloat16)


def nt_dot(a, b):
    return lax.dot_general(a, b, (((1,), (1,)), ((), ())), preferred_element_type=jnp.float32)


def nn_dot(a, b):
    return lax.dot_general(a, b, (((1,), (0,)), ((), ())), preferred_element_type=jnp.float32)


LEVELS = 32000.0
MESH = pl.DeviceIdType.MESH
LANES = 128
whole = pl.BlockSpec(memory_space=pltpu.VMEM)


def place():
    band = lax.axis_index("band")
    vis = lax.axis_index("vis")
    groups = lax.axis_size("vis")
    z = vis // 4
    y = vis // 2 % 2
    core = vis % 2
    return band, z, y, core, groups


def taps_dot(values, tables):
    upper, lower = split(values)
    return nn_dot(upper, tables[0]) + nn_dot(lower, tables[0]) + nn_dot(upper, tables[1])


def level(values):
    return jnp.round(values).astype(jnp.int32)


def step_kernel(
    low,
    kernels_hbm,
    coef_hbm,
    sky_hbm,
    up_hbm,
    edge_hbm,
    base_hbm,
    spin_hbm,
    inv_hbm,
    fwd_hbm,
    near_hbm,
    next_hbm,
    last_hbm,
    order_hbm,
    state_ref,
    data_ref,
    rows_ref,
    counts_ref,
    phase_ref,
    shift_ref,
    tw_ref,
    sky_ref,
    merged_ref,
    vis_out_ref,
    kernels_ref,
    joined_ref,
    up_ref,
    edge_ref,
    base_ref,
    spin_ref,
    inv_ref,
    fwd_ref,
    near_ref,
    next_ref,
    last_ref,
    order_ref,
    load_sem,
    tail_ref,
    halo_ref,
    block_ref,
    all_cols_ref,
    turn_ref,
    total_ref,
    tall_ref,
    smooth_ref,
    fold_ref,
    grid_ref,
    hot_ref,
    half_ref,
    spec_ref,
    rest_ref,
    extrap_ref,
    picked_ref,
    unit_ref,
    got_ref,
    units_ref,
    mid_ref,
    column_ref,
    all_sums_ref,
    send_a,
    send_b,
    recv_a,
    recv_b,
    send_p,
    send_u,
    recv_p,
    recv_u,
    send_s,
    recv_s,
    halo_sem,
):
    x, z, y, core, groups = place()
    levels = groups // 4
    devices = 2 * groups
    half_rows, half_width = coef_hbm.shape[1:]
    rows = 2 * half_rows
    tiles = block_ref.shape[1]
    kept = low // 2 + 1
    wide = LANES

    def index(px, pz, py, pc):
        return px * groups + pz * 4 + py * 2 + pc

    def device(px, pz, py, pc):
        return (px, pz * 4 + py * 2 + pc)

    def ident(number):
        return (number // groups, number % groups)

    def remote(src, dst, send, recv, target):
        return pltpu.make_async_remote_copy(
            src_ref=src,
            dst_ref=dst,
            send_sem=send,
            recv_sem=recv,
            device_id=target,
            device_id_type=MESH,
        )

    me = index(x, z, y, core)
    after, before = (me + 1) % devices, (me + devices - 1) % devices
    twin = device(x, z, y, 1 - core)
    line = [device(x, (z + k) % levels, y, core) for k in range(1, levels)]
    corners = [(1 - x, y), (x, 1 - y), (1 - x, 1 - y)]
    plane = [device(px, z, py, core) for px, py in corners]
    barrier = pltpu.get_barrier_semaphore()
    peers = line + plane + [twin, ident(after), ident(before)]
    for peer in peers:
        pl.semaphore_signal(barrier, inc=1, device_id=peer, device_id_type=MESH)

    sources = [
        (kernels_hbm, kernels_ref),
        (coef_hbm, joined_ref.at[:, pl.ds(8, half_rows), :]),
        (up_hbm, up_ref),
        (edge_hbm, edge_ref),
        (base_hbm, base_ref),
        (spin_hbm, spin_ref),
        (inv_hbm, inv_ref),
        (sky_hbm, sky_ref),
        (fwd_hbm, fwd_ref),
        (near_hbm, near_ref),
        (next_hbm, next_ref),
        (last_hbm, last_ref),
        (order_hbm, order_ref),
    ]
    loads = [
        pltpu.make_async_copy(src, dst, load_sem.at[i]) for i, (src, dst) in enumerate(sources)
    ]
    for load in loads:
        load.start()
    loads[0].wait()
    count = 16
    span = kernels_ref.shape[0] * count // tiles
    width = low * wide
    stripe = width // 2
    slots = rows_ref.shape[1]
    lane = lax.broadcasted_iota(jnp.int32, (tiles, groups), 1)
    tile_id = lax.broadcasted_iota(jnp.int32, (tiles, groups), 0)
    counts = jnp.where(lane == tile_id // slots, counts_ref[...].astype(jnp.float32), 0.0)
    counts = jnp.sum(counts, axis=1, keepdims=True)
    tile_id = lax.broadcasted_iota(jnp.int32, (tiles, 1), 0)
    live = jnp.where((tile_id % slots).astype(jnp.float32) < counts, 1.0, 0.0)
    state = [state_ref[:, part, :] for part in range(2)]
    data = [data_ref[:, part, :] for part in range(2)]
    ours = [part * live for part in state]
    turned = [ours[0], ours[1], ours[0], ours[1]], [ours[1], -ours[0], ours[1], -ours[0]]
    turned = [jnp.concatenate(parts, axis=1) for parts in turned]
    pair_lane = lax.broadcasted_iota(jnp.int32, (count, LANES), 1) // (LANES // 2)
    pair_row = lax.broadcasted_iota(jnp.int32, (count, LANES), 0)
    masks = [pair_lane + 2 * k == pair_row for k in range(count // 2)]
    for i in range(tiles // count):
        spread = [
            jnp.concatenate(
                [jnp.where(mask, part[i * count : (i + 1) * count], 0.0) for mask in masks], axis=1
            )
            for part in turned
        ]
        spread = jnp.concatenate(spread, axis=0).astype(jnp.bfloat16)
        both = nn_dot(spread, kernels_ref[i * span : (i + 1) * span, :])
        both = jnp.concatenate([both[:count], both[count:]], axis=1)
        block_ref[me, i * count : (i + 1) * count, :] = both.astype(jnp.bfloat16)
    lane = lax.broadcasted_iota(jnp.int32, (groups, LANES), 1) % tiles
    owner = lax.broadcasted_iota(jnp.int32, (groups, LANES), 0)
    columns = 0.0
    for slot in range(slots):
        here = rows_ref[:, slot : slot + 1].astype(jnp.float32)
        columns = columns + jnp.where(lane == owner * slots + slot, here, 0.0)
    columns = jnp.sum(columns, axis=0, keepdims=True).astype(jnp.int32)
    all_cols_ref[me] = columns + x * stripe
    loads[1].wait()
    for c in range(4):
        tail_ref[3 * c : 3 * c + 3, :] = joined_ref[c, half_rows + 5 :, :]
    pl.semaphore_wait(barrier, len(peers))

    started = []

    def start(block, target, slot):
        own_a, own_b = block_ref.at[block], all_cols_ref.at[block]
        for own, send, recv in ((own_a, send_a, recv_a), (own_b, send_b, recv_b)):
            copy = remote(own, own, send.at[slot], recv.at[block], target)
            copy.start()
            started.append(copy)

    def got(block):
        for ref, send, recv in ((block_ref, send_a, recv_a), (all_cols_ref, send_b, recv_b)):
            own = ref.at[block]
            remote(own, own, send.at[0], recv.at[block], twin).wait_recv()

    slots_of = iter(range(send_a.shape[0]))
    far = sorted(range(1, levels), key=lambda k: abs(k - levels / 2))
    for k in far:
        start(me, line[k - 1], next(slots_of))
    for target in plane:
        start(me, target, next(slots_of))
    edge = remote(tail_ref, halo_ref, halo_sem.at[0], halo_sem.at[1], ident(after))
    edge.start()
    start(me, twin, next(slots_of))
    line_blocks = [index(x, (z + levels - k) % levels, y, core) for k in far]
    for block in line_blocks:
        got(block)
        for target in plane:
            start(block, target, next(slots_of))
        start(block, twin, next(slots_of))
    edge.wait()
    for c in range(4):
        joined_ref[c, 5:8, :] = halo_ref[3 * c : 3 * c + 3, :]
    strips = half_width // LANES

    def tall(i, carry):
        here = pl.ds(pl.multiple_of(i * LANES, LANES), LANES)
        for c in range(2):
            for k in range(half_rows // 8):
                lows = [joined_ref[c, 8 + 8 * k - d : 16 + 8 * k - d, here] for d in range(4)]
                highs = [joined_ref[c + 2, 8 + 8 * k - d : 16 + 8 * k - d, here] for d in range(4)]
                for parity in range(2):
                    total = 0.0
                    for d in range(4):
                        total = total + low_taps[parity + 2 * d] * lows[d]
                        total = total + high_taps[parity + 2 * d] * highs[d]
                    tall_ref[c * strips + i, pl.ds(16 * k + parity, 8, stride=2), :] = total
        return carry

    lax.fori_loop(0, strips, tall, 0)

    for px, py in corners:
        block = index(px, z, py, core)
        got(block)
        start(block, twin, next(slots_of))
    for load in loads[2:8]:
        load.wait()

    def broad(i, carry):
        there = (i + strips - 1) % strips
        near = jnp.concatenate([tall_ref[i], tall_ref[strips + i]], axis=1)
        last = jnp.concatenate([tall_ref[there], tall_ref[strips + there]], axis=1)
        out = taps_dot(near, up_ref)
        first = taps_dot(last, edge_ref)
        smooth_ref[2 * i] = out[:, :LANES] + first
        smooth_ref[2 * i + 1] = out[:, LANES:]
        return carry

    lax.fori_loop(0, strips // 2, broad, 0)
    spin_cos, spin_sin = spin_ref[0, pl.ds(me, 1), :], spin_ref[1, pl.ds(me, 1), :]
    cosine = (base_ref[0] * spin_cos - base_ref[1] * spin_sin).astype(jnp.bfloat16)
    sine = (base_ref[1] * spin_cos + base_ref[0] * spin_sin).astype(jnp.bfloat16)
    piece = kernels_ref.shape[1]
    turn_ref[:rows, :piece] = cosine
    turn_ref[:rows, piece:] = -sine
    turn_ref[rows:, :piece] = sine
    turn_ref[rows:, piece:] = cosine
    for n, k in enumerate(far):
        for px, py in corners:
            block = index(px, (z + levels - k) % levels, py, core)
            got(block)
            start(block, twin, next(slots_of))
        if n == 0:
            lax.fori_loop(strips // 2, strips, broad, 0)

    total_tiles = devices * tiles
    class_tiles = groups * tiles
    parts = class_tiles // LANES
    lane = lax.broadcasted_iota(jnp.int32, (1, LANES), 1)

    def spread_class(c):
        for i in range(parts):
            columns = jnp.where(
                lane < tiles, all_cols_ref[4 * i + c], all_cols_ref[4 * i + 2 + c]
            )
            k1 = columns % low
            k2 = columns // low
            flip = k1 >= kept
            k1 = jnp.where(flip, low - k1, k1)
            k2 = jnp.where(flip, wide - 1 - k2, k2)
            fold_ref[0, pl.ds(c * parts + i, 1), :] = (k1 * wide + k2).astype(jnp.float32)
            fold_ref[1, pl.ds(c * parts + i, 1), :] = jnp.where(flip, -1.0, 1.0)
        chunk = 4 * LANES
        for j in range(class_tiles // chunk):
            n = chunk // tiles
            some = [block_ref[2 * (j * n + i) + c] for i in range(n)]
            both = nt_dot(turn_ref[...], jnp.concatenate(some, axis=0))
            for i in range(chunk // LANES):
                b = c * parts + j * (chunk // LANES) + i
                at = pl.ds(pl.multiple_of(b * LANES, LANES), LANES)
                real = both[:rows, i * LANES : (i + 1) * LANES]
                imag = both[rows:, i * LANES : (i + 1) * LANES]
                sign = fold_ref[1, pl.ds(b, 1), :]
                out_real = real * phase_ref[0] - imag * phase_ref[1]
                out_imag = (real * phase_ref[1] + imag * phase_ref[0]) * sign
                grid_ref[:rows, at] = out_real.astype(jnp.bfloat16)
                grid_ref[rows:, at] = out_imag.astype(jnp.bfloat16)

    def folded_class(c, p):
        base = pl.multiple_of(p * 2 * wide, 2 * wide)
        row = (lax.broadcasted_iota(jnp.int32, (2 * wide, LANES), 0) + base).astype(jnp.float32)
        hots = []
        for i in range(parts):
            hit = row == fold_ref[0, pl.ds(c * parts + i, 1), :]
            hots.append(jnp.where(hit, 1.0, 0.0).astype(jnp.bfloat16))
        hot = jnp.concatenate(hots, axis=1)
        at = pl.ds(pl.multiple_of(c * class_tiles, class_tiles), class_tiles)
        hot_ref[pl.ds(base, 2 * wide), at] = hot
        return nt_dot(grid_ref[:, at], hot)

    spread_class(core)

    def scatter_own(p, carry):
        total_ref[p] = folded_class(core, p)
        return carry

    lax.fori_loop(0, (kept + 1) // 2, scatter_own, 0)
    for i in range(groups):
        got(2 * i + 1 - core)
    spread_class(1 - core)

    def scatter(p, carry):
        folded = (total_ref[p] + folded_class(1 - core, p)).astype(jnp.bfloat16)
        for e in range(2):
            here = slice(e * wide, (e + 1) * wide)
            pair = jnp.concatenate([folded[:rows, here], folded[rows:, here]], axis=1)
            mid = nn_dot(pair, inv_ref[...])
            k1 = p * 2 + e
            tw_real, tw_imag = tw_ref[0, pl.ds(k1, 1), :], tw_ref[1, pl.ds(k1, 1), :]
            real, imag = mid[:, :wide], mid[:, wide:]
            half_ref[k1, :, :wide] = real * tw_real - imag * tw_imag
            half_ref[k1, :, wide:] = real * tw_imag + imag * tw_real
        return carry

    lax.fori_loop(0, (kept + 1) // 2, scatter, 0)

    def strip(i, carry):
        at = pl.ds(pl.multiple_of(i * 8, 8), 8)
        cos_part = cos_sums([half_ref[k, at, :wide] for k in range(kept)], low)
        sin_part = sin_sums([None] + [half_ref[k, at, wide:] for k in range(1, kept - 1)], low)
        extraps = []
        for a in range(low):
            k = min(a, low - a)
            if a == 0 or a == low // 2:
                adjoint = cos_part[k]
            elif a < low // 2:
                adjoint = cos_part[k] - sin_part[k]
            else:
                adjoint = cos_part[k] + sin_part[k]
            here = slice(a * wide, (a + 1) * wide)
            sky = sky_ref[at, here]
            image = jnp.maximum(sky - smooth_ref[a, at, :] - adjoint, 0.0)
            extrap = 2.0 * image - sky
            sky_ref[at, here] = image
            extrap_ref[a, at, :] = extrap
            extraps.append(extrap)
        even, odd = even_odd(extraps)
        real_part = cos_sums(even, low)
        imag_part = sin_sums(odd, low)
        for k in range(kept):
            tw_real, tw_imag = tw_ref[0, k : k + 1, :], tw_ref[1, k : k + 1, :]
            real = real_part[k] * tw_real
            imag = -real_part[k] * tw_imag
            if 0 < k < kept - 1:
                real = real - imag_part[k] * tw_imag
                imag = imag - imag_part[k] * tw_real
            half_ref[k, at, :wide] = real
            half_ref[k, at, wide:] = imag
        return carry

    lax.fori_loop(0, rows // 8, strip, 0)
    top = remote(
        extrap_ref.at[:, pl.ds(0, 8), :],
        extrap_ref.at[:, pl.ds(rows, 8), :],
        halo_sem.at[2],
        halo_sem.at[3],
        ident(before),
    )
    top.start()
    loads[8].wait()

    def spectrum(k, carry):
        out = taps_dot(half_ref[k], fwd_ref)
        here = pl.ds(pl.multiple_of(k * wide, wide), wide)
        upper, lower = split(out)
        spec_ref[:rows, here] = upper[:, :wide]
        spec_ref[rows:, here] = upper[:, wide:]
        rest_ref[:rows, here] = lower[:, :wide]
        rest_ref[rows:, here] = lower[:, wide:]
        return carry

    lax.fori_loop(0, kept, spectrum, 0)

    def sends(to):
        order = to % 2 * groups + to // 2
        at = pl.ds(pl.multiple_of(order * tiles, tiles), tiles)
        unit = unit_ref.at[order // 2]
        return [
            remote(picked_ref.at[at, :], got_ref.at[me], send_p.at[to], recv_p.at[me], ident(to)),
            remote(unit, units_ref.at[me], send_u.at[to], recv_u.at[me], ident(to)),
        ]

    def arrivals(origin):
        at = pl.ds(0, tiles)
        return [
            remote(
                picked_ref.at[at, :], got_ref.at[origin], send_p.at[0], recv_p.at[origin], twin
            ),
            remote(unit_ref.at[0], units_ref.at[origin], send_u.at[0], recv_u.at[origin], twin),
        ]

    def pick(s, carry):
        half = levels // 2
        to_class, to_x = (core + s) % 2, (x + 1 + s // 2) % 2
        spot = to_x * 2 + (z // half + 1 + s // 4) % 2
        j = to_class * 4 + spot
        at = pl.multiple_of(j * 2 * LANES, 2 * LANES)
        hot = hot_ref[: kept * wide, pl.ds(at, 2 * LANES)]
        both = nn_dot(spec_ref[...], hot) + nn_dot(rest_ref[...], hot)
        for h in range(2):
            sign = fold_ref[1, pl.ds(2 * j + h, 1), :]
            real = both[:rows, h * LANES : (h + 1) * LANES]
            imag = both[rows:, h * LANES : (h + 1) * LANES] * sign
            most = jnp.max(jnp.maximum(jnp.abs(real), jnp.abs(imag)), axis=0, keepdims=True)
            most = jnp.maximum(most, 1e-30)
            unit_ref[2 * j + h] = most * (1.0 / LEVELS)
            to_level = LEVELS / most
            packed = level(real * to_level) * 65536 + level(imag * to_level)
            to = pl.ds(pl.multiple_of(at + h * LANES, LANES), LANES)
            picked_ref[to, :] = packed.T
        for i in range(4):
            to = (spot * 4 + i) * 2 + to_class

            @pl.when(to != me)
            def _():
                for copy in sends(to):
                    copy.start()

        return carry

    lax.fori_loop(0, devices // 4, pick, 0)
    order = core * groups + me // 2
    got_ref[me] = picked_ref[pl.ds(pl.multiple_of(order * tiles, tiles), tiles), :]
    units_ref[me] = unit_ref[order // 2]
    top.wait()
    loads[9].wait()
    loads[10].wait()

    def rows_down(i, carry):
        for k in range(half_rows // 8):
            lows, highs = 0.0, 0.0
            for tap in range(8):
                taken = extrap_ref[i, pl.ds(16 * k + tap, 8, stride=2), :]
                lows = lows + low_taps[tap] * taken
                highs = highs + high_taps[tap] * taken
            tall_ref[i, 8 * k : 8 * k + 8, :] = lows
            tall_ref[i, half_rows + 8 * k : half_rows + 8 * k + 8, :] = highs
        return carry

    lax.fori_loop(0, low, rows_down, 0)

    def cols_down(b, absolute):
        here = jnp.concatenate([tall_ref[2 * b], tall_ref[2 * b + 1]], axis=1)
        out = taps_dot(here, near_ref) + taps_dot(tall_ref[(2 * b + 2) % low], next_ref)
        at = pl.ds(pl.multiple_of(b * LANES, LANES), LANES)
        for c in range(4):
            top_row, left = c // 2 * half_rows, c % 2 * LANES
            part = out[top_row : top_row + half_rows, left : left + LANES]
            absolute = absolute + jnp.abs(part)
            merged_ref[c, :, at] = joined_ref[c, 8:, at] + part
        return absolute

    absolute = lax.fori_loop(0, low // 2, cols_down, jnp.zeros((half_rows, LANES), jnp.float32))
    abs_total = jnp.sum(jnp.sum(absolute, axis=0, keepdims=True), axis=1, keepdims=True)
    loads[11].wait()
    loads[12].wait()

    def landed(k, carry):
        for copy in arrivals((me + k) % devices):
            copy.wait_recv()
        return carry

    lax.fori_loop(1, devices, landed, 0)

    units = jnp.concatenate([units_ref[d] for d in range(devices)], axis=0)
    units = jnp.concatenate([units] * (LANES // devices), axis=0).T
    column_ref[...] = jnp.where(y == 0, units[:tiles], units[tiles:])

    def finish(i, carry):
        here = pl.ds(pl.multiple_of(i * 8, 8), 8)
        cosine, sine = shift_ref[0, here, :], shift_ref[1, here, :]
        reals, imags = [], []
        for d in range(devices):
            packed = got_ref[d, here, :]
            real = (packed + 32768) >> 16
            imag = packed - (real << 16)
            unit = column_ref[here, d : d + 1]
            real = real.astype(jnp.float32) * unit
            imag = imag.astype(jnp.float32) * unit
            reals.append(real * cosine + imag * sine)
            imags.append(imag * cosine - real * sine)
        even, odd = even_odd(reals)
        cos_real, sin_real = cos_sums(even, devices), sin_sums(odd, devices)
        even, odd = even_odd(imags)
        cos_imag, sin_imag = cos_sums(even, devices), sin_sums(odd, devices)
        half = devices // 2
        for k in range(half + 1):
            if k == 0 or k == half:
                outs = [(k, cos_real[k], cos_imag[k])]
            else:
                outs = [
                    (k, cos_real[k] + sin_imag[k], cos_imag[k] - sin_real[k]),
                    (devices - k, cos_real[k] - sin_imag[k], cos_imag[k] + sin_real[k]),
                ]
            for t, real, imag in outs:
                mid_ref[t, here, :rows] = real
                mid_ref[t, here, rows:] = imag
        return carry

    lax.fori_loop(0, tiles // 8, finish, 0)
    group = 2 * LANES // 16
    lane = lax.broadcasted_iota(jnp.int32, (1, 2 * LANES), 1) // 16
    pieces = []
    for g in range(devices // group):
        total = None
        for e in range(group):
            upper, lower = split(mid_ref[g * group + e])
            out = nn_dot(upper, last_ref[0, g]) + nn_dot(lower, last_ref[0, g])
            out = out + nn_dot(upper, last_ref[1, g])
            out = jnp.where(lane == e, out, 0.0)
            total = out if total is None else total + out
        pieces.append(total.astype(jnp.bfloat16))
    tile = nn_dot(jnp.concatenate(pieces, axis=1), order_ref[...]).astype(jnp.bfloat16)
    first, second = [], []
    near_row = pair_row % 2 == 0
    for i in range(tiles // count):
        here = tile[i * count : (i + 1) * count]
        pair = jnp.concatenate([here[:, :piece], here[:, piece:]], axis=0)
        out = nt_dot(pair, kernels_ref[i * span : (i + 1) * span, :])
        for found, half in ((first, out[:count]), (second, out[count:])):
            total = 0.0
            for k in range(count // 2):
                total = total + jnp.where(
                    pair_row // 2 == k, half[:, k * LANES : (k + 1) * LANES], 0.0
                )
            found.append(jnp.where(near_row, total, pltpu.roll(total, LANES // 2, 1)))
    first = jnp.concatenate(first, axis=0)
    second = jnp.concatenate(second, axis=0)
    visits = state_ref.shape[2]
    lane = lax.broadcasted_iota(jnp.int32, first.shape, 1)
    crossed = jnp.where(
        lane // visits % 2 == 0,
        -pltpu.roll(second, LANES - visits, 1),
        pltpu.roll(second, visits, 1),
    )
    keep = jnp.where(lane < 2 * visits, live, 0.0)
    state_wide = jnp.concatenate(state + state, axis=1)
    data_wide = jnp.concatenate(data + data, axis=1)
    residual = keep * (state_wide + first + crossed - data_wide)
    norms = []
    for values in (residual, data_wide * keep):
        norms.append(jnp.sum(jnp.sum(values * values, axis=0, keepdims=True), axis=1, keepdims=True))
    lane = lax.broadcasted_iota(jnp.int32, (1, LANES), 1)
    row = jnp.where(lane == 0, abs_total, jnp.where(lane == 1, norms[0], norms[1]))
    all_sums_ref[me] = row

    def share(k, carry):
        to = (me + k) % devices
        own = all_sums_ref.at[me]
        remote(own, own, send_s.at[to], recv_s.at[me], ident(to)).start()
        return carry

    lax.fori_loop(1, devices, share, 0)
    for copy in started:
        copy.wait_send()

    def shared(k, total):
        other = (me + k) % devices
        own = all_sums_ref.at[other]
        remote(own, own, send_s.at[other], recv_s.at[other], twin).wait_recv()
        return total

    lax.fori_loop(1, devices, shared, 0)
    total = all_sums_ref[0]
    for d in range(1, devices):
        total = total + all_sums_ref[d]
    threshold = 0.5 * total[:, 0:1] / (width * width)
    size = jnp.sqrt(total[:, 1:2] + 1e-06)
    radius = 0.5 * jnp.sqrt(total[:, 2:3] + 1e-06)
    residual = residual * (1.0 - jnp.minimum(1.0, radius / size))
    vis_out_ref[:, 0, :] = residual[:, :visits]
    vis_out_ref[:, 1, :] = residual[:, visits : 2 * visits]

    def clip(i, carry):
        at = pl.ds(pl.multiple_of(i * LANES, LANES), LANES)
        for c in range(4):
            merged_ref[c, :, at] = jnp.clip(merged_ref[c, :, at], -threshold, threshold)
        return carry

    lax.fori_loop(0, half_width // LANES, clip, 0)

    def sent(k, carry):
        to = (me + k) % devices
        for copy in sends(to):
            copy.wait_send()
        own = all_sums_ref.at[me]
        remote(own, own, send_s.at[to], recv_s.at[me], ident(to)).wait_send()
        return carry

    lax.fori_loop(1, devices, sent, 0)


def step(kernels, coef, sky, state, data, tile_rows, tile_counts, groups, devices):
    rows, width = sky.shape
    piece = kernels.shape[1]
    slots = tile_rows.shape[1]
    tiles = groups * slots
    half_rows, half_width = coef.shape[1:]
    low = width // LANES
    kept = low // 2 + 1
    wide = np.arange(LANES)
    matrix = synthesis_matrix(LANES)
    up = matrix[:, :, 3:].transpose(1, 2, 0).reshape(2 * LANES, 2 * LANES)
    edge = np.zeros((2, LANES, LANES))
    edge[:, LANES - 3 :, :] = matrix[:LANES, :, :3].transpose(1, 2, 0)
    matrix = analysis_matrix(LANES).T
    following = np.zeros((LANES, 2 * LANES))
    following[:6] = matrix[2 * LANES :]
    turn = np.arange(piece)
    base = 2 * np.pi * np.arange(rows)[:, None] * turn[None, :] / width
    spin = 2 * np.pi * (np.arange(devices)[:, None] * turn[None, :] % devices) / devices
    owner = wide // slots % groups
    shift = 2 * np.pi * (np.arange(rows)[:, None] * owner[None, :] % groups) / groups
    phase = np.stack([np.cos(shift), np.sin(shift)])
    full = 2 * np.pi * (wide[:, None] * wide[None, :] % LANES) / LANES
    c, s = np.cos(full) / width, np.sin(full) / width
    inverse = np.block([[c, s], [-s, c]])
    forward = np.block([[c, -s], [s, c]])
    twist = 2 * np.pi * np.arange(kept + 1)[:, None] * wide[None, :] / width
    each = piece // devices
    t = np.arange(devices)[:, None] + devices * np.arange(each)[None, :]
    angle = 2 * np.pi * (np.arange(rows)[:, None, None] * t[None] % width) / width
    c, s = np.cos(angle), np.sin(angle)
    last = np.stack([np.stack([c, -s], axis=2), np.stack([s, c], axis=2)])
    last = last.reshape(2 * rows, -1, 2 * LANES).transpose(1, 0, 2)
    order = np.zeros((2 * piece, 2 * piece))
    for a in range(devices):
        for part in range(2):
            for b in range(each):
                order[(a * 2 + part) * each + b, part * piece + a + devices * b] = 1.0
    loaded = [
        kernels,
        coef,
        sky,
        jnp.stack(table_pair(up)),
        jnp.stack(table_pair(edge.reshape(2 * LANES, LANES))),
        f32(np.stack([np.cos(base), np.sin(base)])),
        f32(np.stack([np.cos(spin), np.sin(spin)])),
        bf16(inverse),
        jnp.stack(table_pair(forward)),
        jnp.stack(table_pair(matrix[: 2 * LANES])),
        jnp.stack(table_pair(following)),
        jnp.stack(table_pair(last)),
        bf16(order),
    ]
    held = [
        state,
        data,
        tile_rows,
        tile_counts,
        f32(phase),
        f32(phase[:, :, :tiles].transpose(0, 2, 1)),
        f32(np.stack([np.cos(twist), np.sin(twist)])),
    ]
    buffers = [pltpu.VMEM(value.shape, value.dtype) for value in loaded]
    buffers[1] = pltpu.VMEM((4, half_rows + 8, half_width), jnp.float32)
    copies = 3 * 4 + 7 + 12
    dma = pltpu.SemaphoreType.DMA
    anywhere = pl.BlockSpec(memory_space=pl.ANY)
    return pl.pallas_call(
        lambda *refs: step_kernel(low, *refs),
        out_shape=(
            jax.ShapeDtypeStruct((rows, width), jnp.float32),
            jax.ShapeDtypeStruct(coef.shape, jnp.float32),
            jax.ShapeDtypeStruct(state.shape, jnp.float32),
        ),
        in_specs=[anywhere] * len(loaded) + [whole] * len(held),
        out_specs=(whole, whole, whole),
        scratch_shapes=buffers[:2]
        + buffers[3:]
        + [
            dma((len(loaded),)),
            pltpu.VMEM((16, half_width), jnp.float32),
            pltpu.VMEM((16, half_width), jnp.float32),
            pltpu.VMEM((devices, tiles, 2 * piece), jnp.bfloat16),
            pltpu.VMEM((devices, 1, LANES), jnp.int32),
            pltpu.VMEM((2 * rows, 2 * piece), jnp.bfloat16),
            pltpu.VMEM(((kept + 1) // 2, 2 * rows, 2 * LANES), jnp.float32),
            pltpu.VMEM((low, rows, LANES), jnp.float32),
            pltpu.VMEM((low, rows, LANES), jnp.float32),
            pltpu.VMEM((2, devices // 2, LANES), jnp.float32),
            pltpu.VMEM((2 * rows, devices * tiles), jnp.bfloat16),
            pltpu.VMEM(((kept + 1) * LANES, devices * tiles), jnp.bfloat16),
            pltpu.VMEM((kept + 1, rows, 2 * LANES), jnp.float32),
            pltpu.VMEM((2 * rows, kept * LANES), jnp.bfloat16),
            pltpu.VMEM((2 * rows, kept * LANES), jnp.bfloat16),
            pltpu.VMEM((low, rows + 8, LANES), jnp.float32),
            pltpu.VMEM((devices * tiles, rows), jnp.int32),
            pltpu.VMEM((devices // 2, 1, LANES), jnp.float32),
            pltpu.VMEM((devices, tiles, rows), jnp.int32),
            pltpu.VMEM((devices, 1, LANES), jnp.float32),
            pltpu.VMEM((devices, tiles, 2 * rows), jnp.float32),
            pltpu.VMEM((tiles, LANES), jnp.float32),
            pltpu.VMEM((devices, 1, LANES), jnp.float32),
            dma((copies,)),
            dma((copies,)),
        ]
        + [dma((devices,))] * 8
        + [dma((4,))],
        compiler_params=pltpu.CompilerParams(
            collective_id=0, has_side_effects=True, vmem_limit_bytes=58 * 2**20
        ),
        name="step",
    )(*loaded, *held)


def fast_local(sky_image, coef_dual, vis_dual, visibilities, kernel_blocks, tile_rows, tile_counts):
    groups = lax.axis_size("vis")
    devices = lax.axis_size("band") * groups
    taken = kernel_blocks.shape
    new_image, coef_dual, vis_state = step(
        kernel_blocks.reshape(-1, taken[-1]),
        coef_dual,
        sky_image,
        vis_dual.reshape((-1,) + vis_dual.shape[4:]),
        visibilities.reshape((-1,) + vis_dual.shape[4:]),
        tile_rows[0, 0],
        tile_counts[0],
        groups,
        devices,
    )
    return (new_image, coef_dual, vis_state.reshape(vis_dual.shape))


def body_for(mesh):
    devices = mesh.shape["band"] * mesh.shape["vis"]
    relayed = mesh.shape["band"] == 2 and mesh.shape["vis"] % 4 == 0 and devices == 32

    def body(sky_image, *rest):
        rows, width = sky_image.shape
        piece = width // mesh.shape["vis"]
        tiles = rest[4].shape[2] * rest[4].shape[3]
        if relayed and rows == LANES and piece == 2 * LANES and 2 * tiles == LANES:
            return fast_local(sky_image, *rest)
        return local(sky_image, *rest)

    return body


def solution(mesh):
    return jax.shard_map(
        body_for(mesh),
        mesh=mesh,
        in_specs=(
            P(("band", "vis"), None),
            P(None, ("band", "vis"), None),
            P("band", "vis", None, None, None, None),
            P("band", "vis", None, None, None, None),
            P("band", "vis", None, None, None, None, None),
            P("band", "vis", None, None),
            P("band", "vis", None),
        ),
        out_specs=(
            P(("band", "vis"), None),
            P(None, ("band", "vis"), None),
            P("band", "vis", None, None, None, None),
        ),
        check_vma=False,
    )
```

```python
import math

import jax
import numpy as np
import jax.numpy as jnp
from jax import lax
from jax.experimental import pallas as pl
from jax.experimental.pallas import tpu as pltpu
from jax.sharding import PartitionSpec as P

IMG = 4096


low_taps = (
    -0.010597401784997278,
    0.032883011666982945,
    0.030841381835986965,
    -0.18703481171888114,
    -0.02798376941698385,
    0.6308807679295904,
    0.7148465705525415,
    0.23037781330885523,
)
high_taps = tuple(((-1.0) ** offset * low_taps[7 - offset] for offset in range(8)))
highest = lax.Precision.HIGHEST


def shifted(block, axis, distance):
    devices = range(lax.axis_size(axis))
    route = [((i - distance) % len(devices), i) for i in devices]
    return lax.ppermute(block, axis, route)


def dft_table(table_size, sign):
    positions = jnp.arange(table_size, dtype=jnp.int32)
    phase = positions[:, None] * positions[None, :] % table_size
    angle = 2.0 * math.pi / table_size * phase.astype(jnp.float32)
    return (jnp.cos(angle), sign * jnp.sin(angle))


def section_one(table, values):
    return jnp.einsum("kn,...nm->...km", table, values, precision=highest)


def section_two(table, values):
    return jnp.einsum("qm,...km->...qk", table, values, precision=highest)


def dft_last(real_in, imag_in, sign):
    leading = real_in.shape[:-1]
    length = real_in.shape[-1]
    inner_len = 64
    outer_len = length // inner_len
    split_real = real_in.reshape(leading + (outer_len, inner_len))
    table_real, table_imag = dft_table(outer_len, sign)
    first_real = section_one(table_real, split_real)
    first_imag = section_one(table_imag, split_real)
    if imag_in is not None:
        split_imag = imag_in.reshape(leading + (outer_len, inner_len))
        first_real = first_real - section_one(table_imag, split_imag)
        first_imag = first_imag + section_one(table_real, split_imag)
    outer_index = jnp.arange(outer_len, dtype=jnp.int32)
    inner_index = jnp.arange(inner_len, dtype=jnp.int32)
    twist_phase = outer_index[:, None] * inner_index[None, :] % length
    twist_angle = 2.0 * math.pi / length * twist_phase.astype(jnp.float32)
    twist_real = jnp.cos(twist_angle)
    twist_imag = sign * jnp.sin(twist_angle)
    mid_real = first_real * twist_real - first_imag * twist_imag
    mid_imag = first_real * twist_imag + first_imag * twist_real
    last_real, last_imag = dft_table(inner_len, sign)
    out_real = section_two(last_real, mid_real) - section_two(last_imag, mid_imag)
    out_imag = section_two(last_real, mid_imag) + section_two(last_imag, mid_real)
    factor = 1.0 / math.sqrt(length)
    return (
        (out_real * factor).reshape(leading + (length,)),
        (out_imag * factor).reshape(leading + (length,)),
    )


def pieces_from_image(extrap, band_count, group_count):
    rows_dev = extrap.shape[0]
    image_width = extrap.shape[1]
    stripe = image_width // band_count
    piece_cols = stripe // group_count
    piece_rows = image_width // group_count
    col_real, col_imag = dft_last(extrap, None, -1.0)
    shaped = jnp.stack([col_real, col_imag]).reshape(
        2, 1, 1, rows_dev, band_count, group_count, piece_cols
    )
    moved = lax.all_to_all(
        lax.all_to_all(shaped, "band", split_axis=4, concat_axis=1, tiled=True),
        "vis",
        split_axis=5,
        concat_axis=2,
        tiled=True,
    )
    columns = jnp.transpose(moved.reshape(2, image_width, piece_cols), (2, 0, 1))
    row_real, row_imag = dft_last(columns[:, 0], columns[:, 1], -1.0)
    stacked = (
        jnp.stack([row_real, row_imag], axis=1)
        .astype(jnp.bfloat16)
        .reshape(piece_cols, 2, group_count, piece_rows)
    )
    pieces = lax.all_to_all(stacked, "vis", split_axis=2, concat_axis=0, tiled=True)
    return pieces.reshape(stripe, 2, piece_rows)


def image_from_pieces(piece_sum, band_count, group_count):
    stripe = piece_sum.shape[0]
    piece_rows = piece_sum.shape[2]
    piece_cols = stripe // group_count
    image_width = piece_rows * group_count
    rows_dev = image_width // (band_count * group_count)
    spread = lax.all_to_all(
        piece_sum.reshape(stripe, 2, 1, piece_rows), "vis", split_axis=0, concat_axis=2, tiled=True
    )
    spread = spread.reshape(piece_cols, 2, image_width)
    col_real, col_imag = dft_last(spread[:, 0], spread[:, 1], 1.0)
    stacked = jnp.transpose(jnp.stack([col_real, col_imag]), (0, 2, 1))
    shaped = stacked.reshape(2, band_count, group_count, rows_dev, 1, 1, piece_cols)
    moved = lax.all_to_all(
        lax.all_to_all(shaped, "band", split_axis=1, concat_axis=4, tiled=True),
        "vis",
        split_axis=2,
        concat_axis=5,
        tiled=True,
    )
    moved = moved.reshape(2, rows_dev, image_width)
    out_real, out_imag = dft_last(moved[0], moved[1], 1.0)
    return out_real


def cols_down(field):
    image_width = field.shape[1]
    extended = jnp.concatenate([field, field[:, :6]], axis=1)
    low_part = 0.0
    high_part = 0.0
    for offset in range(8):
        taken = extended[:, offset : offset + image_width : 2]
        low_part = low_part + low_taps[offset] * taken
        high_part = high_part + high_taps[offset] * taken
    return (low_part, high_part)


def cols_up(low_part, high_part):
    halves = []
    for parity in range(2):
        summed = 0.0
        for delay in range(4):
            summed = summed + low_taps[parity + 2 * delay] * jnp.roll(low_part, delay, axis=1)
            summed = summed + high_taps[parity + 2 * delay] * jnp.roll(high_part, delay, axis=1)
        halves.append(summed)
    return jnp.stack(halves, axis=2).reshape(low_part.shape[0], 2 * low_part.shape[1])


def rows_up(low_ext, high_ext, half_rows):
    halves = []
    for parity in range(2):
        summed = 0.0
        for delay in range(4):
            begin = 3 - delay
            summed = summed + low_taps[parity + 2 * delay] * low_ext[begin : begin + half_rows]
            summed = summed + high_taps[parity + 2 * delay] * high_ext[begin : begin + half_rows]
        halves.append(summed)
    return jnp.stack(halves, axis=1).reshape(2 * half_rows, low_ext.shape[1])


def analysis(extrap):
    rows_dev = extrap.shape[0]
    taken_rows = min(6, rows_dev)
    parts_list = [extrap]
    parts_list.append(shifted(extrap[:taken_rows], ("band", "vis"), -1))
    extended = jnp.concatenate(parts_list, axis=0)
    half_rows = rows_dev // 2
    rows_low = 0.0
    rows_high = 0.0
    for offset in range(8):
        taken = extended[offset : offset + 2 * half_rows : 2]
        rows_low = rows_low + low_taps[offset] * taken
        rows_high = rows_high + high_taps[offset] * taken
    low_low, low_high = cols_down(rows_low)
    high_low, high_high = cols_down(rows_high)
    return jnp.stack([low_low, low_high, high_low, high_high])


def synthesis(coef_dual):
    half_rows = coef_dual.shape[1]
    taken_rows = min(3, half_rows)
    parts_list = [shifted(coef_dual[:, half_rows - taken_rows :, :], ("band", "vis"), 1)]
    joined = jnp.concatenate(parts_list[::-1] + [coef_dual], axis=1)
    cols_low = rows_up(joined[0], joined[2], half_rows)
    cols_high = rows_up(joined[1], joined[3], half_rows)
    return cols_up(cols_low, cols_high)


def degrid(kernel_here, tiles):
    kernel_real = kernel_here[:, :, 0]
    kernel_imag = kernel_here[:, :, 1]
    tile_real = tiles[:, :, 0]
    tile_imag = tiles[:, :, 1]
    out_real = jnp.einsum(
        "qsat,qst->qsa", kernel_real, tile_real, preferred_element_type=jnp.float32
    ) - jnp.einsum("qsat,qst->qsa", kernel_imag, tile_imag, preferred_element_type=jnp.float32)
    out_imag = jnp.einsum(
        "qsat,qst->qsa", kernel_real, tile_imag, preferred_element_type=jnp.float32
    ) + jnp.einsum("qsat,qst->qsa", kernel_imag, tile_real, preferred_element_type=jnp.float32)
    return jnp.stack([out_real, out_imag], axis=2)


def grid_back(kernel_here, weights):
    kernel_real = kernel_here[:, :, 0]
    kernel_imag = kernel_here[:, :, 1]
    weight_real = weights[:, :, 0]
    weight_imag = weights[:, :, 1]
    grid_real = jnp.einsum(
        "qsat,qsa->qst", kernel_real, weight_real, preferred_element_type=jnp.float32
    ) + jnp.einsum("qsat,qsa->qst", kernel_imag, weight_imag, preferred_element_type=jnp.float32)
    grid_imag = jnp.einsum(
        "qsat,qsa->qst", kernel_real, weight_imag, preferred_element_type=jnp.float32
    ) - jnp.einsum("qsat,qsa->qst", kernel_imag, weight_real, preferred_element_type=jnp.float32)
    return jnp.stack([grid_real, grid_imag], axis=2)


def local(sky_image, coef_dual, vis_dual, visibilities, kernel_blocks, tile_rows, tile_counts):
    band_count = lax.axis_size("band")
    group_count = lax.axis_size("vis")
    kernel_here = kernel_blocks[0, 0]
    rows_here = tile_rows[0, 0]
    slot_count = rows_here.shape[1]
    live_slots = (
        jnp.arange(slot_count, dtype=jnp.int32)[None, :] < tile_counts[0, 0][:, None]
    ).astype(jnp.float32)[:, :, None, None]
    vis_data = visibilities[0, 0]
    vis_state = vis_dual[0, 0]
    image_width = sky_image.shape[1]
    stripe = image_width // band_count
    piece_rows = image_width // group_count
    incoming_rows = lax.all_to_all(rows_here, "vis", split_axis=0, concat_axis=0, tiled=True)
    data_part = jnp.sum(live_slots * vis_data * vis_data)
    weights = (live_slots * vis_state).astype(jnp.bfloat16)
    contrib = grid_back(kernel_here, weights)
    arrived = lax.all_to_all(contrib, "vis", split_axis=0, concat_axis=0, tiled=True)
    piece_sum = jax.ops.segment_sum(
        arrived.reshape(-1, 2, piece_rows), incoming_rows.reshape(-1), num_segments=stripe
    )
    adjoint_part = image_from_pieces(piece_sum, band_count, group_count)
    smooth = synthesis(coef_dual)
    new_image = jnp.maximum(sky_image - smooth - adjoint_part, 0.0)
    extrap = 2.0 * new_image - sky_image
    coeffs = analysis(extrap)
    abs_total = jnp.sum(jnp.abs(coeffs))
    coef_total = lax.psum(abs_total, ("band", "vis"))
    threshold = 0.5 * coef_total / (IMG * IMG)
    coef_dual = jnp.clip(coef_dual + coeffs, -threshold, threshold)
    piece_grid = pieces_from_image(extrap, band_count, group_count)
    tiles = lax.all_to_all(
        piece_grid[incoming_rows], "vis", split_axis=0, concat_axis=0, tiled=True
    )
    predicted = degrid(kernel_here, tiles)
    residual = live_slots * (vis_state + predicted - vis_data)
    resid_square = jnp.sum(residual * residual)
    norm_square, data_square = lax.psum((resid_square, data_part), ("band", "vis"))
    radius = 0.5 * jnp.sqrt(data_square + 1e-06)
    size_value = jnp.sqrt(norm_square + 1e-06)
    vis_state = residual * (1.0 - jnp.minimum(1.0, radius / size_value))
    return (new_image, coef_dual, vis_state[None, None])


high = lax.Precision.HIGH
everywhere = ("band", "vis")


def wave_tables(length, digit_low):
    digit_high = length // digit_low
    low = np.arange(digit_low)
    wide = np.arange(digit_high)
    full = 2.0 * np.pi
    small = full * (low[:, None] * low[None, :] % digit_low) / digit_low
    twist = full * (low[:, None] * wide[None, :]) / length
    large = full * (wide[:, None] * wide[None, :] % digit_high) / digit_high
    return small, twist, large


def complex_matrix(angle, sign):
    c = np.cos(angle)
    s = sign * np.sin(angle)
    return np.stack([np.stack([c, -s], axis=1), np.stack([s, c], axis=1)])


def f32(values):
    return jnp.asarray(np.asarray(values, np.float32))


def bf16(values):
    return f32(values).astype(jnp.bfloat16)


def analysis_matrix(half):
    matrix = np.zeros((2, half, 2 * half + 6))
    for k in range(half):
        for j in range(8):
            matrix[0, k, 2 * k + j] = low_taps[j]
            matrix[1, k, 2 * k + j] = high_taps[j]
    return matrix.reshape(2 * half, 2 * half + 6)


def synthesis_matrix(half):
    matrix = np.zeros((2 * half, 2, half + 3))
    for n in range(2 * half):
        for delay in range(4):
            tap = n % 2 + 2 * delay
            matrix[n, 0, n // 2 - delay + 3] = low_taps[tap]
            matrix[n, 1, n // 2 - delay + 3] = high_taps[tap]
    return matrix


def cos_sums(values, size):
    half = size // 2
    if half < 2:
        return [values[0] + values[1], values[0] - values[1]]
    quarter = half // 2
    plus = [values[a] + values[half - a] for a in range(quarter)] + [values[quarter]]
    minus = [values[a] - values[half - a] for a in range(quarter)]
    out = [None] * (half + 1)
    out[0::2] = cos_sums(plus, half)
    for k in range(1, half, 2):
        total = minus[0]
        for a in range(1, quarter):
            total = total + minus[a] * math.cos(2 * math.pi * (a * k % size) / size)
        out[k] = total
    return out


def sin_sums(values, size):
    half = size // 2
    if half < 2:
        return [None] * (half + 1)
    quarter = half // 2
    plus = {a: values[a] + values[half - a] for a in range(1, quarter)}
    plus[quarter] = values[quarter]
    minus = [None] + [values[a] - values[half - a] for a in range(1, quarter)]
    out = [None] * (half + 1)
    out[0::2] = sin_sums(minus, half)
    for k in range(1, half, 2):
        total = None
        for a in range(1, quarter + 1):
            factor = math.sin(2 * math.pi * (a * k % size) / size)
            term = plus[a] if a * 4 == size and k % 4 == 1 else plus[a] * factor
            total = term if total is None else total + term
        out[k] = total
    return out


def even_odd(values):
    size = len(values)
    half = size // 2
    even = [values[0]] + [values[a] + values[size - a] for a in range(1, half)] + [values[half]]
    odd = [None] + [values[a] - values[size - a] for a in range(1, half)]
    return even, odd


def split(values):
    upper = values.astype(jnp.bfloat16)
    return upper, (values - upper.astype(jnp.float32)).astype(jnp.bfloat16)


def table_pair(values):
    upper = f32(values).astype(jnp.bfloat16)
    return upper, (f32(values) - upper.astype(jnp.float32)).astype(jnp.bfloat16)


def nt_dot(a, b):
    return lax.dot_general(a, b, (((1,), (1,)), ((), ())), preferred_element_type=jnp.float32)


def nn_dot(a, b):
    return lax.dot_general(a, b, (((1,), (0,)), ((), ())), preferred_element_type=jnp.float32)


LEVELS = 32000.0
MESH = pl.DeviceIdType.MESH
LANES = 128
whole = pl.BlockSpec(memory_space=pltpu.VMEM)


def place():
    band = lax.axis_index("band")
    vis = lax.axis_index("vis")
    groups = lax.axis_size("vis")
    z = vis // 4
    y = vis // 2 % 2
    core = vis % 2
    return band, z, y, core, groups


def taps_dot(values, tables):
    upper, lower = split(values)
    return nn_dot(upper, tables[0]) + nn_dot(lower, tables[0]) + nn_dot(upper, tables[1])


def level(values):
    return jnp.round(values).astype(jnp.int32)


def step_kernel(
    low,
    kernels_hbm,
    coef_hbm,
    sky_hbm,
    up_hbm,
    edge_hbm,
    base_hbm,
    spin_hbm,
    inv_hbm,
    fwd_hbm,
    near_hbm,
    next_hbm,
    last_hbm,
    order_hbm,
    state_ref,
    data_ref,
    rows_ref,
    counts_ref,
    phase_ref,
    shift_ref,
    tw_ref,
    image_hbm,
    coef_out_hbm,
    vis_out_ref,
    kernels_ref,
    joined_ref,
    sky_ref,
    merged_ref,
    up_ref,
    edge_ref,
    base_ref,
    spin_ref,
    inv_ref,
    fwd_ref,
    near_ref,
    next_ref,
    last_ref,
    order_ref,
    load_sem,
    tail_ref,
    halo_ref,
    block_ref,
    all_cols_ref,
    turn_ref,
    total_ref,
    tall_ref,
    smooth_ref,
    fold_ref,
    grid_ref,
    hot_ref,
    half_ref,
    spec_ref,
    rest_ref,
    extrap_ref,
    picked_ref,
    unit_ref,
    got_ref,
    units_ref,
    mid_ref,
    column_ref,
    all_abs_ref,
    all_sums_ref,
    send_a,
    send_b,
    recv_a,
    recv_b,
    send_p,
    send_u,
    recv_p,
    recv_u,
    send_t,
    recv_t,
    send_s,
    recv_s,
    halo_sem,
):
    x, z, y, core, groups = place()
    levels = groups // 4
    devices = 2 * groups
    half_rows, half_width = coef_hbm.shape[1:]
    rows = 2 * half_rows
    tiles = block_ref.shape[1]
    kept = low // 2 + 1
    wide = LANES

    def index(px, pz, py, pc):
        return px * groups + pz * 4 + py * 2 + pc

    def device(px, pz, py, pc):
        return (px, pz * 4 + py * 2 + pc)

    def ident(number):
        return (number // groups, number % groups)

    def remote(src, dst, send, recv, target):
        return pltpu.make_async_remote_copy(
            src_ref=src,
            dst_ref=dst,
            send_sem=send,
            recv_sem=recv,
            device_id=target,
            device_id_type=MESH,
        )

    me = index(x, z, y, core)
    after, before = (me + 1) % devices, (me + devices - 1) % devices
    twin = device(x, z, y, 1 - core)
    line = [device(x, (z + k) % levels, y, core) for k in range(1, levels)]
    corners = [(1 - x, y), (x, 1 - y), (1 - x, 1 - y)]
    plane = [device(px, z, py, core) for px, py in corners]
    barrier = pltpu.get_barrier_semaphore()
    peers = line + plane + [twin, ident(after), ident(before)]
    for peer in peers:
        pl.semaphore_signal(barrier, inc=1, device_id=peer, device_id_type=MESH)

    sources = [
        (kernels_hbm, kernels_ref),
        (coef_hbm, joined_ref.at[:, pl.ds(8, half_rows), :]),
        (up_hbm, up_ref),
        (edge_hbm, edge_ref),
        (base_hbm, base_ref),
        (spin_hbm, spin_ref),
        (inv_hbm, inv_ref),
        (sky_hbm, sky_ref),
        (fwd_hbm, fwd_ref),
        (near_hbm, near_ref),
        (next_hbm, next_ref),
        (last_hbm, last_ref),
        (order_hbm, order_ref),
    ]
    loads = [
        pltpu.make_async_copy(src, dst, load_sem.at[i]) for i, (src, dst) in enumerate(sources)
    ]
    for load in loads:
        load.start()
    loads[0].wait()
    count = 16
    span = kernels_ref.shape[0] * count // tiles
    width = low * wide
    stripe = width // 2
    slots = rows_ref.shape[0]
    lane = lax.broadcasted_iota(jnp.int32, (tiles, groups), 1)
    tile_id = lax.broadcasted_iota(jnp.int32, (tiles, groups), 0)
    counts = jnp.where(lane == tile_id // slots, counts_ref[...].astype(jnp.float32), 0.0)
    counts = jnp.sum(counts, axis=1, keepdims=True)
    tile_id = lax.broadcasted_iota(jnp.int32, (tiles, 1), 0)
    live = jnp.where((tile_id % slots).astype(jnp.float32) < counts, 1.0, 0.0)
    state = [state_ref[:, part, :] for part in range(2)]
    data = [data_ref[:, part, :] for part in range(2)]
    ours = [part * live for part in state]
    turned = [ours[0], ours[1], ours[0], ours[1]], [ours[1], -ours[0], ours[1], -ours[0]]
    turned = [jnp.concatenate(parts, axis=1) for parts in turned]
    pair_lane = lax.broadcasted_iota(jnp.int32, (count, LANES), 1) // (LANES // 2)
    pair_row = lax.broadcasted_iota(jnp.int32, (count, LANES), 0)
    masks = [pair_lane + 2 * k == pair_row for k in range(count // 2)]
    for i in range(tiles // count):
        spread = [
            jnp.concatenate(
                [jnp.where(mask, part[i * count : (i + 1) * count], 0.0) for mask in masks], axis=1
            )
            for part in turned
        ]
        spread = jnp.concatenate(spread, axis=0).astype(jnp.bfloat16)
        both = nn_dot(spread, kernels_ref[i * span : (i + 1) * span, :])
        both = jnp.concatenate([both[:count], both[count:]], axis=1)
        block_ref[me, i * count : (i + 1) * count, :] = both.astype(jnp.bfloat16)
    lane = lax.broadcasted_iota(jnp.int32, (groups, LANES), 1) % tiles
    owner = lax.broadcasted_iota(jnp.int32, (groups, LANES), 0)
    columns = 0.0
    by_owner = rows_ref[...].astype(jnp.float32).T
    for slot in range(slots):
        here = by_owner[:, slot : slot + 1]
        columns = columns + jnp.where(lane == owner * slots + slot, here, 0.0)
    columns = jnp.sum(columns, axis=0, keepdims=True).astype(jnp.int32)
    all_cols_ref[me] = columns + x * stripe
    loads[1].wait()
    for c in range(4):
        tail_ref[3 * c : 3 * c + 3, :] = joined_ref[c, half_rows + 5 :, :]
    pl.semaphore_wait(barrier, len(peers))

    started = []

    def start(block, target, slot):
        own_a, own_b = block_ref.at[block], all_cols_ref.at[block]
        for own, send, recv in ((own_a, send_a, recv_a), (own_b, send_b, recv_b)):
            copy = remote(own, own, send.at[slot], recv.at[block], target)
            copy.start()
            started.append(copy)

    def got(block):
        for ref, send, recv in ((block_ref, send_a, recv_a), (all_cols_ref, send_b, recv_b)):
            own = ref.at[block]
            remote(own, own, send.at[0], recv.at[block], twin).wait_recv()

    slots_of = iter(range(send_a.shape[0]))
    far = sorted(range(1, levels), key=lambda k: abs(k - levels / 2))
    for k in far:
        start(me, line[k - 1], next(slots_of))
    for target in plane:
        start(me, target, next(slots_of))
    edge = remote(tail_ref, halo_ref, halo_sem.at[0], halo_sem.at[1], ident(after))
    edge.start()
    start(me, twin, next(slots_of))
    line_blocks = [index(x, (z + levels - k) % levels, y, core) for k in far]
    for block in line_blocks:
        got(block)
        for target in plane:
            start(block, target, next(slots_of))
        start(block, twin, next(slots_of))
    edge.wait()
    for c in range(4):
        joined_ref[c, 5:8, :] = halo_ref[3 * c : 3 * c + 3, :]
    strips = half_width // LANES

    def tall(i, carry):
        here = pl.ds(pl.multiple_of(i * LANES, LANES), LANES)
        for c in range(2):
            for k in range(half_rows // 8):
                lows = [joined_ref[c, 8 + 8 * k - d : 16 + 8 * k - d, here] for d in range(4)]
                highs = [joined_ref[c + 2, 8 + 8 * k - d : 16 + 8 * k - d, here] for d in range(4)]
                for parity in range(2):
                    total = 0.0
                    for d in range(4):
                        total = total + low_taps[parity + 2 * d] * lows[d]
                        total = total + high_taps[parity + 2 * d] * highs[d]
                    tall_ref[c * strips + i, pl.ds(16 * k + parity, 8, stride=2), :] = total
        return carry

    lax.fori_loop(0, strips, tall, 0)

    for px, py in corners:
        block = index(px, z, py, core)
        got(block)
        start(block, twin, next(slots_of))
    for load in loads[2:8]:
        load.wait()

    def broad(i, carry):
        there = (i + strips - 1) % strips
        near = jnp.concatenate([tall_ref[i], tall_ref[strips + i]], axis=1)
        last = jnp.concatenate([tall_ref[there], tall_ref[strips + there]], axis=1)
        out = taps_dot(near, up_ref)
        first = taps_dot(last, edge_ref)
        smooth_ref[2 * i] = out[:, :LANES] + first
        smooth_ref[2 * i + 1] = out[:, LANES:]
        return carry

    lax.fori_loop(0, strips // 2, broad, 0)
    spin_cos, spin_sin = spin_ref[0, pl.ds(me, 1), :], spin_ref[1, pl.ds(me, 1), :]
    cosine = (base_ref[0] * spin_cos - base_ref[1] * spin_sin).astype(jnp.bfloat16)
    sine = (base_ref[1] * spin_cos + base_ref[0] * spin_sin).astype(jnp.bfloat16)
    piece = kernels_ref.shape[1]
    turn_ref[:rows, :piece] = cosine
    turn_ref[:rows, piece:] = -sine
    turn_ref[rows:, :piece] = sine
    turn_ref[rows:, piece:] = cosine
    for n, k in enumerate(far):
        for px, py in corners:
            block = index(px, (z + levels - k) % levels, py, core)
            got(block)
            start(block, twin, next(slots_of))
        if n == 0:
            lax.fori_loop(strips // 2, strips, broad, 0)

    total_tiles = devices * tiles
    class_tiles = groups * tiles
    parts = class_tiles // LANES
    lane = lax.broadcasted_iota(jnp.int32, (1, LANES), 1)

    def spread_class(c):
        for i in range(parts):
            columns = jnp.where(
                lane < tiles, all_cols_ref[4 * i + c], all_cols_ref[4 * i + 2 + c]
            )
            k1 = columns % low
            k2 = columns // low
            flip = k1 >= kept
            k1 = jnp.where(flip, low - k1, k1)
            k2 = jnp.where(flip, wide - 1 - k2, k2)
            fold_ref[0, pl.ds(c * parts + i, 1), :] = (k1 * wide + k2).astype(jnp.float32)
            fold_ref[1, pl.ds(c * parts + i, 1), :] = jnp.where(flip, -1.0, 1.0)
        chunk = 4 * LANES
        for j in range(class_tiles // chunk):
            n = chunk // tiles
            some = [block_ref[2 * (j * n + i) + c] for i in range(n)]
            both = nt_dot(turn_ref[...], jnp.concatenate(some, axis=0))
            for i in range(chunk // LANES):
                b = c * parts + j * (chunk // LANES) + i
                at = pl.ds(pl.multiple_of(b * LANES, LANES), LANES)
                real = both[:rows, i * LANES : (i + 1) * LANES]
                imag = both[rows:, i * LANES : (i + 1) * LANES]
                sign = fold_ref[1, pl.ds(b, 1), :]
                out_real = real * phase_ref[0] - imag * phase_ref[1]
                out_imag = (real * phase_ref[1] + imag * phase_ref[0]) * sign
                grid_ref[:rows, at] = out_real.astype(jnp.bfloat16)
                grid_ref[rows:, at] = out_imag.astype(jnp.bfloat16)

    def folded_class(c, p):
        base = pl.multiple_of(p * 2 * wide, 2 * wide)
        row = (lax.broadcasted_iota(jnp.int32, (2 * wide, LANES), 0) + base).astype(jnp.float32)
        hots = []
        for i in range(parts):
            hit = row == fold_ref[0, pl.ds(c * parts + i, 1), :]
            hots.append(jnp.where(hit, 1.0, 0.0).astype(jnp.bfloat16))
        hot = jnp.concatenate(hots, axis=1)
        at = pl.ds(pl.multiple_of(c * class_tiles, class_tiles), class_tiles)
        hot_ref[pl.ds(base, 2 * wide), at] = hot
        return nt_dot(grid_ref[:, at], hot)

    spread_class(core)

    def scatter_own(p, carry):
        total_ref[p] = folded_class(core, p)
        return carry

    lax.fori_loop(0, (kept + 1) // 2, scatter_own, 0)
    for i in range(groups):
        got(2 * i + 1 - core)
    spread_class(1 - core)

    def scatter(p, carry):
        folded = (total_ref[p] + folded_class(1 - core, p)).astype(jnp.bfloat16)
        for e in range(2):
            here = slice(e * wide, (e + 1) * wide)
            pair = jnp.concatenate([folded[:rows, here], folded[rows:, here]], axis=1)
            mid = nn_dot(pair, inv_ref[...])
            k1 = p * 2 + e
            tw_real, tw_imag = tw_ref[0, pl.ds(k1, 1), :], tw_ref[1, pl.ds(k1, 1), :]
            real, imag = mid[:, :wide], mid[:, wide:]
            half_ref[k1, :, :wide] = real * tw_real - imag * tw_imag
            half_ref[k1, :, wide:] = real * tw_imag + imag * tw_real
        return carry

    lax.fori_loop(0, (kept + 1) // 2, scatter, 0)

    def strip(i, carry):
        at = pl.ds(pl.multiple_of(i * 8, 8), 8)
        cos_part = cos_sums([half_ref[k, at, :wide] for k in range(kept)], low)
        sin_part = sin_sums([None] + [half_ref[k, at, wide:] for k in range(1, kept - 1)], low)
        extraps = []
        for a in range(low):
            k = min(a, low - a)
            if a == 0 or a == low // 2:
                adjoint = cos_part[k]
            elif a < low // 2:
                adjoint = cos_part[k] - sin_part[k]
            else:
                adjoint = cos_part[k] + sin_part[k]
            here = slice(a * wide, (a + 1) * wide)
            sky = sky_ref[at, here]
            image = jnp.maximum(sky - smooth_ref[a, at, :] - adjoint, 0.0)
            extrap = 2.0 * image - sky
            sky_ref[at, here] = image
            extrap_ref[a, at, :] = extrap
            extraps.append(extrap)
        even, odd = even_odd(extraps)
        real_part = cos_sums(even, low)
        imag_part = sin_sums(odd, low)
        for k in range(kept):
            tw_real, tw_imag = tw_ref[0, k : k + 1, :], tw_ref[1, k : k + 1, :]
            real = real_part[k] * tw_real
            imag = -real_part[k] * tw_imag
            if 0 < k < kept - 1:
                real = real - imag_part[k] * tw_imag
                imag = imag - imag_part[k] * tw_real
            half_ref[k, at, :wide] = real
            half_ref[k, at, wide:] = imag
        return carry

    lax.fori_loop(0, rows // 8, strip, 0)
    store = pltpu.make_async_copy(sky_ref, image_hbm, load_sem.at[len(loads)])
    store.start()
    top = remote(
        extrap_ref.at[:, pl.ds(0, 8), :],
        extrap_ref.at[:, pl.ds(rows, 8), :],
        halo_sem.at[2],
        halo_sem.at[3],
        ident(before),
    )
    top.start()
    loads[8].wait()

    def spectrum(k, carry):
        out = taps_dot(half_ref[k], fwd_ref)
        here = pl.ds(pl.multiple_of(k * wide, wide), wide)
        upper, lower = split(out)
        spec_ref[:rows, here] = upper[:, :wide]
        spec_ref[rows:, here] = upper[:, wide:]
        rest_ref[:rows, here] = lower[:, :wide]
        rest_ref[rows:, here] = lower[:, wide:]
        return carry

    lax.fori_loop(0, kept, spectrum, 0)

    def sends(to):
        order = to % 2 * groups + to // 2
        at = pl.ds(pl.multiple_of(order * tiles, tiles), tiles)
        unit = unit_ref.at[order // 2]
        return [
            remote(picked_ref.at[at, :], got_ref.at[me], send_p.at[0], recv_p.at[0], ident(to)),
            remote(unit, units_ref.at[me], send_u.at[0], recv_u.at[0], ident(to)),
        ]

    others = pl.ds(0, devices - 1)

    def total_of(ref, send, recv):
        return remote(ref.at[others], ref.at[others], send.at[0], recv.at[0], twin)

    def share_row(ref, send, recv):
        def one(k, carry):
            to = (me + k) % devices
            remote(ref.at[me], ref.at[me], send.at[0], recv.at[0], ident(to)).start()
            return carry

        lax.fori_loop(1, devices, one, 0)

    def row_total(ref):
        total = ref[0]
        for d in range(1, devices):
            total = total + ref[d]
        return total

    def pick(s, carry):
        half = levels // 2
        to_class, to_x = (core + s) % 2, (x + 1 + s // 2) % 2
        spot = to_x * 2 + (z // half + 1 + s // 4) % 2
        j = to_class * 4 + spot
        at = pl.multiple_of(j * 2 * LANES, 2 * LANES)
        hot = hot_ref[: kept * wide, pl.ds(at, 2 * LANES)]
        both = nn_dot(spec_ref[...], hot) + nn_dot(rest_ref[...], hot)
        for h in range(2):
            sign = fold_ref[1, pl.ds(2 * j + h, 1), :]
            real = both[:rows, h * LANES : (h + 1) * LANES]
            imag = both[rows:, h * LANES : (h + 1) * LANES] * sign
            most = jnp.max(jnp.maximum(jnp.abs(real), jnp.abs(imag)), axis=0, keepdims=True)
            most = jnp.maximum(most, 1e-30)
            unit_ref[2 * j + h] = most * (1.0 / LEVELS)
            to_level = LEVELS / most
            packed = level(real * to_level) * 65536 + level(imag * to_level)
            to = pl.ds(pl.multiple_of(at + h * LANES, LANES), LANES)
            picked_ref[to, :] = packed.T
        for i in range(4):
            to = (spot * 4 + i) * 2 + to_class

            @pl.when(to != me)
            def _():
                for copy in sends(to):
                    copy.start()

        return carry

    lax.fori_loop(0, devices // 4, pick, 0)
    order = core * groups + me // 2
    got_ref[me] = picked_ref[pl.ds(pl.multiple_of(order * tiles, tiles), tiles), :]
    units_ref[me] = unit_ref[order // 2]
    top.wait()
    loads[9].wait()
    loads[10].wait()

    def rows_down(i, carry):
        for k in range(half_rows // 8):
            lows, highs = 0.0, 0.0
            for tap in range(8):
                taken = extrap_ref[i, pl.ds(16 * k + tap, 8, stride=2), :]
                lows = lows + low_taps[tap] * taken
                highs = highs + high_taps[tap] * taken
            tall_ref[i, 8 * k : 8 * k + 8, :] = lows
            tall_ref[i, half_rows + 8 * k : half_rows + 8 * k + 8, :] = highs
        return carry

    lax.fori_loop(0, low, rows_down, 0)

    def cols_down(b, absolute):
        here = jnp.concatenate([tall_ref[2 * b], tall_ref[2 * b + 1]], axis=1)
        out = taps_dot(here, near_ref) + taps_dot(tall_ref[(2 * b + 2) % low], next_ref)
        at = pl.ds(pl.multiple_of(b * LANES, LANES), LANES)
        for c in range(4):
            top_row, left = c // 2 * half_rows, c % 2 * LANES
            part = out[top_row : top_row + half_rows, left : left + LANES]
            absolute = absolute + jnp.abs(part)
            merged_ref[c, :, at] = joined_ref[c, 8:, at] + part
        return absolute

    absolute = lax.fori_loop(0, low // 2, cols_down, jnp.zeros((half_rows, LANES), jnp.float32))
    abs_total = jnp.sum(jnp.sum(absolute, axis=0, keepdims=True), axis=1, keepdims=True)
    loads[11].wait()
    loads[12].wait()

    lane = lax.broadcasted_iota(jnp.int32, (1, LANES), 1)
    all_abs_ref[me] = jnp.where(lane == 0, abs_total, 0.0)
    share_row(all_abs_ref, send_t, recv_t)
    total_of(got_ref, send_p, recv_p).wait_recv()
    total_of(units_ref, send_u, recv_u).wait_recv()

    units = jnp.concatenate([units_ref[d] for d in range(devices)], axis=0)
    units = jnp.concatenate([units] * (LANES // devices), axis=0).T
    column_ref[...] = jnp.where(y == 0, units[:tiles], units[tiles:])

    def finish(i, carry):
        here = pl.ds(pl.multiple_of(i * 8, 8), 8)
        cosine, sine = shift_ref[0, here, :], shift_ref[1, here, :]
        reals, imags = [], []
        for d in range(devices):
            packed = got_ref[d, here, :]
            real = (packed + 32768) >> 16
            imag = packed - (real << 16)
            unit = column_ref[here, d : d + 1]
            real = real.astype(jnp.float32) * unit
            imag = imag.astype(jnp.float32) * unit
            reals.append(real * cosine + imag * sine)
            imags.append(imag * cosine - real * sine)
        even, odd = even_odd(reals)
        cos_real, sin_real = cos_sums(even, devices), sin_sums(odd, devices)
        even, odd = even_odd(imags)
        cos_imag, sin_imag = cos_sums(even, devices), sin_sums(odd, devices)
        half = devices // 2
        for k in range(half + 1):
            if k == 0 or k == half:
                outs = [(k, cos_real[k], cos_imag[k])]
            else:
                outs = [
                    (k, cos_real[k] + sin_imag[k], cos_imag[k] - sin_real[k]),
                    (devices - k, cos_real[k] - sin_imag[k], cos_imag[k] + sin_real[k]),
                ]
            for t, real, imag in outs:
                mid_ref[t, here, :rows] = real
                mid_ref[t, here, rows:] = imag
        return carry

    lax.fori_loop(0, tiles // 8, finish, 0)
    group = 2 * LANES // 16
    lane = lax.broadcasted_iota(jnp.int32, (1, 2 * LANES), 1) // 16
    pieces = []
    for g in range(devices // group):
        total = None
        for e in range(group):
            upper, lower = split(mid_ref[g * group + e])
            out = nn_dot(upper, last_ref[0, g]) + nn_dot(lower, last_ref[0, g])
            out = out + nn_dot(upper, last_ref[1, g])
            out = jnp.where(lane == e, out, 0.0)
            total = out if total is None else total + out
        pieces.append(total.astype(jnp.bfloat16))
    tile = nn_dot(jnp.concatenate(pieces, axis=1), order_ref[...]).astype(jnp.bfloat16)
    first, second = [], []
    near_row = pair_row % 2 == 0
    for i in range(tiles // count):
        here = tile[i * count : (i + 1) * count]
        pair = jnp.concatenate([here[:, :piece], here[:, piece:]], axis=0)
        out = nt_dot(pair, kernels_ref[i * span : (i + 1) * span, :])
        for found, half in ((first, out[:count]), (second, out[count:])):
            total = 0.0
            for k in range(count // 2):
                total = total + jnp.where(
                    pair_row // 2 == k, half[:, k * LANES : (k + 1) * LANES], 0.0
                )
            found.append(jnp.where(near_row, total, pltpu.roll(total, LANES // 2, 1)))
    first = jnp.concatenate(first, axis=0)
    second = jnp.concatenate(second, axis=0)
    visits = state_ref.shape[2]
    lane = lax.broadcasted_iota(jnp.int32, first.shape, 1)
    crossed = jnp.where(
        lane // visits % 2 == 0,
        -pltpu.roll(second, LANES - visits, 1),
        pltpu.roll(second, visits, 1),
    )
    keep = jnp.where(lane < 2 * visits, live, 0.0)
    state_wide = jnp.concatenate(state + state, axis=1)
    data_wide = jnp.concatenate(data + data, axis=1)
    residual = keep * (state_wide + first + crossed - data_wide)
    norms = []
    for values in (residual, data_wide * keep):
        norms.append(jnp.sum(jnp.sum(values * values, axis=0, keepdims=True), axis=1, keepdims=True))
    lane = lax.broadcasted_iota(jnp.int32, (1, LANES), 1)
    all_sums_ref[me] = jnp.where(lane == 0, norms[0], norms[1])
    share_row(all_sums_ref, send_s, recv_s)
    total_of(all_abs_ref, send_t, recv_t).wait_recv()
    threshold = 0.5 * row_total(all_abs_ref)[:, 0:1] / (width * width)

    def clip(i, carry):
        at = pl.ds(pl.multiple_of(i * LANES, LANES), LANES)
        for c in range(4):
            merged_ref[c, :, at] = jnp.clip(merged_ref[c, :, at], -threshold, threshold)
        return carry

    lax.fori_loop(0, half_width // LANES, clip, 0)
    store_coef = pltpu.make_async_copy(merged_ref, coef_out_hbm, load_sem.at[len(loads) + 1])
    store_coef.start()
    for copy in started:
        copy.wait_send()
    total_of(got_ref, send_p, recv_p).wait_send()
    total_of(units_ref, send_u, recv_u).wait_send()
    total_of(all_abs_ref, send_t, recv_t).wait_send()
    total_of(all_sums_ref, send_s, recv_s).wait()
    total = row_total(all_sums_ref)
    size = jnp.sqrt(total[:, 0:1] + 1e-06)
    radius = 0.5 * jnp.sqrt(total[:, 1:2] + 1e-06)
    residual = residual * (1.0 - jnp.minimum(1.0, radius / size))
    vis_out_ref[:, 0, :] = residual[:, :visits]
    vis_out_ref[:, 1, :] = residual[:, visits : 2 * visits]
    store.wait()
    store_coef.wait()


def step(kernels, coef, sky, state, data, tile_rows, tile_counts, groups, devices):
    rows, width = sky.shape
    piece = kernels.shape[1]
    slots = tile_rows.shape[0]
    tiles = groups * slots
    half_rows, half_width = coef.shape[1:]
    low = width // LANES
    kept = low // 2 + 1
    wide = np.arange(LANES)
    matrix = synthesis_matrix(LANES)
    up = matrix[:, :, 3:].transpose(1, 2, 0).reshape(2 * LANES, 2 * LANES)
    edge = np.zeros((2, LANES, LANES))
    edge[:, LANES - 3 :, :] = matrix[:LANES, :, :3].transpose(1, 2, 0)
    matrix = analysis_matrix(LANES).T
    following = np.zeros((LANES, 2 * LANES))
    following[:6] = matrix[2 * LANES :]
    turn = np.arange(piece)
    base = 2 * np.pi * np.arange(rows)[:, None] * turn[None, :] / width
    spin = 2 * np.pi * (np.arange(devices)[:, None] * turn[None, :] % devices) / devices
    owner = wide // slots % groups
    shift = 2 * np.pi * (np.arange(rows)[:, None] * owner[None, :] % groups) / groups
    phase = np.stack([np.cos(shift), np.sin(shift)])
    full = 2 * np.pi * (wide[:, None] * wide[None, :] % LANES) / LANES
    c, s = np.cos(full) / width, np.sin(full) / width
    inverse = np.block([[c, s], [-s, c]])
    forward = np.block([[c, -s], [s, c]])
    twist = 2 * np.pi * np.arange(kept + 1)[:, None] * wide[None, :] / width
    each = piece // devices
    t = np.arange(devices)[:, None] + devices * np.arange(each)[None, :]
    angle = 2 * np.pi * (np.arange(rows)[:, None, None] * t[None] % width) / width
    c, s = np.cos(angle), np.sin(angle)
    last = np.stack([np.stack([c, -s], axis=2), np.stack([s, c], axis=2)])
    last = last.reshape(2 * rows, -1, 2 * LANES).transpose(1, 0, 2)
    order = np.zeros((2 * piece, 2 * piece))
    for a in range(devices):
        for part in range(2):
            for b in range(each):
                order[(a * 2 + part) * each + b, part * piece + a + devices * b] = 1.0
    loaded = [
        kernels,
        coef,
        sky,
        jnp.stack(table_pair(up)),
        jnp.stack(table_pair(edge.reshape(2 * LANES, LANES))),
        f32(np.stack([np.cos(base), np.sin(base)])),
        f32(np.stack([np.cos(spin), np.sin(spin)])),
        bf16(inverse),
        jnp.stack(table_pair(forward)),
        jnp.stack(table_pair(matrix[: 2 * LANES])),
        jnp.stack(table_pair(following)),
        jnp.stack(table_pair(last)),
        bf16(order),
    ]
    held = [
        state,
        data,
        tile_rows,
        tile_counts,
        f32(phase),
        f32(phase[:, :, :tiles].transpose(0, 2, 1)),
        f32(np.stack([np.cos(twist), np.sin(twist)])),
    ]
    buffers = [pltpu.VMEM(value.shape, value.dtype) for value in loaded]
    buffers[1] = pltpu.VMEM((4, half_rows + 8, half_width), jnp.float32)
    copies = 3 * 4 + 7 + 12
    dma = pltpu.SemaphoreType.DMA
    anywhere = pl.BlockSpec(memory_space=pltpu.HBM)
    return pl.pallas_call(
        lambda *refs: step_kernel(low, *refs),
        out_shape=(
            jax.ShapeDtypeStruct((rows, width), jnp.float32),
            jax.ShapeDtypeStruct(coef.shape, jnp.float32),
            jax.ShapeDtypeStruct(state.shape, jnp.float32),
        ),
        in_specs=[anywhere] * len(loaded) + [whole] * len(held),
        out_specs=(anywhere, anywhere, whole),
        scratch_shapes=buffers[:3]
        + [pltpu.VMEM(coef.shape, jnp.float32)]
        + buffers[3:]
        + [
            dma((len(loaded) + 2,)),
            pltpu.VMEM((16, half_width), jnp.float32),
            pltpu.VMEM((16, half_width), jnp.float32),
            pltpu.VMEM((devices, tiles, 2 * piece), jnp.bfloat16),
            pltpu.VMEM((devices, 1, LANES), jnp.int32),
            pltpu.VMEM((2 * rows, 2 * piece), jnp.bfloat16),
            pltpu.VMEM(((kept + 1) // 2, 2 * rows, 2 * LANES), jnp.float32),
            pltpu.VMEM((low, rows, LANES), jnp.float32),
            pltpu.VMEM((low, rows, LANES), jnp.float32),
            pltpu.VMEM((2, devices // 2, LANES), jnp.float32),
            pltpu.VMEM((2 * rows, devices * tiles), jnp.bfloat16),
            pltpu.VMEM(((kept + 1) * LANES, devices * tiles), jnp.bfloat16),
            pltpu.VMEM((kept + 1, rows, 2 * LANES), jnp.float32),
            pltpu.VMEM((2 * rows, kept * LANES), jnp.bfloat16),
            pltpu.VMEM((2 * rows, kept * LANES), jnp.bfloat16),
            pltpu.VMEM((low, rows + 8, LANES), jnp.float32),
            pltpu.VMEM((devices * tiles, rows), jnp.int32),
            pltpu.VMEM((devices // 2, 1, LANES), jnp.float32),
            pltpu.VMEM((devices, tiles, rows), jnp.int32),
            pltpu.VMEM((devices, 1, LANES), jnp.float32),
            pltpu.VMEM((devices, tiles, 2 * rows), jnp.float32),
            pltpu.VMEM((tiles, LANES), jnp.float32),
            pltpu.VMEM((devices, 1, LANES), jnp.float32),
            pltpu.VMEM((devices, 1, LANES), jnp.float32),
            dma((copies,)),
            dma((copies,)),
        ]
        + [dma((devices,))] * 2
        + [dma((1,))] * 8
        + [dma((4,))],
        compiler_params=pltpu.CompilerParams(
            collective_id=0, has_side_effects=True, vmem_limit_bytes=60 * 2**20
        ),
        name="step",
    )(*loaded, *held)


def fast_local(sky_image, coef_dual, vis_dual, visibilities, kernel_blocks, tile_rows, tile_counts):
    groups = lax.axis_size("vis")
    devices = lax.axis_size("band") * groups
    taken = kernel_blocks.shape
    new_image, coef_dual, vis_state = step(
        kernel_blocks.reshape(-1, taken[-1]),
        coef_dual,
        sky_image,
        vis_dual.reshape((-1,) + vis_dual.shape[4:]),
        visibilities.reshape((-1,) + vis_dual.shape[4:]),
        tile_rows[0, 0].T,
        tile_counts[0],
        groups,
        devices,
    )
    return (new_image, coef_dual, vis_state.reshape(vis_dual.shape))


def body_for(mesh):
    devices = mesh.shape["band"] * mesh.shape["vis"]
    relayed = mesh.shape["band"] == 2 and mesh.shape["vis"] % 4 == 0 and devices == 32

    def body(sky_image, *rest):
        rows, width = sky_image.shape
        piece = width // mesh.shape["vis"]
        tiles = rest[4].shape[2] * rest[4].shape[3]
        if relayed and rows == LANES and piece == 2 * LANES and 2 * tiles == LANES:
            return fast_local(sky_image, *rest)
        return local(sky_image, *rest)

    return body


def solution(mesh):
    return jax.shard_map(
        body_for(mesh),
        mesh=mesh,
        in_specs=(
            P(("band", "vis"), None),
            P(None, ("band", "vis"), None),
            P("band", "vis", None, None, None, None),
            P("band", "vis", None, None, None, None),
            P("band", "vis", None, None, None, None, None),
            P("band", "vis", None, None),
            P("band", "vis", None),
        ),
        out_specs=(
            P(("band", "vis"), None),
            P(None, ("band", "vis"), None),
            P("band", "vis", None, None, None, None),
        ),
        check_vma=False,
    )
```

```python
import math

import jax
import numpy as np
import jax.numpy as jnp
from jax import lax
from jax.experimental import pallas as pl
from jax.experimental.pallas import tpu as pltpu
from jax.sharding import PartitionSpec as P

IMG = 4096


low_taps = (
    -0.010597401784997278,
    0.032883011666982945,
    0.030841381835986965,
    -0.18703481171888114,
    -0.02798376941698385,
    0.6308807679295904,
    0.7148465705525415,
    0.23037781330885523,
)
high_taps = tuple(((-1.0) ** offset * low_taps[7 - offset] for offset in range(8)))
highest = lax.Precision.HIGHEST


def shifted(block, axis, distance):
    devices = range(lax.axis_size(axis))
    route = [((i - distance) % len(devices), i) for i in devices]
    return lax.ppermute(block, axis, route)


def dft_table(table_size, sign):
    positions = jnp.arange(table_size, dtype=jnp.int32)
    phase = positions[:, None] * positions[None, :] % table_size
    angle = 2.0 * math.pi / table_size * phase.astype(jnp.float32)
    return (jnp.cos(angle), sign * jnp.sin(angle))


def section_one(table, values):
    return jnp.einsum("kn,...nm->...km", table, values, precision=highest)


def section_two(table, values):
    return jnp.einsum("qm,...km->...qk", table, values, precision=highest)


def dft_last(real_in, imag_in, sign):
    leading = real_in.shape[:-1]
    length = real_in.shape[-1]
    inner_len = 64
    outer_len = length // inner_len
    split_real = real_in.reshape(leading + (outer_len, inner_len))
    table_real, table_imag = dft_table(outer_len, sign)
    first_real = section_one(table_real, split_real)
    first_imag = section_one(table_imag, split_real)
    if imag_in is not None:
        split_imag = imag_in.reshape(leading + (outer_len, inner_len))
        first_real = first_real - section_one(table_imag, split_imag)
        first_imag = first_imag + section_one(table_real, split_imag)
    outer_index = jnp.arange(outer_len, dtype=jnp.int32)
    inner_index = jnp.arange(inner_len, dtype=jnp.int32)
    twist_phase = outer_index[:, None] * inner_index[None, :] % length
    twist_angle = 2.0 * math.pi / length * twist_phase.astype(jnp.float32)
    twist_real = jnp.cos(twist_angle)
    twist_imag = sign * jnp.sin(twist_angle)
    mid_real = first_real * twist_real - first_imag * twist_imag
    mid_imag = first_real * twist_imag + first_imag * twist_real
    last_real, last_imag = dft_table(inner_len, sign)
    out_real = section_two(last_real, mid_real) - section_two(last_imag, mid_imag)
    out_imag = section_two(last_real, mid_imag) + section_two(last_imag, mid_real)
    factor = 1.0 / math.sqrt(length)
    return (
        (out_real * factor).reshape(leading + (length,)),
        (out_imag * factor).reshape(leading + (length,)),
    )


def pieces_from_image(extrap, band_count, group_count):
    rows_dev = extrap.shape[0]
    image_width = extrap.shape[1]
    stripe = image_width // band_count
    piece_cols = stripe // group_count
    piece_rows = image_width // group_count
    col_real, col_imag = dft_last(extrap, None, -1.0)
    shaped = jnp.stack([col_real, col_imag]).reshape(
        2, 1, 1, rows_dev, band_count, group_count, piece_cols
    )
    moved = lax.all_to_all(
        lax.all_to_all(shaped, "band", split_axis=4, concat_axis=1, tiled=True),
        "vis",
        split_axis=5,
        concat_axis=2,
        tiled=True,
    )
    columns = jnp.transpose(moved.reshape(2, image_width, piece_cols), (2, 0, 1))
    row_real, row_imag = dft_last(columns[:, 0], columns[:, 1], -1.0)
    stacked = (
        jnp.stack([row_real, row_imag], axis=1)
        .astype(jnp.bfloat16)
        .reshape(piece_cols, 2, group_count, piece_rows)
    )
    pieces = lax.all_to_all(stacked, "vis", split_axis=2, concat_axis=0, tiled=True)
    return pieces.reshape(stripe, 2, piece_rows)


def image_from_pieces(piece_sum, band_count, group_count):
    stripe = piece_sum.shape[0]
    piece_rows = piece_sum.shape[2]
    piece_cols = stripe // group_count
    image_width = piece_rows * group_count
    rows_dev = image_width // (band_count * group_count)
    spread = lax.all_to_all(
        piece_sum.reshape(stripe, 2, 1, piece_rows), "vis", split_axis=0, concat_axis=2, tiled=True
    )
    spread = spread.reshape(piece_cols, 2, image_width)
    col_real, col_imag = dft_last(spread[:, 0], spread[:, 1], 1.0)
    stacked = jnp.transpose(jnp.stack([col_real, col_imag]), (0, 2, 1))
    shaped = stacked.reshape(2, band_count, group_count, rows_dev, 1, 1, piece_cols)
    moved = lax.all_to_all(
        lax.all_to_all(shaped, "band", split_axis=1, concat_axis=4, tiled=True),
        "vis",
        split_axis=2,
        concat_axis=5,
        tiled=True,
    )
    moved = moved.reshape(2, rows_dev, image_width)
    out_real, out_imag = dft_last(moved[0], moved[1], 1.0)
    return out_real


def cols_down(field):
    image_width = field.shape[1]
    extended = jnp.concatenate([field, field[:, :6]], axis=1)
    low_part = 0.0
    high_part = 0.0
    for offset in range(8):
        taken = extended[:, offset : offset + image_width : 2]
        low_part = low_part + low_taps[offset] * taken
        high_part = high_part + high_taps[offset] * taken
    return (low_part, high_part)


def cols_up(low_part, high_part):
    halves = []
    for parity in range(2):
        summed = 0.0
        for delay in range(4):
            summed = summed + low_taps[parity + 2 * delay] * jnp.roll(low_part, delay, axis=1)
            summed = summed + high_taps[parity + 2 * delay] * jnp.roll(high_part, delay, axis=1)
        halves.append(summed)
    return jnp.stack(halves, axis=2).reshape(low_part.shape[0], 2 * low_part.shape[1])


def rows_up(low_ext, high_ext, half_rows):
    halves = []
    for parity in range(2):
        summed = 0.0
        for delay in range(4):
            begin = 3 - delay
            summed = summed + low_taps[parity + 2 * delay] * low_ext[begin : begin + half_rows]
            summed = summed + high_taps[parity + 2 * delay] * high_ext[begin : begin + half_rows]
        halves.append(summed)
    return jnp.stack(halves, axis=1).reshape(2 * half_rows, low_ext.shape[1])


def analysis(extrap):
    rows_dev = extrap.shape[0]
    taken_rows = min(6, rows_dev)
    parts_list = [extrap]
    parts_list.append(shifted(extrap[:taken_rows], ("band", "vis"), -1))
    extended = jnp.concatenate(parts_list, axis=0)
    half_rows = rows_dev // 2
    rows_low = 0.0
    rows_high = 0.0
    for offset in range(8):
        taken = extended[offset : offset + 2 * half_rows : 2]
        rows_low = rows_low + low_taps[offset] * taken
        rows_high = rows_high + high_taps[offset] * taken
    low_low, low_high = cols_down(rows_low)
    high_low, high_high = cols_down(rows_high)
    return jnp.stack([low_low, low_high, high_low, high_high])


def synthesis(coef_dual):
    half_rows = coef_dual.shape[1]
    taken_rows = min(3, half_rows)
    parts_list = [shifted(coef_dual[:, half_rows - taken_rows :, :], ("band", "vis"), 1)]
    joined = jnp.concatenate(parts_list[::-1] + [coef_dual], axis=1)
    cols_low = rows_up(joined[0], joined[2], half_rows)
    cols_high = rows_up(joined[1], joined[3], half_rows)
    return cols_up(cols_low, cols_high)


def degrid(kernel_here, tiles):
    kernel_real = kernel_here[:, :, 0]
    kernel_imag = kernel_here[:, :, 1]
    tile_real = tiles[:, :, 0]
    tile_imag = tiles[:, :, 1]
    out_real = jnp.einsum(
        "qsat,qst->qsa", kernel_real, tile_real, preferred_element_type=jnp.float32
    ) - jnp.einsum("qsat,qst->qsa", kernel_imag, tile_imag, preferred_element_type=jnp.float32)
    out_imag = jnp.einsum(
        "qsat,qst->qsa", kernel_real, tile_imag, preferred_element_type=jnp.float32
    ) + jnp.einsum("qsat,qst->qsa", kernel_imag, tile_real, preferred_element_type=jnp.float32)
    return jnp.stack([out_real, out_imag], axis=2)


def grid_back(kernel_here, weights):
    kernel_real = kernel_here[:, :, 0]
    kernel_imag = kernel_here[:, :, 1]
    weight_real = weights[:, :, 0]
    weight_imag = weights[:, :, 1]
    grid_real = jnp.einsum(
        "qsat,qsa->qst", kernel_real, weight_real, preferred_element_type=jnp.float32
    ) + jnp.einsum("qsat,qsa->qst", kernel_imag, weight_imag, preferred_element_type=jnp.float32)
    grid_imag = jnp.einsum(
        "qsat,qsa->qst", kernel_real, weight_imag, preferred_element_type=jnp.float32
    ) - jnp.einsum("qsat,qsa->qst", kernel_imag, weight_real, preferred_element_type=jnp.float32)
    return jnp.stack([grid_real, grid_imag], axis=2)


def local(sky_image, coef_dual, vis_dual, visibilities, kernel_blocks, tile_rows, tile_counts):
    band_count = lax.axis_size("band")
    group_count = lax.axis_size("vis")
    kernel_here = kernel_blocks[0, 0]
    rows_here = tile_rows[0, 0]
    slot_count = rows_here.shape[1]
    live_slots = (
        jnp.arange(slot_count, dtype=jnp.int32)[None, :] < tile_counts[0, 0][:, None]
    ).astype(jnp.float32)[:, :, None, None]
    vis_data = visibilities[0, 0]
    vis_state = vis_dual[0, 0]
    image_width = sky_image.shape[1]
    stripe = image_width // band_count
    piece_rows = image_width // group_count
    incoming_rows = lax.all_to_all(rows_here, "vis", split_axis=0, concat_axis=0, tiled=True)
    data_part = jnp.sum(live_slots * vis_data * vis_data)
    weights = (live_slots * vis_state).astype(jnp.bfloat16)
    contrib = grid_back(kernel_here, weights)
    arrived = lax.all_to_all(contrib, "vis", split_axis=0, concat_axis=0, tiled=True)
    piece_sum = jax.ops.segment_sum(
        arrived.reshape(-1, 2, piece_rows), incoming_rows.reshape(-1), num_segments=stripe
    )
    adjoint_part = image_from_pieces(piece_sum, band_count, group_count)
    smooth = synthesis(coef_dual)
    new_image = jnp.maximum(sky_image - smooth - adjoint_part, 0.0)
    extrap = 2.0 * new_image - sky_image
    coeffs = analysis(extrap)
    abs_total = jnp.sum(jnp.abs(coeffs))
    coef_total = lax.psum(abs_total, ("band", "vis"))
    threshold = 0.5 * coef_total / (IMG * IMG)
    coef_dual = jnp.clip(coef_dual + coeffs, -threshold, threshold)
    piece_grid = pieces_from_image(extrap, band_count, group_count)
    tiles = lax.all_to_all(
        piece_grid[incoming_rows], "vis", split_axis=0, concat_axis=0, tiled=True
    )
    predicted = degrid(kernel_here, tiles)
    residual = live_slots * (vis_state + predicted - vis_data)
    resid_square = jnp.sum(residual * residual)
    norm_square, data_square = lax.psum((resid_square, data_part), ("band", "vis"))
    radius = 0.5 * jnp.sqrt(data_square + 1e-06)
    size_value = jnp.sqrt(norm_square + 1e-06)
    vis_state = residual * (1.0 - jnp.minimum(1.0, radius / size_value))
    return (new_image, coef_dual, vis_state[None, None])


high = lax.Precision.HIGH
everywhere = ("band", "vis")


def wave_tables(length, digit_low):
    digit_high = length // digit_low
    low = np.arange(digit_low)
    wide = np.arange(digit_high)
    full = 2.0 * np.pi
    small = full * (low[:, None] * low[None, :] % digit_low) / digit_low
    twist = full * (low[:, None] * wide[None, :]) / length
    large = full * (wide[:, None] * wide[None, :] % digit_high) / digit_high
    return small, twist, large


def complex_matrix(angle, sign):
    c = np.cos(angle)
    s = sign * np.sin(angle)
    return np.stack([np.stack([c, -s], axis=1), np.stack([s, c], axis=1)])


def f32(values):
    return jnp.asarray(np.asarray(values, np.float32))


def bf16(values):
    return f32(values).astype(jnp.bfloat16)


def analysis_matrix(half):
    matrix = np.zeros((2, half, 2 * half + 6))
    for k in range(half):
        for j in range(8):
            matrix[0, k, 2 * k + j] = low_taps[j]
            matrix[1, k, 2 * k + j] = high_taps[j]
    return matrix.reshape(2 * half, 2 * half + 6)


def synthesis_matrix(half):
    matrix = np.zeros((2 * half, 2, half + 3))
    for n in range(2 * half):
        for delay in range(4):
            tap = n % 2 + 2 * delay
            matrix[n, 0, n // 2 - delay + 3] = low_taps[tap]
            matrix[n, 1, n // 2 - delay + 3] = high_taps[tap]
    return matrix


def cos_sums(values, size):
    half = size // 2
    if half < 2:
        return [values[0] + values[1], values[0] - values[1]]
    quarter = half // 2
    plus = [values[a] + values[half - a] for a in range(quarter)] + [values[quarter]]
    minus = [values[a] - values[half - a] for a in range(quarter)]
    out = [None] * (half + 1)
    out[0::2] = cos_sums(plus, half)
    for k in range(1, half, 2):
        total = minus[0]
        for a in range(1, quarter):
            total = total + minus[a] * math.cos(2 * math.pi * (a * k % size) / size)
        out[k] = total
    return out


def sin_sums(values, size):
    half = size // 2
    if half < 2:
        return [None] * (half + 1)
    quarter = half // 2
    plus = {a: values[a] + values[half - a] for a in range(1, quarter)}
    plus[quarter] = values[quarter]
    minus = [None] + [values[a] - values[half - a] for a in range(1, quarter)]
    out = [None] * (half + 1)
    out[0::2] = sin_sums(minus, half)
    for k in range(1, half, 2):
        total = None
        for a in range(1, quarter + 1):
            factor = math.sin(2 * math.pi * (a * k % size) / size)
            term = plus[a] if a * 4 == size and k % 4 == 1 else plus[a] * factor
            total = term if total is None else total + term
        out[k] = total
    return out


def even_odd(values):
    size = len(values)
    half = size // 2
    even = [values[0]] + [values[a] + values[size - a] for a in range(1, half)] + [values[half]]
    odd = [None] + [values[a] - values[size - a] for a in range(1, half)]
    return even, odd


def split(values):
    upper = values.astype(jnp.bfloat16)
    return upper, (values - upper.astype(jnp.float32)).astype(jnp.bfloat16)


def table_pair(values):
    upper = f32(values).astype(jnp.bfloat16)
    return upper, (f32(values) - upper.astype(jnp.float32)).astype(jnp.bfloat16)


def nt_dot(a, b):
    return lax.dot_general(a, b, (((1,), (1,)), ((), ())), preferred_element_type=jnp.float32)


def nn_dot(a, b):
    return lax.dot_general(a, b, (((1,), (0,)), ((), ())), preferred_element_type=jnp.float32)


LEVELS = 32000.0
MESH = pl.DeviceIdType.MESH
LANES = 128
whole = pl.BlockSpec(memory_space=pltpu.VMEM)


def place():
    band = lax.axis_index("band")
    vis = lax.axis_index("vis")
    groups = lax.axis_size("vis")
    z = vis // 4
    y = vis // 2 % 2
    core = vis % 2
    return band, z, y, core, groups


def taps_dot(values, tables):
    upper, lower = split(values)
    return nn_dot(upper, tables[0]) + nn_dot(lower, tables[0]) + nn_dot(upper, tables[1])


def level(values):
    return jnp.round(values).astype(jnp.int32)


def step_kernel(
    low,
    kernels_hbm,
    coef_hbm,
    sky_hbm,
    up_hbm,
    edge_hbm,
    base_hbm,
    spin_hbm,
    inv_hbm,
    fwd_hbm,
    near_hbm,
    next_hbm,
    half_base_hbm,
    half_spin_hbm,
    order_hbm,
    state_ref,
    data_ref,
    rows_ref,
    counts_ref,
    phase_ref,
    shift_ref,
    tw_ref,
    image_hbm,
    coef_out_hbm,
    vis_out_ref,
    kernels_ref,
    joined_ref,
    sky_ref,
    merged_ref,
    up_ref,
    edge_ref,
    base_ref,
    spin_ref,
    inv_ref,
    fwd_ref,
    near_ref,
    next_ref,
    half_base_ref,
    half_spin_ref,
    order_ref,
    load_sem,
    tail_ref,
    halo_ref,
    block_ref,
    all_cols_ref,
    turn_ref,
    total_ref,
    tall_ref,
    smooth_ref,
    fold_ref,
    grid_ref,
    hot_ref,
    half_ref,
    spec_ref,
    rest_ref,
    extrap_ref,
    picked_ref,
    unit_ref,
    got_ref,
    units_ref,
    sum_table_ref,
    terms_ref,
    own_ref,
    sums_out_ref,
    sums_unit_ref,
    sums_got_ref,
    sums_units_ref,
    all_abs_ref,
    all_sums_ref,
    send_a,
    send_b,
    recv_a,
    recv_b,
    send_p,
    send_u,
    recv_p,
    recv_u,
    send_z,
    recv_z,
    send_w,
    recv_w,
    send_t,
    recv_t,
    send_s,
    recv_s,
    halo_sem,
):
    x, z, y, core, groups = place()
    levels = groups // 4
    devices = 2 * groups
    half_rows, half_width = coef_hbm.shape[1:]
    rows = 2 * half_rows
    tiles = block_ref.shape[1]
    kept = low // 2 + 1
    wide = LANES

    def index(px, pz, py, pc):
        return px * groups + pz * 4 + py * 2 + pc

    def device(px, pz, py, pc):
        return (px, pz * 4 + py * 2 + pc)

    def ident(number):
        return (number // groups, number % groups)

    def remote(src, dst, send, recv, target):
        return pltpu.make_async_remote_copy(
            src_ref=src,
            dst_ref=dst,
            send_sem=send,
            recv_sem=recv,
            device_id=target,
            device_id_type=MESH,
        )

    me = index(x, z, y, core)
    after, before = (me + 1) % devices, (me + devices - 1) % devices
    twin = device(x, z, y, 1 - core)
    line = [device(x, (z + k) % levels, y, core) for k in range(1, levels)]
    corners = [(1 - x, y), (x, 1 - y), (1 - x, 1 - y)]
    plane = [device(px, z, py, core) for px, py in corners]
    barrier = pltpu.get_barrier_semaphore()
    peers = line + plane + [twin, ident(after), ident(before)]
    for peer in peers:
        pl.semaphore_signal(barrier, inc=1, device_id=peer, device_id_type=MESH)

    sources = [
        (kernels_hbm, kernels_ref),
        (coef_hbm, joined_ref.at[:, pl.ds(8, half_rows), :]),
        (up_hbm, up_ref),
        (edge_hbm, edge_ref),
        (base_hbm, base_ref),
        (spin_hbm, spin_ref),
        (inv_hbm, inv_ref),
        (sky_hbm, sky_ref),
        (fwd_hbm, fwd_ref),
        (near_hbm, near_ref),
        (next_hbm, next_ref),
        (half_base_hbm, half_base_ref),
        (half_spin_hbm, half_spin_ref),
        (order_hbm, order_ref),
    ]
    loads = [
        pltpu.make_async_copy(src, dst, load_sem.at[i]) for i, (src, dst) in enumerate(sources)
    ]
    for load in loads:
        load.start()
    loads[0].wait()
    count = 16
    span = kernels_ref.shape[0] * count // tiles
    width = low * wide
    stripe = width // 2
    slots = rows_ref.shape[0]
    lane = lax.broadcasted_iota(jnp.int32, (tiles, groups), 1)
    tile_id = lax.broadcasted_iota(jnp.int32, (tiles, groups), 0)
    counts = jnp.where(lane == tile_id // slots, counts_ref[...].astype(jnp.float32), 0.0)
    counts = jnp.sum(counts, axis=1, keepdims=True)
    tile_id = lax.broadcasted_iota(jnp.int32, (tiles, 1), 0)
    live = jnp.where((tile_id % slots).astype(jnp.float32) < counts, 1.0, 0.0)
    state = [state_ref[:, part, :] for part in range(2)]
    data = [data_ref[:, part, :] for part in range(2)]
    ours = [part * live for part in state]
    turned = [ours[0], ours[1], ours[0], ours[1]], [ours[1], -ours[0], ours[1], -ours[0]]
    turned = [jnp.concatenate(parts, axis=1) for parts in turned]
    pair_lane = lax.broadcasted_iota(jnp.int32, (count, LANES), 1) // (LANES // 2)
    pair_row = lax.broadcasted_iota(jnp.int32, (count, LANES), 0)
    masks = [pair_lane + 2 * k == pair_row for k in range(count // 2)]
    for i in range(tiles // count):
        spread = [
            jnp.concatenate(
                [jnp.where(mask, part[i * count : (i + 1) * count], 0.0) for mask in masks], axis=1
            )
            for part in turned
        ]
        spread = jnp.concatenate(spread, axis=0).astype(jnp.bfloat16)
        both = nn_dot(spread, kernels_ref[i * span : (i + 1) * span, :])
        both = jnp.concatenate([both[:count], both[count:]], axis=1)
        block_ref[me, i * count : (i + 1) * count, :] = both.astype(jnp.bfloat16)
    lane = lax.broadcasted_iota(jnp.int32, (groups, LANES), 1) % tiles
    owner = lax.broadcasted_iota(jnp.int32, (groups, LANES), 0)
    columns = 0.0
    by_owner = rows_ref[...].astype(jnp.float32).T
    for slot in range(slots):
        here = by_owner[:, slot : slot + 1]
        columns = columns + jnp.where(lane == owner * slots + slot, here, 0.0)
    columns = jnp.sum(columns, axis=0, keepdims=True).astype(jnp.int32)
    all_cols_ref[me] = columns + x * stripe
    loads[1].wait()
    for c in range(4):
        tail_ref[3 * c : 3 * c + 3, :] = joined_ref[c, half_rows + 5 :, :]
    pl.semaphore_wait(barrier, len(peers))

    started = []

    def start(block, target, slot):
        own_a, own_b = block_ref.at[block], all_cols_ref.at[block]
        for own, send, recv in ((own_a, send_a, recv_a), (own_b, send_b, recv_b)):
            copy = remote(own, own, send.at[slot], recv.at[block], target)
            copy.start()
            started.append(copy)

    def got(block):
        for ref, send, recv in ((block_ref, send_a, recv_a), (all_cols_ref, send_b, recv_b)):
            own = ref.at[block]
            remote(own, own, send.at[0], recv.at[block], twin).wait_recv()

    slots_of = iter(range(send_a.shape[0]))
    far = sorted(range(1, levels), key=lambda k: abs(k - levels / 2))
    for k in far:
        start(me, line[k - 1], next(slots_of))
    for target in plane:
        start(me, target, next(slots_of))
    edge = remote(tail_ref, halo_ref, halo_sem.at[0], halo_sem.at[1], ident(after))
    edge.start()
    start(me, twin, next(slots_of))
    line_blocks = [index(x, (z + levels - k) % levels, y, core) for k in far]
    for block in line_blocks:
        got(block)
        for target in plane:
            start(block, target, next(slots_of))
        start(block, twin, next(slots_of))
    edge.wait()
    for c in range(4):
        joined_ref[c, 5:8, :] = halo_ref[3 * c : 3 * c + 3, :]
    strips = half_width // LANES

    def tall(i, carry):
        here = pl.ds(pl.multiple_of(i * LANES, LANES), LANES)
        for c in range(2):
            for k in range(half_rows // 8):
                lows = [joined_ref[c, 8 + 8 * k - d : 16 + 8 * k - d, here] for d in range(4)]
                highs = [joined_ref[c + 2, 8 + 8 * k - d : 16 + 8 * k - d, here] for d in range(4)]
                for parity in range(2):
                    total = 0.0
                    for d in range(4):
                        total = total + low_taps[parity + 2 * d] * lows[d]
                        total = total + high_taps[parity + 2 * d] * highs[d]
                    tall_ref[c * strips + i, pl.ds(16 * k + parity, 8, stride=2), :] = total
        return carry

    lax.fori_loop(0, strips, tall, 0)

    for px, py in corners:
        block = index(px, z, py, core)
        got(block)
        start(block, twin, next(slots_of))
    for load in loads[2:8]:
        load.wait()

    def broad(i, carry):
        there = (i + strips - 1) % strips
        near = jnp.concatenate([tall_ref[i], tall_ref[strips + i]], axis=1)
        last = jnp.concatenate([tall_ref[there], tall_ref[strips + there]], axis=1)
        out = taps_dot(near, up_ref)
        first = taps_dot(last, edge_ref)
        smooth_ref[2 * i] = out[:, :LANES] + first
        smooth_ref[2 * i + 1] = out[:, LANES:]
        return carry

    lax.fori_loop(0, strips // 2, broad, 0)
    spin_cos, spin_sin = spin_ref[0, pl.ds(me, 1), :], spin_ref[1, pl.ds(me, 1), :]
    cosine = (base_ref[0] * spin_cos - base_ref[1] * spin_sin).astype(jnp.bfloat16)
    sine = (base_ref[1] * spin_cos + base_ref[0] * spin_sin).astype(jnp.bfloat16)
    piece = kernels_ref.shape[1]
    turn_ref[:rows, :piece] = cosine
    turn_ref[:rows, piece:] = -sine
    turn_ref[rows:, :piece] = sine
    turn_ref[rows:, piece:] = cosine
    for load in loads[11:13]:
        load.wait()
    for n in range(4):
        spin_cos, spin_sin = half_spin_ref[0, n : n + 1, :], half_spin_ref[1, n : n + 1, :]
        cosine = half_base_ref[0] * spin_cos - half_base_ref[1] * spin_sin
        sine = half_base_ref[1] * spin_cos + half_base_ref[0] * spin_sin
        for p in range(2):
            part = slice(p * LANES, (p + 1) * LANES)
            c, d = split(cosine[:, part]), split(sine[:, part])
            real_rows = slice(2 * n * rows, (2 * n + 1) * rows)
            imag_rows = slice((2 * n + 1) * rows, (2 * n + 2) * rows)
            for e in range(2):
                sum_table_ref[e, p, real_rows, :LANES] = c[e]
                sum_table_ref[e, p, real_rows, LANES:] = -d[e]
                sum_table_ref[e, p, imag_rows, :LANES] = d[e]
                sum_table_ref[e, p, imag_rows, LANES:] = c[e]
    for n, k in enumerate(far):
        for px, py in corners:
            block = index(px, (z + levels - k) % levels, py, core)
            got(block)
            start(block, twin, next(slots_of))
        if n == 0:
            lax.fori_loop(strips // 2, strips, broad, 0)

    total_tiles = devices * tiles
    class_tiles = groups * tiles
    parts = class_tiles // LANES
    lane = lax.broadcasted_iota(jnp.int32, (1, LANES), 1)

    def block_of(u):
        return u // 2 % 2 * groups + u // 4 * 4 + u % 2 * 2

    def spread_class(c):
        for i in range(parts):
            first = block_of(2 * i) + c
            columns = jnp.where(lane < tiles, all_cols_ref[first], all_cols_ref[first + 2])
            k1 = columns % low
            k2 = columns // low
            flip = k1 >= kept
            k1 = jnp.where(flip, low - k1, k1)
            k2 = jnp.where(flip, wide - 1 - k2, k2)
            fold_ref[0, pl.ds(c * parts + i, 1), :] = (k1 * wide + k2).astype(jnp.float32)
            fold_ref[1, pl.ds(c * parts + i, 1), :] = jnp.where(flip, -1.0, 1.0)
        chunk = 4 * LANES
        for j in range(class_tiles // chunk):
            n = chunk // tiles
            some = [block_ref[block_of(j * n + i) + c] for i in range(n)]
            both = nt_dot(turn_ref[...], jnp.concatenate(some, axis=0))
            for i in range(chunk // LANES):
                b = c * parts + j * (chunk // LANES) + i
                at = pl.ds(pl.multiple_of(b * LANES, LANES), LANES)
                real = both[:rows, i * LANES : (i + 1) * LANES]
                imag = both[rows:, i * LANES : (i + 1) * LANES]
                sign = fold_ref[1, pl.ds(b, 1), :]
                out_real = real * phase_ref[0] - imag * phase_ref[1]
                out_imag = (real * phase_ref[1] + imag * phase_ref[0]) * sign
                grid_ref[:rows, at] = out_real.astype(jnp.bfloat16)
                grid_ref[rows:, at] = out_imag.astype(jnp.bfloat16)

    def folded_class(c, p):
        base = pl.multiple_of(p * 2 * wide, 2 * wide)
        row = (lax.broadcasted_iota(jnp.int32, (2 * wide, LANES), 0) + base).astype(jnp.float32)
        hots = []
        for i in range(parts):
            hit = row == fold_ref[0, pl.ds(c * parts + i, 1), :]
            hots.append(jnp.where(hit, 1.0, 0.0).astype(jnp.bfloat16))
        hot = jnp.concatenate(hots, axis=1)
        at = pl.ds(pl.multiple_of(c * class_tiles, class_tiles), class_tiles)
        hot_ref[pl.ds(base, 2 * wide), at] = hot
        return nt_dot(grid_ref[:, at], hot)

    spread_class(core)

    def scatter_own(p, carry):
        total_ref[p] = folded_class(core, p)
        return carry

    lax.fori_loop(0, (kept + 1) // 2, scatter_own, 0)
    for i in range(groups):
        got(2 * i + 1 - core)
    spread_class(1 - core)

    def scatter(p, carry):
        folded = (total_ref[p] + folded_class(1 - core, p)).astype(jnp.bfloat16)
        for e in range(2):
            here = slice(e * wide, (e + 1) * wide)
            pair = jnp.concatenate([folded[:rows, here], folded[rows:, here]], axis=1)
            mid = nn_dot(pair, inv_ref[...])
            k1 = p * 2 + e
            tw_real, tw_imag = tw_ref[0, pl.ds(k1, 1), :], tw_ref[1, pl.ds(k1, 1), :]
            real, imag = mid[:, :wide], mid[:, wide:]
            half_ref[k1, :, :wide] = real * tw_real - imag * tw_imag
            half_ref[k1, :, wide:] = real * tw_imag + imag * tw_real
        return carry

    lax.fori_loop(0, (kept + 1) // 2, scatter, 0)

    def strip(i, carry):
        at = pl.ds(pl.multiple_of(i * 8, 8), 8)
        cos_part = cos_sums([half_ref[k, at, :wide] for k in range(kept)], low)
        sin_part = sin_sums([None] + [half_ref[k, at, wide:] for k in range(1, kept - 1)], low)
        extraps = []
        for a in range(low):
            k = min(a, low - a)
            if a == 0 or a == low // 2:
                adjoint = cos_part[k]
            elif a < low // 2:
                adjoint = cos_part[k] - sin_part[k]
            else:
                adjoint = cos_part[k] + sin_part[k]
            here = slice(a * wide, (a + 1) * wide)
            sky = sky_ref[at, here]
            image = jnp.maximum(sky - smooth_ref[a, at, :] - adjoint, 0.0)
            extrap = 2.0 * image - sky
            sky_ref[at, here] = image
            extrap_ref[a, at, :] = extrap
            extraps.append(extrap)
        even, odd = even_odd(extraps)
        real_part = cos_sums(even, low)
        imag_part = sin_sums(odd, low)
        for k in range(kept):
            tw_real, tw_imag = tw_ref[0, k : k + 1, :], tw_ref[1, k : k + 1, :]
            real = real_part[k] * tw_real
            imag = -real_part[k] * tw_imag
            if 0 < k < kept - 1:
                real = real - imag_part[k] * tw_imag
                imag = imag - imag_part[k] * tw_real
            half_ref[k, at, :wide] = real
            half_ref[k, at, wide:] = imag
        return carry

    lax.fori_loop(0, rows // 8, strip, 0)
    store = pltpu.make_async_copy(sky_ref, image_hbm, load_sem.at[len(loads)])
    store.start()
    top = remote(
        extrap_ref.at[:, pl.ds(0, 8), :],
        extrap_ref.at[:, pl.ds(rows, 8), :],
        halo_sem.at[2],
        halo_sem.at[3],
        ident(before),
    )
    top.start()
    loads[8].wait()

    def spectrum(k, carry):
        out = taps_dot(half_ref[k], fwd_ref)
        here = pl.ds(pl.multiple_of(k * wide, wide), wide)
        upper, lower = split(out)
        spec_ref[:rows, here] = upper[:, :wide]
        spec_ref[rows:, here] = upper[:, wide:]
        rest_ref[:rows, here] = lower[:, :wide]
        rest_ref[rows:, here] = lower[:, wide:]
        return carry

    lax.fori_loop(0, kept, spectrum, 0)

    mate = x * 4 + y * 2 + core

    def sends(to_z, to_x, to_y, to_class):
        at = to_class * class_tiles + (to_z * 4 + to_x * 2 + to_y) * tiles
        at = pl.ds(pl.multiple_of(at, tiles), tiles)
        unit = unit_ref.at[to_class * parts + to_z * 2 + to_x]
        spot, half, target = to_z * 8 + mate, to_z // 2, device(to_x, z, to_y, to_class)
        return [
            remote(picked_ref.at[at, :], got_ref.at[spot], send_p.at[0], recv_p.at[half], target),
            remote(unit, units_ref.at[spot], send_u.at[0], recv_u.at[half], target),
        ]

    def total_of(ref, send, recv, count=devices - 1, at=0):
        some = ref.at[pl.ds(0, count)]
        return remote(some, some, send.at[0], recv.at[at], twin)

    def share_row(ref, send, recv):
        def one(k, carry):
            to = (me + k) % devices
            remote(ref.at[me], ref.at[me], send.at[0], recv.at[0], ident(to)).start()
            return carry

        lax.fori_loop(1, devices, one, 0)

    def row_total(ref):
        total = ref[0]
        for d in range(1, devices):
            total = total + ref[d]
        return total

    def ordered(n):
        return (z // 2 + 1 + n // 2) % 2 * 2 + (z + 1 + n) % 2

    def pick(s, carry):
        to_z = ordered(s // 2)
        to_class = (core + 1 + s) % 2
        j = to_class * 4 + to_z
        at = pl.multiple_of(j * 2 * LANES, 2 * LANES)
        hot = hot_ref[: kept * wide, pl.ds(at, 2 * LANES)]
        both = nn_dot(spec_ref[...], hot) + nn_dot(rest_ref[...], hot)
        for h in range(2):
            sign = fold_ref[1, pl.ds(2 * j + h, 1), :]
            real = both[:rows, h * LANES : (h + 1) * LANES]
            imag = both[rows:, h * LANES : (h + 1) * LANES] * sign
            most = jnp.max(jnp.maximum(jnp.abs(real), jnp.abs(imag)), axis=0, keepdims=True)
            most = jnp.maximum(most, 1e-30)
            unit_ref[2 * j + h] = most * (1.0 / LEVELS)
            to_level = LEVELS / most
            packed = level(real * to_level) * 65536 + level(imag * to_level)
            to = pl.ds(pl.multiple_of(at + h * LANES, LANES), LANES)
            picked_ref[to, :] = packed.T
        for to_x in range(2):
            for to_y in range(2):
                away = (to_x - x) * (to_x - x) + (to_y - y) * (to_y - y)

                @pl.when(away + (to_class - core) * (to_class - core) != 0)
                def _():
                    for copy in sends(to_z, to_x, to_y, to_class):
                        copy.start()

        return carry

    lax.fori_loop(0, devices // 4, pick, 0)
    for to_z in range(levels):
        at = core * class_tiles + (to_z * 4 + x * 2 + y) * tiles
        got_ref[to_z * 8 + mate] = picked_ref[pl.ds(pl.multiple_of(at, tiles), tiles), :]
        units_ref[to_z * 8 + mate] = unit_ref[core * parts + to_z * 2 + x]
    top.wait()
    loads[9].wait()
    loads[10].wait()

    def rows_down(i, carry):
        for k in range(half_rows // 8):
            lows, highs = 0.0, 0.0
            for tap in range(8):
                taken = extrap_ref[i, pl.ds(16 * k + tap, 8, stride=2), :]
                lows = lows + low_taps[tap] * taken
                highs = highs + high_taps[tap] * taken
            tall_ref[i, 8 * k : 8 * k + 8, :] = lows
            tall_ref[i, half_rows + 8 * k : half_rows + 8 * k + 8, :] = highs
        return carry

    lax.fori_loop(0, low, rows_down, 0)

    def cols_down(b, absolute):
        here = jnp.concatenate([tall_ref[2 * b], tall_ref[2 * b + 1]], axis=1)
        out = taps_dot(here, near_ref) + taps_dot(tall_ref[(2 * b + 2) % low], next_ref)
        at = pl.ds(pl.multiple_of(b * LANES, LANES), LANES)
        for c in range(4):
            top_row, left = c // 2 * half_rows, c % 2 * LANES
            part = out[top_row : top_row + half_rows, left : left + LANES]
            absolute = absolute + jnp.abs(part)
            merged_ref[c, :, at] = joined_ref[c, 8:, at] + part
        return absolute

    def plane_sums(n, absolute):
        half = (z // 2 + 1 + n) % 2
        total_of(got_ref, send_p, recv_p, 14, half).wait_recv()
        total_of(units_ref, send_u, recv_u, 14, half).wait_recv()
        rows_of = [units_ref[half * 16 + i] for i in range(16)]
        units = jnp.concatenate(rows_of * (LANES // 16), axis=0).T
        units = jnp.where(y == 0, units[:tiles], units[tiles:])
        cosine, sine = shift_ref[0], shift_ref[1]
        level_cos = half_spin_ref[0, pl.ds(4 * z, 1), :]
        level_sin = half_spin_ref[1, pl.ds(4 * z, 1), :]
        for e in range(2):
            strip_rows = slice(e * tiles, (e + 1) * tiles)
            for pair in range(4):
                reals, imags = [], []
                for side in range(2):
                    m = side * 4 + pair
                    packed = got_ref[half * 16 + e * 8 + m]
                    real = (packed + 32768) >> 16
                    imag = packed - (real << 16)
                    unit = units[:, e * 8 + m : e * 8 + m + 1]
                    real = real.astype(jnp.float32) * unit
                    imag = imag.astype(jnp.float32) * unit
                    reals.append(real * cosine + imag * sine)
                    imags.append(imag * cosine - real * sine)
                at = 2 * pair * LANES
                for p, values in ((0, (reals[0] + reals[1], imags[0] + imags[1])),
                                  (1, (reals[0] - reals[1], imags[0] - imags[1]))):
                    for part in range(2):
                        upper, lower = split(values[part])
                        here = slice(at + part * LANES, at + (part + 1) * LANES)
                        terms_ref[0, p, strip_rows, here] = upper
                        terms_ref[1, p, strip_rows, here] = lower
        reals, imags = [], []
        for p in range(2):
            out = nn_dot(terms_ref[0, p], sum_table_ref[0, p])
            out = out + nn_dot(terms_ref[1, p], sum_table_ref[0, p])
            out = out + nn_dot(terms_ref[0, p], sum_table_ref[1, p])
            part = slice(p * LANES, (p + 1) * LANES)
            turn_cos, turn_sin = level_cos[:, part], level_sin[:, part]
            real, imag = out[:, :LANES], out[:, LANES:]
            reals.append(real * turn_cos + imag * turn_sin)
            imags.append(imag * turn_cos - real * turn_sin)
        real = jnp.concatenate(reals, axis=1)
        imag = jnp.concatenate(imags, axis=1)
        most = jnp.max(jnp.maximum(jnp.abs(real), jnp.abs(imag)), axis=1, keepdims=True)
        most = jnp.maximum(most, 1e-30)
        to_level = LEVELS / most
        packed = level(real * to_level) * 65536 + level(imag * to_level)
        sums_unit_ref[half] = jnp.broadcast_to(most * (1.0 / LEVELS), (LANES, LANES)).T[:1]
        for e in range(2):
            strip_rows = slice(e * tiles, (e + 1) * tiles)
            to_z = half * 2 + e
            sums_out_ref[to_z] = packed[strip_rows]

            @pl.when(to_z == z)
            def _():
                own_ref[:, : 2 * LANES] = real[strip_rows]
                own_ref[:, 2 * LANES :] = imag[strip_rows]

            @pl.when(to_z != z)
            def _():
                target = device(x, to_z, y, core)
                remote(
                    sums_out_ref.at[to_z], sums_got_ref.at[z], send_z.at[0], recv_z.at[0], target
                ).start()
                remote(
                    sums_unit_ref.at[half],
                    sums_units_ref.at[z],
                    send_w.at[0],
                    recv_w.at[0],
                    target,
                ).start()

        return lax.fori_loop(n * (low // 4), (n + 1) * (low // 4), cols_down, absolute)

    absolute = lax.fori_loop(0, 2, plane_sums, jnp.zeros((half_rows, LANES), jnp.float32))
    abs_total = jnp.sum(jnp.sum(absolute, axis=0, keepdims=True), axis=1, keepdims=True)
    loads[13].wait()

    lane = lax.broadcasted_iota(jnp.int32, (1, LANES), 1)
    all_abs_ref[me] = jnp.where(lane == 0, abs_total, 0.0)
    share_row(all_abs_ref, send_t, recv_t)
    total_of(sums_got_ref, send_z, recv_z, levels - 1).wait_recv()
    total_of(sums_units_ref, send_w, recv_w, levels - 1).wait_recv()
    units = [sums_units_ref[(z + k) % levels] for k in range(1, levels)]
    units = jnp.concatenate(units + [units[0]] * (LANES - levels + 1), axis=0).T
    units = jnp.where(z % 2 == 0, units[:tiles], units[tiles:])
    real, imag = own_ref[:, : 2 * LANES], own_ref[:, 2 * LANES :]
    for k in range(1, levels):
        packed = sums_got_ref[(z + k) % levels]
        upper = (packed + 32768) >> 16
        lower = packed - (upper << 16)
        unit = units[:, k - 1 : k]
        real = real + upper.astype(jnp.float32) * unit
        imag = imag + lower.astype(jnp.float32) * unit
    tile = jnp.concatenate([real, imag], axis=1).astype(jnp.bfloat16)
    tile = nn_dot(tile, order_ref[...]).astype(jnp.bfloat16)
    first, second = [], []
    near_row = pair_row % 2 == 0
    for i in range(tiles // count):
        here = tile[i * count : (i + 1) * count]
        pair = jnp.concatenate([here[:, :piece], here[:, piece:]], axis=0)
        out = nt_dot(pair, kernels_ref[i * span : (i + 1) * span, :])
        for found, half in ((first, out[:count]), (second, out[count:])):
            total = 0.0
            for k in range(count // 2):
                total = total + jnp.where(
                    pair_row // 2 == k, half[:, k * LANES : (k + 1) * LANES], 0.0
                )
            found.append(jnp.where(near_row, total, pltpu.roll(total, LANES // 2, 1)))
    first = jnp.concatenate(first, axis=0)
    second = jnp.concatenate(second, axis=0)
    visits = state_ref.shape[2]
    lane = lax.broadcasted_iota(jnp.int32, first.shape, 1)
    crossed = jnp.where(
        lane // visits % 2 == 0,
        -pltpu.roll(second, LANES - visits, 1),
        pltpu.roll(second, visits, 1),
    )
    keep = jnp.where(lane < 2 * visits, live, 0.0)
    state_wide = jnp.concatenate(state + state, axis=1)
    data_wide = jnp.concatenate(data + data, axis=1)
    residual = keep * (state_wide + first + crossed - data_wide)
    norms = []
    for values in (residual, data_wide * keep):
        norms.append(jnp.sum(jnp.sum(values * values, axis=0, keepdims=True), axis=1, keepdims=True))
    lane = lax.broadcasted_iota(jnp.int32, (1, LANES), 1)
    all_sums_ref[me] = jnp.where(lane == 0, norms[0], norms[1])
    share_row(all_sums_ref, send_s, recv_s)
    total_of(all_abs_ref, send_t, recv_t).wait_recv()
    threshold = 0.5 * row_total(all_abs_ref)[:, 0:1] / (width * width)

    def clip(i, carry):
        at = pl.ds(pl.multiple_of(i * LANES, LANES), LANES)
        for c in range(4):
            merged_ref[c, :, at] = jnp.clip(merged_ref[c, :, at], -threshold, threshold)
        return carry

    lax.fori_loop(0, half_width // LANES, clip, 0)
    store_coef = pltpu.make_async_copy(merged_ref, coef_out_hbm, load_sem.at[len(loads) + 1])
    store_coef.start()
    for copy in started:
        copy.wait_send()
    total_of(got_ref, send_p, recv_p, 28).wait_send()
    total_of(units_ref, send_u, recv_u, 28).wait_send()
    total_of(sums_got_ref, send_z, recv_z, levels - 1).wait_send()
    total_of(sums_units_ref, send_w, recv_w, levels - 1).wait_send()
    total_of(all_abs_ref, send_t, recv_t).wait_send()
    total_of(all_sums_ref, send_s, recv_s).wait()
    total = row_total(all_sums_ref)
    size = jnp.sqrt(total[:, 0:1] + 1e-06)
    radius = 0.5 * jnp.sqrt(total[:, 1:2] + 1e-06)
    residual = residual * (1.0 - jnp.minimum(1.0, radius / size))
    vis_out_ref[:, 0, :] = residual[:, :visits]
    vis_out_ref[:, 1, :] = residual[:, visits : 2 * visits]
    store.wait()
    store_coef.wait()


def step(kernels, coef, sky, state, data, tile_rows, tile_counts, groups, devices):
    rows, width = sky.shape
    piece = kernels.shape[1]
    slots = tile_rows.shape[0]
    tiles = groups * slots
    half_rows, half_width = coef.shape[1:]
    low = width // LANES
    kept = low // 2 + 1
    wide = np.arange(LANES)
    matrix = synthesis_matrix(LANES)
    up = matrix[:, :, 3:].transpose(1, 2, 0).reshape(2 * LANES, 2 * LANES)
    edge = np.zeros((2, LANES, LANES))
    edge[:, LANES - 3 :, :] = matrix[:LANES, :, :3].transpose(1, 2, 0)
    matrix = analysis_matrix(LANES).T
    following = np.zeros((LANES, 2 * LANES))
    following[:6] = matrix[2 * LANES :]
    turn = np.arange(piece)
    base = 2 * np.pi * np.arange(rows)[:, None] * turn[None, :] / width
    spin = 2 * np.pi * (np.arange(devices)[:, None] * turn[None, :] % devices) / devices
    owner = wide // slots % groups
    shift = 2 * np.pi * (np.arange(rows)[:, None] * owner[None, :] % groups) / groups
    phase = np.stack([np.cos(shift), np.sin(shift)])
    full = 2 * np.pi * (wide[:, None] * wide[None, :] % LANES) / LANES
    c, s = np.cos(full) / width, np.sin(full) / width
    inverse = np.block([[c, s], [-s, c]])
    forward = np.block([[c, -s], [s, c]])
    twist = 2 * np.pi * np.arange(kept + 1)[:, None] * wide[None, :] / width
    halves = np.concatenate([turn[0::2], turn[1::2]])
    half_base = 2 * np.pi * np.arange(rows)[:, None] * halves[None, :] / width
    half_spin = 2 * np.pi * (np.arange(devices)[:, None] * halves[None, :] % devices) / devices
    order = np.zeros((2 * piece, 2 * piece))
    for part in range(2):
        order[part * piece + np.arange(piece), part * piece + halves] = 1.0
    loaded = [
        kernels,
        coef,
        sky,
        jnp.stack(table_pair(up)),
        jnp.stack(table_pair(edge.reshape(2 * LANES, LANES))),
        f32(np.stack([np.cos(base), np.sin(base)])),
        f32(np.stack([np.cos(spin), np.sin(spin)])),
        bf16(inverse),
        jnp.stack(table_pair(forward)),
        jnp.stack(table_pair(matrix[: 2 * LANES])),
        jnp.stack(table_pair(following)),
        f32(np.stack([np.cos(half_base), np.sin(half_base)])),
        f32(np.stack([np.cos(half_spin), np.sin(half_spin)])),
        bf16(order),
    ]
    held = [
        state,
        data,
        tile_rows,
        tile_counts,
        f32(phase),
        f32(phase[:, :, :tiles].transpose(0, 2, 1)),
        f32(np.stack([np.cos(twist), np.sin(twist)])),
    ]
    buffers = [pltpu.VMEM(value.shape, value.dtype) for value in loaded]
    buffers[1] = pltpu.VMEM((4, half_rows + 8, half_width), jnp.float32)
    copies = 3 * 4 + 7 + 12
    dma = pltpu.SemaphoreType.DMA
    anywhere = pl.BlockSpec(memory_space=pltpu.HBM)
    return pl.pallas_call(
        lambda *refs: step_kernel(low, *refs),
        out_shape=(
            jax.ShapeDtypeStruct((rows, width), jnp.float32),
            jax.ShapeDtypeStruct(coef.shape, jnp.float32),
            jax.ShapeDtypeStruct(state.shape, jnp.float32),
        ),
        in_specs=[anywhere] * len(loaded) + [whole] * len(held),
        out_specs=(anywhere, anywhere, whole),
        scratch_shapes=buffers[:3]
        + [pltpu.VMEM(coef.shape, jnp.float32)]
        + buffers[3:]
        + [
            dma((len(loaded) + 2,)),
            pltpu.VMEM((16, half_width), jnp.float32),
            pltpu.VMEM((16, half_width), jnp.float32),
            pltpu.VMEM((devices, tiles, 2 * piece), jnp.bfloat16),
            pltpu.VMEM((devices, 1, LANES), jnp.int32),
            pltpu.VMEM((2 * rows, 2 * piece), jnp.bfloat16),
            pltpu.VMEM(((kept + 1) // 2, 2 * rows, 2 * LANES), jnp.float32),
            pltpu.VMEM((low, rows, LANES), jnp.float32),
            pltpu.VMEM((low, rows, LANES), jnp.float32),
            pltpu.VMEM((2, devices // 2, LANES), jnp.float32),
            pltpu.VMEM((2 * rows, devices * tiles), jnp.bfloat16),
            pltpu.VMEM(((kept + 1) * LANES, devices * tiles), jnp.bfloat16),
            pltpu.VMEM((kept + 1, rows, 2 * LANES), jnp.float32),
            pltpu.VMEM((2 * rows, kept * LANES), jnp.bfloat16),
            pltpu.VMEM((2 * rows, kept * LANES), jnp.bfloat16),
            pltpu.VMEM((low, rows + 8, LANES), jnp.float32),
            pltpu.VMEM((devices * tiles, rows), jnp.int32),
            pltpu.VMEM((devices // 2, 1, LANES), jnp.float32),
            pltpu.VMEM((devices, tiles, rows), jnp.int32),
            pltpu.VMEM((devices, 1, LANES), jnp.float32),
            pltpu.VMEM((2, 2, 8 * rows, 2 * LANES), jnp.bfloat16),
            pltpu.VMEM((2, 2, 2 * tiles, 8 * rows), jnp.bfloat16),
            pltpu.VMEM((tiles, 2 * piece), jnp.float32),
            pltpu.VMEM((groups // 4, tiles, piece), jnp.int32),
            pltpu.VMEM((2, 1, LANES), jnp.float32),
            pltpu.VMEM((groups // 4, tiles, piece), jnp.int32),
            pltpu.VMEM((groups // 4, 1, LANES), jnp.float32),
            pltpu.VMEM((devices, 1, LANES), jnp.float32),
            pltpu.VMEM((devices, 1, LANES), jnp.float32),
            dma((copies,)),
            dma((copies,)),
        ]
        + [dma((devices,))] * 2
        + [dma((2,))] * 4
        + [dma((1,))] * 8
        + [dma((4,))],
        compiler_params=pltpu.CompilerParams(
            collective_id=0, has_side_effects=True, vmem_limit_bytes=60 * 2**20
        ),
        name="step",
    )(*loaded, *held)


def fast_local(sky_image, coef_dual, vis_dual, visibilities, kernel_blocks, tile_rows, tile_counts):
    groups = lax.axis_size("vis")
    devices = lax.axis_size("band") * groups
    taken = kernel_blocks.shape
    new_image, coef_dual, vis_state = step(
        kernel_blocks.reshape(-1, taken[-1]),
        coef_dual,
        sky_image,
        vis_dual.reshape((-1,) + vis_dual.shape[4:]),
        visibilities.reshape((-1,) + vis_dual.shape[4:]),
        tile_rows[0, 0].T,
        tile_counts[0],
        groups,
        devices,
    )
    return (new_image, coef_dual, vis_state.reshape(vis_dual.shape))


def body_for(mesh):
    devices = mesh.shape["band"] * mesh.shape["vis"]
    relayed = mesh.shape["band"] == 2 and mesh.shape["vis"] % 4 == 0 and devices == 32

    def body(sky_image, *rest):
        rows, width = sky_image.shape
        piece = width // mesh.shape["vis"]
        tiles = rest[4].shape[2] * rest[4].shape[3]
        if relayed and rows == LANES and piece == 2 * LANES and 2 * tiles == LANES:
            return fast_local(sky_image, *rest)
        return local(sky_image, *rest)

    return body


def solution(mesh):
    return jax.shard_map(
        body_for(mesh),
        mesh=mesh,
        in_specs=(
            P(("band", "vis"), None),
            P(None, ("band", "vis"), None),
            P("band", "vis", None, None, None, None),
            P("band", "vis", None, None, None, None),
            P("band", "vis", None, None, None, None, None),
            P("band", "vis", None, None),
            P("band", "vis", None),
        ),
        out_specs=(
            P(("band", "vis"), None),
            P(None, ("band", "vis"), None),
            P("band", "vis", None, None, None, None),
        ),
        check_vma=False,
    )
```

```python
import math

import jax
import numpy as np
import jax.numpy as jnp
from jax import lax
from jax.experimental import pallas as pl
from jax.experimental.pallas import tpu as pltpu
from jax.sharding import PartitionSpec as P

IMG = 4096


low_taps = (
    -0.010597401784997278,
    0.032883011666982945,
    0.030841381835986965,
    -0.18703481171888114,
    -0.02798376941698385,
    0.6308807679295904,
    0.7148465705525415,
    0.23037781330885523,
)
high_taps = tuple(((-1.0) ** offset * low_taps[7 - offset] for offset in range(8)))
highest = lax.Precision.HIGHEST


def shifted(block, axis, distance):
    devices = range(lax.axis_size(axis))
    route = [((i - distance) % len(devices), i) for i in devices]
    return lax.ppermute(block, axis, route)


def dft_table(table_size, sign):
    positions = jnp.arange(table_size, dtype=jnp.int32)
    phase = positions[:, None] * positions[None, :] % table_size
    angle = 2.0 * math.pi / table_size * phase.astype(jnp.float32)
    return (jnp.cos(angle), sign * jnp.sin(angle))


def section_one(table, values):
    return jnp.einsum("kn,...nm->...km", table, values, precision=highest)


def section_two(table, values):
    return jnp.einsum("qm,...km->...qk", table, values, precision=highest)


def dft_last(real_in, imag_in, sign):
    leading = real_in.shape[:-1]
    length = real_in.shape[-1]
    inner_len = 64
    outer_len = length // inner_len
    split_real = real_in.reshape(leading + (outer_len, inner_len))
    table_real, table_imag = dft_table(outer_len, sign)
    first_real = section_one(table_real, split_real)
    first_imag = section_one(table_imag, split_real)
    if imag_in is not None:
        split_imag = imag_in.reshape(leading + (outer_len, inner_len))
        first_real = first_real - section_one(table_imag, split_imag)
        first_imag = first_imag + section_one(table_real, split_imag)
    outer_index = jnp.arange(outer_len, dtype=jnp.int32)
    inner_index = jnp.arange(inner_len, dtype=jnp.int32)
    twist_phase = outer_index[:, None] * inner_index[None, :] % length
    twist_angle = 2.0 * math.pi / length * twist_phase.astype(jnp.float32)
    twist_real = jnp.cos(twist_angle)
    twist_imag = sign * jnp.sin(twist_angle)
    mid_real = first_real * twist_real - first_imag * twist_imag
    mid_imag = first_real * twist_imag + first_imag * twist_real
    last_real, last_imag = dft_table(inner_len, sign)
    out_real = section_two(last_real, mid_real) - section_two(last_imag, mid_imag)
    out_imag = section_two(last_real, mid_imag) + section_two(last_imag, mid_real)
    factor = 1.0 / math.sqrt(length)
    return (
        (out_real * factor).reshape(leading + (length,)),
        (out_imag * factor).reshape(leading + (length,)),
    )


def pieces_from_image(extrap, band_count, group_count):
    rows_dev = extrap.shape[0]
    image_width = extrap.shape[1]
    stripe = image_width // band_count
    piece_cols = stripe // group_count
    piece_rows = image_width // group_count
    col_real, col_imag = dft_last(extrap, None, -1.0)
    shaped = jnp.stack([col_real, col_imag]).reshape(
        2, 1, 1, rows_dev, band_count, group_count, piece_cols
    )
    moved = lax.all_to_all(
        lax.all_to_all(shaped, "band", split_axis=4, concat_axis=1, tiled=True),
        "vis",
        split_axis=5,
        concat_axis=2,
        tiled=True,
    )
    columns = jnp.transpose(moved.reshape(2, image_width, piece_cols), (2, 0, 1))
    row_real, row_imag = dft_last(columns[:, 0], columns[:, 1], -1.0)
    stacked = (
        jnp.stack([row_real, row_imag], axis=1)
        .astype(jnp.bfloat16)
        .reshape(piece_cols, 2, group_count, piece_rows)
    )
    pieces = lax.all_to_all(stacked, "vis", split_axis=2, concat_axis=0, tiled=True)
    return pieces.reshape(stripe, 2, piece_rows)


def image_from_pieces(piece_sum, band_count, group_count):
    stripe = piece_sum.shape[0]
    piece_rows = piece_sum.shape[2]
    piece_cols = stripe // group_count
    image_width = piece_rows * group_count
    rows_dev = image_width // (band_count * group_count)
    spread = lax.all_to_all(
        piece_sum.reshape(stripe, 2, 1, piece_rows), "vis", split_axis=0, concat_axis=2, tiled=True
    )
    spread = spread.reshape(piece_cols, 2, image_width)
    col_real, col_imag = dft_last(spread[:, 0], spread[:, 1], 1.0)
    stacked = jnp.transpose(jnp.stack([col_real, col_imag]), (0, 2, 1))
    shaped = stacked.reshape(2, band_count, group_count, rows_dev, 1, 1, piece_cols)
    moved = lax.all_to_all(
        lax.all_to_all(shaped, "band", split_axis=1, concat_axis=4, tiled=True),
        "vis",
        split_axis=2,
        concat_axis=5,
        tiled=True,
    )
    moved = moved.reshape(2, rows_dev, image_width)
    out_real, out_imag = dft_last(moved[0], moved[1], 1.0)
    return out_real


def cols_down(field):
    image_width = field.shape[1]
    extended = jnp.concatenate([field, field[:, :6]], axis=1)
    low_part = 0.0
    high_part = 0.0
    for offset in range(8):
        taken = extended[:, offset : offset + image_width : 2]
        low_part = low_part + low_taps[offset] * taken
        high_part = high_part + high_taps[offset] * taken
    return (low_part, high_part)


def cols_up(low_part, high_part):
    halves = []
    for parity in range(2):
        summed = 0.0
        for delay in range(4):
            summed = summed + low_taps[parity + 2 * delay] * jnp.roll(low_part, delay, axis=1)
            summed = summed + high_taps[parity + 2 * delay] * jnp.roll(high_part, delay, axis=1)
        halves.append(summed)
    return jnp.stack(halves, axis=2).reshape(low_part.shape[0], 2 * low_part.shape[1])


def rows_up(low_ext, high_ext, half_rows):
    halves = []
    for parity in range(2):
        summed = 0.0
        for delay in range(4):
            begin = 3 - delay
            summed = summed + low_taps[parity + 2 * delay] * low_ext[begin : begin + half_rows]
            summed = summed + high_taps[parity + 2 * delay] * high_ext[begin : begin + half_rows]
        halves.append(summed)
    return jnp.stack(halves, axis=1).reshape(2 * half_rows, low_ext.shape[1])


def analysis(extrap):
    rows_dev = extrap.shape[0]
    taken_rows = min(6, rows_dev)
    parts_list = [extrap]
    parts_list.append(shifted(extrap[:taken_rows], ("band", "vis"), -1))
    extended = jnp.concatenate(parts_list, axis=0)
    half_rows = rows_dev // 2
    rows_low = 0.0
    rows_high = 0.0
    for offset in range(8):
        taken = extended[offset : offset + 2 * half_rows : 2]
        rows_low = rows_low + low_taps[offset] * taken
        rows_high = rows_high + high_taps[offset] * taken
    low_low, low_high = cols_down(rows_low)
    high_low, high_high = cols_down(rows_high)
    return jnp.stack([low_low, low_high, high_low, high_high])


def synthesis(coef_dual):
    half_rows = coef_dual.shape[1]
    taken_rows = min(3, half_rows)
    parts_list = [shifted(coef_dual[:, half_rows - taken_rows :, :], ("band", "vis"), 1)]
    joined = jnp.concatenate(parts_list[::-1] + [coef_dual], axis=1)
    cols_low = rows_up(joined[0], joined[2], half_rows)
    cols_high = rows_up(joined[1], joined[3], half_rows)
    return cols_up(cols_low, cols_high)


def degrid(kernel_here, tiles):
    kernel_real = kernel_here[:, :, 0]
    kernel_imag = kernel_here[:, :, 1]
    tile_real = tiles[:, :, 0]
    tile_imag = tiles[:, :, 1]
    out_real = jnp.einsum(
        "qsat,qst->qsa", kernel_real, tile_real, preferred_element_type=jnp.float32
    ) - jnp.einsum("qsat,qst->qsa", kernel_imag, tile_imag, preferred_element_type=jnp.float32)
    out_imag = jnp.einsum(
        "qsat,qst->qsa", kernel_real, tile_imag, preferred_element_type=jnp.float32
    ) + jnp.einsum("qsat,qst->qsa", kernel_imag, tile_real, preferred_element_type=jnp.float32)
    return jnp.stack([out_real, out_imag], axis=2)


def grid_back(kernel_here, weights):
    kernel_real = kernel_here[:, :, 0]
    kernel_imag = kernel_here[:, :, 1]
    weight_real = weights[:, :, 0]
    weight_imag = weights[:, :, 1]
    grid_real = jnp.einsum(
        "qsat,qsa->qst", kernel_real, weight_real, preferred_element_type=jnp.float32
    ) + jnp.einsum("qsat,qsa->qst", kernel_imag, weight_imag, preferred_element_type=jnp.float32)
    grid_imag = jnp.einsum(
        "qsat,qsa->qst", kernel_real, weight_imag, preferred_element_type=jnp.float32
    ) - jnp.einsum("qsat,qsa->qst", kernel_imag, weight_real, preferred_element_type=jnp.float32)
    return jnp.stack([grid_real, grid_imag], axis=2)


def local(sky_image, coef_dual, vis_dual, visibilities, kernel_blocks, tile_rows, tile_counts):
    band_count = lax.axis_size("band")
    group_count = lax.axis_size("vis")
    kernel_here = kernel_blocks[0, 0]
    rows_here = tile_rows[0, 0]
    slot_count = rows_here.shape[1]
    live_slots = (
        jnp.arange(slot_count, dtype=jnp.int32)[None, :] < tile_counts[0, 0][:, None]
    ).astype(jnp.float32)[:, :, None, None]
    vis_data = visibilities[0, 0]
    vis_state = vis_dual[0, 0]
    image_width = sky_image.shape[1]
    stripe = image_width // band_count
    piece_rows = image_width // group_count
    incoming_rows = lax.all_to_all(rows_here, "vis", split_axis=0, concat_axis=0, tiled=True)
    data_part = jnp.sum(live_slots * vis_data * vis_data)
    weights = (live_slots * vis_state).astype(jnp.bfloat16)
    contrib = grid_back(kernel_here, weights)
    arrived = lax.all_to_all(contrib, "vis", split_axis=0, concat_axis=0, tiled=True)
    piece_sum = jax.ops.segment_sum(
        arrived.reshape(-1, 2, piece_rows), incoming_rows.reshape(-1), num_segments=stripe
    )
    adjoint_part = image_from_pieces(piece_sum, band_count, group_count)
    smooth = synthesis(coef_dual)
    new_image = jnp.maximum(sky_image - smooth - adjoint_part, 0.0)
    extrap = 2.0 * new_image - sky_image
    coeffs = analysis(extrap)
    abs_total = jnp.sum(jnp.abs(coeffs))
    coef_total = lax.psum(abs_total, ("band", "vis"))
    threshold = 0.5 * coef_total / (IMG * IMG)
    coef_dual = jnp.clip(coef_dual + coeffs, -threshold, threshold)
    piece_grid = pieces_from_image(extrap, band_count, group_count)
    tiles = lax.all_to_all(
        piece_grid[incoming_rows], "vis", split_axis=0, concat_axis=0, tiled=True
    )
    predicted = degrid(kernel_here, tiles)
    residual = live_slots * (vis_state + predicted - vis_data)
    resid_square = jnp.sum(residual * residual)
    norm_square, data_square = lax.psum((resid_square, data_part), ("band", "vis"))
    radius = 0.5 * jnp.sqrt(data_square + 1e-06)
    size_value = jnp.sqrt(norm_square + 1e-06)
    vis_state = residual * (1.0 - jnp.minimum(1.0, radius / size_value))
    return (new_image, coef_dual, vis_state[None, None])


high = lax.Precision.HIGH
everywhere = ("band", "vis")


def wave_tables(length, digit_low):
    digit_high = length // digit_low
    low = np.arange(digit_low)
    wide = np.arange(digit_high)
    full = 2.0 * np.pi
    small = full * (low[:, None] * low[None, :] % digit_low) / digit_low
    twist = full * (low[:, None] * wide[None, :]) / length
    large = full * (wide[:, None] * wide[None, :] % digit_high) / digit_high
    return small, twist, large


def complex_matrix(angle, sign):
    c = np.cos(angle)
    s = sign * np.sin(angle)
    return np.stack([np.stack([c, -s], axis=1), np.stack([s, c], axis=1)])


def f32(values):
    return jnp.asarray(np.asarray(values, np.float32))


def bf16(values):
    return f32(values).astype(jnp.bfloat16)


def analysis_matrix(half):
    matrix = np.zeros((2, half, 2 * half + 6))
    for k in range(half):
        for j in range(8):
            matrix[0, k, 2 * k + j] = low_taps[j]
            matrix[1, k, 2 * k + j] = high_taps[j]
    return matrix.reshape(2 * half, 2 * half + 6)


def synthesis_matrix(half):
    matrix = np.zeros((2 * half, 2, half + 3))
    for n in range(2 * half):
        for delay in range(4):
            tap = n % 2 + 2 * delay
            matrix[n, 0, n // 2 - delay + 3] = low_taps[tap]
            matrix[n, 1, n // 2 - delay + 3] = high_taps[tap]
    return matrix


def cos_sums(values, size):
    half = size // 2
    if half < 2:
        return [values[0] + values[1], values[0] - values[1]]
    quarter = half // 2
    plus = [values[a] + values[half - a] for a in range(quarter)] + [values[quarter]]
    minus = [values[a] - values[half - a] for a in range(quarter)]
    out = [None] * (half + 1)
    out[0::2] = cos_sums(plus, half)
    for k in range(1, half, 2):
        total = minus[0]
        for a in range(1, quarter):
            total = total + minus[a] * math.cos(2 * math.pi * (a * k % size) / size)
        out[k] = total
    return out


def sin_sums(values, size):
    half = size // 2
    if half < 2:
        return [None] * (half + 1)
    quarter = half // 2
    plus = {a: values[a] + values[half - a] for a in range(1, quarter)}
    plus[quarter] = values[quarter]
    minus = [None] + [values[a] - values[half - a] for a in range(1, quarter)]
    out = [None] * (half + 1)
    out[0::2] = sin_sums(minus, half)
    for k in range(1, half, 2):
        total = None
        for a in range(1, quarter + 1):
            factor = math.sin(2 * math.pi * (a * k % size) / size)
            term = plus[a] if a * 4 == size and k % 4 == 1 else plus[a] * factor
            total = term if total is None else total + term
        out[k] = total
    return out


def even_odd(values):
    size = len(values)
    half = size // 2
    even = [values[0]] + [values[a] + values[size - a] for a in range(1, half)] + [values[half]]
    odd = [None] + [values[a] - values[size - a] for a in range(1, half)]
    return even, odd


def split(values):
    upper = values.astype(jnp.bfloat16)
    return upper, (values - upper.astype(jnp.float32)).astype(jnp.bfloat16)


def table_pair(values):
    upper = f32(values).astype(jnp.bfloat16)
    return upper, (f32(values) - upper.astype(jnp.float32)).astype(jnp.bfloat16)


def nt_dot(a, b):
    return lax.dot_general(a, b, (((1,), (1,)), ((), ())), preferred_element_type=jnp.float32)


def nn_dot(a, b):
    return lax.dot_general(a, b, (((1,), (0,)), ((), ())), preferred_element_type=jnp.float32)


LEVELS = 32000.0
MESH = pl.DeviceIdType.MESH
LANES = 128
whole = pl.BlockSpec(memory_space=pltpu.VMEM)


def place():
    band = lax.axis_index("band")
    vis = lax.axis_index("vis")
    groups = lax.axis_size("vis")
    z = vis // 4
    y = vis // 2 % 2
    core = vis % 2
    return band, z, y, core, groups


def taps_dot(values, tables):
    upper, lower = split(values)
    return nn_dot(upper, tables[0]) + nn_dot(lower, tables[0]) + nn_dot(upper, tables[1])


def level(values):
    return jnp.round(values).astype(jnp.int32)


def step_kernel(
    low,
    kernels_hbm,
    coef_hbm,
    sky_hbm,
    up_hbm,
    edge_hbm,
    base_hbm,
    spin_hbm,
    inv_hbm,
    fwd_hbm,
    near_hbm,
    next_hbm,
    half_base_hbm,
    half_spin_hbm,
    order_hbm,
    state_ref,
    data_ref,
    rows_ref,
    counts_ref,
    phase_ref,
    shift_ref,
    tw_ref,
    image_hbm,
    coef_out_hbm,
    vis_out_ref,
    kernels_ref,
    joined_ref,
    sky_ref,
    merged_ref,
    up_ref,
    edge_ref,
    base_ref,
    spin_ref,
    inv_ref,
    fwd_ref,
    near_ref,
    next_ref,
    half_base_ref,
    half_spin_ref,
    order_ref,
    load_sem,
    tail_ref,
    halo_ref,
    block_ref,
    all_cols_ref,
    turn_ref,
    total_ref,
    tall_ref,
    smooth_ref,
    fold_ref,
    grid_ref,
    hot_ref,
    half_ref,
    spec_ref,
    rest_ref,
    extrap_ref,
    picked_ref,
    unit_ref,
    got_ref,
    units_ref,
    sum_table_ref,
    terms_ref,
    own_ref,
    sums_out_ref,
    sums_unit_ref,
    sums_got_ref,
    sums_units_ref,
    all_abs_ref,
    all_sums_ref,
    send_a,
    send_b,
    recv_a,
    recv_b,
    send_p,
    send_u,
    recv_p,
    recv_u,
    send_z,
    recv_z,
    send_w,
    recv_w,
    send_t,
    recv_t,
    send_s,
    recv_s,
    halo_sem,
):
    x, z, y, core, groups = place()
    levels = groups // 4
    devices = 2 * groups
    half_rows, half_width = coef_hbm.shape[1:]
    rows = 2 * half_rows
    tiles = block_ref.shape[1]
    kept = low // 2 + 1
    wide = LANES

    def index(px, pz, py, pc):
        return px * groups + pz * 4 + py * 2 + pc

    def device(px, pz, py, pc):
        return (px, pz * 4 + py * 2 + pc)

    def ident(number):
        return (number // groups, number % groups)

    def remote(src, dst, send, recv, target):
        return pltpu.make_async_remote_copy(
            src_ref=src,
            dst_ref=dst,
            send_sem=send,
            recv_sem=recv,
            device_id=target,
            device_id_type=MESH,
        )

    me = index(x, z, y, core)
    after, before = (me + 1) % devices, (me + devices - 1) % devices
    twin = device(x, z, y, 1 - core)
    line = [device(x, (z + k) % levels, y, core) for k in range(1, levels)]
    corners = [(1 - x, y), (x, 1 - y), (1 - x, 1 - y)]
    plane = [device(px, z, py, core) for px, py in corners]
    barrier = pltpu.get_barrier_semaphore()
    peers = line + plane + [twin, ident(after), ident(before)]
    for peer in peers:
        pl.semaphore_signal(barrier, inc=1, device_id=peer, device_id_type=MESH)

    sources = [
        (kernels_hbm, kernels_ref),
        (coef_hbm, joined_ref.at[:, pl.ds(8, half_rows), :]),
        (up_hbm, up_ref),
        (edge_hbm, edge_ref),
        (base_hbm, base_ref),
        (spin_hbm, spin_ref),
        (inv_hbm, inv_ref),
        (sky_hbm, sky_ref),
        (fwd_hbm, fwd_ref),
        (near_hbm, near_ref),
        (next_hbm, next_ref),
        (half_base_hbm, half_base_ref),
        (half_spin_hbm, half_spin_ref),
        (order_hbm, order_ref),
    ]
    loads = [
        pltpu.make_async_copy(src, dst, load_sem.at[i]) for i, (src, dst) in enumerate(sources)
    ]
    for load in loads:
        load.start()
    loads[0].wait()
    count = 16
    span = kernels_ref.shape[0] * count // tiles
    width = low * wide
    stripe = width // 2
    slots = rows_ref.shape[0]
    lane = lax.broadcasted_iota(jnp.int32, (tiles, groups), 1)
    tile_id = lax.broadcasted_iota(jnp.int32, (tiles, groups), 0)
    counts = jnp.where(lane == tile_id // slots, counts_ref[...].astype(jnp.float32), 0.0)
    counts = jnp.sum(counts, axis=1, keepdims=True)
    tile_id = lax.broadcasted_iota(jnp.int32, (tiles, 1), 0)
    live = jnp.where((tile_id % slots).astype(jnp.float32) < counts, 1.0, 0.0)
    state = [state_ref[:, part, :] for part in range(2)]
    data = [data_ref[:, part, :] for part in range(2)]
    ours = [part * live for part in state]
    turned = [ours[0], ours[1], ours[0], ours[1]], [ours[1], -ours[0], ours[1], -ours[0]]
    turned = [jnp.concatenate(parts, axis=1) for parts in turned]
    pair_lane = lax.broadcasted_iota(jnp.int32, (count, LANES), 1) // (LANES // 2)
    pair_row = lax.broadcasted_iota(jnp.int32, (count, LANES), 0)
    masks = [pair_lane + 2 * k == pair_row for k in range(count // 2)]
    for i in range(tiles // count):
        spread = [
            jnp.concatenate(
                [jnp.where(mask, part[i * count : (i + 1) * count], 0.0) for mask in masks], axis=1
            )
            for part in turned
        ]
        spread = jnp.concatenate(spread, axis=0).astype(jnp.bfloat16)
        both = nn_dot(spread, kernels_ref[i * span : (i + 1) * span, :])
        both = jnp.concatenate([both[:count], both[count:]], axis=1)
        block_ref[me, i * count : (i + 1) * count, :] = both.astype(jnp.bfloat16)
    lane = lax.broadcasted_iota(jnp.int32, (groups, LANES), 1) % tiles
    owner = lax.broadcasted_iota(jnp.int32, (groups, LANES), 0)
    columns = 0.0
    by_owner = rows_ref[...].astype(jnp.float32).T
    for slot in range(slots):
        here = by_owner[:, slot : slot + 1]
        columns = columns + jnp.where(lane == owner * slots + slot, here, 0.0)
    columns = jnp.sum(columns, axis=0, keepdims=True).astype(jnp.int32)
    all_cols_ref[me] = columns + x * stripe
    loads[1].wait()
    for c in range(4):
        tail_ref[3 * c : 3 * c + 3, :] = joined_ref[c, half_rows + 5 :, :]
    pl.semaphore_wait(barrier, len(peers))

    started = []

    def start(block, target, slot):
        own_a, own_b = block_ref.at[block], all_cols_ref.at[block]
        for own, send, recv in ((own_a, send_a, recv_a), (own_b, send_b, recv_b)):
            copy = remote(own, own, send.at[slot], recv.at[block], target)
            copy.start()
            started.append(copy)

    def got(block):
        for ref, send, recv in ((block_ref, send_a, recv_a), (all_cols_ref, send_b, recv_b)):
            own = ref.at[block]
            remote(own, own, send.at[0], recv.at[block], twin).wait_recv()

    slots_of = iter(range(send_a.shape[0]))
    far = sorted(range(1, levels), key=lambda k: abs(k - levels / 2))
    for k in far:
        start(me, line[k - 1], next(slots_of))
    for target in plane:
        start(me, target, next(slots_of))
    edge = remote(tail_ref, halo_ref, halo_sem.at[0], halo_sem.at[1], ident(after))
    edge.start()
    start(me, twin, next(slots_of))
    line_blocks = [index(x, (z + levels - k) % levels, y, core) for k in far]
    for block in line_blocks:
        got(block)
        for target in plane:
            start(block, target, next(slots_of))
        start(block, twin, next(slots_of))
    edge.wait()
    for c in range(4):
        joined_ref[c, 5:8, :] = halo_ref[3 * c : 3 * c + 3, :]
    strips = half_width // LANES

    def tall(i, carry):
        here = pl.ds(pl.multiple_of(i * LANES, LANES), LANES)
        for c in range(2):
            for k in range(half_rows // 8):
                lows = [joined_ref[c, 8 + 8 * k - d : 16 + 8 * k - d, here] for d in range(4)]
                highs = [joined_ref[c + 2, 8 + 8 * k - d : 16 + 8 * k - d, here] for d in range(4)]
                for parity in range(2):
                    total = 0.0
                    for d in range(4):
                        total = total + low_taps[parity + 2 * d] * lows[d]
                        total = total + high_taps[parity + 2 * d] * highs[d]
                    tall_ref[c * strips + i, pl.ds(16 * k + parity, 8, stride=2), :] = total
        return carry

    lax.fori_loop(0, strips, tall, 0)

    for px, py in corners:
        block = index(px, z, py, core)
        got(block)
        start(block, twin, next(slots_of))
    for load in loads[2:8]:
        load.wait()

    def broad(i, carry):
        there = (i + strips - 1) % strips
        near = jnp.concatenate([tall_ref[i], tall_ref[strips + i]], axis=1)
        last = jnp.concatenate([tall_ref[there], tall_ref[strips + there]], axis=1)
        out = taps_dot(near, up_ref)
        first = taps_dot(last, edge_ref)
        smooth_ref[2 * i] = out[:, :LANES] + first
        smooth_ref[2 * i + 1] = out[:, LANES:]
        return carry

    lax.fori_loop(0, strips // 2, broad, 0)
    spin_cos, spin_sin = spin_ref[0, pl.ds(me, 1), :], spin_ref[1, pl.ds(me, 1), :]
    cosine = (base_ref[0] * spin_cos - base_ref[1] * spin_sin).astype(jnp.bfloat16)
    sine = (base_ref[1] * spin_cos + base_ref[0] * spin_sin).astype(jnp.bfloat16)
    piece = kernels_ref.shape[1]
    turn_ref[:rows, :piece] = cosine
    turn_ref[:rows, piece:] = -sine
    turn_ref[rows:, :piece] = sine
    turn_ref[rows:, piece:] = cosine
    for load in loads[11:13]:
        load.wait()
    for n in range(4):
        spin_cos, spin_sin = half_spin_ref[0, n : n + 1, :], half_spin_ref[1, n : n + 1, :]
        cosine = half_base_ref[0] * spin_cos - half_base_ref[1] * spin_sin
        sine = half_base_ref[1] * spin_cos + half_base_ref[0] * spin_sin
        for p in range(2):
            part = slice(p * LANES, (p + 1) * LANES)
            c, d = split(cosine[:, part]), split(sine[:, part])
            real_rows = slice(2 * n * rows, (2 * n + 1) * rows)
            imag_rows = slice((2 * n + 1) * rows, (2 * n + 2) * rows)
            for e in range(2):
                sum_table_ref[e, p, real_rows, :LANES] = c[e]
                sum_table_ref[e, p, real_rows, LANES:] = -d[e]
                sum_table_ref[e, p, imag_rows, :LANES] = d[e]
                sum_table_ref[e, p, imag_rows, LANES:] = c[e]
    for n, k in enumerate(far):
        for px, py in corners:
            block = index(px, (z + levels - k) % levels, py, core)
            got(block)
            start(block, twin, next(slots_of))
        if n == 0:
            lax.fori_loop(strips // 2, strips, broad, 0)

    total_tiles = devices * tiles
    class_tiles = groups * tiles
    parts = class_tiles // LANES
    lane = lax.broadcasted_iota(jnp.int32, (1, LANES), 1)

    def spread(c, levels_taken):
        for zz in levels_taken:
            for side in range(2):
                b = c * parts + zz * 2 + side
                first = side * groups + zz * 4 + c
                columns = jnp.where(lane < tiles, all_cols_ref[first], all_cols_ref[first + 2])
                k1 = columns % low
                k2 = columns // low
                flip = k1 >= kept
                k1 = jnp.where(flip, low - k1, k1)
                k2 = jnp.where(flip, wide - 1 - k2, k2)
                fold_ref[0, pl.ds(b, 1), :] = (k1 * wide + k2).astype(jnp.float32)
                fold_ref[1, pl.ds(b, 1), :] = jnp.where(flip, -1.0, 1.0)
            some = [block_ref[i // 2 * groups + zz * 4 + i % 2 * 2 + c] for i in range(4)]
            both = nt_dot(turn_ref[...], jnp.concatenate(some, axis=0))
            for side in range(2):
                b = c * parts + zz * 2 + side
                at = pl.ds(pl.multiple_of(b * LANES, LANES), LANES)
                real = both[:rows, side * LANES : (side + 1) * LANES]
                imag = both[rows:, side * LANES : (side + 1) * LANES]
                sign = fold_ref[1, pl.ds(b, 1), :]
                out_real = real * phase_ref[0] - imag * phase_ref[1]
                out_imag = (real * phase_ref[1] + imag * phase_ref[0]) * sign
                grid_ref[:rows, at] = out_real.astype(jnp.bfloat16)
                grid_ref[rows:, at] = out_imag.astype(jnp.bfloat16)

    def folded_sum(c, levels_taken, p):
        base = pl.multiple_of(p * 2 * wide, 2 * wide)
        row = (lax.broadcasted_iota(jnp.int32, (2 * wide, LANES), 0) + base).astype(jnp.float32)
        total = None
        for zz in levels_taken:
            hots = []
            for side in range(2):
                hit = row == fold_ref[0, pl.ds(c * parts + zz * 2 + side, 1), :]
                hots.append(jnp.where(hit, 1.0, 0.0).astype(jnp.bfloat16))
            hot = jnp.concatenate(hots, axis=1)
            at = c * class_tiles + zz * 2 * LANES
            at = pl.ds(pl.multiple_of(at, 2 * LANES), 2 * LANES)
            hot_ref[pl.ds(base, 2 * wide), at] = hot
            out = nt_dot(grid_ref[:, at], hot)
            total = out if total is None else total + out
        return total

    everything = list(range(levels))
    spread(core, everything)

    def scatter_own(p, carry):
        total_ref[p] = folded_sum(core, everything, p)
        return carry

    lax.fori_loop(0, (kept + 1) // 2, scatter_own, 0)
    coming = [z] + [(z + levels - k) % levels for k in far]

    def from_twin(zz):
        for i in range(4):
            got(i // 2 * groups + zz * 4 + i % 2 * 2 + 1 - core)

    for zz in coming[:-1]:
        from_twin(zz)
    spread(1 - core, coming[:-1])

    def scatter_more(p, carry):
        total_ref[p] = total_ref[p] + folded_sum(1 - core, coming[:-1], p)
        return carry

    lax.fori_loop(0, (kept + 1) // 2, scatter_more, 0)
    from_twin(coming[-1])
    spread(1 - core, coming[-1:])

    def scatter(p, carry):
        folded = (total_ref[p] + folded_sum(1 - core, coming[-1:], p)).astype(jnp.bfloat16)
        pairs = []
        for e in range(2):
            here = slice(e * wide, (e + 1) * wide)
            pairs.append(jnp.concatenate([folded[:rows, here], folded[rows:, here]], axis=1))
        mids = nn_dot(jnp.concatenate(pairs, axis=0), inv_ref[...])
        for e in range(2):
            mid = mids[e * rows : (e + 1) * rows]
            k1 = p * 2 + e
            tw_real, tw_imag = tw_ref[0, pl.ds(k1, 1), :], tw_ref[1, pl.ds(k1, 1), :]
            real, imag = mid[:, :wide], mid[:, wide:]
            half_ref[k1, :, :wide] = real * tw_real - imag * tw_imag
            half_ref[k1, :, wide:] = real * tw_imag + imag * tw_real
        return carry

    lax.fori_loop(0, (kept + 1) // 2, scatter, 0)

    def strip(i, carry):
        at = pl.ds(pl.multiple_of(i * 8, 8), 8)
        cos_part = cos_sums([half_ref[k, at, :wide] for k in range(kept)], low)
        sin_part = sin_sums([None] + [half_ref[k, at, wide:] for k in range(1, kept - 1)], low)
        extraps = []
        for a in range(low):
            k = min(a, low - a)
            if a == 0 or a == low // 2:
                adjoint = cos_part[k]
            elif a < low // 2:
                adjoint = cos_part[k] - sin_part[k]
            else:
                adjoint = cos_part[k] + sin_part[k]
            here = slice(a * wide, (a + 1) * wide)
            sky = sky_ref[at, here]
            image = jnp.maximum(sky - smooth_ref[a, at, :] - adjoint, 0.0)
            extrap = 2.0 * image - sky
            sky_ref[at, here] = image
            extrap_ref[a, at, :] = extrap
            extraps.append(extrap)
        even, odd = even_odd(extraps)
        real_part = cos_sums(even, low)
        imag_part = sin_sums(odd, low)
        for k in range(kept):
            tw_real, tw_imag = tw_ref[0, k : k + 1, :], tw_ref[1, k : k + 1, :]
            real = real_part[k] * tw_real
            imag = -real_part[k] * tw_imag
            if 0 < k < kept - 1:
                real = real - imag_part[k] * tw_imag
                imag = imag - imag_part[k] * tw_real
            half_ref[k, at, :wide] = real
            half_ref[k, at, wide:] = imag
        return carry

    lax.fori_loop(0, rows // 8, strip, 0)
    store = pltpu.make_async_copy(sky_ref, image_hbm, load_sem.at[len(loads)])
    store.start()
    top = remote(
        extrap_ref.at[:, pl.ds(0, 8), :],
        extrap_ref.at[:, pl.ds(rows, 8), :],
        halo_sem.at[2],
        halo_sem.at[3],
        ident(before),
    )
    top.start()
    loads[8].wait()

    batch = (kept + 1) // 3

    def spectrum(i, carry):
        some = half_ref[pl.ds(i * batch, batch)].reshape(batch * rows, 2 * wide)
        out = taps_dot(some, fwd_ref)
        for e in range(batch):
            here = pl.ds(pl.multiple_of((i * batch + e) * wide, wide), wide)
            upper, lower = split(out[e * rows : (e + 1) * rows])
            spec_ref[:rows, here] = upper[:, :wide]
            spec_ref[rows:, here] = upper[:, wide:]
            rest_ref[:rows, here] = lower[:, :wide]
            rest_ref[rows:, here] = lower[:, wide:]
        return carry

    lax.fori_loop(0, 3, spectrum, 0)

    mate = x * 4 + y * 2 + core

    def sends(to_z, to_x, to_y, to_class):
        at = to_class * class_tiles + (to_z * 4 + to_x * 2 + to_y) * tiles
        at = pl.ds(pl.multiple_of(at, tiles), tiles)
        unit = unit_ref.at[to_class * parts + to_z * 2 + to_x]
        spot, target = to_z * 8 + mate, device(to_x, z, to_y, to_class)
        return [
            remote(picked_ref.at[at, :], got_ref.at[spot], send_p.at[0], recv_p.at[to_z], target),
            remote(unit, units_ref.at[spot], send_u.at[0], recv_u.at[to_z], target),
        ]

    def total_of(ref, send, recv, count=devices - 1, at=0):
        some = ref.at[pl.ds(0, count)]
        return remote(some, some, send.at[0], recv.at[at], twin)

    def share_row(ref, send, recv):
        def one(k, carry):
            to = (me + k) % devices
            remote(ref.at[me], ref.at[me], send.at[0], recv.at[0], ident(to)).start()
            return carry

        lax.fori_loop(1, devices, one, 0)

    def row_total(ref):
        total = ref[0]
        for d in range(1, devices):
            total = total + ref[d]
        return total

    def ordered(n):
        return (z // 2 + 1 + n // 2) % 2 * 2 + (z + 1 + n) % 2

    def pick(s, carry):
        to_z = ordered(s // 2)
        to_class = (core + 1 + s) % 2
        j = to_class * 4 + to_z
        at = pl.multiple_of(j * 2 * LANES, 2 * LANES)
        hot = hot_ref[: kept * wide, pl.ds(at, 2 * LANES)]
        both = nn_dot(spec_ref[:, : kept * wide], hot) + nn_dot(rest_ref[:, : kept * wide], hot)
        for h in range(2):
            sign = fold_ref[1, pl.ds(2 * j + h, 1), :]
            real = both[:rows, h * LANES : (h + 1) * LANES]
            imag = both[rows:, h * LANES : (h + 1) * LANES] * sign
            most = jnp.max(jnp.maximum(jnp.abs(real), jnp.abs(imag)), axis=0, keepdims=True)
            most = jnp.maximum(most, 1e-30)
            unit_ref[2 * j + h] = most * (1.0 / LEVELS)
            to_level = LEVELS / most
            packed = level(real * to_level) * 65536 + level(imag * to_level)
            to = pl.ds(pl.multiple_of(at + h * LANES, LANES), LANES)
            picked_ref[to, :] = packed.T
        for to_x in range(2):
            for to_y in range(2):
                away = (to_x - x) * (to_x - x) + (to_y - y) * (to_y - y)

                @pl.when(away + (to_class - core) * (to_class - core) != 0)
                def _():
                    for copy in sends(to_z, to_x, to_y, to_class):
                        copy.start()

        return carry

    lax.fori_loop(0, devices // 4, pick, 0)
    for to_z in range(levels):
        at = core * class_tiles + (to_z * 4 + x * 2 + y) * tiles
        got_ref[to_z * 8 + mate] = picked_ref[pl.ds(pl.multiple_of(at, tiles), tiles), :]
        units_ref[to_z * 8 + mate] = unit_ref[core * parts + to_z * 2 + x]
    top.wait()
    loads[9].wait()
    loads[10].wait()

    def rows_down(i, carry):
        for k in range(half_rows // 8):
            lows, highs = 0.0, 0.0
            for tap in range(8):
                taken = extrap_ref[i, pl.ds(16 * k + tap, 8, stride=2), :]
                lows = lows + low_taps[tap] * taken
                highs = highs + high_taps[tap] * taken
            tall_ref[i, 8 * k : 8 * k + 8, :] = lows
            tall_ref[i, half_rows + 8 * k : half_rows + 8 * k + 8, :] = highs
        return carry

    lax.fori_loop(0, low, rows_down, 0)

    def cols_down(b, absolute):
        here = jnp.concatenate([tall_ref[2 * b], tall_ref[2 * b + 1]], axis=1)
        out = taps_dot(here, near_ref) + taps_dot(tall_ref[(2 * b + 2) % low], next_ref)
        at = pl.ds(pl.multiple_of(b * LANES, LANES), LANES)
        for c in range(4):
            top_row, left = c // 2 * half_rows, c % 2 * LANES
            part = out[top_row : top_row + half_rows, left : left + LANES]
            absolute = absolute + jnp.abs(part)
            merged_ref[c, :, at] = joined_ref[c, 8:, at] + part
        return absolute

    def plane_sums(taken):
        many = len(taken) * tiles
        rows_of = []
        for zz in taken:
            total_of(got_ref, send_p, recv_p, 7, zz).wait_recv()
            total_of(units_ref, send_u, recv_u, 7, zz).wait_recv()
            rows_of += [units_ref[zz * 8 + m] for m in range(8)]
        units = jnp.concatenate(rows_of * (LANES // len(rows_of)), axis=0).T
        units = jnp.where(y == 0, units[:tiles], units[tiles:])
        cosine, sine = shift_ref[0], shift_ref[1]
        level_cos = half_spin_ref[0, pl.ds(4 * z, 1), :]
        level_sin = half_spin_ref[1, pl.ds(4 * z, 1), :]
        for e, zz in enumerate(taken):
            strip_rows = slice(e * tiles, (e + 1) * tiles)
            for pair in range(4):
                reals, imags = [], []
                for side in range(2):
                    m = side * 4 + pair
                    packed = got_ref[zz * 8 + m]
                    real = (packed + 32768) >> 16
                    imag = packed - (real << 16)
                    unit = units[:, e * 8 + m : e * 8 + m + 1]
                    real = real.astype(jnp.float32) * unit
                    imag = imag.astype(jnp.float32) * unit
                    reals.append(real * cosine + imag * sine)
                    imags.append(imag * cosine - real * sine)
                at = 2 * pair * LANES
                for p, values in ((0, (reals[0] + reals[1], imags[0] + imags[1])),
                                  (1, (reals[0] - reals[1], imags[0] - imags[1]))):
                    for part in range(2):
                        upper, lower = split(values[part])
                        here = slice(at + part * LANES, at + (part + 1) * LANES)
                        terms_ref[0, p, strip_rows, here] = upper
                        terms_ref[1, p, strip_rows, here] = lower
        reals, imags = [], []
        for p in range(2):
            out = nn_dot(terms_ref[0, p, :many], sum_table_ref[0, p])
            out = out + nn_dot(terms_ref[1, p, :many], sum_table_ref[0, p])
            out = out + nn_dot(terms_ref[0, p, :many], sum_table_ref[1, p])
            part = slice(p * LANES, (p + 1) * LANES)
            turn_cos, turn_sin = level_cos[:, part], level_sin[:, part]
            real, imag = out[:, :LANES], out[:, LANES:]
            reals.append(real * turn_cos + imag * turn_sin)
            imags.append(imag * turn_cos - real * turn_sin)
        real = jnp.concatenate(reals, axis=1)
        imag = jnp.concatenate(imags, axis=1)
        most = jnp.max(jnp.maximum(jnp.abs(real), jnp.abs(imag)), axis=1, keepdims=True)
        most = jnp.maximum(most, 1e-30)
        to_level = LEVELS / most
        packed = level(real * to_level) * 65536 + level(imag * to_level)
        unit = most * (1.0 / LEVELS)
        for e, zz in enumerate(taken):
            strip_rows = slice(e * tiles, (e + 1) * tiles)
            if zz is z:
                own_ref[:, : 2 * LANES] = real[strip_rows]
                own_ref[:, 2 * LANES :] = imag[strip_rows]
                continue
            sums_out_ref[zz] = packed[strip_rows]
            wide_unit = jnp.broadcast_to(unit[strip_rows], (tiles, LANES))
            sums_unit_ref[zz] = jnp.concatenate([wide_unit, wide_unit], axis=0).T[:1]
            target = device(x, zz, y, core)
            remote(
                sums_out_ref.at[zz], sums_got_ref.at[z], send_z.at[0], recv_z.at[0], target
            ).start()
            remote(
                sums_unit_ref.at[zz], sums_units_ref.at[z], send_w.at[0], recv_w.at[0], target
            ).start()

    plane_sums([ordered(0), ordered(1)])
    absolute = jnp.zeros((half_rows, LANES), jnp.float32)
    absolute = lax.fori_loop(0, low // 4, cols_down, absolute)
    plane_sums([ordered(2)])
    plane_sums([z])
    absolute = lax.fori_loop(low // 4, low // 2, cols_down, absolute)
    abs_total = jnp.sum(jnp.sum(absolute, axis=0, keepdims=True), axis=1, keepdims=True)
    loads[13].wait()

    lane = lax.broadcasted_iota(jnp.int32, (1, LANES), 1)
    all_abs_ref[me] = jnp.where(lane == 0, abs_total, 0.0)
    share_row(all_abs_ref, send_t, recv_t)
    total_of(sums_got_ref, send_z, recv_z, levels - 1).wait_recv()
    total_of(sums_units_ref, send_w, recv_w, levels - 1).wait_recv()
    units = [sums_units_ref[(z + k) % levels] for k in range(1, levels)]
    units = jnp.concatenate(units + [units[0]] * (LANES - levels + 1), axis=0).T
    units = units[:tiles]
    real, imag = own_ref[:, : 2 * LANES], own_ref[:, 2 * LANES :]
    for k in range(1, levels):
        packed = sums_got_ref[(z + k) % levels]
        upper = (packed + 32768) >> 16
        lower = packed - (upper << 16)
        unit = units[:, k - 1 : k]
        real = real + upper.astype(jnp.float32) * unit
        imag = imag + lower.astype(jnp.float32) * unit
    tile = jnp.concatenate([real, imag], axis=1).astype(jnp.bfloat16)
    tile = nn_dot(tile, order_ref[...]).astype(jnp.bfloat16)
    first, second = [], []
    near_row = pair_row % 2 == 0
    for i in range(tiles // count):
        here = tile[i * count : (i + 1) * count]
        pair = jnp.concatenate([here[:, :piece], here[:, piece:]], axis=0)
        out = nt_dot(pair, kernels_ref[i * span : (i + 1) * span, :])
        for found, half in ((first, out[:count]), (second, out[count:])):
            total = 0.0
            for k in range(count // 2):
                total = total + jnp.where(
                    pair_row // 2 == k, half[:, k * LANES : (k + 1) * LANES], 0.0
                )
            found.append(jnp.where(near_row, total, pltpu.roll(total, LANES // 2, 1)))
    first = jnp.concatenate(first, axis=0)
    second = jnp.concatenate(second, axis=0)
    visits = state_ref.shape[2]
    lane = lax.broadcasted_iota(jnp.int32, first.shape, 1)
    crossed = jnp.where(
        lane // visits % 2 == 0,
        -pltpu.roll(second, LANES - visits, 1),
        pltpu.roll(second, visits, 1),
    )
    keep = jnp.where(lane < 2 * visits, live, 0.0)
    state_wide = jnp.concatenate(state + state, axis=1)
    data_wide = jnp.concatenate(data + data, axis=1)
    residual = keep * (state_wide + first + crossed - data_wide)
    norms = []
    for values in (residual, data_wide * keep):
        norms.append(jnp.sum(jnp.sum(values * values, axis=0, keepdims=True), axis=1, keepdims=True))
    lane = lax.broadcasted_iota(jnp.int32, (1, LANES), 1)
    all_sums_ref[me] = jnp.where(lane == 0, norms[0], norms[1])
    share_row(all_sums_ref, send_s, recv_s)
    total_of(all_abs_ref, send_t, recv_t).wait_recv()
    threshold = 0.5 * row_total(all_abs_ref)[:, 0:1] / (width * width)

    def clip(i, carry):
        at = pl.ds(pl.multiple_of(i * LANES, LANES), LANES)
        for c in range(4):
            merged_ref[c, :, at] = jnp.clip(merged_ref[c, :, at], -threshold, threshold)
        return carry

    lax.fori_loop(0, half_width // LANES, clip, 0)
    store_coef = pltpu.make_async_copy(merged_ref, coef_out_hbm, load_sem.at[len(loads) + 1])
    store_coef.start()
    for copy in started:
        copy.wait_send()
    total_of(got_ref, send_p, recv_p, 28).wait_send()
    total_of(units_ref, send_u, recv_u, 28).wait_send()
    total_of(sums_got_ref, send_z, recv_z, levels - 1).wait_send()
    total_of(sums_units_ref, send_w, recv_w, levels - 1).wait_send()
    total_of(all_abs_ref, send_t, recv_t).wait_send()
    total_of(all_sums_ref, send_s, recv_s).wait()
    total = row_total(all_sums_ref)
    size = jnp.sqrt(total[:, 0:1] + 1e-06)
    radius = 0.5 * jnp.sqrt(total[:, 1:2] + 1e-06)
    residual = residual * (1.0 - jnp.minimum(1.0, radius / size))
    vis_out_ref[:, 0, :] = residual[:, :visits]
    vis_out_ref[:, 1, :] = residual[:, visits : 2 * visits]
    store.wait()
    store_coef.wait()


def step(kernels, coef, sky, state, data, tile_rows, tile_counts, groups, devices):
    rows, width = sky.shape
    piece = kernels.shape[1]
    slots = tile_rows.shape[0]
    tiles = groups * slots
    half_rows, half_width = coef.shape[1:]
    low = width // LANES
    kept = low // 2 + 1
    wide = np.arange(LANES)
    matrix = synthesis_matrix(LANES)
    up = matrix[:, :, 3:].transpose(1, 2, 0).reshape(2 * LANES, 2 * LANES)
    edge = np.zeros((2, LANES, LANES))
    edge[:, LANES - 3 :, :] = matrix[:LANES, :, :3].transpose(1, 2, 0)
    matrix = analysis_matrix(LANES).T
    following = np.zeros((LANES, 2 * LANES))
    following[:6] = matrix[2 * LANES :]
    turn = np.arange(piece)
    base = 2 * np.pi * np.arange(rows)[:, None] * turn[None, :] / width
    spin = 2 * np.pi * (np.arange(devices)[:, None] * turn[None, :] % devices) / devices
    owner = wide // slots % groups
    shift = 2 * np.pi * (np.arange(rows)[:, None] * owner[None, :] % groups) / groups
    phase = np.stack([np.cos(shift), np.sin(shift)])
    full = 2 * np.pi * (wide[:, None] * wide[None, :] % LANES) / LANES
    c, s = np.cos(full) / width, np.sin(full) / width
    inverse = np.block([[c, s], [-s, c]])
    forward = np.block([[c, -s], [s, c]])
    twist = 2 * np.pi * np.arange(kept + 1)[:, None] * wide[None, :] / width
    halves = np.concatenate([turn[0::2], turn[1::2]])
    half_base = 2 * np.pi * np.arange(rows)[:, None] * halves[None, :] / width
    half_spin = 2 * np.pi * (np.arange(devices)[:, None] * halves[None, :] % devices) / devices
    order = np.zeros((2 * piece, 2 * piece))
    for part in range(2):
        order[part * piece + np.arange(piece), part * piece + halves] = 1.0
    loaded = [
        kernels,
        coef,
        sky,
        jnp.stack(table_pair(up)),
        jnp.stack(table_pair(edge.reshape(2 * LANES, LANES))),
        f32(np.stack([np.cos(base), np.sin(base)])),
        f32(np.stack([np.cos(spin), np.sin(spin)])),
        bf16(inverse),
        jnp.stack(table_pair(forward)),
        jnp.stack(table_pair(matrix[: 2 * LANES])),
        jnp.stack(table_pair(following)),
        f32(np.stack([np.cos(half_base), np.sin(half_base)])),
        f32(np.stack([np.cos(half_spin), np.sin(half_spin)])),
        bf16(order),
    ]
    held = [
        state,
        data,
        tile_rows,
        tile_counts,
        f32(phase),
        f32(phase[:, :, :tiles].transpose(0, 2, 1)),
        f32(np.stack([np.cos(twist), np.sin(twist)])),
    ]
    buffers = [pltpu.VMEM(value.shape, value.dtype) for value in loaded]
    buffers[1] = pltpu.VMEM((4, half_rows + 8, half_width), jnp.float32)
    copies = 3 * 4 + 7 + 12
    dma = pltpu.SemaphoreType.DMA
    anywhere = pl.BlockSpec(memory_space=pltpu.HBM)
    return pl.pallas_call(
        lambda *refs: step_kernel(low, *refs),
        out_shape=(
            jax.ShapeDtypeStruct((rows, width), jnp.float32),
            jax.ShapeDtypeStruct(coef.shape, jnp.float32),
            jax.ShapeDtypeStruct(state.shape, jnp.float32),
        ),
        in_specs=[anywhere] * len(loaded) + [whole] * len(held),
        out_specs=(anywhere, anywhere, whole),
        scratch_shapes=buffers[:3]
        + [pltpu.VMEM(coef.shape, jnp.float32)]
        + buffers[3:]
        + [
            dma((len(loaded) + 2,)),
            pltpu.VMEM((16, half_width), jnp.float32),
            pltpu.VMEM((16, half_width), jnp.float32),
            pltpu.VMEM((devices, tiles, 2 * piece), jnp.bfloat16),
            pltpu.VMEM((devices, 1, LANES), jnp.int32),
            pltpu.VMEM((2 * rows, 2 * piece), jnp.bfloat16),
            pltpu.VMEM(((kept + 1) // 2, 2 * rows, 2 * LANES), jnp.float32),
            pltpu.VMEM((low, rows, LANES), jnp.float32),
            pltpu.VMEM((low, rows, LANES), jnp.float32),
            pltpu.VMEM((2, devices // 2, LANES), jnp.float32),
            pltpu.VMEM((2 * rows, devices * tiles), jnp.bfloat16),
            pltpu.VMEM(((kept + 1) * LANES, devices * tiles), jnp.bfloat16),
            pltpu.VMEM((kept + 1, rows, 2 * LANES), jnp.float32),
            pltpu.VMEM((2 * rows, (kept + 1) * LANES), jnp.bfloat16),
            pltpu.VMEM((2 * rows, (kept + 1) * LANES), jnp.bfloat16),
            pltpu.VMEM((low, rows + 8, LANES), jnp.float32),
            pltpu.VMEM((devices * tiles, rows), jnp.int32),
            pltpu.VMEM((devices // 2, 1, LANES), jnp.float32),
            pltpu.VMEM((devices, tiles, rows), jnp.int32),
            pltpu.VMEM((devices, 1, LANES), jnp.float32),
            pltpu.VMEM((2, 2, 8 * rows, 2 * LANES), jnp.bfloat16),
            pltpu.VMEM((2, 2, 2 * tiles, 8 * rows), jnp.bfloat16),
            pltpu.VMEM((tiles, 2 * piece), jnp.float32),
            pltpu.VMEM((groups // 4, tiles, piece), jnp.int32),
            pltpu.VMEM((groups // 4, 1, LANES), jnp.float32),
            pltpu.VMEM((groups // 4, tiles, piece), jnp.int32),
            pltpu.VMEM((groups // 4, 1, LANES), jnp.float32),
            pltpu.VMEM((devices, 1, LANES), jnp.float32),
            pltpu.VMEM((devices, 1, LANES), jnp.float32),
            dma((copies,)),
            dma((copies,)),
        ]
        + [dma((devices,))] * 2
        + [dma((groups // 4,))] * 4
        + [dma((1,))] * 8
        + [dma((4,))],
        compiler_params=pltpu.CompilerParams(
            collective_id=0, has_side_effects=True, vmem_limit_bytes=60 * 2**20
        ),
        name="step",
    )(*loaded, *held)


def fast_local(sky_image, coef_dual, vis_dual, visibilities, kernel_blocks, tile_rows, tile_counts):
    groups = lax.axis_size("vis")
    devices = lax.axis_size("band") * groups
    taken = kernel_blocks.shape
    new_image, coef_dual, vis_state = step(
        kernel_blocks.reshape(-1, taken[-1]),
        coef_dual,
        sky_image,
        vis_dual.reshape((-1,) + vis_dual.shape[4:]),
        visibilities.reshape((-1,) + vis_dual.shape[4:]),
        tile_rows[0, 0].T,
        tile_counts[0],
        groups,
        devices,
    )
    return (new_image, coef_dual, vis_state.reshape(vis_dual.shape))


def body_for(mesh):
    devices = mesh.shape["band"] * mesh.shape["vis"]
    relayed = mesh.shape["band"] == 2 and mesh.shape["vis"] % 4 == 0 and devices == 32

    def body(sky_image, *rest):
        rows, width = sky_image.shape
        piece = width // mesh.shape["vis"]
        tiles = rest[4].shape[2] * rest[4].shape[3]
        if relayed and rows == LANES and piece == 2 * LANES and 2 * tiles == LANES:
            return fast_local(sky_image, *rest)
        return local(sky_image, *rest)

    return body


def solution(mesh):
    return jax.shard_map(
        body_for(mesh),
        mesh=mesh,
        in_specs=(
            P(("band", "vis"), None),
            P(None, ("band", "vis"), None),
            P("band", "vis", None, None, None, None),
            P("band", "vis", None, None, None, None),
            P("band", "vis", None, None, None, None, None),
            P("band", "vis", None, None),
            P("band", "vis", None),
        ),
        out_specs=(
            P(("band", "vis"), None),
            P(None, ("band", "vis"), None),
            P("band", "vis", None, None, None, None),
        ),
        check_vma=False,
    )
```

```python
import math

import jax
import numpy as np
import jax.numpy as jnp
from jax import lax
from jax.experimental import pallas as pl
from jax.experimental.pallas import tpu as pltpu
from jax.sharding import PartitionSpec as P

IMG = 4096


low_taps = (
    -0.010597401784997278,
    0.032883011666982945,
    0.030841381835986965,
    -0.18703481171888114,
    -0.02798376941698385,
    0.6308807679295904,
    0.7148465705525415,
    0.23037781330885523,
)
high_taps = tuple(((-1.0) ** offset * low_taps[7 - offset] for offset in range(8)))
highest = lax.Precision.HIGHEST


def shifted(block, axis, distance):
    devices = range(lax.axis_size(axis))
    route = [((i - distance) % len(devices), i) for i in devices]
    return lax.ppermute(block, axis, route)


def dft_table(table_size, sign):
    positions = jnp.arange(table_size, dtype=jnp.int32)
    phase = positions[:, None] * positions[None, :] % table_size
    angle = 2.0 * math.pi / table_size * phase.astype(jnp.float32)
    return (jnp.cos(angle), sign * jnp.sin(angle))


def section_one(table, values):
    return jnp.einsum("kn,...nm->...km", table, values, precision=highest)


def section_two(table, values):
    return jnp.einsum("qm,...km->...qk", table, values, precision=highest)


def dft_last(real_in, imag_in, sign):
    leading = real_in.shape[:-1]
    length = real_in.shape[-1]
    inner_len = 64
    outer_len = length // inner_len
    split_real = real_in.reshape(leading + (outer_len, inner_len))
    table_real, table_imag = dft_table(outer_len, sign)
    first_real = section_one(table_real, split_real)
    first_imag = section_one(table_imag, split_real)
    if imag_in is not None:
        split_imag = imag_in.reshape(leading + (outer_len, inner_len))
        first_real = first_real - section_one(table_imag, split_imag)
        first_imag = first_imag + section_one(table_real, split_imag)
    outer_index = jnp.arange(outer_len, dtype=jnp.int32)
    inner_index = jnp.arange(inner_len, dtype=jnp.int32)
    twist_phase = outer_index[:, None] * inner_index[None, :] % length
    twist_angle = 2.0 * math.pi / length * twist_phase.astype(jnp.float32)
    twist_real = jnp.cos(twist_angle)
    twist_imag = sign * jnp.sin(twist_angle)
    mid_real = first_real * twist_real - first_imag * twist_imag
    mid_imag = first_real * twist_imag + first_imag * twist_real
    last_real, last_imag = dft_table(inner_len, sign)
    out_real = section_two(last_real, mid_real) - section_two(last_imag, mid_imag)
    out_imag = section_two(last_real, mid_imag) + section_two(last_imag, mid_real)
    factor = 1.0 / math.sqrt(length)
    return (
        (out_real * factor).reshape(leading + (length,)),
        (out_imag * factor).reshape(leading + (length,)),
    )


def pieces_from_image(extrap, band_count, group_count):
    rows_dev = extrap.shape[0]
    image_width = extrap.shape[1]
    stripe = image_width // band_count
    piece_cols = stripe // group_count
    piece_rows = image_width // group_count
    col_real, col_imag = dft_last(extrap, None, -1.0)
    shaped = jnp.stack([col_real, col_imag]).reshape(
        2, 1, 1, rows_dev, band_count, group_count, piece_cols
    )
    moved = lax.all_to_all(
        lax.all_to_all(shaped, "band", split_axis=4, concat_axis=1, tiled=True),
        "vis",
        split_axis=5,
        concat_axis=2,
        tiled=True,
    )
    columns = jnp.transpose(moved.reshape(2, image_width, piece_cols), (2, 0, 1))
    row_real, row_imag = dft_last(columns[:, 0], columns[:, 1], -1.0)
    stacked = (
        jnp.stack([row_real, row_imag], axis=1)
        .astype(jnp.bfloat16)
        .reshape(piece_cols, 2, group_count, piece_rows)
    )
    pieces = lax.all_to_all(stacked, "vis", split_axis=2, concat_axis=0, tiled=True)
    return pieces.reshape(stripe, 2, piece_rows)


def image_from_pieces(piece_sum, band_count, group_count):
    stripe = piece_sum.shape[0]
    piece_rows = piece_sum.shape[2]
    piece_cols = stripe // group_count
    image_width = piece_rows * group_count
    rows_dev = image_width // (band_count * group_count)
    spread = lax.all_to_all(
        piece_sum.reshape(stripe, 2, 1, piece_rows), "vis", split_axis=0, concat_axis=2, tiled=True
    )
    spread = spread.reshape(piece_cols, 2, image_width)
    col_real, col_imag = dft_last(spread[:, 0], spread[:, 1], 1.0)
    stacked = jnp.transpose(jnp.stack([col_real, col_imag]), (0, 2, 1))
    shaped = stacked.reshape(2, band_count, group_count, rows_dev, 1, 1, piece_cols)
    moved = lax.all_to_all(
        lax.all_to_all(shaped, "band", split_axis=1, concat_axis=4, tiled=True),
        "vis",
        split_axis=2,
        concat_axis=5,
        tiled=True,
    )
    moved = moved.reshape(2, rows_dev, image_width)
    out_real, out_imag = dft_last(moved[0], moved[1], 1.0)
    return out_real


def cols_down(field):
    image_width = field.shape[1]
    extended = jnp.concatenate([field, field[:, :6]], axis=1)
    low_part = 0.0
    high_part = 0.0
    for offset in range(8):
        taken = extended[:, offset : offset + image_width : 2]
        low_part = low_part + low_taps[offset] * taken
        high_part = high_part + high_taps[offset] * taken
    return (low_part, high_part)


def cols_up(low_part, high_part):
    halves = []
    for parity in range(2):
        summed = 0.0
        for delay in range(4):
            summed = summed + low_taps[parity + 2 * delay] * jnp.roll(low_part, delay, axis=1)
            summed = summed + high_taps[parity + 2 * delay] * jnp.roll(high_part, delay, axis=1)
        halves.append(summed)
    return jnp.stack(halves, axis=2).reshape(low_part.shape[0], 2 * low_part.shape[1])


def rows_up(low_ext, high_ext, half_rows):
    halves = []
    for parity in range(2):
        summed = 0.0
        for delay in range(4):
            begin = 3 - delay
            summed = summed + low_taps[parity + 2 * delay] * low_ext[begin : begin + half_rows]
            summed = summed + high_taps[parity + 2 * delay] * high_ext[begin : begin + half_rows]
        halves.append(summed)
    return jnp.stack(halves, axis=1).reshape(2 * half_rows, low_ext.shape[1])


def analysis(extrap):
    rows_dev = extrap.shape[0]
    taken_rows = min(6, rows_dev)
    parts_list = [extrap]
    parts_list.append(shifted(extrap[:taken_rows], ("band", "vis"), -1))
    extended = jnp.concatenate(parts_list, axis=0)
    half_rows = rows_dev // 2
    rows_low = 0.0
    rows_high = 0.0
    for offset in range(8):
        taken = extended[offset : offset + 2 * half_rows : 2]
        rows_low = rows_low + low_taps[offset] * taken
        rows_high = rows_high + high_taps[offset] * taken
    low_low, low_high = cols_down(rows_low)
    high_low, high_high = cols_down(rows_high)
    return jnp.stack([low_low, low_high, high_low, high_high])


def synthesis(coef_dual):
    half_rows = coef_dual.shape[1]
    taken_rows = min(3, half_rows)
    parts_list = [shifted(coef_dual[:, half_rows - taken_rows :, :], ("band", "vis"), 1)]
    joined = jnp.concatenate(parts_list[::-1] + [coef_dual], axis=1)
    cols_low = rows_up(joined[0], joined[2], half_rows)
    cols_high = rows_up(joined[1], joined[3], half_rows)
    return cols_up(cols_low, cols_high)


def degrid(kernel_here, tiles):
    kernel_real = kernel_here[:, :, 0]
    kernel_imag = kernel_here[:, :, 1]
    tile_real = tiles[:, :, 0]
    tile_imag = tiles[:, :, 1]
    out_real = jnp.einsum(
        "qsat,qst->qsa", kernel_real, tile_real, preferred_element_type=jnp.float32
    ) - jnp.einsum("qsat,qst->qsa", kernel_imag, tile_imag, preferred_element_type=jnp.float32)
    out_imag = jnp.einsum(
        "qsat,qst->qsa", kernel_real, tile_imag, preferred_element_type=jnp.float32
    ) + jnp.einsum("qsat,qst->qsa", kernel_imag, tile_real, preferred_element_type=jnp.float32)
    return jnp.stack([out_real, out_imag], axis=2)


def grid_back(kernel_here, weights):
    kernel_real = kernel_here[:, :, 0]
    kernel_imag = kernel_here[:, :, 1]
    weight_real = weights[:, :, 0]
    weight_imag = weights[:, :, 1]
    grid_real = jnp.einsum(
        "qsat,qsa->qst", kernel_real, weight_real, preferred_element_type=jnp.float32
    ) + jnp.einsum("qsat,qsa->qst", kernel_imag, weight_imag, preferred_element_type=jnp.float32)
    grid_imag = jnp.einsum(
        "qsat,qsa->qst", kernel_real, weight_imag, preferred_element_type=jnp.float32
    ) - jnp.einsum("qsat,qsa->qst", kernel_imag, weight_real, preferred_element_type=jnp.float32)
    return jnp.stack([grid_real, grid_imag], axis=2)


def local(sky_image, coef_dual, vis_dual, visibilities, kernel_blocks, tile_rows, tile_counts):
    band_count = lax.axis_size("band")
    group_count = lax.axis_size("vis")
    kernel_here = kernel_blocks[0, 0]
    rows_here = tile_rows[0, 0]
    slot_count = rows_here.shape[1]
    live_slots = (
        jnp.arange(slot_count, dtype=jnp.int32)[None, :] < tile_counts[0, 0][:, None]
    ).astype(jnp.float32)[:, :, None, None]
    vis_data = visibilities[0, 0]
    vis_state = vis_dual[0, 0]
    image_width = sky_image.shape[1]
    stripe = image_width // band_count
    piece_rows = image_width // group_count
    incoming_rows = lax.all_to_all(rows_here, "vis", split_axis=0, concat_axis=0, tiled=True)
    data_part = jnp.sum(live_slots * vis_data * vis_data)
    weights = (live_slots * vis_state).astype(jnp.bfloat16)
    contrib = grid_back(kernel_here, weights)
    arrived = lax.all_to_all(contrib, "vis", split_axis=0, concat_axis=0, tiled=True)
    piece_sum = jax.ops.segment_sum(
        arrived.reshape(-1, 2, piece_rows), incoming_rows.reshape(-1), num_segments=stripe
    )
    adjoint_part = image_from_pieces(piece_sum, band_count, group_count)
    smooth = synthesis(coef_dual)
    new_image = jnp.maximum(sky_image - smooth - adjoint_part, 0.0)
    extrap = 2.0 * new_image - sky_image
    coeffs = analysis(extrap)
    abs_total = jnp.sum(jnp.abs(coeffs))
    coef_total = lax.psum(abs_total, ("band", "vis"))
    threshold = 0.5 * coef_total / (IMG * IMG)
    coef_dual = jnp.clip(coef_dual + coeffs, -threshold, threshold)
    piece_grid = pieces_from_image(extrap, band_count, group_count)
    tiles = lax.all_to_all(
        piece_grid[incoming_rows], "vis", split_axis=0, concat_axis=0, tiled=True
    )
    predicted = degrid(kernel_here, tiles)
    residual = live_slots * (vis_state + predicted - vis_data)
    resid_square = jnp.sum(residual * residual)
    norm_square, data_square = lax.psum((resid_square, data_part), ("band", "vis"))
    radius = 0.5 * jnp.sqrt(data_square + 1e-06)
    size_value = jnp.sqrt(norm_square + 1e-06)
    vis_state = residual * (1.0 - jnp.minimum(1.0, radius / size_value))
    return (new_image, coef_dual, vis_state[None, None])


high = lax.Precision.HIGH
everywhere = ("band", "vis")


def wave_tables(length, digit_low):
    digit_high = length // digit_low
    low = np.arange(digit_low)
    wide = np.arange(digit_high)
    full = 2.0 * np.pi
    small = full * (low[:, None] * low[None, :] % digit_low) / digit_low
    twist = full * (low[:, None] * wide[None, :]) / length
    large = full * (wide[:, None] * wide[None, :] % digit_high) / digit_high
    return small, twist, large


def complex_matrix(angle, sign):
    c = np.cos(angle)
    s = sign * np.sin(angle)
    return np.stack([np.stack([c, -s], axis=1), np.stack([s, c], axis=1)])


def f32(values):
    return jnp.asarray(np.asarray(values, np.float32))


def bf16(values):
    return f32(values).astype(jnp.bfloat16)


def analysis_matrix(half):
    matrix = np.zeros((2, half, 2 * half + 6))
    for k in range(half):
        for j in range(8):
            matrix[0, k, 2 * k + j] = low_taps[j]
            matrix[1, k, 2 * k + j] = high_taps[j]
    return matrix.reshape(2 * half, 2 * half + 6)


def synthesis_matrix(half):
    matrix = np.zeros((2 * half, 2, half + 3))
    for n in range(2 * half):
        for delay in range(4):
            tap = n % 2 + 2 * delay
            matrix[n, 0, n // 2 - delay + 3] = low_taps[tap]
            matrix[n, 1, n // 2 - delay + 3] = high_taps[tap]
    return matrix


def cos_sums(values, size):
    half = size // 2
    if half < 2:
        return [values[0] + values[1], values[0] - values[1]]
    quarter = half // 2
    plus = [values[a] + values[half - a] for a in range(quarter)] + [values[quarter]]
    minus = [values[a] - values[half - a] for a in range(quarter)]
    out = [None] * (half + 1)
    out[0::2] = cos_sums(plus, half)
    for k in range(1, half, 2):
        total = minus[0]
        for a in range(1, quarter):
            total = total + minus[a] * math.cos(2 * math.pi * (a * k % size) / size)
        out[k] = total
    return out


def sin_sums(values, size):
    half = size // 2
    if half < 2:
        return [None] * (half + 1)
    quarter = half // 2
    plus = {a: values[a] + values[half - a] for a in range(1, quarter)}
    plus[quarter] = values[quarter]
    minus = [None] + [values[a] - values[half - a] for a in range(1, quarter)]
    out = [None] * (half + 1)
    out[0::2] = sin_sums(minus, half)
    for k in range(1, half, 2):
        total = None
        for a in range(1, quarter + 1):
            factor = math.sin(2 * math.pi * (a * k % size) / size)
            term = plus[a] if a * 4 == size and k % 4 == 1 else plus[a] * factor
            total = term if total is None else total + term
        out[k] = total
    return out


def even_odd(values):
    size = len(values)
    half = size // 2
    even = [values[0]] + [values[a] + values[size - a] for a in range(1, half)] + [values[half]]
    odd = [None] + [values[a] - values[size - a] for a in range(1, half)]
    return even, odd


def split(values):
    upper = values.astype(jnp.bfloat16)
    return upper, (values - upper.astype(jnp.float32)).astype(jnp.bfloat16)


def table_pair(values):
    upper = f32(values).astype(jnp.bfloat16)
    return upper, (f32(values) - upper.astype(jnp.float32)).astype(jnp.bfloat16)


def nt_dot(a, b):
    return lax.dot_general(a, b, (((1,), (1,)), ((), ())), preferred_element_type=jnp.float32)


def nn_dot(a, b):
    return lax.dot_general(a, b, (((1,), (0,)), ((), ())), preferred_element_type=jnp.float32)


LEVELS = 32000.0
MESH = pl.DeviceIdType.MESH
LANES = 128
whole = pl.BlockSpec(memory_space=pltpu.VMEM)


def place():
    band = lax.axis_index("band")
    vis = lax.axis_index("vis")
    groups = lax.axis_size("vis")
    z = vis // 4
    y = vis // 2 % 2
    core = vis % 2
    return band, z, y, core, groups


def taps_dot(values, tables):
    upper, lower = split(values)
    return nn_dot(upper, tables[0]) + nn_dot(lower, tables[0]) + nn_dot(upper, tables[1])


def level(values):
    return jnp.round(values).astype(jnp.int32)


def step_kernel(
    low,
    kernels_hbm,
    coef_hbm,
    sky_hbm,
    up_hbm,
    edge_hbm,
    base_hbm,
    spin_hbm,
    inv_hbm,
    fwd_hbm,
    near_hbm,
    next_hbm,
    half_base_hbm,
    half_spin_hbm,
    order_hbm,
    state_ref,
    data_ref,
    rows_ref,
    counts_ref,
    phase_ref,
    shift_ref,
    tw_ref,
    image_hbm,
    coef_out_hbm,
    vis_out_ref,
    kernels_ref,
    joined_ref,
    sky_ref,
    merged_ref,
    up_ref,
    edge_ref,
    base_ref,
    spin_ref,
    inv_ref,
    fwd_ref,
    near_ref,
    next_ref,
    half_base_ref,
    half_spin_ref,
    order_ref,
    load_sem,
    tail_ref,
    halo_ref,
    block_ref,
    all_cols_ref,
    turn_ref,
    total_ref,
    tall_ref,
    smooth_ref,
    fold_ref,
    grid_ref,
    hot_ref,
    half_ref,
    spec_ref,
    rest_ref,
    extrap_ref,
    picked_ref,
    unit_ref,
    got_ref,
    units_ref,
    sum_table_ref,
    terms_ref,
    own_ref,
    sums_out_ref,
    sums_unit_ref,
    sums_got_ref,
    sums_units_ref,
    all_abs_ref,
    all_sums_ref,
    send_a,
    send_b,
    recv_a,
    recv_b,
    send_p,
    send_u,
    recv_p,
    recv_u,
    send_z,
    recv_z,
    send_w,
    recv_w,
    send_t,
    recv_t,
    send_s,
    recv_s,
    halo_sem,
):
    x, z, y, core, groups = place()
    levels = groups // 4
    devices = 2 * groups
    half_rows, half_width = coef_hbm.shape[1:]
    rows = 2 * half_rows
    tiles = block_ref.shape[1]
    kept = low // 2 + 1
    wide = LANES

    def index(px, pz, py, pc):
        return px * groups + pz * 4 + py * 2 + pc

    def device(px, pz, py, pc):
        return (px, pz * 4 + py * 2 + pc)

    def ident(number):
        return (number // groups, number % groups)

    def remote(src, dst, send, recv, target):
        return pltpu.make_async_remote_copy(
            src_ref=src,
            dst_ref=dst,
            send_sem=send,
            recv_sem=recv,
            device_id=target,
            device_id_type=MESH,
        )

    me = index(x, z, y, core)
    after, before = (me + 1) % devices, (me + devices - 1) % devices
    twin = device(x, z, y, 1 - core)
    line = [device(x, (z + k) % levels, y, core) for k in range(1, levels)]
    corners = [(1 - x, y), (x, 1 - y), (1 - x, 1 - y)]
    plane = [device(px, z, py, core) for px, py in corners]
    barrier = pltpu.get_barrier_semaphore()
    peers = line + plane + [twin, ident(after), ident(before)]
    for peer in peers:
        pl.semaphore_signal(barrier, inc=1, device_id=peer, device_id_type=MESH)

    sources = [
        (kernels_hbm, kernels_ref),
        (coef_hbm, joined_ref.at[:, pl.ds(8, half_rows), :]),
        (up_hbm, up_ref),
        (edge_hbm, edge_ref),
        (base_hbm, base_ref),
        (spin_hbm, spin_ref),
        (inv_hbm, inv_ref),
        (sky_hbm, sky_ref),
        (fwd_hbm, fwd_ref),
        (near_hbm, near_ref),
        (next_hbm, next_ref),
        (half_base_hbm, half_base_ref),
        (half_spin_hbm, half_spin_ref),
        (order_hbm, order_ref),
    ]
    loads = [
        pltpu.make_async_copy(src, dst, load_sem.at[i]) for i, (src, dst) in enumerate(sources)
    ]
    for load in loads:
        load.start()
    loads[0].wait()
    count = 16
    span = kernels_ref.shape[0] * count // tiles
    width = low * wide
    stripe = width // 2
    slots = rows_ref.shape[0]
    lane = lax.broadcasted_iota(jnp.int32, (tiles, groups), 1)
    tile_id = lax.broadcasted_iota(jnp.int32, (tiles, groups), 0)
    counts = jnp.where(lane == tile_id // slots, counts_ref[...].astype(jnp.float32), 0.0)
    counts = jnp.sum(counts, axis=1, keepdims=True)
    tile_id = lax.broadcasted_iota(jnp.int32, (tiles, 1), 0)
    live = jnp.where((tile_id % slots).astype(jnp.float32) < counts, 1.0, 0.0)
    state = [state_ref[:, part, :] for part in range(2)]
    data = [data_ref[:, part, :] for part in range(2)]
    ours = [part * live for part in state]
    turned = [ours[0], ours[1], ours[0], ours[1]], [ours[1], -ours[0], ours[1], -ours[0]]
    turned = [jnp.concatenate(parts, axis=1) for parts in turned]
    pair_lane = lax.broadcasted_iota(jnp.int32, (count, LANES), 1) // (LANES // 2)
    pair_row = lax.broadcasted_iota(jnp.int32, (count, LANES), 0)
    masks = [pair_lane + 2 * k == pair_row for k in range(count // 2)]
    for i in range(tiles // count):
        spread = [
            jnp.concatenate(
                [jnp.where(mask, part[i * count : (i + 1) * count], 0.0) for mask in masks], axis=1
            )
            for part in turned
        ]
        spread = jnp.concatenate(spread, axis=0).astype(jnp.bfloat16)
        both = nn_dot(spread, kernels_ref[i * span : (i + 1) * span, :])
        both = jnp.concatenate([both[:count], both[count:]], axis=1)
        block_ref[me, i * count : (i + 1) * count, :] = both.astype(jnp.bfloat16)
    lane = lax.broadcasted_iota(jnp.int32, (groups, LANES), 1) % tiles
    owner = lax.broadcasted_iota(jnp.int32, (groups, LANES), 0)
    columns = 0.0
    by_owner = rows_ref[...].astype(jnp.float32).T
    for slot in range(slots):
        here = by_owner[:, slot : slot + 1]
        columns = columns + jnp.where(lane == owner * slots + slot, here, 0.0)
    columns = jnp.sum(columns, axis=0, keepdims=True).astype(jnp.int32)
    all_cols_ref[me] = columns + x * stripe
    loads[1].wait()
    for c in range(4):
        tail_ref[3 * c : 3 * c + 3, :] = joined_ref[c, half_rows + 5 :, :]
    pl.semaphore_wait(barrier, len(peers))

    started = []

    def start(block, target, slot):
        own_a, own_b = block_ref.at[block], all_cols_ref.at[block]
        for own, send, recv in ((own_a, send_a, recv_a), (own_b, send_b, recv_b)):
            copy = remote(own, own, send.at[slot], recv.at[block], target)
            copy.start()
            started.append(copy)

    def got(block):
        for ref, send, recv in ((block_ref, send_a, recv_a), (all_cols_ref, send_b, recv_b)):
            own = ref.at[block]
            remote(own, own, send.at[0], recv.at[block], twin).wait_recv()

    slots_of = iter(range(send_a.shape[0]))
    far = sorted(range(1, levels), key=lambda k: abs(k - levels / 2))
    for k in far:
        start(me, line[k - 1], next(slots_of))
    for target in plane:
        start(me, target, next(slots_of))
    edge = remote(tail_ref, halo_ref, halo_sem.at[0], halo_sem.at[1], ident(after))
    edge.start()
    start(me, twin, next(slots_of))
    for load in loads[2:8]:
        load.wait()
    piece = kernels_ref.shape[1]
    spin_cos, spin_sin = spin_ref[0, pl.ds(me, 1), :], spin_ref[1, pl.ds(me, 1), :]
    cosine = (base_ref[0] * spin_cos - base_ref[1] * spin_sin).astype(jnp.bfloat16)
    sine = (base_ref[1] * spin_cos + base_ref[0] * spin_sin).astype(jnp.bfloat16)
    turn_ref[:rows, :piece] = cosine
    turn_ref[:rows, piece:] = -sine
    turn_ref[rows:, :piece] = sine
    turn_ref[rows:, piece:] = cosine
    line_blocks = [index(x, (z + levels - k) % levels, y, core) for k in far]
    for block in line_blocks:
        got(block)
        for target in plane:
            start(block, target, next(slots_of))
        start(block, twin, next(slots_of))
    for px, py in corners:
        block = index(px, z, py, core)
        got(block)
        start(block, twin, next(slots_of))
    edge.wait()
    for c in range(4):
        joined_ref[c, 5:8, :] = halo_ref[3 * c : 3 * c + 3, :]
    strips = half_width // LANES

    def tall(i, carry):
        here = pl.ds(pl.multiple_of(i * LANES, LANES), LANES)
        for c in range(2):
            for k in range(half_rows // 8):
                lows = [joined_ref[c, 8 + 8 * k - d : 16 + 8 * k - d, here] for d in range(4)]
                highs = [joined_ref[c + 2, 8 + 8 * k - d : 16 + 8 * k - d, here] for d in range(4)]
                for parity in range(2):
                    total = 0.0
                    for d in range(4):
                        total = total + low_taps[parity + 2 * d] * lows[d]
                        total = total + high_taps[parity + 2 * d] * highs[d]
                    tall_ref[c * strips + i, pl.ds(16 * k + parity, 8, stride=2), :] = total
        return carry

    lax.fori_loop(0, strips, tall, 0)


    def broad(i, carry):
        there = (i + strips - 1) % strips
        near = jnp.concatenate([tall_ref[i], tall_ref[strips + i]], axis=1)
        last = jnp.concatenate([tall_ref[there], tall_ref[strips + there]], axis=1)
        out = taps_dot(near, up_ref)
        first = taps_dot(last, edge_ref)
        smooth_ref[2 * i] = out[:, :LANES] + first
        smooth_ref[2 * i + 1] = out[:, LANES:]
        return carry

    lax.fori_loop(0, strips // 2, broad, 0)
    for n, k in enumerate(far):
        for px, py in corners:
            block = index(px, (z + levels - k) % levels, py, core)
            got(block)
            start(block, twin, next(slots_of))
        if n == 0:
            lax.fori_loop(strips // 2, strips, broad, 0)

    total_tiles = devices * tiles
    class_tiles = groups * tiles
    parts = class_tiles // LANES
    lane = lax.broadcasted_iota(jnp.int32, (1, LANES), 1)

    def spread(c, levels_taken):
        for zz in levels_taken:
            for side in range(2):
                b = c * parts + zz * 2 + side
                first = side * groups + zz * 4 + c
                columns = jnp.where(lane < tiles, all_cols_ref[first], all_cols_ref[first + 2])
                k1 = columns % low
                k2 = columns // low
                flip = k1 >= kept
                k1 = jnp.where(flip, low - k1, k1)
                k2 = jnp.where(flip, wide - 1 - k2, k2)
                fold_ref[0, pl.ds(b, 1), :] = (k1 * wide + k2).astype(jnp.float32)
                fold_ref[1, pl.ds(b, 1), :] = jnp.where(flip, -1.0, 1.0)
            some = [block_ref[i // 2 * groups + zz * 4 + i % 2 * 2 + c] for i in range(4)]
            both = nt_dot(turn_ref[...], jnp.concatenate(some, axis=0))
            for side in range(2):
                b = c * parts + zz * 2 + side
                at = pl.ds(pl.multiple_of(b * LANES, LANES), LANES)
                real = both[:rows, side * LANES : (side + 1) * LANES]
                imag = both[rows:, side * LANES : (side + 1) * LANES]
                sign = fold_ref[1, pl.ds(b, 1), :]
                out_real = real * phase_ref[0] - imag * phase_ref[1]
                out_imag = (real * phase_ref[1] + imag * phase_ref[0]) * sign
                grid_ref[:rows, at] = out_real.astype(jnp.bfloat16)
                grid_ref[rows:, at] = out_imag.astype(jnp.bfloat16)

    def folded_sum(c, p):
        base = pl.multiple_of(p * 2 * wide, 2 * wide)
        row = (lax.broadcasted_iota(jnp.int32, (2 * wide, LANES), 0) + base).astype(jnp.float32)
        hots = []
        for i in range(parts):
            hit = row == fold_ref[0, pl.ds(c * parts + i, 1), :]
            hots.append(jnp.where(hit, 1.0, 0.0).astype(jnp.bfloat16))
        hot = jnp.concatenate(hots, axis=1)
        at = pl.ds(pl.multiple_of(c * class_tiles, class_tiles), class_tiles)
        hot_ref[pl.ds(base, 2 * wide), at] = hot
        return nt_dot(grid_ref[:, at], hot)

    everything = list(range(levels))
    spread(core, everything)

    def scatter_own(p, carry):
        total_ref[p] = folded_sum(core, p)
        return carry

    lax.fori_loop(0, (kept + 1) // 2, scatter_own, 0)
    coming = [z] + [(z + levels - k) % levels for k in far]

    def from_twin(zz):
        for i in range(4):
            got(i // 2 * groups + zz * 4 + i % 2 * 2 + 1 - core)

    for zz in coming:
        from_twin(zz)
    spread(1 - core, everything)

    def scatter(p, carry):
        folded = (total_ref[p] + folded_sum(1 - core, p)).astype(jnp.bfloat16)
        pairs = []
        for e in range(2):
            here = slice(e * wide, (e + 1) * wide)
            pairs.append(jnp.concatenate([folded[:rows, here], folded[rows:, here]], axis=1))
        mids = nn_dot(jnp.concatenate(pairs, axis=0), inv_ref[...])
        for e in range(2):
            mid = mids[e * rows : (e + 1) * rows]
            k1 = p * 2 + e
            tw_real, tw_imag = tw_ref[0, pl.ds(k1, 1), :], tw_ref[1, pl.ds(k1, 1), :]
            real, imag = mid[:, :wide], mid[:, wide:]
            half_ref[k1, :, :wide] = real * tw_real - imag * tw_imag
            half_ref[k1, :, wide:] = real * tw_imag + imag * tw_real
        return carry

    lax.fori_loop(0, (kept + 1) // 2, scatter, 0)

    def strip(i, carry):
        at = pl.ds(pl.multiple_of(i * 8, 8), 8)
        cos_part = cos_sums([half_ref[k, at, :wide] for k in range(kept)], low)
        sin_part = sin_sums([None] + [half_ref[k, at, wide:] for k in range(1, kept - 1)], low)
        extraps = []
        for a in range(low):
            k = min(a, low - a)
            if a == 0 or a == low // 2:
                adjoint = cos_part[k]
            elif a < low // 2:
                adjoint = cos_part[k] - sin_part[k]
            else:
                adjoint = cos_part[k] + sin_part[k]
            here = slice(a * wide, (a + 1) * wide)
            sky = sky_ref[at, here]
            image = jnp.maximum(sky - smooth_ref[a, at, :] - adjoint, 0.0)
            extrap = 2.0 * image - sky
            sky_ref[at, here] = image
            extrap_ref[a, at, :] = extrap
            extraps.append(extrap)
        even, odd = even_odd(extraps)
        real_part = cos_sums(even, low)
        imag_part = sin_sums(odd, low)
        for k in range(kept):
            tw_real, tw_imag = tw_ref[0, k : k + 1, :], tw_ref[1, k : k + 1, :]
            real = real_part[k] * tw_real
            imag = -real_part[k] * tw_imag
            if 0 < k < kept - 1:
                real = real - imag_part[k] * tw_imag
                imag = imag - imag_part[k] * tw_real
            half_ref[k, at, :wide] = real
            half_ref[k, at, wide:] = imag
        return carry

    lax.fori_loop(0, rows // 8, strip, 0)
    store = pltpu.make_async_copy(sky_ref, image_hbm, load_sem.at[len(loads)])
    store.start()
    top = remote(
        extrap_ref.at[:, pl.ds(0, 8), :],
        extrap_ref.at[:, pl.ds(rows, 8), :],
        halo_sem.at[2],
        halo_sem.at[3],
        ident(before),
    )
    top.start()
    loads[8].wait()

    batch = (kept + 1) // 3

    def spectrum(i, carry):
        some = half_ref[pl.ds(i * batch, batch)].reshape(batch * rows, 2 * wide)
        out = taps_dot(some, fwd_ref)
        for e in range(batch):
            here = pl.ds(pl.multiple_of((i * batch + e) * wide, wide), wide)
            upper, lower = split(out[e * rows : (e + 1) * rows])
            spec_ref[:rows, here] = upper[:, :wide]
            spec_ref[rows:, here] = upper[:, wide:]
            rest_ref[:rows, here] = lower[:, :wide]
            rest_ref[rows:, here] = lower[:, wide:]
        return carry

    lax.fori_loop(0, 3, spectrum, 0)

    mate = x * 4 + y * 2 + core

    def sends(to_z, to_x, to_y, to_class):
        at = to_class * class_tiles + (to_z * 4 + to_x * 2 + to_y) * tiles
        at = pl.ds(pl.multiple_of(at, tiles), tiles)
        unit = unit_ref.at[to_class * parts + to_z * 2 + to_x]
        spot, target = to_z * 8 + mate, device(to_x, z, to_y, to_class)
        return [
            remote(picked_ref.at[at, :], got_ref.at[spot], send_p.at[0], recv_p.at[to_z], target),
            remote(unit, units_ref.at[spot], send_u.at[0], recv_u.at[to_z], target),
        ]

    def total_of(ref, send, recv, count=devices - 1, at=0):
        some = ref.at[pl.ds(0, count)]
        return remote(some, some, send.at[0], recv.at[at], twin)

    def share_row(ref, send, recv):
        def one(k, carry):
            to = (me + k) % devices
            remote(ref.at[me], ref.at[me], send.at[0], recv.at[0], ident(to)).start()
            return carry

        lax.fori_loop(1, devices, one, 0)

    def row_total(ref):
        total = ref[0]
        for d in range(1, devices):
            total = total + ref[d]
        return total

    def ordered(n):
        return (z // 2 + 1 + n // 2) % 2 * 2 + (z + 1 + n) % 2

    def pick(s, carry):
        to_z = ordered(s // 2)
        to_class = (core + 1 + s) % 2
        j = to_class * 4 + to_z
        at = pl.multiple_of(j * 2 * LANES, 2 * LANES)
        hot = hot_ref[: kept * wide, pl.ds(at, 2 * LANES)]
        both = nn_dot(spec_ref[:, : kept * wide], hot) + nn_dot(rest_ref[:, : kept * wide], hot)
        for h in range(2):
            sign = fold_ref[1, pl.ds(2 * j + h, 1), :]
            real = both[:rows, h * LANES : (h + 1) * LANES]
            imag = both[rows:, h * LANES : (h + 1) * LANES] * sign
            most = jnp.max(jnp.maximum(jnp.abs(real), jnp.abs(imag)), axis=0, keepdims=True)
            most = jnp.maximum(most, 1e-30)
            unit_ref[2 * j + h] = most * (1.0 / LEVELS)
            to_level = LEVELS / most
            packed = level(real * to_level) * 65536 + level(imag * to_level)
            to = pl.ds(pl.multiple_of(at + h * LANES, LANES), LANES)
            picked_ref[to, :] = packed.T
        for to_x in range(2):
            for to_y in range(2):
                away = (to_x - x) * (to_x - x) + (to_y - y) * (to_y - y)

                @pl.when(away + (to_class - core) * (to_class - core) != 0)
                def _():
                    for copy in sends(to_z, to_x, to_y, to_class):
                        copy.start()

        return carry

    lax.fori_loop(0, devices // 4, pick, 0)
    for load in loads[11:13]:
        load.wait()
    for n in range(4):
        spin_cos, spin_sin = half_spin_ref[0, n : n + 1, :], half_spin_ref[1, n : n + 1, :]
        cosine = half_base_ref[0] * spin_cos - half_base_ref[1] * spin_sin
        sine = half_base_ref[1] * spin_cos + half_base_ref[0] * spin_sin
        for p in range(2):
            part = slice(p * LANES, (p + 1) * LANES)
            c, d = split(cosine[:, part]), split(sine[:, part])
            real_rows = slice(2 * n * rows, (2 * n + 1) * rows)
            imag_rows = slice((2 * n + 1) * rows, (2 * n + 2) * rows)
            for e in range(2):
                sum_table_ref[e, p, real_rows, :LANES] = c[e]
                sum_table_ref[e, p, real_rows, LANES:] = -d[e]
                sum_table_ref[e, p, imag_rows, :LANES] = d[e]
                sum_table_ref[e, p, imag_rows, LANES:] = c[e]
    for to_z in range(levels):
        at = core * class_tiles + (to_z * 4 + x * 2 + y) * tiles
        got_ref[to_z * 8 + mate] = picked_ref[pl.ds(pl.multiple_of(at, tiles), tiles), :]
        units_ref[to_z * 8 + mate] = unit_ref[core * parts + to_z * 2 + x]
    top.wait()
    loads[9].wait()
    loads[10].wait()

    def rows_down(i, carry):
        for k in range(half_rows // 8):
            lows, highs = 0.0, 0.0
            for tap in range(8):
                taken = extrap_ref[i, pl.ds(16 * k + tap, 8, stride=2), :]
                lows = lows + low_taps[tap] * taken
                highs = highs + high_taps[tap] * taken
            tall_ref[i, 8 * k : 8 * k + 8, :] = lows
            tall_ref[i, half_rows + 8 * k : half_rows + 8 * k + 8, :] = highs
        return carry

    lax.fori_loop(0, low, rows_down, 0)

    def cols_down(b, absolute):
        here = jnp.concatenate([tall_ref[2 * b], tall_ref[2 * b + 1]], axis=1)
        out = taps_dot(here, near_ref) + taps_dot(tall_ref[(2 * b + 2) % low], next_ref)
        at = pl.ds(pl.multiple_of(b * LANES, LANES), LANES)
        for c in range(4):
            top_row, left = c // 2 * half_rows, c % 2 * LANES
            part = out[top_row : top_row + half_rows, left : left + LANES]
            absolute = absolute + jnp.abs(part)
            merged_ref[c, :, at] = joined_ref[c, 8:, at] + part
        return absolute

    def plane_sums(taken):
        many = len(taken) * tiles
        rows_of = []
        for zz in taken:
            total_of(got_ref, send_p, recv_p, 7, zz).wait_recv()
            total_of(units_ref, send_u, recv_u, 7, zz).wait_recv()
            rows_of += [units_ref[zz * 8 + m] for m in range(8)]
        units = jnp.concatenate(rows_of * (LANES // len(rows_of)), axis=0).T
        units = jnp.where(y == 0, units[:tiles], units[tiles:])
        cosine, sine = shift_ref[0], shift_ref[1]
        level_cos = half_spin_ref[0, pl.ds(4 * z, 1), :]
        level_sin = half_spin_ref[1, pl.ds(4 * z, 1), :]
        for e, zz in enumerate(taken):
            strip_rows = slice(e * tiles, (e + 1) * tiles)
            for pair in range(4):
                reals, imags = [], []
                for side in range(2):
                    m = side * 4 + pair
                    packed = got_ref[zz * 8 + m]
                    real = (packed + 32768) >> 16
                    imag = packed - (real << 16)
                    unit = units[:, e * 8 + m : e * 8 + m + 1]
                    real = real.astype(jnp.float32) * unit
                    imag = imag.astype(jnp.float32) * unit
                    reals.append(real * cosine + imag * sine)
                    imags.append(imag * cosine - real * sine)
                at = 2 * pair * LANES
                for p, values in ((0, (reals[0] + reals[1], imags[0] + imags[1])),
                                  (1, (reals[0] - reals[1], imags[0] - imags[1]))):
                    for part in range(2):
                        upper, lower = split(values[part])
                        here = slice(at + part * LANES, at + (part + 1) * LANES)
                        terms_ref[0, p, strip_rows, here] = upper
                        terms_ref[1, p, strip_rows, here] = lower
        reals, imags = [], []
        for p in range(2):
            out = nn_dot(terms_ref[0, p, :many], sum_table_ref[0, p])
            out = out + nn_dot(terms_ref[1, p, :many], sum_table_ref[0, p])
            out = out + nn_dot(terms_ref[0, p, :many], sum_table_ref[1, p])
            part = slice(p * LANES, (p + 1) * LANES)
            turn_cos, turn_sin = level_cos[:, part], level_sin[:, part]
            real, imag = out[:, :LANES], out[:, LANES:]
            reals.append(real * turn_cos + imag * turn_sin)
            imags.append(imag * turn_cos - real * turn_sin)
        real = jnp.concatenate(reals, axis=1)
        imag = jnp.concatenate(imags, axis=1)
        most = jnp.max(jnp.maximum(jnp.abs(real), jnp.abs(imag)), axis=1, keepdims=True)
        most = jnp.maximum(most, 1e-30)
        to_level = LEVELS / most
        packed = level(real * to_level) * 65536 + level(imag * to_level)
        unit = most * (1.0 / LEVELS)
        for e, zz in enumerate(taken):
            strip_rows = slice(e * tiles, (e + 1) * tiles)
            if zz is z:
                own_ref[:, : 2 * LANES] = real[strip_rows]
                own_ref[:, 2 * LANES :] = imag[strip_rows]
                continue
            sums_out_ref[zz] = packed[strip_rows]
            wide_unit = jnp.broadcast_to(unit[strip_rows], (tiles, LANES))
            sums_unit_ref[zz] = jnp.concatenate([wide_unit, wide_unit], axis=0).T[:1]
            target = device(x, zz, y, core)
            remote(
                sums_out_ref.at[zz], sums_got_ref.at[z], send_z.at[0], recv_z.at[0], target
            ).start()
            remote(
                sums_unit_ref.at[zz], sums_units_ref.at[z], send_w.at[0], recv_w.at[0], target
            ).start()

    plane_sums([ordered(0), ordered(1)])
    absolute = jnp.zeros((half_rows, LANES), jnp.float32)
    absolute = lax.fori_loop(0, low // 4, cols_down, absolute)
    plane_sums([ordered(2), z])
    absolute = lax.fori_loop(low // 4, low // 2, cols_down, absolute)
    abs_total = jnp.sum(jnp.sum(absolute, axis=0, keepdims=True), axis=1, keepdims=True)
    loads[13].wait()

    lane = lax.broadcasted_iota(jnp.int32, (1, LANES), 1)
    all_abs_ref[me] = jnp.where(lane == 0, abs_total, 0.0)
    share_row(all_abs_ref, send_t, recv_t)
    total_of(sums_got_ref, send_z, recv_z, levels - 1).wait_recv()
    total_of(sums_units_ref, send_w, recv_w, levels - 1).wait_recv()
    units = [sums_units_ref[(z + k) % levels] for k in range(1, levels)]
    units = jnp.concatenate(units + [units[0]] * (LANES - levels + 1), axis=0).T
    units = units[:tiles]
    real, imag = own_ref[:, : 2 * LANES], own_ref[:, 2 * LANES :]
    for k in range(1, levels):
        packed = sums_got_ref[(z + k) % levels]
        upper = (packed + 32768) >> 16
        lower = packed - (upper << 16)
        unit = units[:, k - 1 : k]
        real = real + upper.astype(jnp.float32) * unit
        imag = imag + lower.astype(jnp.float32) * unit
    tile = jnp.concatenate([real, imag], axis=1).astype(jnp.bfloat16)
    tile = nn_dot(tile, order_ref[...]).astype(jnp.bfloat16)
    first, second = [], []
    near_row = pair_row % 2 == 0
    for i in range(tiles // count):
        here = tile[i * count : (i + 1) * count]
        pair = jnp.concatenate([here[:, :piece], here[:, piece:]], axis=0)
        out = nt_dot(pair, kernels_ref[i * span : (i + 1) * span, :])
        for found, half in ((first, out[:count]), (second, out[count:])):
            total = 0.0
            for k in range(count // 2):
                total = total + jnp.where(
                    pair_row // 2 == k, half[:, k * LANES : (k + 1) * LANES], 0.0
                )
            found.append(jnp.where(near_row, total, pltpu.roll(total, LANES // 2, 1)))
    first = jnp.concatenate(first, axis=0)
    second = jnp.concatenate(second, axis=0)
    visits = state_ref.shape[2]
    lane = lax.broadcasted_iota(jnp.int32, first.shape, 1)
    crossed = jnp.where(
        lane // visits % 2 == 0,
        -pltpu.roll(second, LANES - visits, 1),
        pltpu.roll(second, visits, 1),
    )
    keep = jnp.where(lane < 2 * visits, live, 0.0)
    state_wide = jnp.concatenate(state + state, axis=1)
    data_wide = jnp.concatenate(data + data, axis=1)
    residual = keep * (state_wide + first + crossed - data_wide)
    norms = []
    for values in (residual, data_wide * keep):
        norms.append(jnp.sum(jnp.sum(values * values, axis=0, keepdims=True), axis=1, keepdims=True))
    lane = lax.broadcasted_iota(jnp.int32, (1, LANES), 1)
    all_sums_ref[me] = jnp.where(lane == 0, norms[0], norms[1])
    share_row(all_sums_ref, send_s, recv_s)
    total_of(all_abs_ref, send_t, recv_t).wait_recv()
    threshold = 0.5 * row_total(all_abs_ref)[:, 0:1] / (width * width)

    def clip(i, carry):
        at = pl.ds(pl.multiple_of(i * LANES, LANES), LANES)
        for c in range(4):
            merged_ref[c, :, at] = jnp.clip(merged_ref[c, :, at], -threshold, threshold)
        return carry

    lax.fori_loop(0, half_width // LANES, clip, 0)
    store_coef = pltpu.make_async_copy(merged_ref, coef_out_hbm, load_sem.at[len(loads) + 1])
    store_coef.start()
    for copy in started:
        copy.wait_send()
    total_of(got_ref, send_p, recv_p, 28).wait_send()
    total_of(units_ref, send_u, recv_u, 28).wait_send()
    total_of(sums_got_ref, send_z, recv_z, levels - 1).wait_send()
    total_of(sums_units_ref, send_w, recv_w, levels - 1).wait_send()
    total_of(all_abs_ref, send_t, recv_t).wait_send()
    total_of(all_sums_ref, send_s, recv_s).wait()
    total = row_total(all_sums_ref)
    size = jnp.sqrt(total[:, 0:1] + 1e-06)
    radius = 0.5 * jnp.sqrt(total[:, 1:2] + 1e-06)
    residual = residual * (1.0 - jnp.minimum(1.0, radius / size))
    vis_out_ref[:, 0, :] = residual[:, :visits]
    vis_out_ref[:, 1, :] = residual[:, visits : 2 * visits]
    store.wait()
    store_coef.wait()


def step(kernels, coef, sky, state, data, tile_rows, tile_counts, groups, devices):
    rows, width = sky.shape
    piece = kernels.shape[1]
    slots = tile_rows.shape[0]
    tiles = groups * slots
    half_rows, half_width = coef.shape[1:]
    low = width // LANES
    kept = low // 2 + 1
    wide = np.arange(LANES)
    matrix = synthesis_matrix(LANES)
    up = matrix[:, :, 3:].transpose(1, 2, 0).reshape(2 * LANES, 2 * LANES)
    edge = np.zeros((2, LANES, LANES))
    edge[:, LANES - 3 :, :] = matrix[:LANES, :, :3].transpose(1, 2, 0)
    matrix = analysis_matrix(LANES).T
    following = np.zeros((LANES, 2 * LANES))
    following[:6] = matrix[2 * LANES :]
    turn = np.arange(piece)
    base = 2 * np.pi * np.arange(rows)[:, None] * turn[None, :] / width
    spin = 2 * np.pi * (np.arange(devices)[:, None] * turn[None, :] % devices) / devices
    owner = wide // slots % groups
    shift = 2 * np.pi * (np.arange(rows)[:, None] * owner[None, :] % groups) / groups
    phase = np.stack([np.cos(shift), np.sin(shift)])
    full = 2 * np.pi * (wide[:, None] * wide[None, :] % LANES) / LANES
    c, s = np.cos(full) / width, np.sin(full) / width
    inverse = np.block([[c, s], [-s, c]])
    forward = np.block([[c, -s], [s, c]])
    twist = 2 * np.pi * np.arange(kept + 1)[:, None] * wide[None, :] / width
    halves = np.concatenate([turn[0::2], turn[1::2]])
    half_base = 2 * np.pi * np.arange(rows)[:, None] * halves[None, :] / width
    half_spin = 2 * np.pi * (np.arange(devices)[:, None] * halves[None, :] % devices) / devices
    order = np.zeros((2 * piece, 2 * piece))
    for part in range(2):
        order[part * piece + np.arange(piece), part * piece + halves] = 1.0
    loaded = [
        kernels,
        coef,
        sky,
        jnp.stack(table_pair(up)),
        jnp.stack(table_pair(edge.reshape(2 * LANES, LANES))),
        f32(np.stack([np.cos(base), np.sin(base)])),
        f32(np.stack([np.cos(spin), np.sin(spin)])),
        bf16(inverse),
        jnp.stack(table_pair(forward)),
        jnp.stack(table_pair(matrix[: 2 * LANES])),
        jnp.stack(table_pair(following)),
        f32(np.stack([np.cos(half_base), np.sin(half_base)])),
        f32(np.stack([np.cos(half_spin), np.sin(half_spin)])),
        bf16(order),
    ]
    held = [
        state,
        data,
        tile_rows,
        tile_counts,
        f32(phase),
        f32(phase[:, :, :tiles].transpose(0, 2, 1)),
        f32(np.stack([np.cos(twist), np.sin(twist)])),
    ]
    buffers = [pltpu.VMEM(value.shape, value.dtype) for value in loaded]
    buffers[1] = pltpu.VMEM((4, half_rows + 8, half_width), jnp.float32)
    copies = 3 * 4 + 7 + 12
    dma = pltpu.SemaphoreType.DMA
    anywhere = pl.BlockSpec(memory_space=pltpu.HBM)
    return pl.pallas_call(
        lambda *refs: step_kernel(low, *refs),
        out_shape=(
            jax.ShapeDtypeStruct((rows, width), jnp.float32),
            jax.ShapeDtypeStruct(coef.shape, jnp.float32),
            jax.ShapeDtypeStruct(state.shape, jnp.float32),
        ),
        in_specs=[anywhere] * len(loaded) + [whole] * len(held),
        out_specs=(anywhere, anywhere, whole),
        scratch_shapes=buffers[:3]
        + [pltpu.VMEM(coef.shape, jnp.float32)]
        + buffers[3:]
        + [
            dma((len(loaded) + 2,)),
            pltpu.VMEM((16, half_width), jnp.float32),
            pltpu.VMEM((16, half_width), jnp.float32),
            pltpu.VMEM((devices, tiles, 2 * piece), jnp.bfloat16),
            pltpu.VMEM((devices, 1, LANES), jnp.int32),
            pltpu.VMEM((2 * rows, 2 * piece), jnp.bfloat16),
            pltpu.VMEM(((kept + 1) // 2, 2 * rows, 2 * LANES), jnp.float32),
            pltpu.VMEM((low, rows, LANES), jnp.float32),
            pltpu.VMEM((low, rows, LANES), jnp.float32),
            pltpu.VMEM((2, devices // 2, LANES), jnp.float32),
            pltpu.VMEM((2 * rows, devices * tiles), jnp.bfloat16),
            pltpu.VMEM(((kept + 1) * LANES, devices * tiles), jnp.bfloat16),
            pltpu.VMEM((kept + 1, rows, 2 * LANES), jnp.float32),
            pltpu.VMEM((2 * rows, (kept + 1) * LANES), jnp.bfloat16),
            pltpu.VMEM((2 * rows, (kept + 1) * LANES), jnp.bfloat16),
            pltpu.VMEM((low, rows + 8, LANES), jnp.float32),
            pltpu.VMEM((devices * tiles, rows), jnp.int32),
            pltpu.VMEM((devices // 2, 1, LANES), jnp.float32),
            pltpu.VMEM((devices, tiles, rows), jnp.int32),
            pltpu.VMEM((devices, 1, LANES), jnp.float32),
            pltpu.VMEM((2, 2, 8 * rows, 2 * LANES), jnp.bfloat16),
            pltpu.VMEM((2, 2, 2 * tiles, 8 * rows), jnp.bfloat16),
            pltpu.VMEM((tiles, 2 * piece), jnp.float32),
            pltpu.VMEM((groups // 4, tiles, piece), jnp.int32),
            pltpu.VMEM((groups // 4, 1, LANES), jnp.float32),
            pltpu.VMEM((groups // 4, tiles, piece), jnp.int32),
            pltpu.VMEM((groups // 4, 1, LANES), jnp.float32),
            pltpu.VMEM((devices, 1, LANES), jnp.float32),
            pltpu.VMEM((devices, 1, LANES), jnp.float32),
            dma((copies,)),
            dma((copies,)),
        ]
        + [dma((devices,))] * 2
        + [dma((groups // 4,))] * 4
        + [dma((1,))] * 8
        + [dma((4,))],
        compiler_params=pltpu.CompilerParams(
            collective_id=0, has_side_effects=True, vmem_limit_bytes=60 * 2**20
        ),
        name="step",
    )(*loaded, *held)


def fast_local(sky_image, coef_dual, vis_dual, visibilities, kernel_blocks, tile_rows, tile_counts):
    groups = lax.axis_size("vis")
    devices = lax.axis_size("band") * groups
    taken = kernel_blocks.shape
    new_image, coef_dual, vis_state = step(
        kernel_blocks.reshape(-1, taken[-1]),
        coef_dual,
        sky_image,
        vis_dual.reshape((-1,) + vis_dual.shape[4:]),
        visibilities.reshape((-1,) + vis_dual.shape[4:]),
        tile_rows[0, 0].T,
        tile_counts[0],
        groups,
        devices,
    )
    return (new_image, coef_dual, vis_state.reshape(vis_dual.shape))


def body_for(mesh):
    devices = mesh.shape["band"] * mesh.shape["vis"]
    relayed = mesh.shape["band"] == 2 and mesh.shape["vis"] % 4 == 0 and devices == 32

    def body(sky_image, *rest):
        rows, width = sky_image.shape
        piece = width // mesh.shape["vis"]
        tiles = rest[4].shape[2] * rest[4].shape[3]
        if relayed and rows == LANES and piece == 2 * LANES and 2 * tiles == LANES:
            return fast_local(sky_image, *rest)
        return local(sky_image, *rest)

    return body


def solution(mesh):
    return jax.shard_map(
        body_for(mesh),
        mesh=mesh,
        in_specs=(
            P(("band", "vis"), None),
            P(None, ("band", "vis"), None),
            P("band", "vis", None, None, None, None),
            P("band", "vis", None, None, None, None),
            P("band", "vis", None, None, None, None, None),
            P("band", "vis", None, None),
            P("band", "vis", None),
        ),
        out_specs=(
            P(("band", "vis"), None),
            P(None, ("band", "vis"), None),
            P("band", "vis", None, None, None, None),
        ),
        check_vma=False,
    )
```

```python
import math

import jax
import numpy as np
import jax.numpy as jnp
from jax import lax
from jax.experimental import pallas as pl
from jax.experimental.pallas import tpu as pltpu
from jax.sharding import PartitionSpec as P

IMG = 4096


low_taps = (
    -0.010597401784997278,
    0.032883011666982945,
    0.030841381835986965,
    -0.18703481171888114,
    -0.02798376941698385,
    0.6308807679295904,
    0.7148465705525415,
    0.23037781330885523,
)
high_taps = tuple(((-1.0) ** offset * low_taps[7 - offset] for offset in range(8)))
highest = lax.Precision.HIGHEST


def shifted(block, axis, distance):
    devices = range(lax.axis_size(axis))
    route = [((i - distance) % len(devices), i) for i in devices]
    return lax.ppermute(block, axis, route)


def dft_table(table_size, sign):
    positions = jnp.arange(table_size, dtype=jnp.int32)
    phase = positions[:, None] * positions[None, :] % table_size
    angle = 2.0 * math.pi / table_size * phase.astype(jnp.float32)
    return (jnp.cos(angle), sign * jnp.sin(angle))


def section_one(table, values):
    return jnp.einsum("kn,...nm->...km", table, values, precision=highest)


def section_two(table, values):
    return jnp.einsum("qm,...km->...qk", table, values, precision=highest)


def dft_last(real_in, imag_in, sign):
    leading = real_in.shape[:-1]
    length = real_in.shape[-1]
    inner_len = 64
    outer_len = length // inner_len
    split_real = real_in.reshape(leading + (outer_len, inner_len))
    table_real, table_imag = dft_table(outer_len, sign)
    first_real = section_one(table_real, split_real)
    first_imag = section_one(table_imag, split_real)
    if imag_in is not None:
        split_imag = imag_in.reshape(leading + (outer_len, inner_len))
        first_real = first_real - section_one(table_imag, split_imag)
        first_imag = first_imag + section_one(table_real, split_imag)
    outer_index = jnp.arange(outer_len, dtype=jnp.int32)
    inner_index = jnp.arange(inner_len, dtype=jnp.int32)
    twist_phase = outer_index[:, None] * inner_index[None, :] % length
    twist_angle = 2.0 * math.pi / length * twist_phase.astype(jnp.float32)
    twist_real = jnp.cos(twist_angle)
    twist_imag = sign * jnp.sin(twist_angle)
    mid_real = first_real * twist_real - first_imag * twist_imag
    mid_imag = first_real * twist_imag + first_imag * twist_real
    last_real, last_imag = dft_table(inner_len, sign)
    out_real = section_two(last_real, mid_real) - section_two(last_imag, mid_imag)
    out_imag = section_two(last_real, mid_imag) + section_two(last_imag, mid_real)
    factor = 1.0 / math.sqrt(length)
    return (
        (out_real * factor).reshape(leading + (length,)),
        (out_imag * factor).reshape(leading + (length,)),
    )


def pieces_from_image(extrap, band_count, group_count):
    rows_dev = extrap.shape[0]
    image_width = extrap.shape[1]
    stripe = image_width // band_count
    piece_cols = stripe // group_count
    piece_rows = image_width // group_count
    col_real, col_imag = dft_last(extrap, None, -1.0)
    shaped = jnp.stack([col_real, col_imag]).reshape(
        2, 1, 1, rows_dev, band_count, group_count, piece_cols
    )
    moved = lax.all_to_all(
        lax.all_to_all(shaped, "band", split_axis=4, concat_axis=1, tiled=True),
        "vis",
        split_axis=5,
        concat_axis=2,
        tiled=True,
    )
    columns = jnp.transpose(moved.reshape(2, image_width, piece_cols), (2, 0, 1))
    row_real, row_imag = dft_last(columns[:, 0], columns[:, 1], -1.0)
    stacked = (
        jnp.stack([row_real, row_imag], axis=1)
        .astype(jnp.bfloat16)
        .reshape(piece_cols, 2, group_count, piece_rows)
    )
    pieces = lax.all_to_all(stacked, "vis", split_axis=2, concat_axis=0, tiled=True)
    return pieces.reshape(stripe, 2, piece_rows)


def image_from_pieces(piece_sum, band_count, group_count):
    stripe = piece_sum.shape[0]
    piece_rows = piece_sum.shape[2]
    piece_cols = stripe // group_count
    image_width = piece_rows * group_count
    rows_dev = image_width // (band_count * group_count)
    spread = lax.all_to_all(
        piece_sum.reshape(stripe, 2, 1, piece_rows), "vis", split_axis=0, concat_axis=2, tiled=True
    )
    spread = spread.reshape(piece_cols, 2, image_width)
    col_real, col_imag = dft_last(spread[:, 0], spread[:, 1], 1.0)
    stacked = jnp.transpose(jnp.stack([col_real, col_imag]), (0, 2, 1))
    shaped = stacked.reshape(2, band_count, group_count, rows_dev, 1, 1, piece_cols)
    moved = lax.all_to_all(
        lax.all_to_all(shaped, "band", split_axis=1, concat_axis=4, tiled=True),
        "vis",
        split_axis=2,
        concat_axis=5,
        tiled=True,
    )
    moved = moved.reshape(2, rows_dev, image_width)
    out_real, out_imag = dft_last(moved[0], moved[1], 1.0)
    return out_real


def cols_down(field):
    image_width = field.shape[1]
    extended = jnp.concatenate([field, field[:, :6]], axis=1)
    low_part = 0.0
    high_part = 0.0
    for offset in range(8):
        taken = extended[:, offset : offset + image_width : 2]
        low_part = low_part + low_taps[offset] * taken
        high_part = high_part + high_taps[offset] * taken
    return (low_part, high_part)


def cols_up(low_part, high_part):
    halves = []
    for parity in range(2):
        summed = 0.0
        for delay in range(4):
            summed = summed + low_taps[parity + 2 * delay] * jnp.roll(low_part, delay, axis=1)
            summed = summed + high_taps[parity + 2 * delay] * jnp.roll(high_part, delay, axis=1)
        halves.append(summed)
    return jnp.stack(halves, axis=2).reshape(low_part.shape[0], 2 * low_part.shape[1])


def rows_up(low_ext, high_ext, half_rows):
    halves = []
    for parity in range(2):
        summed = 0.0
        for delay in range(4):
            begin = 3 - delay
            summed = summed + low_taps[parity + 2 * delay] * low_ext[begin : begin + half_rows]
            summed = summed + high_taps[parity + 2 * delay] * high_ext[begin : begin + half_rows]
        halves.append(summed)
    return jnp.stack(halves, axis=1).reshape(2 * half_rows, low_ext.shape[1])


def analysis(extrap):
    rows_dev = extrap.shape[0]
    taken_rows = min(6, rows_dev)
    parts_list = [extrap]
    parts_list.append(shifted(extrap[:taken_rows], ("band", "vis"), -1))
    extended = jnp.concatenate(parts_list, axis=0)
    half_rows = rows_dev // 2
    rows_low = 0.0
    rows_high = 0.0
    for offset in range(8):
        taken = extended[offset : offset + 2 * half_rows : 2]
        rows_low = rows_low + low_taps[offset] * taken
        rows_high = rows_high + high_taps[offset] * taken
    low_low, low_high = cols_down(rows_low)
    high_low, high_high = cols_down(rows_high)
    return jnp.stack([low_low, low_high, high_low, high_high])


def synthesis(coef_dual):
    half_rows = coef_dual.shape[1]
    taken_rows = min(3, half_rows)
    parts_list = [shifted(coef_dual[:, half_rows - taken_rows :, :], ("band", "vis"), 1)]
    joined = jnp.concatenate(parts_list[::-1] + [coef_dual], axis=1)
    cols_low = rows_up(joined[0], joined[2], half_rows)
    cols_high = rows_up(joined[1], joined[3], half_rows)
    return cols_up(cols_low, cols_high)


def degrid(kernel_here, tiles):
    kernel_real = kernel_here[:, :, 0]
    kernel_imag = kernel_here[:, :, 1]
    tile_real = tiles[:, :, 0]
    tile_imag = tiles[:, :, 1]
    out_real = jnp.einsum(
        "qsat,qst->qsa", kernel_real, tile_real, preferred_element_type=jnp.float32
    ) - jnp.einsum("qsat,qst->qsa", kernel_imag, tile_imag, preferred_element_type=jnp.float32)
    out_imag = jnp.einsum(
        "qsat,qst->qsa", kernel_real, tile_imag, preferred_element_type=jnp.float32
    ) + jnp.einsum("qsat,qst->qsa", kernel_imag, tile_real, preferred_element_type=jnp.float32)
    return jnp.stack([out_real, out_imag], axis=2)


def grid_back(kernel_here, weights):
    kernel_real = kernel_here[:, :, 0]
    kernel_imag = kernel_here[:, :, 1]
    weight_real = weights[:, :, 0]
    weight_imag = weights[:, :, 1]
    grid_real = jnp.einsum(
        "qsat,qsa->qst", kernel_real, weight_real, preferred_element_type=jnp.float32
    ) + jnp.einsum("qsat,qsa->qst", kernel_imag, weight_imag, preferred_element_type=jnp.float32)
    grid_imag = jnp.einsum(
        "qsat,qsa->qst", kernel_real, weight_imag, preferred_element_type=jnp.float32
    ) - jnp.einsum("qsat,qsa->qst", kernel_imag, weight_real, preferred_element_type=jnp.float32)
    return jnp.stack([grid_real, grid_imag], axis=2)


def local(sky_image, coef_dual, vis_dual, visibilities, kernel_blocks, tile_rows, tile_counts):
    band_count = lax.axis_size("band")
    group_count = lax.axis_size("vis")
    kernel_here = kernel_blocks[0, 0]
    rows_here = tile_rows[0, 0]
    slot_count = rows_here.shape[1]
    live_slots = (
        jnp.arange(slot_count, dtype=jnp.int32)[None, :] < tile_counts[0, 0][:, None]
    ).astype(jnp.float32)[:, :, None, None]
    vis_data = visibilities[0, 0]
    vis_state = vis_dual[0, 0]
    image_width = sky_image.shape[1]
    stripe = image_width // band_count
    piece_rows = image_width // group_count
    incoming_rows = lax.all_to_all(rows_here, "vis", split_axis=0, concat_axis=0, tiled=True)
    data_part = jnp.sum(live_slots * vis_data * vis_data)
    weights = (live_slots * vis_state).astype(jnp.bfloat16)
    contrib = grid_back(kernel_here, weights)
    arrived = lax.all_to_all(contrib, "vis", split_axis=0, concat_axis=0, tiled=True)
    piece_sum = jax.ops.segment_sum(
        arrived.reshape(-1, 2, piece_rows), incoming_rows.reshape(-1), num_segments=stripe
    )
    adjoint_part = image_from_pieces(piece_sum, band_count, group_count)
    smooth = synthesis(coef_dual)
    new_image = jnp.maximum(sky_image - smooth - adjoint_part, 0.0)
    extrap = 2.0 * new_image - sky_image
    coeffs = analysis(extrap)
    abs_total = jnp.sum(jnp.abs(coeffs))
    coef_total = lax.psum(abs_total, ("band", "vis"))
    threshold = 0.5 * coef_total / (IMG * IMG)
    coef_dual = jnp.clip(coef_dual + coeffs, -threshold, threshold)
    piece_grid = pieces_from_image(extrap, band_count, group_count)
    tiles = lax.all_to_all(
        piece_grid[incoming_rows], "vis", split_axis=0, concat_axis=0, tiled=True
    )
    predicted = degrid(kernel_here, tiles)
    residual = live_slots * (vis_state + predicted - vis_data)
    resid_square = jnp.sum(residual * residual)
    norm_square, data_square = lax.psum((resid_square, data_part), ("band", "vis"))
    radius = 0.5 * jnp.sqrt(data_square + 1e-06)
    size_value = jnp.sqrt(norm_square + 1e-06)
    vis_state = residual * (1.0 - jnp.minimum(1.0, radius / size_value))
    return (new_image, coef_dual, vis_state[None, None])


high = lax.Precision.HIGH
everywhere = ("band", "vis")


def wave_tables(length, digit_low):
    digit_high = length // digit_low
    low = np.arange(digit_low)
    wide = np.arange(digit_high)
    full = 2.0 * np.pi
    small = full * (low[:, None] * low[None, :] % digit_low) / digit_low
    twist = full * (low[:, None] * wide[None, :]) / length
    large = full * (wide[:, None] * wide[None, :] % digit_high) / digit_high
    return small, twist, large


def complex_matrix(angle, sign):
    c = np.cos(angle)
    s = sign * np.sin(angle)
    return np.stack([np.stack([c, -s], axis=1), np.stack([s, c], axis=1)])


def f32(values):
    return jnp.asarray(np.asarray(values, np.float32))


def bf16(values):
    return f32(values).astype(jnp.bfloat16)


def analysis_matrix(half):
    matrix = np.zeros((2, half, 2 * half + 6))
    for k in range(half):
        for j in range(8):
            matrix[0, k, 2 * k + j] = low_taps[j]
            matrix[1, k, 2 * k + j] = high_taps[j]
    return matrix.reshape(2 * half, 2 * half + 6)


def synthesis_matrix(half):
    matrix = np.zeros((2 * half, 2, half + 3))
    for n in range(2 * half):
        for delay in range(4):
            tap = n % 2 + 2 * delay
            matrix[n, 0, n // 2 - delay + 3] = low_taps[tap]
            matrix[n, 1, n // 2 - delay + 3] = high_taps[tap]
    return matrix


def cos_sums(values, size):
    half = size // 2
    if half < 2:
        return [values[0] + values[1], values[0] - values[1]]
    quarter = half // 2
    plus = [values[a] + values[half - a] for a in range(quarter)] + [values[quarter]]
    minus = [values[a] - values[half - a] for a in range(quarter)]
    out = [None] * (half + 1)
    out[0::2] = cos_sums(plus, half)
    for k in range(1, half, 2):
        total = minus[0]
        for a in range(1, quarter):
            total = total + minus[a] * math.cos(2 * math.pi * (a * k % size) / size)
        out[k] = total
    return out


def sin_sums(values, size):
    half = size // 2
    if half < 2:
        return [None] * (half + 1)
    quarter = half // 2
    plus = {a: values[a] + values[half - a] for a in range(1, quarter)}
    plus[quarter] = values[quarter]
    minus = [None] + [values[a] - values[half - a] for a in range(1, quarter)]
    out = [None] * (half + 1)
    out[0::2] = sin_sums(minus, half)
    for k in range(1, half, 2):
        total = None
        for a in range(1, quarter + 1):
            factor = math.sin(2 * math.pi * (a * k % size) / size)
            term = plus[a] if a * 4 == size and k % 4 == 1 else plus[a] * factor
            total = term if total is None else total + term
        out[k] = total
    return out


def even_odd(values):
    size = len(values)
    half = size // 2
    even = [values[0]] + [values[a] + values[size - a] for a in range(1, half)] + [values[half]]
    odd = [None] + [values[a] - values[size - a] for a in range(1, half)]
    return even, odd


def split(values):
    upper = values.astype(jnp.bfloat16)
    return upper, (values - upper.astype(jnp.float32)).astype(jnp.bfloat16)


def table_pair(values):
    upper = f32(values).astype(jnp.bfloat16)
    return upper, (f32(values) - upper.astype(jnp.float32)).astype(jnp.bfloat16)


def nt_dot(a, b):
    return lax.dot_general(a, b, (((1,), (1,)), ((), ())), preferred_element_type=jnp.float32)


def nn_dot(a, b):
    return lax.dot_general(a, b, (((1,), (0,)), ((), ())), preferred_element_type=jnp.float32)


LEVELS = 32000.0
MESH = pl.DeviceIdType.MESH
LANES = 128
whole = pl.BlockSpec(memory_space=pltpu.VMEM)


def place():
    band = lax.axis_index("band")
    vis = lax.axis_index("vis")
    groups = lax.axis_size("vis")
    z = vis // 4
    y = vis // 2 % 2
    core = vis % 2
    return band, z, y, core, groups


def taps_dot(values, tables):
    upper, lower = split(values)
    return nn_dot(upper, tables[0]) + nn_dot(lower, tables[0]) + nn_dot(upper, tables[1])


def level(values):
    return jnp.round(values).astype(jnp.int32)


def step_kernel(
    low,
    kernels_hbm,
    coef_hbm,
    sky_hbm,
    up_hbm,
    edge_hbm,
    base_hbm,
    spin_hbm,
    inv_hbm,
    fwd_hbm,
    near_hbm,
    next_hbm,
    half_base_hbm,
    half_spin_hbm,
    order_hbm,
    state_ref,
    data_ref,
    rows_ref,
    counts_ref,
    phase_ref,
    shift_ref,
    tw_ref,
    image_hbm,
    coef_out_hbm,
    vis_out_ref,
    kernels_ref,
    joined_ref,
    sky_ref,
    merged_ref,
    up_ref,
    edge_ref,
    base_ref,
    spin_ref,
    inv_ref,
    fwd_ref,
    near_ref,
    next_ref,
    half_base_ref,
    half_spin_ref,
    order_ref,
    load_sem,
    tail_ref,
    halo_ref,
    block_ref,
    all_cols_ref,
    turn_ref,
    total_ref,
    tall_ref,
    smooth_ref,
    fold_ref,
    grid_ref,
    hot_ref,
    half_ref,
    spec_ref,
    rest_ref,
    extrap_ref,
    picked_ref,
    unit_ref,
    got_ref,
    units_ref,
    sum_table_ref,
    terms_ref,
    own_ref,
    sums_out_ref,
    sums_unit_ref,
    sums_got_ref,
    sums_units_ref,
    all_abs_ref,
    all_sums_ref,
    send_a,
    send_b,
    recv_a,
    recv_b,
    send_p,
    send_u,
    recv_p,
    recv_u,
    send_z,
    recv_z,
    send_w,
    recv_w,
    send_t,
    recv_t,
    send_s,
    recv_s,
    halo_sem,
):
    x, z, y, core, groups = place()
    levels = groups // 4
    devices = 2 * groups
    half_rows, half_width = coef_hbm.shape[1:]
    rows = 2 * half_rows
    tiles = block_ref.shape[1]
    kept = low // 2 + 1
    wide = LANES

    def index(px, pz, py, pc):
        return px * groups + pz * 4 + py * 2 + pc

    def device(px, pz, py, pc):
        return (px, pz * 4 + py * 2 + pc)

    def ident(number):
        return (number // groups, number % groups)

    def remote(src, dst, send, recv, target):
        return pltpu.make_async_remote_copy(
            src_ref=src,
            dst_ref=dst,
            send_sem=send,
            recv_sem=recv,
            device_id=target,
            device_id_type=MESH,
        )

    me = index(x, z, y, core)
    after, before = (me + 1) % devices, (me + devices - 1) % devices
    twin = device(x, z, y, 1 - core)
    line = [device(x, (z + k) % levels, y, core) for k in range(1, levels)]
    corners = [(1 - x, y), (x, 1 - y), (1 - x, 1 - y)]
    plane = [device(px, z, py, core) for px, py in corners]
    barrier = pltpu.get_barrier_semaphore()
    peers = line + plane + [twin, ident(after), ident(before)]
    for peer in peers:
        pl.semaphore_signal(barrier, inc=1, device_id=peer, device_id_type=MESH)

    sources = [
        (kernels_hbm, kernels_ref),
        (coef_hbm, joined_ref.at[:, pl.ds(8, half_rows), :]),
        (up_hbm, up_ref),
        (edge_hbm, edge_ref),
        (base_hbm, base_ref),
        (spin_hbm, spin_ref),
        (inv_hbm, inv_ref),
        (sky_hbm, sky_ref),
        (fwd_hbm, fwd_ref),
        (near_hbm, near_ref),
        (next_hbm, next_ref),
        (half_base_hbm, half_base_ref),
        (half_spin_hbm, half_spin_ref),
        (order_hbm, order_ref),
    ]
    loads = [
        pltpu.make_async_copy(src, dst, load_sem.at[i]) for i, (src, dst) in enumerate(sources)
    ]
    for load in loads:
        load.start()
    loads[0].wait()
    count = 16
    span = kernels_ref.shape[0] * count // tiles
    width = low * wide
    stripe = width // 2
    slots = rows_ref.shape[0]
    lane = lax.broadcasted_iota(jnp.int32, (tiles, groups), 1)
    tile_id = lax.broadcasted_iota(jnp.int32, (tiles, groups), 0)
    counts = jnp.where(lane == tile_id // slots, counts_ref[...].astype(jnp.float32), 0.0)
    counts = jnp.sum(counts, axis=1, keepdims=True)
    tile_id = lax.broadcasted_iota(jnp.int32, (tiles, 1), 0)
    live = jnp.where((tile_id % slots).astype(jnp.float32) < counts, 1.0, 0.0)
    state = [state_ref[:, part, :] for part in range(2)]
    data = [data_ref[:, part, :] for part in range(2)]
    ours = [part * live for part in state]
    turned = [ours[0], ours[1], ours[0], ours[1]], [ours[1], -ours[0], ours[1], -ours[0]]
    turned = [jnp.concatenate(parts, axis=1) for parts in turned]
    pair_lane = lax.broadcasted_iota(jnp.int32, (count, LANES), 1) // (LANES // 2)
    pair_row = lax.broadcasted_iota(jnp.int32, (count, LANES), 0)
    masks = [pair_lane + 2 * k == pair_row for k in range(count // 2)]
    for i in range(tiles // count):
        spread = [
            jnp.concatenate(
                [jnp.where(mask, part[i * count : (i + 1) * count], 0.0) for mask in masks], axis=1
            )
            for part in turned
        ]
        spread = jnp.concatenate(spread, axis=0).astype(jnp.bfloat16)
        both = nn_dot(spread, kernels_ref[i * span : (i + 1) * span, :])
        both = jnp.concatenate([both[:count], both[count:]], axis=1)
        block_ref[me, i * count : (i + 1) * count, :] = both.astype(jnp.bfloat16)
    lane = lax.broadcasted_iota(jnp.int32, (groups, LANES), 1) % tiles
    owner = lax.broadcasted_iota(jnp.int32, (groups, LANES), 0)
    columns = 0.0
    by_owner = rows_ref[...].astype(jnp.float32).T
    for slot in range(slots):
        here = by_owner[:, slot : slot + 1]
        columns = columns + jnp.where(lane == owner * slots + slot, here, 0.0)
    columns = jnp.sum(columns, axis=0, keepdims=True).astype(jnp.int32)
    all_cols_ref[me] = columns + x * stripe
    loads[1].wait()
    for c in range(4):
        tail_ref[3 * c : 3 * c + 3, :] = joined_ref[c, half_rows + 5 :, :]
    pl.semaphore_wait(barrier, len(peers))

    started = []

    def start(block, target, slot):
        own_a, own_b = block_ref.at[block], all_cols_ref.at[block]
        for own, send, recv in ((own_a, send_a, recv_a), (own_b, send_b, recv_b)):
            copy = remote(own, own, send.at[slot], recv.at[block], target)
            copy.start()
            started.append(copy)

    def got(block):
        for ref, send, recv in ((block_ref, send_a, recv_a), (all_cols_ref, send_b, recv_b)):
            own = ref.at[block]
            remote(own, own, send.at[0], recv.at[block], twin).wait_recv()

    slots_of = iter(range(send_a.shape[0]))
    far = sorted(range(1, levels), key=lambda k: abs(k - levels / 2))
    for k in far:
        start(me, line[k - 1], next(slots_of))
    for target in plane:
        start(me, target, next(slots_of))
    edge = remote(tail_ref, halo_ref, halo_sem.at[0], halo_sem.at[1], ident(after))
    edge.start()
    start(me, twin, next(slots_of))
    for load in loads[2:8]:
        load.wait()
    piece = kernels_ref.shape[1]
    spin_cos, spin_sin = spin_ref[0, pl.ds(me, 1), :], spin_ref[1, pl.ds(me, 1), :]
    cosine = (base_ref[0] * spin_cos - base_ref[1] * spin_sin).astype(jnp.bfloat16)
    sine = (base_ref[1] * spin_cos + base_ref[0] * spin_sin).astype(jnp.bfloat16)
    turn_ref[:rows, :piece] = cosine
    turn_ref[:rows, piece:] = -sine
    turn_ref[rows:, :piece] = sine
    turn_ref[rows:, piece:] = cosine
    line_blocks = [index(x, (z + levels - k) % levels, y, core) for k in far]
    for block in line_blocks:
        got(block)
        for target in plane:
            start(block, target, next(slots_of))
        start(block, twin, next(slots_of))
    for px, py in corners:
        block = index(px, z, py, core)
        got(block)
        start(block, twin, next(slots_of))
    edge.wait()
    for c in range(4):
        joined_ref[c, 5:8, :] = halo_ref[3 * c : 3 * c + 3, :]
    strips = half_width // LANES

    def tall(i, carry):
        here = pl.ds(pl.multiple_of(i * LANES, LANES), LANES)
        for c in range(2):
            for k in range(half_rows // 8):
                lows = [joined_ref[c, 8 + 8 * k - d : 16 + 8 * k - d, here] for d in range(4)]
                highs = [joined_ref[c + 2, 8 + 8 * k - d : 16 + 8 * k - d, here] for d in range(4)]
                for parity in range(2):
                    total = 0.0
                    for d in range(4):
                        total = total + low_taps[parity + 2 * d] * lows[d]
                        total = total + high_taps[parity + 2 * d] * highs[d]
                    tall_ref[c * strips + i, pl.ds(16 * k + parity, 8, stride=2), :] = total
        return carry

    lax.fori_loop(0, strips, tall, 0)


    def broad(i, carry):
        there = (i + strips - 1) % strips
        near = jnp.concatenate([tall_ref[i], tall_ref[strips + i]], axis=1)
        last = jnp.concatenate([tall_ref[there], tall_ref[strips + there]], axis=1)
        out = taps_dot(near, up_ref)
        first = taps_dot(last, edge_ref)
        smooth_ref[2 * i] = out[:, :LANES] + first
        smooth_ref[2 * i + 1] = out[:, LANES:]
        return carry

    lax.fori_loop(0, strips // 2, broad, 0)
    for n, k in enumerate(far):
        for px, py in corners:
            block = index(px, (z + levels - k) % levels, py, core)
            got(block)
            start(block, twin, next(slots_of))
        if n == 0:
            lax.fori_loop(strips // 2, strips, broad, 0)

    total_tiles = devices * tiles
    class_tiles = groups * tiles
    parts = class_tiles // LANES
    lane = lax.broadcasted_iota(jnp.int32, (1, LANES), 1)

    def spread(c, levels_taken):
        for zz in levels_taken:
            for side in range(2):
                b = c * parts + zz * 2 + side
                first = side * groups + zz * 4 + c
                columns = jnp.where(lane < tiles, all_cols_ref[first], all_cols_ref[first + 2])
                k1 = columns % low
                k2 = columns // low
                flip = k1 >= kept
                k1 = jnp.where(flip, low - k1, k1)
                k2 = jnp.where(flip, wide - 1 - k2, k2)
                fold_ref[0, pl.ds(b, 1), :] = (k1 * wide + k2).astype(jnp.float32)
                fold_ref[1, pl.ds(b, 1), :] = jnp.where(flip, -1.0, 1.0)
            some = [block_ref[i // 2 * groups + zz * 4 + i % 2 * 2 + c] for i in range(4)]
            both = nt_dot(turn_ref[...], jnp.concatenate(some, axis=0))
            for side in range(2):
                b = c * parts + zz * 2 + side
                at = pl.ds(pl.multiple_of(b * LANES, LANES), LANES)
                real = both[:rows, side * LANES : (side + 1) * LANES]
                imag = both[rows:, side * LANES : (side + 1) * LANES]
                sign = fold_ref[1, pl.ds(b, 1), :]
                out_real = real * phase_ref[0] - imag * phase_ref[1]
                out_imag = (real * phase_ref[1] + imag * phase_ref[0]) * sign
                grid_ref[:rows, at] = out_real.astype(jnp.bfloat16)
                grid_ref[rows:, at] = out_imag.astype(jnp.bfloat16)

    some = (kept + 1) // 3

    def folded_sum(c, p):
        base = pl.multiple_of(p * some * wide, some * wide)
        row = (lax.broadcasted_iota(jnp.int32, (some * wide, LANES), 0) + base).astype(jnp.float32)
        hots = []
        for i in range(parts):
            hit = row == fold_ref[0, pl.ds(c * parts + i, 1), :]
            hots.append(jnp.where(hit, 1.0, 0.0).astype(jnp.bfloat16))
        hot = jnp.concatenate(hots, axis=1)
        at = pl.ds(pl.multiple_of(c * class_tiles, class_tiles), class_tiles)
        hot_ref[pl.ds(base, some * wide), at] = hot
        return nt_dot(grid_ref[:, at], hot)

    everything = list(range(levels))
    spread(core, everything)

    def scatter_own(p, carry):
        total_ref[p] = folded_sum(core, p)
        return carry

    lax.fori_loop(0, 3, scatter_own, 0)
    coming = [z] + [(z + levels - k) % levels for k in far]

    def from_twin(zz):
        for i in range(4):
            got(i // 2 * groups + zz * 4 + i % 2 * 2 + 1 - core)

    for zz in coming:
        from_twin(zz)
    spread(1 - core, everything)

    def scatter(p, carry):
        folded = (total_ref[p] + folded_sum(1 - core, p)).astype(jnp.bfloat16)
        pairs = []
        for e in range(some):
            here = slice(e * wide, (e + 1) * wide)
            pairs.append(jnp.concatenate([folded[:rows, here], folded[rows:, here]], axis=1))
        mids = nn_dot(jnp.concatenate(pairs, axis=0), inv_ref[...])
        for e in range(some):
            mid = mids[e * rows : (e + 1) * rows]
            k1 = p * some + e
            tw_real, tw_imag = tw_ref[0, pl.ds(k1, 1), :], tw_ref[1, pl.ds(k1, 1), :]
            real, imag = mid[:, :wide], mid[:, wide:]
            half_ref[k1, :, :wide] = real * tw_real - imag * tw_imag
            half_ref[k1, :, wide:] = real * tw_imag + imag * tw_real
        return carry

    lax.fori_loop(0, 3, scatter, 0)

    def strip(i, carry):
        at = pl.ds(pl.multiple_of(i * 8, 8), 8)
        cos_part = cos_sums([half_ref[k, at, :wide] for k in range(kept)], low)
        sin_part = sin_sums([None] + [half_ref[k, at, wide:] for k in range(1, kept - 1)], low)
        extraps = []
        for a in range(low):
            k = min(a, low - a)
            if a == 0 or a == low // 2:
                adjoint = cos_part[k]
            elif a < low // 2:
                adjoint = cos_part[k] - sin_part[k]
            else:
                adjoint = cos_part[k] + sin_part[k]
            here = slice(a * wide, (a + 1) * wide)
            sky = sky_ref[at, here]
            image = jnp.maximum(sky - smooth_ref[a, at, :] - adjoint, 0.0)
            extrap = 2.0 * image - sky
            sky_ref[at, here] = image
            extrap_ref[a, at, :] = extrap
            extraps.append(extrap)
        even, odd = even_odd(extraps)
        real_part = cos_sums(even, low)
        imag_part = sin_sums(odd, low)
        for k in range(kept):
            tw_real, tw_imag = tw_ref[0, k : k + 1, :], tw_ref[1, k : k + 1, :]
            real = real_part[k] * tw_real
            imag = -real_part[k] * tw_imag
            if 0 < k < kept - 1:
                real = real - imag_part[k] * tw_imag
                imag = imag - imag_part[k] * tw_real
            half_ref[k, at, :wide] = real
            half_ref[k, at, wide:] = imag
        return carry

    lax.fori_loop(0, rows // 8, strip, 0)
    store = pltpu.make_async_copy(sky_ref, image_hbm, load_sem.at[len(loads)])
    store.start()
    top = remote(
        extrap_ref.at[:, pl.ds(0, 8), :],
        extrap_ref.at[:, pl.ds(rows, 8), :],
        halo_sem.at[2],
        halo_sem.at[3],
        ident(before),
    )
    top.start()
    loads[8].wait()

    batch = (kept + 1) // 3

    def spectrum(i, carry):
        some = half_ref[pl.ds(i * batch, batch)].reshape(batch * rows, 2 * wide)
        out = taps_dot(some, fwd_ref)
        for e in range(batch):
            here = pl.ds(pl.multiple_of((i * batch + e) * wide, wide), wide)
            upper, lower = split(out[e * rows : (e + 1) * rows])
            spec_ref[:rows, here] = upper[:, :wide]
            spec_ref[rows:, here] = upper[:, wide:]
            rest_ref[:rows, here] = lower[:, :wide]
            rest_ref[rows:, here] = lower[:, wide:]
        return carry

    lax.fori_loop(0, 3, spectrum, 0)

    mate = x * 4 + y * 2 + core

    def sends(to_z, to_x, to_y, to_class):
        at = to_class * class_tiles + (to_z * 4 + to_x * 2 + to_y) * tiles
        at = pl.ds(pl.multiple_of(at, tiles), tiles)
        unit = unit_ref.at[to_class * parts + to_z * 2 + to_x]
        spot, target = to_z * 8 + mate, device(to_x, z, to_y, to_class)
        return [
            remote(picked_ref.at[at, :], got_ref.at[spot], send_p.at[0], recv_p.at[to_z], target),
            remote(unit, units_ref.at[spot], send_u.at[0], recv_u.at[to_z], target),
        ]

    def total_of(ref, send, recv, count=devices - 1, at=0):
        some = ref.at[pl.ds(0, count)]
        return remote(some, some, send.at[0], recv.at[at], twin)

    def share_row(ref, send, recv):
        def one(k, carry):
            to = (me + k) % devices
            remote(ref.at[me], ref.at[me], send.at[0], recv.at[0], ident(to)).start()
            return carry

        lax.fori_loop(1, devices, one, 0)

    def row_total(ref):
        total = ref[0]
        for d in range(1, devices):
            total = total + ref[d]
        return total

    def ordered(n):
        return (z // 2 + 1 + n // 2) % 2 * 2 + (z + 1 + n) % 2

    def pick(s, carry):
        to_z = ordered(s // 2)
        to_class = (core + 1 + s) % 2
        j = to_class * 4 + to_z
        at = pl.multiple_of(j * 2 * LANES, 2 * LANES)
        hot = hot_ref[: kept * wide, pl.ds(at, 2 * LANES)]
        both = nn_dot(spec_ref[:, : kept * wide], hot) + nn_dot(rest_ref[:, : kept * wide], hot)
        for h in range(2):
            sign = fold_ref[1, pl.ds(2 * j + h, 1), :]
            real = both[:rows, h * LANES : (h + 1) * LANES]
            imag = both[rows:, h * LANES : (h + 1) * LANES] * sign
            most = jnp.max(jnp.maximum(jnp.abs(real), jnp.abs(imag)), axis=0, keepdims=True)
            most = jnp.maximum(most, 1e-30)
            unit_ref[2 * j + h] = most * (1.0 / LEVELS)
            to_level = LEVELS / most
            packed = level(real * to_level) * 65536 + level(imag * to_level)
            to = pl.ds(pl.multiple_of(at + h * LANES, LANES), LANES)
            picked_ref[to, :] = packed.T
        for to_x in range(2):
            for to_y in range(2):
                away = (to_x - x) * (to_x - x) + (to_y - y) * (to_y - y)

                @pl.when(away + (to_class - core) * (to_class - core) != 0)
                def _():
                    for copy in sends(to_z, to_x, to_y, to_class):
                        copy.start()

        return carry

    lax.fori_loop(0, devices // 4, pick, 0)
    for load in loads[11:13]:
        load.wait()
    for n in range(4):
        spin_cos, spin_sin = half_spin_ref[0, n : n + 1, :], half_spin_ref[1, n : n + 1, :]
        cosine = half_base_ref[0] * spin_cos - half_base_ref[1] * spin_sin
        sine = half_base_ref[1] * spin_cos + half_base_ref[0] * spin_sin
        for p in range(2):
            part = slice(p * LANES, (p + 1) * LANES)
            c, d = split(cosine[:, part]), split(sine[:, part])
            real_rows = slice(2 * n * rows, (2 * n + 1) * rows)
            imag_rows = slice((2 * n + 1) * rows, (2 * n + 2) * rows)
            for e in range(2):
                sum_table_ref[e, p, real_rows, :LANES] = c[e]
                sum_table_ref[e, p, real_rows, LANES:] = -d[e]
                sum_table_ref[e, p, imag_rows, :LANES] = d[e]
                sum_table_ref[e, p, imag_rows, LANES:] = c[e]
    for to_z in range(levels):
        at = core * class_tiles + (to_z * 4 + x * 2 + y) * tiles
        got_ref[to_z * 8 + mate] = picked_ref[pl.ds(pl.multiple_of(at, tiles), tiles), :]
        units_ref[to_z * 8 + mate] = unit_ref[core * parts + to_z * 2 + x]
    top.wait()
    loads[9].wait()
    loads[10].wait()

    def rows_down(i, carry):
        for k in range(half_rows // 8):
            lows, highs = 0.0, 0.0
            for tap in range(8):
                taken = extrap_ref[i, pl.ds(16 * k + tap, 8, stride=2), :]
                lows = lows + low_taps[tap] * taken
                highs = highs + high_taps[tap] * taken
            tall_ref[i, 8 * k : 8 * k + 8, :] = lows
            tall_ref[i, half_rows + 8 * k : half_rows + 8 * k + 8, :] = highs
        return carry

    lax.fori_loop(0, low, rows_down, 0)

    def cols_down(b, absolute):
        here = jnp.concatenate([tall_ref[2 * b], tall_ref[2 * b + 1]], axis=1)
        out = taps_dot(here, near_ref) + taps_dot(tall_ref[(2 * b + 2) % low], next_ref)
        at = pl.ds(pl.multiple_of(b * LANES, LANES), LANES)
        for c in range(4):
            top_row, left = c // 2 * half_rows, c % 2 * LANES
            part = out[top_row : top_row + half_rows, left : left + LANES]
            absolute = absolute + jnp.abs(part)
            merged_ref[c, :, at] = joined_ref[c, 8:, at] + part
        return absolute

    def plane_sums(taken):
        many = len(taken) * tiles
        rows_of = []
        for zz in taken:
            total_of(got_ref, send_p, recv_p, 7, zz).wait_recv()
            total_of(units_ref, send_u, recv_u, 7, zz).wait_recv()
            rows_of += [units_ref[zz * 8 + m] for m in range(8)]
        units = jnp.concatenate(rows_of * (LANES // len(rows_of)), axis=0).T
        units = jnp.where(y == 0, units[:tiles], units[tiles:])
        cosine, sine = shift_ref[0], shift_ref[1]
        level_cos = half_spin_ref[0, pl.ds(4 * z, 1), :]
        level_sin = half_spin_ref[1, pl.ds(4 * z, 1), :]
        for e, zz in enumerate(taken):
            strip_rows = slice(e * tiles, (e + 1) * tiles)
            for pair in range(4):
                reals, imags = [], []
                for side in range(2):
                    m = side * 4 + pair
                    packed = got_ref[zz * 8 + m]
                    real = (packed + 32768) >> 16
                    imag = packed - (real << 16)
                    unit = units[:, e * 8 + m : e * 8 + m + 1]
                    real = real.astype(jnp.float32) * unit
                    imag = imag.astype(jnp.float32) * unit
                    reals.append(real * cosine + imag * sine)
                    imags.append(imag * cosine - real * sine)
                at = 2 * pair * LANES
                for p, values in ((0, (reals[0] + reals[1], imags[0] + imags[1])),
                                  (1, (reals[0] - reals[1], imags[0] - imags[1]))):
                    for part in range(2):
                        upper, lower = split(values[part])
                        here = slice(at + part * LANES, at + (part + 1) * LANES)
                        terms_ref[0, p, strip_rows, here] = upper
                        terms_ref[1, p, strip_rows, here] = lower
        reals, imags = [], []
        for p in range(2):
            out = nn_dot(terms_ref[0, p, :many], sum_table_ref[0, p])
            out = out + nn_dot(terms_ref[1, p, :many], sum_table_ref[0, p])
            out = out + nn_dot(terms_ref[0, p, :many], sum_table_ref[1, p])
            part = slice(p * LANES, (p + 1) * LANES)
            turn_cos, turn_sin = level_cos[:, part], level_sin[:, part]
            real, imag = out[:, :LANES], out[:, LANES:]
            reals.append(real * turn_cos + imag * turn_sin)
            imags.append(imag * turn_cos - real * turn_sin)
        real = jnp.concatenate(reals, axis=1)
        imag = jnp.concatenate(imags, axis=1)
        most = jnp.max(jnp.maximum(jnp.abs(real), jnp.abs(imag)), axis=1, keepdims=True)
        most = jnp.maximum(most, 1e-30)
        to_level = LEVELS / most
        packed = level(real * to_level) * 65536 + level(imag * to_level)
        unit = most * (1.0 / LEVELS)
        for e, zz in enumerate(taken):
            strip_rows = slice(e * tiles, (e + 1) * tiles)
            if zz is z:
                own_ref[:, : 2 * LANES] = real[strip_rows]
                own_ref[:, 2 * LANES :] = imag[strip_rows]
                continue
            sums_out_ref[zz] = packed[strip_rows]
            wide_unit = jnp.broadcast_to(unit[strip_rows], (tiles, LANES))
            sums_unit_ref[zz] = jnp.concatenate([wide_unit, wide_unit], axis=0).T[:1]
            target = device(x, zz, y, core)
            remote(
                sums_out_ref.at[zz], sums_got_ref.at[z], send_z.at[0], recv_z.at[0], target
            ).start()
            remote(
                sums_unit_ref.at[zz], sums_units_ref.at[z], send_w.at[0], recv_w.at[0], target
            ).start()

    plane_sums([ordered(0), ordered(1)])
    absolute = jnp.zeros((half_rows, LANES), jnp.float32)
    absolute = lax.fori_loop(0, low // 4, cols_down, absolute)
    plane_sums([ordered(2), z])
    absolute = lax.fori_loop(low // 4, low // 2, cols_down, absolute)
    abs_total = jnp.sum(jnp.sum(absolute, axis=0, keepdims=True), axis=1, keepdims=True)
    loads[13].wait()

    lane = lax.broadcasted_iota(jnp.int32, (1, LANES), 1)
    all_abs_ref[me] = jnp.where(lane == 0, abs_total, 0.0)
    share_row(all_abs_ref, send_t, recv_t)
    total_of(sums_got_ref, send_z, recv_z, levels - 1).wait_recv()
    total_of(sums_units_ref, send_w, recv_w, levels - 1).wait_recv()
    units = [sums_units_ref[(z + k) % levels] for k in range(1, levels)]
    units = jnp.concatenate(units + [units[0]] * (LANES - levels + 1), axis=0).T
    units = units[:tiles]
    real, imag = own_ref[:, : 2 * LANES], own_ref[:, 2 * LANES :]
    for k in range(1, levels):
        packed = sums_got_ref[(z + k) % levels]
        upper = (packed + 32768) >> 16
        lower = packed - (upper << 16)
        unit = units[:, k - 1 : k]
        real = real + upper.astype(jnp.float32) * unit
        imag = imag + lower.astype(jnp.float32) * unit
    tile = jnp.concatenate([real, imag], axis=1).astype(jnp.bfloat16)
    tile = nn_dot(tile, order_ref[...]).astype(jnp.bfloat16)
    first, second = [], []
    near_row = pair_row % 2 == 0
    for i in range(tiles // count):
        here = tile[i * count : (i + 1) * count]
        pair = jnp.concatenate([here[:, :piece], here[:, piece:]], axis=0)
        out = nt_dot(pair, kernels_ref[i * span : (i + 1) * span, :])
        for found, half in ((first, out[:count]), (second, out[count:])):
            total = 0.0
            for k in range(count // 2):
                total = total + jnp.where(
                    pair_row // 2 == k, half[:, k * LANES : (k + 1) * LANES], 0.0
                )
            found.append(jnp.where(near_row, total, pltpu.roll(total, LANES // 2, 1)))
    first = jnp.concatenate(first, axis=0)
    second = jnp.concatenate(second, axis=0)
    visits = state_ref.shape[2]
    lane = lax.broadcasted_iota(jnp.int32, first.shape, 1)
    crossed = jnp.where(
        lane // visits % 2 == 0,
        -pltpu.roll(second, LANES - visits, 1),
        pltpu.roll(second, visits, 1),
    )
    keep = jnp.where(lane < 2 * visits, live, 0.0)
    state_wide = jnp.concatenate(state + state, axis=1)
    data_wide = jnp.concatenate(data + data, axis=1)
    residual = keep * (state_wide + first + crossed - data_wide)
    norms = []
    for values in (residual, data_wide * keep):
        norms.append(jnp.sum(jnp.sum(values * values, axis=0, keepdims=True), axis=1, keepdims=True))
    lane = lax.broadcasted_iota(jnp.int32, (1, LANES), 1)
    all_sums_ref[me] = jnp.where(lane == 0, norms[0], norms[1])
    share_row(all_sums_ref, send_s, recv_s)
    total_of(all_abs_ref, send_t, recv_t).wait_recv()
    threshold = 0.5 * row_total(all_abs_ref)[:, 0:1] / (width * width)

    def clip(i, carry):
        at = pl.ds(pl.multiple_of(i * LANES, LANES), LANES)
        for c in range(4):
            merged_ref[c, :, at] = jnp.clip(merged_ref[c, :, at], -threshold, threshold)
        return carry

    lax.fori_loop(0, half_width // LANES, clip, 0)
    store_coef = pltpu.make_async_copy(merged_ref, coef_out_hbm, load_sem.at[len(loads) + 1])
    store_coef.start()
    for copy in started:
        copy.wait_send()
    total_of(got_ref, send_p, recv_p, 28).wait_send()
    total_of(units_ref, send_u, recv_u, 28).wait_send()
    total_of(sums_got_ref, send_z, recv_z, levels - 1).wait_send()
    total_of(sums_units_ref, send_w, recv_w, levels - 1).wait_send()
    total_of(all_abs_ref, send_t, recv_t).wait_send()
    total_of(all_sums_ref, send_s, recv_s).wait()
    total = row_total(all_sums_ref)
    size = jnp.sqrt(total[:, 0:1] + 1e-06)
    radius = 0.5 * jnp.sqrt(total[:, 1:2] + 1e-06)
    residual = residual * (1.0 - jnp.minimum(1.0, radius / size))
    vis_out_ref[:, 0, :] = residual[:, :visits]
    vis_out_ref[:, 1, :] = residual[:, visits : 2 * visits]
    store.wait()
    store_coef.wait()


def step(kernels, coef, sky, state, data, tile_rows, tile_counts, groups, devices):
    rows, width = sky.shape
    piece = kernels.shape[1]
    slots = tile_rows.shape[0]
    tiles = groups * slots
    half_rows, half_width = coef.shape[1:]
    low = width // LANES
    kept = low // 2 + 1
    wide = np.arange(LANES)
    matrix = synthesis_matrix(LANES)
    up = matrix[:, :, 3:].transpose(1, 2, 0).reshape(2 * LANES, 2 * LANES)
    edge = np.zeros((2, LANES, LANES))
    edge[:, LANES - 3 :, :] = matrix[:LANES, :, :3].transpose(1, 2, 0)
    matrix = analysis_matrix(LANES).T
    following = np.zeros((LANES, 2 * LANES))
    following[:6] = matrix[2 * LANES :]
    turn = np.arange(piece)
    base = 2 * np.pi * np.arange(rows)[:, None] * turn[None, :] / width
    spin = 2 * np.pi * (np.arange(devices)[:, None] * turn[None, :] % devices) / devices
    owner = wide // slots % groups
    shift = 2 * np.pi * (np.arange(rows)[:, None] * owner[None, :] % groups) / groups
    phase = np.stack([np.cos(shift), np.sin(shift)])
    full = 2 * np.pi * (wide[:, None] * wide[None, :] % LANES) / LANES
    c, s = np.cos(full) / width, np.sin(full) / width
    inverse = np.block([[c, s], [-s, c]])
    forward = np.block([[c, -s], [s, c]])
    twist = 2 * np.pi * np.arange(kept + 1)[:, None] * wide[None, :] / width
    halves = np.concatenate([turn[0::2], turn[1::2]])
    half_base = 2 * np.pi * np.arange(rows)[:, None] * halves[None, :] / width
    half_spin = 2 * np.pi * (np.arange(devices)[:, None] * halves[None, :] % devices) / devices
    order = np.zeros((2 * piece, 2 * piece))
    for part in range(2):
        order[part * piece + np.arange(piece), part * piece + halves] = 1.0
    loaded = [
        kernels,
        coef,
        sky,
        jnp.stack(table_pair(up)),
        jnp.stack(table_pair(edge.reshape(2 * LANES, LANES))),
        f32(np.stack([np.cos(base), np.sin(base)])),
        f32(np.stack([np.cos(spin), np.sin(spin)])),
        bf16(inverse),
        jnp.stack(table_pair(forward)),
        jnp.stack(table_pair(matrix[: 2 * LANES])),
        jnp.stack(table_pair(following)),
        f32(np.stack([np.cos(half_base), np.sin(half_base)])),
        f32(np.stack([np.cos(half_spin), np.sin(half_spin)])),
        bf16(order),
    ]
    held = [
        state,
        data,
        tile_rows,
        tile_counts,
        f32(phase),
        f32(phase[:, :, :tiles].transpose(0, 2, 1)),
        f32(np.stack([np.cos(twist), np.sin(twist)])),
    ]
    buffers = [pltpu.VMEM(value.shape, value.dtype) for value in loaded]
    buffers[1] = pltpu.VMEM((4, half_rows + 8, half_width), jnp.float32)
    copies = 3 * 4 + 7 + 12
    dma = pltpu.SemaphoreType.DMA
    anywhere = pl.BlockSpec(memory_space=pltpu.HBM)
    return pl.pallas_call(
        lambda *refs: step_kernel(low, *refs),
        out_shape=(
            jax.ShapeDtypeStruct((rows, width), jnp.float32),
            jax.ShapeDtypeStruct(coef.shape, jnp.float32),
            jax.ShapeDtypeStruct(state.shape, jnp.float32),
        ),
        in_specs=[anywhere] * len(loaded) + [whole] * len(held),
        out_specs=(anywhere, anywhere, whole),
        scratch_shapes=buffers[:3]
        + [pltpu.VMEM(coef.shape, jnp.float32)]
        + buffers[3:]
        + [
            dma((len(loaded) + 2,)),
            pltpu.VMEM((16, half_width), jnp.float32),
            pltpu.VMEM((16, half_width), jnp.float32),
            pltpu.VMEM((devices, tiles, 2 * piece), jnp.bfloat16),
            pltpu.VMEM((devices, 1, LANES), jnp.int32),
            pltpu.VMEM((2 * rows, 2 * piece), jnp.bfloat16),
            pltpu.VMEM((3, 2 * rows, (kept + 1) // 3 * LANES), jnp.float32),
            pltpu.VMEM((low, rows, LANES), jnp.float32),
            pltpu.VMEM((low, rows, LANES), jnp.float32),
            pltpu.VMEM((2, devices // 2, LANES), jnp.float32),
            pltpu.VMEM((2 * rows, devices * tiles), jnp.bfloat16),
            pltpu.VMEM(((kept + 1) * LANES, devices * tiles), jnp.bfloat16),
            pltpu.VMEM((kept + 1, rows, 2 * LANES), jnp.float32),
            pltpu.VMEM((2 * rows, (kept + 1) * LANES), jnp.bfloat16),
            pltpu.VMEM((2 * rows, (kept + 1) * LANES), jnp.bfloat16),
            pltpu.VMEM((low, rows + 8, LANES), jnp.float32),
            pltpu.VMEM((devices * tiles, rows), jnp.int32),
            pltpu.VMEM((devices // 2, 1, LANES), jnp.float32),
            pltpu.VMEM((devices, tiles, rows), jnp.int32),
            pltpu.VMEM((devices, 1, LANES), jnp.float32),
            pltpu.VMEM((2, 2, 8 * rows, 2 * LANES), jnp.bfloat16),
            pltpu.VMEM((2, 2, 2 * tiles, 8 * rows), jnp.bfloat16),
            pltpu.VMEM((tiles, 2 * piece), jnp.float32),
            pltpu.VMEM((groups // 4, tiles, piece), jnp.int32),
            pltpu.VMEM((groups // 4, 1, LANES), jnp.float32),
            pltpu.VMEM((groups // 4, tiles, piece), jnp.int32),
            pltpu.VMEM((groups // 4, 1, LANES), jnp.float32),
            pltpu.VMEM((devices, 1, LANES), jnp.float32),
            pltpu.VMEM((devices, 1, LANES), jnp.float32),
            dma((copies,)),
            dma((copies,)),
        ]
        + [dma((devices,))] * 2
        + [dma((groups // 4,))] * 4
        + [dma((1,))] * 8
        + [dma((4,))],
        compiler_params=pltpu.CompilerParams(
            collective_id=0, has_side_effects=True, vmem_limit_bytes=60 * 2**20
        ),
        name="step",
    )(*loaded, *held)


def fast_local(sky_image, coef_dual, vis_dual, visibilities, kernel_blocks, tile_rows, tile_counts):
    groups = lax.axis_size("vis")
    devices = lax.axis_size("band") * groups
    taken = kernel_blocks.shape
    new_image, coef_dual, vis_state = step(
        kernel_blocks.reshape(-1, taken[-1]),
        coef_dual,
        sky_image,
        vis_dual.reshape((-1,) + vis_dual.shape[4:]),
        visibilities.reshape((-1,) + vis_dual.shape[4:]),
        tile_rows[0, 0].T,
        tile_counts[0],
        groups,
        devices,
    )
    return (new_image, coef_dual, vis_state.reshape(vis_dual.shape))


def body_for(mesh):
    devices = mesh.shape["band"] * mesh.shape["vis"]
    relayed = mesh.shape["band"] == 2 and mesh.shape["vis"] % 4 == 0 and devices == 32

    def body(sky_image, *rest):
        rows, width = sky_image.shape
        piece = width // mesh.shape["vis"]
        tiles = rest[4].shape[2] * rest[4].shape[3]
        if relayed and rows == LANES and piece == 2 * LANES and 2 * tiles == LANES:
            return fast_local(sky_image, *rest)
        return local(sky_image, *rest)

    return body


def solution(mesh):
    return jax.shard_map(
        body_for(mesh),
        mesh=mesh,
        in_specs=(
            P(("band", "vis"), None),
            P(None, ("band", "vis"), None),
            P("band", "vis", None, None, None, None),
            P("band", "vis", None, None, None, None),
            P("band", "vis", None, None, None, None, None),
            P("band", "vis", None, None),
            P("band", "vis", None),
        ),
        out_specs=(
            P(("band", "vis"), None),
            P(None, ("band", "vis"), None),
            P("band", "vis", None, None, None, None),
        ),
        check_vma=False,
    )
```
